32 devices in a mesh: dp: 4 (over y, z), tp: 8 (over x, core).
Axes of the slice: x: 4, y: 2, z: 2, core: 2. Of those that a mesh axis runs over, the one named last changes fastest.
The devices are a block of a 4x4x8 slice.
Arguments:
- hidden: bfloat16 [48, 512, 2560], P('dp', 'tp'), parts along dimension 0
- lengths: int32 [48], P('dp'), parts along dimension 0
- rope_cos: float32 [48, 512, 16], P('dp'), parts along dimension 0
- rope_sin: float32 [48, 512, 16], P('dp'), parts along dimension 0
- cache_lat: bfloat16 [48, 1024, 256], P('dp'), parts along dimension 0
- cache_pe: bfloat16 [48, 1024, 32], P('dp'), parts along dimension 0
- norm_in: float32 [2560], replicated
- w_dq: bfloat16 [2560, 768], replicated
- norm_q: float32 [768], replicated
- w_dkv: bfloat16 [2560, 288], replicated
- norm_kv: float32 [256], replicated
- w_uq: bfloat16 [768, 40, 96], P(None, 'tp')
- w_uk: bfloat16 [256, 40, 64], P(None, 'tp')
- w_uv: bfloat16 [256, 40, 64], P(None, 'tp')
- w_out: bfloat16 [2560, 2560], P('tp')
Outputs:
- output 1: bfloat16 [48, 512, 2560], P('dp', 'tp'), parts along dimension 0
- output 2: bfloat16 [48, 1024, 256], P('dp'), parts along dimension 0
- output 3: bfloat16 [48, 1024, 32], P('dp'), parts along dimension 0
There are 4 independent parts. The reference program is written for one: setup_inputs(seed, part) draws one part's arguments, and reference() takes and returns one part's arrays. A program takes and returns all parts, laid end to end along the dimension named above; an argument that names none is the same for every part.
All inputs are finite; a program needn't handle non-finite values.
Results may differ from the reference program's by a relative error of at most 0.0169221.
Values are sent between devices in bfloat16 or wider.
A program may use at most 768 MiB of HBM per device.

```python
import jax
import jax.numpy as jnp
from jax import lax

MODEL_DIM = 2560
NUM_HEADS = 40
Q_RANK = 768
KV_RANK = 256
NOPE_DIM = 64
ROPE_DIM = 32
VALUE_DIM = 64
SEQ_COUNT = 12
CHUNK_LEN = 512
PREFIX_MAX = 512
CACHE_LEN = 1024

HEAD_BLOCK = min(8, NUM_HEADS)


def rms_norm(values, gain_vec):
    inv_rms = lax.rsqrt(jnp.mean(values * values, axis=-1, keepdims=True) + 1e-6)
    return values * inv_rms * gain_vec


def apply_rope(values, cos_tab, sin_tab):
    half_dim = values.shape[-1] // 2
    lower_half = values[..., :half_dim]
    upper_half = values[..., half_dim:]
    return jnp.concatenate([lower_half * cos_tab - upper_half * sin_tab, upper_half * cos_tab + lower_half * sin_tab], axis=-1)


def write_rows(old_rows, new_rows, start_row):
    zero_col = jnp.zeros((), start_row.dtype)
    return lax.dynamic_update_slice(old_rows, new_rows.astype(old_rows.dtype), (start_row, zero_col))


def rope_tables(lengths):
    positions = (lengths[:, None] + jnp.arange(CHUNK_LEN)[None, :]).astype(jnp.float32)
    inv_freq = 10000.0 ** (-2.0 * jnp.arange(ROPE_DIM // 2).astype(jnp.float32) / ROPE_DIM)
    angles = positions[:, :, None] * inv_freq[None, None, :]
    return jnp.cos(angles), jnp.sin(angles)


def normal_draw(key_in, array_shape, std_scale):
    return jax.random.normal(key_in, array_shape, jnp.float32) * std_scale


def setup_inputs(seed: int = 0, part: int = 0) -> dict:
    base_key = jax.random.key(seed)
    part_keys = jax.random.split(jax.random.fold_in(base_key, part), 5)
    weight_keys = jax.random.split(base_key, 9)
    draw_vals = jax.random.randint(part_keys[0], (SEQ_COUNT,), PREFIX_MAX // 4, PREFIX_MAX + 1)
    top_slot = jax.random.randint(part_keys[1], (), 0, SEQ_COUNT)
    lengths = jnp.where(jnp.arange(SEQ_COUNT) == top_slot, PREFIX_MAX, draw_vals).astype(jnp.int32)
    rope_cos, rope_sin = rope_tables(lengths)
    out_scale = (NUM_HEADS * VALUE_DIM) ** -0.5 * (CACHE_LEN / 4.0) ** 0.5
    return {
        "hidden": normal_draw(part_keys[2], (SEQ_COUNT, CHUNK_LEN, MODEL_DIM), 1.0).astype(jnp.bfloat16),
        "lengths": lengths,
        "rope_cos": rope_cos,
        "rope_sin": rope_sin,
        "cache_lat": normal_draw(part_keys[3], (SEQ_COUNT, CACHE_LEN, KV_RANK), 1.0).astype(jnp.bfloat16),
        "cache_pe": normal_draw(part_keys[4], (SEQ_COUNT, CACHE_LEN, ROPE_DIM), 1.0).astype(jnp.bfloat16),
        "norm_in": jax.random.uniform(weight_keys[0], (MODEL_DIM,), jnp.float32, 0.5, 1.5),
        "w_dq": normal_draw(weight_keys[1], (MODEL_DIM, Q_RANK), MODEL_DIM ** -0.5).astype(jnp.bfloat16),
        "norm_q": jax.random.uniform(weight_keys[2], (Q_RANK,), jnp.float32, 0.5, 1.5),
        "w_dkv": normal_draw(weight_keys[3], (MODEL_DIM, KV_RANK + ROPE_DIM), MODEL_DIM ** -0.5).astype(jnp.bfloat16),
        "norm_kv": jax.random.uniform(weight_keys[4], (KV_RANK,), jnp.float32, 0.5, 1.5),
        "w_uq": normal_draw(weight_keys[5], (Q_RANK, NUM_HEADS, NOPE_DIM + ROPE_DIM), Q_RANK ** -0.5).astype(jnp.bfloat16),
        "w_uk": normal_draw(weight_keys[6], (KV_RANK, NUM_HEADS, NOPE_DIM), KV_RANK ** -0.5).astype(jnp.bfloat16),
        "w_uv": normal_draw(weight_keys[7], (KV_RANK, NUM_HEADS, VALUE_DIM), KV_RANK ** -0.5).astype(jnp.bfloat16),
        "w_out": normal_draw(weight_keys[8], (NUM_HEADS * VALUE_DIM, MODEL_DIM), out_scale).astype(jnp.bfloat16),
    }


def reference(hidden, lengths, rope_cos, rope_sin, cache_lat, cache_pe, norm_in, w_dq, norm_q, w_dkv, norm_kv, w_uq, w_uk, w_uv, w_out):
    hidden_f = hidden.astype(jnp.float32)
    normed = rms_norm(hidden_f, norm_in).astype(jnp.bfloat16).reshape(SEQ_COUNT * CHUNK_LEN, MODEL_DIM)
    q_latent = rms_norm(jnp.dot(normed, w_dq, preferred_element_type=jnp.float32), norm_q).astype(jnp.bfloat16)
    kv_proj = jnp.dot(normed, w_dkv, preferred_element_type=jnp.float32).reshape(SEQ_COUNT, CHUNK_LEN, KV_RANK + ROPE_DIM)
    new_lat = rms_norm(kv_proj[..., :KV_RANK], norm_kv).astype(jnp.bfloat16)
    new_pe = apply_rope(kv_proj[..., KV_RANK:], rope_cos, rope_sin).astype(jnp.bfloat16)
    lat_all = jax.vmap(write_rows)(cache_lat, new_lat, lengths)
    pe_all = jax.vmap(write_rows)(cache_pe, new_pe, lengths)
    q_full = jnp.einsum("nc,chd->nhd", q_latent.astype(jnp.float32), w_uq.astype(jnp.float32)).reshape(SEQ_COUNT, CHUNK_LEN, NUM_HEADS, NOPE_DIM + ROPE_DIM)
    q_nope = q_full[..., :NOPE_DIM].astype(jnp.bfloat16)
    q_pe = apply_rope(q_full[..., NOPE_DIM:], rope_cos[:, :, None, :], rope_sin[:, :, None, :]).astype(jnp.bfloat16)
    block_count = NUM_HEADS // HEAD_BLOCK
    uk_blocks = w_uk.reshape(KV_RANK, block_count, HEAD_BLOCK, NOPE_DIM).transpose(1, 0, 2, 3)
    uv_blocks = w_uv.reshape(KV_RANK, block_count, HEAD_BLOCK, VALUE_DIM).transpose(1, 0, 2, 3)
    score_scale = (NOPE_DIM + ROPE_DIM) ** -0.5
    query_pos = jnp.arange(CHUNK_LEN)[:, None]
    key_pos = jnp.arange(CACHE_LEN)[None, :]

    def one_sequence(seq_args):
        qn_seq, qp_seq, lat_seq, pe_seq, length = seq_args
        visible = key_pos < length + query_pos + 1
        qn_blocks = qn_seq.reshape(CHUNK_LEN, block_count, HEAD_BLOCK, NOPE_DIM).transpose(1, 0, 2, 3)
        qp_blocks = qp_seq.reshape(CHUNK_LEN, block_count, HEAD_BLOCK, ROPE_DIM).transpose(1, 0, 2, 3)
        lat_f = lat_seq.astype(jnp.float32)
        pe_f = pe_seq.astype(jnp.float32)

        def one_block(blk_args):
            qn_blk, qp_blk, uk_blk, uv_blk = blk_args
            keys_nope = jnp.einsum("sc,chd->shd", lat_f, uk_blk.astype(jnp.float32)).astype(jnp.bfloat16)
            values_blk = jnp.einsum("sc,chv->shv", lat_f, uv_blk.astype(jnp.float32)).astype(jnp.bfloat16)
            scores = jnp.einsum("thd,shd->hts", qn_blk.astype(jnp.float32), keys_nope.astype(jnp.float32))
            scores = scores + jnp.einsum("thr,sr->hts", qp_blk.astype(jnp.float32), pe_f)
            scores = jnp.where(visible[None], scores * score_scale, -1e30)
            attn_probs = jax.nn.softmax(scores, axis=-1).astype(jnp.bfloat16)
            return jnp.einsum("hts,shv->thv", attn_probs.astype(jnp.float32), values_blk.astype(jnp.float32)).astype(jnp.bfloat16)

        out_blocks = lax.map(one_block, (qn_blocks, qp_blocks, uk_blocks, uv_blocks))
        return out_blocks.transpose(1, 0, 2, 3).reshape(CHUNK_LEN, NUM_HEADS * VALUE_DIM)

    attn_out = lax.map(one_sequence, (q_nope, q_pe, lat_all, pe_all, lengths))
    out_proj = jnp.dot(attn_out.reshape(SEQ_COUNT * CHUNK_LEN, NUM_HEADS * VALUE_DIM), w_out, preferred_element_type=jnp.float32)
    block_out = (out_proj.reshape(SEQ_COUNT, CHUNK_LEN, MODEL_DIM) + hidden_f).astype(jnp.bfloat16)
    return (block_out, lat_all, pe_all)
```

```python
import functools

import jax
import jax.numpy as jnp
from jax import lax
from jax.experimental import pallas as pl
from jax.experimental.pallas import tpu as pltpu
from jax.sharding import PartitionSpec as P

BLOCK = 128
LOG2E = 1.4426950408889634
F32 = jnp.float32
BF16 = jnp.bfloat16


def dot(a, b):
    return lax.dot_general(a, b, (((1,), (0,)), ((), ())), preferred_element_type=F32)


def dot_t(a, b):
    return lax.dot_general(a, b, (((1,), (1,)), ((), ())), preferred_element_type=F32)


def project_kernel(where_ref, x_ref, g1_ref, wdq_ref, gq_ref, wkv_ref, gkv_ref, cos_ref, sin_ref, cq_ref, kv_ref):
    seqs, toks, dim = x_ref.shape
    rank = gkv_ref.shape[1]
    half = cos_ref.shape[1]
    odd = where_ref[1]
    x = x_ref[...].reshape(seqs * toks, dim).astype(F32)
    inv = lax.rsqrt(jnp.mean(x * x, axis=-1, keepdims=True) + 1e-6)
    a = (x * inv * g1_ref[...]).astype(BF16)
    kv = dot_t(a, wkv_ref[...])
    c = kv[:, :rank]
    inv = lax.rsqrt(jnp.mean(c * c, axis=-1, keepdims=True) + 1e-6)
    kv_ref[:, :, :rank] = (c * inv * gkv_ref[...]).astype(BF16).reshape(seqs, toks, rank)
    for s in range(seqs):
        cos_pair, sin_pair = cos_ref[s], sin_ref[s]
        cos = jnp.where(odd == 1, cos_pair[:, toks:], cos_pair[:, :toks])
        sin = jnp.where(odd == 1, sin_pair[:, toks:], sin_pair[:, :toks])
        table = jnp.concatenate([cos, cos, -sin, sin], axis=0).T
        p = kv[s * toks : (s + 1) * toks, rank:]
        swapped = jnp.concatenate([p[:, half:], p[:, :half]], axis=1)
        kv_ref[s, :, rank:] = (p * table[:, : 2 * half] + swapped * table[:, 2 * half :]).astype(BF16)
    h = dot(a, wdq_ref[...])
    inv = lax.rsqrt(jnp.mean(h * h, axis=-1, keepdims=True) + 1e-6)
    cq_ref[...] = (h * inv * gq_ref[...]).astype(BF16).reshape(cq_ref.shape)


def attend_kernel(
    where_ref,
    len_ref,
    wq_ref,
    wkv_ref,
    cq_ref,
    cos_ref,
    sin_ref,
    new_ref,
    lat_ref,
    pe_ref,
    own_ref,
    send_ref,
    lat_out,
    pe_out,
    qraw,
    qbd,
    rows,
    rot,
    kbuf,
    vbuf,
    s_a,
    s_b,
    pbuf,
    obuf,
    fresh,
    fresh_pe,
):
    step = pl.program_id(0)
    chip, odd = where_ref[0], where_ref[1]
    peers, seqs, toks, _ = new_ref.shape
    rank = lat_ref.shape[2]
    rope = pe_ref.shape[1]
    half = rope // 2
    shards, q_rows, q_rank = wq_ref.shape
    kv_rows = wkv_ref.shape[1] // 2
    nope = qbd.shape[2] // 4
    head = nope + rope
    local_heads = q_rows // head
    pairs = qbd.shape[1]
    cache_len = lat_ref.shape[1]
    chunk = peers * toks
    width = 2 * BLOCK
    factor = LOG2E * head**-0.5

    @pl.when(step == 0)
    def _():
        qbd[...] = jnp.zeros_like(qbd)
        rot[...] = jnp.zeros_like(rot)
        fresh_pe[...] = jnp.zeros_like(fresh_pe)

    cq = jnp.concatenate([cq_ref[c, s] for s in range(seqs) for c in range(2)], axis=0)
    for shard in range(shards):
        qraw[...] = dot_t(wq_ref[shard], cq)
        for h in range(local_heads):
            index = shard * local_heads + h
            pair, side = index // 2, index % 2
            base = h * head
            for s in range(seqs):
                lanes = slice(s * BLOCK, (s + 1) * BLOCK)
                cols = slice(side * BLOCK, (side + 1) * BLOCK)
                qbd[s, pair, side * nope : (side + 1) * nope, cols] = qraw[base : base + nope, lanes].astype(BF16)
                lo = qraw[base + nope : base + nope + half, lanes]
                hi = qraw[base + nope + half : base + head, lanes]
                cos, sin = cos_ref[s], sin_ref[s]
                qbd[s, pair, 2 * nope : 2 * nope + half, cols] = (lo * cos - hi * sin).astype(BF16)
                qbd[s, pair, 2 * nope + half : 2 * nope + rope, cols] = (hi * cos + lo * sin).astype(BF16)

    def one_sequence(s, _):
        length = len_ref[step * seqs + s]
        prefix_blocks = (length + BLOCK - 1) // BLOCK
        last = prefix_blocks - 1
        total = prefix_blocks + chip + 1
        old_pe = pe_ref[s].astype(F32)

        def new_block(b, at):
            for c in range(2):
                piece = new_ref[2 * b + c, s]
                start = pl.multiple_of(at + c * toks, toks)
                rows[pl.ds(start, toks), :] = piece[:, :rank]
                rot[pl.ds(start, toks), :rope] = piece[:, rank:]

        def old_block(b, at):
            start = pl.multiple_of(b * BLOCK, BLOCK)
            rows[pl.ds(at, BLOCK), :] = lat_ref[s, pl.ds(start, BLOCK), :]
            rot[pl.ds(at, BLOCK), :rope] = pe_ref[s, :, pl.ds(start, BLOCK)].astype(F32).T.astype(BF16)

        new_block(chip, 0)
        old_block(last, BLOCK)

        def place_old(b, _):
            old_block(b, pl.multiple_of((2 + b) * BLOCK, BLOCK))
            return 0

        def place_new(b, _):
            new_block(b, pl.multiple_of((2 + last + b) * BLOCK, BLOCK))
            return 0

        lax.fori_loop(0, last, place_old, 0)
        lax.fori_loop(0, chip, place_new, 0)

        def attend(blocks):
            t = blocks * BLOCK
            for j in range(shards * kv_rows // width):
                lo = j * width
                parts = []
                while lo < (j + 1) * width:
                    shard, at = lo // kv_rows, lo % kv_rows
                    take = min(kv_rows - at, (j + 1) * width - lo)
                    parts.append((shard, at, take))
                    lo += take
                wk = jnp.concatenate([wkv_ref[g, at : at + n] for g, at, n in parts], axis=0)
                wv = jnp.concatenate([wkv_ref[g, kv_rows + at : kv_rows + at + n] for g, at, n in parts], axis=0)
                k = dot_t(rows[:t], wk).astype(BF16)
                kbuf[2 * j, :t] = k[:, :BLOCK]
                kbuf[2 * j + 1, :t] = k[:, BLOCK:]
                vbuf[2 * j : 2 * j + 2, :, :t] = dot_t(wv, rows[:t]).astype(BF16).reshape(2, BLOCK, t)

            lane = lax.broadcasted_iota(jnp.int32, (BLOCK, width), 1) % BLOCK
            row = lax.broadcasted_iota(jnp.int32, (BLOCK, width), 0)
            near = row <= lane
            tail = row < length - last * BLOCK

            def score(pair, out):
                keys = jnp.concatenate([kbuf[pair, :t], rot[:t]], axis=1)
                value = dot(keys, qbd[s, pair])
                top = jnp.where(near, value[:BLOCK], -1e30)
                out[:BLOCK] = top
                second = jnp.where(tail, value[BLOCK : 2 * BLOCK], -1e30)
                out[BLOCK : 2 * BLOCK] = second
                most = jnp.maximum(top, second)
                for b in range(2, blocks):
                    part = value[b * BLOCK : (b + 1) * BLOCK]
                    out[b * BLOCK : (b + 1) * BLOCK] = part
                    most = jnp.maximum(most, part)
                return jnp.max(most, axis=0, keepdims=True)

            def mix(pair, source, most):
                total = jnp.zeros((8, width), F32)
                for b in range(blocks):
                    e = jnp.exp2((source[b * BLOCK : (b + 1) * BLOCK] - most) * factor)
                    total = total + jnp.sum(e.reshape(BLOCK // 8, 8, width), axis=0)
                    pbuf[b * BLOCK : (b + 1) * BLOCK] = e.astype(BF16)
                inv = 1.0 / jnp.sum(total, axis=0, keepdims=True)
                o = dot(vbuf[pair, :, :t], pbuf[:t]) * inv
                obuf[pair, :nope] = o[:nope, :BLOCK].astype(BF16)
                obuf[pair, nope:] = o[nope:, BLOCK:].astype(BF16)

            def two_pairs(j, most):
                most_b = score(2 * j + 1, s_b)
                mix(2 * j, s_a, most)
                most = score(jnp.minimum(2 * j + 2, pairs - 1), s_a)
                mix(2 * j + 1, s_b, most_b)
                return most

            lax.fori_loop(0, pairs // 2, two_pairs, score(0, s_a))

        for blocks in range(2, cache_len // BLOCK + 1):
            pl.when(total == blocks)(functools.partial(attend, blocks))

        for pair in range(pairs):
            o = obuf[pair].astype(F32).T.astype(BF16)
            cols = slice(pair * BLOCK, (pair + 1) * BLOCK)
            first, second = o[:toks], o[toks:]
            own_ref[s, :, cols] = jnp.where(odd == 1, second, first)
            send_ref[s, :, cols] = jnp.where(odd == 1, first, second)

        lat_out[s] = lat_ref[s]
        for c in range(peers):
            piece = new_ref[c, s].astype(F32)
            for w in range(rank // BLOCK):
                fresh[w, BLOCK + c * toks : BLOCK + (c + 1) * toks] = piece[:, w * BLOCK : (w + 1) * BLOCK]
        base = (length // 16) * 16
        skew = length - base
        tile_row = lax.broadcasted_iota(jnp.int32, (16, BLOCK), 0)

        def shift(k, _):
            at = pl.multiple_of(base + k * 16, 16)
            for w in range(rank // BLOCK):
                moved = fresh[w, pl.ds(BLOCK - skew + k * 16, 16), :]
                local = tile_row + k * 16 - skew
                cols = slice(w * BLOCK, (w + 1) * BLOCK)
                old = lat_ref[s, pl.ds(at, 16), cols].astype(F32)
                lat_out[s, pl.ds(at, 16), cols] = jnp.where((local >= 0) & (local < chunk), moved, old).astype(BF16)
            return 0

        lax.fori_loop(0, chunk // 16 + (skew > 0).astype(jnp.int32), shift, 0)
        for b in range(cache_len // BLOCK):
            fresh_pe[b * BLOCK : (b + 1) * BLOCK, :rope] = old_pe[:, b * BLOCK : (b + 1) * BLOCK].T
        for c in range(peers):
            fresh_pe[pl.ds(length + c * toks, toks), :rope] = new_ref[c, s, :, rank:].astype(F32)
        for b in range(cache_len // BLOCK):
            pe_out[s, :, b * BLOCK : (b + 1) * BLOCK] = fresh_pe[b * BLOCK : (b + 1) * BLOCK].T[:rope].astype(BF16)
        return 0

    lax.fori_loop(0, seqs, one_sequence, 0)


def output_kernel(where_ref, own_ref, other_ref, w_ref, x_ref, y_ref):
    odd = where_ref[1]
    seqs, toks, depth = own_ref.shape
    shards = w_ref.shape[0] // 2

    def side(o, parity):
        w = jnp.concatenate([w_ref[2 * g + parity] for g in range(shards)], axis=0)
        return dot(o[...].reshape(seqs * toks, depth), w)

    y = side(own_ref, odd) + side(other_ref, 1 - odd)
    y = y + x_ref[...].reshape(y.shape).astype(F32)
    y_ref[...] = y.astype(BF16).reshape(y_ref.shape)


def solution(mesh):
    size = mesh.shape["tp"]
    even_odd = [[2 * c + p for c in range(size // 2)] for p in range(2)]
    chip_pairs = [[2 * c, 2 * c + 1] for c in range(size // 2)]
    swap = [(i, i ^ 1) for i in range(size)]

    def local_step(hidden, lengths, rope_cos, rope_sin, cache_lat, cache_pe, norm_in, w_dq, norm_q, w_dkv, norm_kv, w_uq, w_uk, w_uv, w_out):
        seqs, toks, dim = hidden.shape
        q_rank = w_dq.shape[1]
        rank, heads, nope = w_uk.shape
        rope = cache_pe.shape[2]
        cache_len = cache_lat.shape[1]
        chips = size // 2
        head = nope + rope
        pairs = chips * heads // 2
        index = lax.axis_index("tp")
        where = jnp.stack([index // 2, index % 2]).astype(jnp.int32)

        wq = w_uq.transpose(1, 2, 0).reshape(heads * head, q_rank)
        wkv = jnp.concatenate([w.transpose(1, 2, 0).reshape(heads * nope, rank) for w in (w_uk, w_uv)], axis=0)
        wkv_all = lax.all_gather(wkv, "tp", axis_index_groups=even_odd)
        wq_all = lax.all_gather(wq, "tp", axis_index_groups=even_odd)
        cos_t, sin_t = rope_cos.transpose(0, 2, 1), rope_sin.transpose(0, 2, 1)
        pe_t = cache_pe.transpose(0, 2, 1)
        wkv_down = w_dkv.transpose(1, 0)

        group = 4
        whole = lambda shape: pl.BlockSpec(shape, lambda i, w: (0,) * len(shape), pipeline_mode=pl.Buffered(1))
        cq, kv = pl.pallas_call(
            project_kernel,
            grid_spec=pltpu.PrefetchScalarGridSpec(
                num_scalar_prefetch=1,
                grid=(seqs // group,),
                in_specs=[
                    pl.BlockSpec((group, toks, dim), lambda i, w: (i, 0, 0)),
                    whole((1, dim)),
                    whole(w_dq.shape),
                    whole((1, q_rank)),
                    whole(wkv_down.shape),
                    whole((1, rank)),
                    pl.BlockSpec((group, rope // 2, BLOCK), lambda i, w: (i, 0, w[0])),
                    pl.BlockSpec((group, rope // 2, BLOCK), lambda i, w: (i, 0, w[0])),
                ],
                out_specs=[
                    pl.BlockSpec((group, toks, q_rank), lambda i, w: (i, 0, 0)),
                    pl.BlockSpec((group, toks, rank + rope), lambda i, w: (i, 0, 0)),
                ],
            ),
            out_shape=[jax.ShapeDtypeStruct((seqs, toks, q_rank), BF16), jax.ShapeDtypeStruct((seqs, toks, rank + rope), BF16)],
            cost_estimate=pl.CostEstimate(flops=2 * seqs * toks * dim * (q_rank + rank + rope), bytes_accessed=12 * 2**20, transcendentals=0),
            name="project",
        )(where, hidden, norm_in[None], w_dq, norm_q[None], wkv_down, norm_kv[None], cos_t, sin_t)

        new_all = lax.all_gather(kv, "tp")
        cq_all = lax.all_gather(cq, "tp", axis_index_groups=chip_pairs)
        w_all = lax.all_gather(w_out, "tp")

        step = 2
        whole = lambda shape: pl.BlockSpec(shape, lambda i, w, n: (0,) * len(shape), pipeline_mode=pl.Buffered(1))
        o_shape = jax.ShapeDtypeStruct((seqs, toks, pairs * 2 * nope), BF16)
        own, send, lat_new, pe_new = pl.pallas_call(
            attend_kernel,
            grid_spec=pltpu.PrefetchScalarGridSpec(
                num_scalar_prefetch=2,
                grid=(seqs // step,),
                in_specs=[
                    whole(wq_all.shape),
                    whole(wkv_all.shape),
                    pl.BlockSpec((2, step, toks, q_rank), lambda i, w, n: (0, i, 0, 0)),
                    pl.BlockSpec((step, rope // 2, BLOCK), lambda i, w, n: (i, 0, w[0])),
                    pl.BlockSpec((step, rope // 2, BLOCK), lambda i, w, n: (i, 0, w[0])),
                    pl.BlockSpec((size, step, toks, rank + rope), lambda i, w, n: (0, i, 0, 0)),
                    pl.BlockSpec((step, cache_len, rank), lambda i, w, n: (i, 0, 0)),
                    pl.BlockSpec((step, rope, cache_len), lambda i, w, n: (i, 0, 0)),
                ],
                out_specs=[
                    pl.BlockSpec((step, toks, pairs * 2 * nope), lambda i, w, n: (i, 0, 0)),
                    pl.BlockSpec((step, toks, pairs * 2 * nope), lambda i, w, n: (i, 0, 0)),
                    pl.BlockSpec((step, cache_len, rank), lambda i, w, n: (i, 0, 0)),
                    pl.BlockSpec((step, rope, cache_len), lambda i, w, n: (i, 0, 0)),
                ],
                scratch_shapes=[
                    pltpu.VMEM((heads * head, step * BLOCK), F32),
                    pltpu.VMEM((step, pairs, 2 * BLOCK, 2 * BLOCK), BF16),
                    pltpu.VMEM((cache_len, rank), BF16),
                    pltpu.VMEM((cache_len, BLOCK), BF16),
                    pltpu.VMEM((pairs, cache_len, BLOCK), BF16),
                    pltpu.VMEM((pairs, BLOCK, cache_len), BF16),
                    pltpu.VMEM((cache_len, 2 * BLOCK), F32),
                    pltpu.VMEM((cache_len, 2 * BLOCK), F32),
                    pltpu.VMEM((cache_len, 2 * BLOCK), BF16),
                    pltpu.VMEM((pairs, BLOCK, BLOCK), BF16),
                    pltpu.VMEM((rank // BLOCK, size * toks + 2 * BLOCK, BLOCK), F32),
                    pltpu.VMEM((cache_len, BLOCK), F32),
                ],
            ),
            out_shape=[
                o_shape,
                o_shape,
                jax.ShapeDtypeStruct(cache_lat.shape, BF16),
                jax.ShapeDtypeStruct(pe_t.shape, BF16),
            ],
            compiler_params=pltpu.CompilerParams(vmem_limit_bytes=60 * 2**20),
            cost_estimate=pl.CostEstimate(flops=40 * 10**9, bytes_accessed=30 * 2**20, transcendentals=30 * 10**6),
            name="attend",
        )(where, lengths, wq_all, wkv_all, cq_all, cos_t, sin_t, new_all, cache_lat, pe_t)

        other = lax.ppermute(send, "tp", swap)

        wide = 512
        y = pl.pallas_call(
            output_kernel,
            grid_spec=pltpu.PrefetchScalarGridSpec(
                num_scalar_prefetch=1,
                grid=(dim // wide,),
                in_specs=[
                    pl.BlockSpec(own.shape, lambda i, w: (0, 0, 0), pipeline_mode=pl.Buffered(1)),
                    pl.BlockSpec(own.shape, lambda i, w: (0, 0, 0), pipeline_mode=pl.Buffered(1)),
                    pl.BlockSpec(w_all.shape[:2] + (wide,), lambda i, w: (0, 0, i)),
                    pl.BlockSpec((seqs, toks, wide), lambda i, w: (0, 0, i)),
                ],
                out_specs=pl.BlockSpec((seqs, toks, wide), lambda i, w: (0, 0, i)),
            ),
            out_shape=jax.ShapeDtypeStruct(hidden.shape, BF16),
            cost_estimate=pl.CostEstimate(flops=2 * seqs * toks * dim * dim, bytes_accessed=30 * 2**20, transcendentals=0),
            name="output",
        )(where, own, other, w_all, hidden)
        return y, lat_new, pe_new.transpose(0, 2, 1)

    spec_tok = P("dp", "tp", None)
    spec_len = P("dp")
    spec_seq = P("dp", None, None)
    spec_vec = P(None)
    spec_mat = P(None, None)
    spec_head = P(None, "tp", None)
    spec_rows = P("tp", None)
    in_specs = (spec_tok, spec_len, spec_seq, spec_seq, spec_seq, spec_seq, spec_vec, spec_mat, spec_vec, spec_mat, spec_vec, spec_head, spec_head, spec_head, spec_rows)
    return jax.shard_map(local_step, mesh=mesh, in_specs=in_specs, out_specs=(spec_tok, spec_seq, spec_seq), check_vma=False)
```

```python
import functools

import jax
import jax.numpy as jnp
from jax import lax
from jax.experimental import pallas as pl
from jax.experimental.pallas import tpu as pltpu
from jax.sharding import PartitionSpec as P

BLOCK = 128
LOG2E = 1.4426950408889634
NEVER = -1e30
F32 = jnp.float32
BF16 = jnp.bfloat16
MESH = pl.DeviceIdType.MESH
MIB = 2**20


def dot(a, b):
    return lax.dot_general(a, b, (((1,), (0,)), ((), ())), preferred_element_type=F32)


def dot_t(a, b):
    return lax.dot_general(a, b, (((1,), (1,)), ((), ())), preferred_element_type=F32)


def unit(x):
    return x * lax.rsqrt(jnp.mean(x * x, axis=-1, keepdims=True) + 1e-6)


def project_kernel(
    size,
    x_hbm,
    g1_ref,
    wdq_hbm,
    gq_ref,
    wkv_hbm,
    gkv_ref,
    cos_ref,
    sin_ref,
    c_all,
    p_all,
    cq_pair,
    x_buf,
    wdq,
    wkv,
    a_buf,
    c_own,
    p_own,
    cq_own,
    load_sem,
    keep_sem,
    send_sem,
    recv_sem,
):
    me = lax.axis_index("tp")
    odd = lax.rem(me, 2)
    chip = me // 2
    right, left = lax.rem(me + 2, size), lax.rem(me + size - 2, size)
    other = me + 1 - 2 * odd
    seqs, toks, dim = x_hbm.shape
    groups = p_own.shape[0]
    per = seqs // groups
    rank = c_own.shape[2]
    rope = BLOCK // per
    half = rope // 2

    loads = [pltpu.make_async_copy(x_hbm.at[pl.ds(0, per)], x_buf.at[pl.ds(0, per)], load_sem.at[0])]
    loads.append(pltpu.make_async_copy(wkv_hbm, wkv, load_sem.at[1]))
    for g in range(1, groups):
        rows = pl.ds(g * per, per)
        loads.append(pltpu.make_async_copy(x_hbm.at[rows], x_buf.at[rows], load_sem.at[1 + g]))
    loads.append(pltpu.make_async_copy(wdq_hbm, wdq, load_sem.at[1 + groups]))
    for load in loads:
        load.start()

    barrier = pltpu.get_barrier_semaphore()
    for peer in (left, right, other):
        pl.semaphore_signal(barrier, inc=1, device_id={"tp": peer}, device_id_type=MESH)
    pl.semaphore_wait(barrier, 3)

    def copies(g, slot_from, slot_to, kind, peer, fresh=False):
        rows = pl.ds(g * per, per)
        c_src = c_own.at[rows] if fresh else c_all.at[rows, slot_from, odd]
        p_src = p_own.at[g] if fresh else p_all.at[g, slot_from, odd]
        out = []
        for which, (src, dst) in enumerate(((c_src, c_all.at[rows, slot_to, odd]), (p_src, p_all.at[g, slot_to, odd]))):
            at = (kind, g, which)
            out.append(pltpu.make_async_remote_copy(src, dst, send_sem.at[at], recv_sem.at[at], device_id={"tp": peer}, device_id_type=MESH))
        return out

    def keep(g):
        rows = pl.ds(g * per, per)
        return [
            pltpu.make_async_copy(c_own.at[rows], c_all.at[rows, 0, odd], keep_sem.at[0, g]),
            pltpu.make_async_copy(p_own.at[g], p_all.at[g, 0, odd], keep_sem.at[1, g]),
            pltpu.make_async_copy(cq_own.at[rows], cq_pair.at[odd, rows], keep_sem.at[2, g]),
        ]

    def send_cq(g):
        rows = pl.ds(g * per, per)
        return pltpu.make_async_remote_copy(
            cq_own.at[rows], cq_pair.at[odd, rows], send_sem.at[7, g, 0], recv_sem.at[7, g, 0], device_id={"tp": other}, device_id_type=MESH
        )

    started = []

    def go(list_of_copies):
        for copy in list_of_copies:
            copy.start()
        started.extend(list_of_copies)

    load_x = [loads[0]] + loads[2 : 1 + groups]
    for g in range(groups):
        load_x[g].wait()
        if g == 0:
            loads[1].wait()
        x = x_buf[g * per : (g + 1) * per].reshape(per * toks, dim).astype(F32)
        a = (unit(x) * g1_ref[...]).astype(BF16)
        a_buf[g] = a
        kv = dot_t(a, wkv[...])
        c_own[g * per : (g + 1) * per] = (unit(kv[:, :rank]) * gkv_ref[...]).astype(BF16).reshape(per, toks, rank)
        turned = []
        for s in range(per):
            lanes = pl.ds(pl.multiple_of(chip * BLOCK, BLOCK), BLOCK)
            cos_pair, sin_pair = cos_ref[g * per + s, :, lanes], sin_ref[g * per + s, :, lanes]
            cos = jnp.where(odd == 1, cos_pair[:, toks:], cos_pair[:, :toks])
            sin = jnp.where(odd == 1, sin_pair[:, toks:], sin_pair[:, :toks])
            table = jnp.concatenate([cos, cos, -sin, sin], axis=0).T
            p = kv[s * toks : (s + 1) * toks, rank:]
            swapped = jnp.concatenate([p[:, half:], p[:, :half]], axis=1)
            turned.append(p * table[:, :rope] + swapped * table[:, rope:])
        p_own[g] = jnp.concatenate(turned, axis=1).astype(BF16)
        go(copies(g, 0, 1, 0, right, True) + copies(g, 0, 3, 1, left, True) + copies(g, 0, 0, 3, other, True))
        for copy in keep(g)[:2]:
            copy.start()

    loads[-1].wait()
    for g in range(groups):
        h = dot(a_buf[g], wdq[...])
        cq_own[g * per : (g + 1) * per] = (unit(h) * gq_ref[...]).astype(BF16).reshape(per, toks, h.shape[-1])
        go([send_cq(g)])
        keep(g)[2].start()

    for g in range(groups):
        for copy in copies(g, 0, 1, 0, right, True):
            copy.wait_recv()
        go(copies(g, 1, 1, 4, other))

        @pl.when(odd == 0)
        def _():
            for copy in copies(g, 1, 2, 2, right):
                copy.start()

        for copy in copies(g, 0, 3, 1, left, True):
            copy.wait_recv()
        go(copies(g, 3, 3, 5, other))

        @pl.when(odd == 1)
        def _():
            for copy in copies(g, 3, 2, 2, left):
                copy.start()

    for g in range(groups):
        for copy in copies(g, 1, 2, 2, right):
            copy.wait_recv()
        go(copies(g, 2, 2, 6, other))

    for g in range(groups):
        for kind, slot in ((3, 0), (4, 1), (5, 3), (6, 2)):
            for copy in copies(g, slot, slot, kind, other, slot == 0):
                copy.wait_recv()
        send_cq(g).wait_recv()
        for copy in copies(g, 1, 2, 2, right):
            copy.wait_send()
        for copy in keep(g):
            copy.wait()
    for copy in started:
        copy.wait_send()


def cache_kernel(len_ref, c_ref, p_ref, lat_ref, pe_ref, lat_out, pe_out, fresh, fresh_pe):
    step = pl.program_id(0)
    chip = lax.axis_index("tp") // 2
    per, slots, _, toks, rank = c_ref.shape
    rope = pe_ref.shape[1]
    cache_len = lat_ref.shape[1]
    chunk = slots * 2 * toks
    words = rank // BLOCK
    tile_row = lax.broadcasted_iota(jnp.int32, (16, BLOCK), 0)

    def slot_of(j):
        return lax.rem(chip - j + slots, slots)

    def one_sequence(s, _):
        length = len_ref[step * per + s]
        for j in range(slots):
            piece = c_ref[s, slot_of(j)].reshape(2 * toks, rank).astype(F32)
            for w in range(words):
                fresh[w, BLOCK + j * 2 * toks : BLOCK + (j + 1) * 2 * toks] = piece[:, w * BLOCK : (w + 1) * BLOCK]
        lat_out[s] = lat_ref[s]
        base = (length // 16) * 16
        skew = length - base

        def tile(k, partial):
            at = pl.multiple_of(base + k * 16, 16)
            for w in range(words):
                moved = fresh[w, pl.ds(BLOCK - skew + k * 16, 16), :].astype(BF16)
                cols = slice(w * BLOCK, (w + 1) * BLOCK)
                if partial:
                    local = tile_row + k * 16 - skew
                    moved = jnp.where((local >= 0) & (local < chunk), moved.astype(F32), lat_ref[s, pl.ds(at, 16), cols].astype(F32)).astype(BF16)
                lat_out[s, pl.ds(at, 16), cols] = moved

        for k in range(chunk // 16):
            tile(k, k == 0)
        pl.when(skew > 0)(functools.partial(tile, chunk // 16, True))
        return 0

    lax.fori_loop(0, per, one_sequence, 0)

    for j in range(slots):
        fresh_pe[cache_len - chunk + j * 2 * toks : cache_len - chunk + (j + 1) * 2 * toks] = p_ref[0, slot_of(j)].reshape(2 * toks, BLOCK).astype(F32)
    old = pe_ref[...].reshape(per * rope, cache_len).astype(F32)
    lane_seq = lax.broadcasted_iota(jnp.int32, (BLOCK, BLOCK), 1) // rope
    row = lax.broadcasted_iota(jnp.int32, (BLOCK, BLOCK), 0)
    for b in range(cache_len // BLOCK):
        value = old[:, b * BLOCK : (b + 1) * BLOCK].T
        for s in range(per):
            length = len_ref[step * per + s]
            moved = fresh_pe[pl.ds(b * BLOCK + cache_len - chunk - length, BLOCK), :]
            local = row + (b * BLOCK - length)
            value = jnp.where((lane_seq == s) & (local >= 0) & (local < chunk), moved, value)
        pe_out[:, :, b * BLOCK : (b + 1) * BLOCK] = value.T.astype(BF16).reshape(per, rope, BLOCK)


def attend_kernel(
    sizes,
    len_ref,
    w0_ref,
    w1_ref,
    w2a_ref,
    w2b_ref,
    w3_ref,
    cq_ref,
    cos_ref,
    sin_ref,
    c_ref,
    p_ref,
    lat_ref,
    pe_ref,
    own_ref,
    send_ref,
    qraw,
    qbd,
    rows,
    rot,
    kbuf,
    vbuf,
    s_bufs,
    p_bufs,
    obuf,
):
    heads, nope, rope, q_rank, rank = sizes
    step = pl.program_id(0)
    me = lax.axis_index("tp")
    chip, odd = me // 2, lax.rem(me, 2)
    seqs, chunk, _ = c_ref.shape
    per = pe_ref.shape[0]
    prefix_max = pe_ref.shape[2]
    toks = own_ref.shape[1]
    half = rope // 2
    head = nope + rope
    q_rows = heads * head
    slots = chunk // BLOCK
    pairs = slots * heads // 2
    quads = pairs // 2
    wide = 2 * BLOCK
    factor = LOG2E * head**-0.5
    cut = w2a_ref.shape[0]
    new_rows = pl.multiple_of((chip + 1) * BLOCK, BLOCK)

    def weight_rows(slot, start, count):
        if slot != 2:
            return (w0_ref, w1_ref, None, w3_ref)[slot][start : start + count]
        if start + count <= cut:
            return w2a_ref[start : start + count]
        if start >= cut:
            return w2b_ref[start - cut : start - cut + count]
        return jnp.concatenate([w2a_ref[start:cut], w2b_ref[0 : start + count - cut]], axis=0)

    def head_rows(first, count, base):
        parts = []
        for h in range(first, first + count):
            parts.append(weight_rows(h // heads, base + (h % heads) * nope, nope))
        return jnp.concatenate(parts, axis=0)

    @pl.when(step == 0)
    def _():
        qbd[...] = jnp.zeros_like(qbd)

    ring = qbd.shape[0]
    first_slot = lax.rem(step * seqs, ring)

    @pl.when(first_slot == 0)
    def _():
        rot[:chunk] = p_ref[0]
        old = pe_ref[...].reshape(per * rope, prefix_max).astype(F32)
        for b in range(prefix_max // BLOCK):
            rot[pl.ds(new_rows + b * BLOCK, BLOCK), :] = old[:, b * BLOCK : (b + 1) * BLOCK].T.astype(BF16)

    cq = jnp.concatenate([cq_ref[c, s] for s in range(seqs) for c in range(2)], axis=0)
    lanes_chip = pl.ds(pl.multiple_of(chip * BLOCK, BLOCK), BLOCK)
    for slot in range(slots):
        raw = qraw.at[slot % 2]
        total = None
        for k in range(q_rank // rank):
            part = dot_t(weight_rows(slot, k * q_rows, q_rows), cq[:, k * rank : (k + 1) * rank])
            total = part if total is None else total + part
        raw[...] = total
        for h in range(heads):
            index = slot * heads + h
            pair, side = index // 2, index % 2
            base = h * head
            cols = slice(side * BLOCK, (side + 1) * BLOCK)
            for s in range(seqs):
                lanes = slice(s * BLOCK, (s + 1) * BLOCK)
                at = first_slot + s
                qbd[at, pair, side * nope : (side + 1) * nope, cols] = raw[base : base + nope, lanes].astype(BF16)
                lo = raw[base + nope : base + nope + half, lanes]
                hi = raw[base + nope + half : base + head, lanes]
                cos, sin = cos_ref[s, :, lanes_chip], sin_ref[s, :, lanes_chip]
                lo, hi = lo * cos - hi * sin, hi * cos + lo * sin
                start = pl.multiple_of(BLOCK + at * rope, rope)
                qbd[at, pair, pl.ds(start, rope), cols] = jnp.concatenate([lo, hi], axis=0).astype(BF16)

    def one_sequence(s, _):
        length = len_ref[step * seqs + s]
        prefix_blocks = (length + BLOCK - 1) // BLOCK
        count = prefix_blocks + chip + 1
        at = first_slot + s
        rows[:chunk] = c_ref[s]
        rows[pl.ds(new_rows, prefix_max), :] = lat_ref[s]

        def attend(blocks):
            t = blocks * BLOCK
            lane = lax.broadcasted_iota(jnp.int32, (BLOCK, wide), 1) % BLOCK
            row = lax.broadcasted_iota(jnp.int32, (BLOCK, wide), 0)
            near = row <= lane
            tail = row < length - (prefix_blocks - 1) * BLOCK

            def keys_values(j):
                kbuf[j, :t] = dot_t(rows[:t], head_rows(4 * j, 4, (q_rank // rank) * q_rows)).astype(BF16)
                vbuf[j, :, :t] = dot_t(head_rows(4 * j, 4, (q_rank // rank) * q_rows + heads * nope), rows[:t]).astype(BF16)

            def score(pair):
                out = s_bufs[pair % 3]
                keys = jnp.concatenate([kbuf[pair // 2, :t, (pair % 2) * BLOCK : (pair % 2 + 1) * BLOCK], rot[:t]], axis=1)
                value = dot(keys, qbd[at, pair])
                most = None
                for b in range(blocks):
                    part = value[b * BLOCK : (b + 1) * BLOCK]
                    if b == 0:
                        part = jnp.where(near, part, NEVER)
                    if b == blocks - 1:
                        part = jnp.where(tail, part, NEVER)
                    out[b * BLOCK : (b + 1) * BLOCK] = part
                    part = jnp.max(part.reshape(BLOCK // 8, 8, wide), axis=0)
                    most = part if most is None else jnp.maximum(most, part)
                return jnp.max(most, axis=0, keepdims=True)

            def mix(pair, most):
                source, probs = s_bufs[pair % 3], p_bufs[pair % 2]
                total = None
                for b in range(blocks):
                    e = jnp.exp2((source[b * BLOCK : (b + 1) * BLOCK] - most) * factor)
                    part = jnp.sum(e.reshape(BLOCK // 8, 8, wide), axis=0)
                    total = part if total is None else total + part
                    probs[b * BLOCK : (b + 1) * BLOCK] = e.astype(BF16)
                inv = 1.0 / jnp.sum(total, axis=0, keepdims=True)
                value = vbuf[pair // 2, (pair % 2) * BLOCK : (pair % 2 + 1) * BLOCK, :t]
                o = dot(value, probs[:t]) * inv
                obuf[pair, :nope] = o[:nope, :BLOCK].astype(BF16)
                obuf[pair, nope:] = o[nope:, BLOCK:].astype(BF16)

            keys_values(0)
            most = {0: score(0), 1: score(1)}
            for pair in range(pairs):
                if pair % 2 == 0 and pair // 2 + 1 < quads:
                    keys_values(pair // 2 + 1)
                if pair + 2 < pairs:
                    most[pair + 2] = score(pair + 2)
                mix(pair, most.pop(pair))

        for blocks in range(2, (chunk + prefix_max) // BLOCK + 1):
            pl.when(count == blocks)(functools.partial(attend, blocks))

        for pair in range(pairs):
            o = obuf[pair].astype(F32).T.astype(BF16)
            cols = slice(pair * BLOCK, (pair + 1) * BLOCK)
            first, second = o[:toks], o[toks:]
            own_ref[s, :, cols] = jnp.where(odd == 1, second, first)
            send_ref[s, :, cols] = jnp.where(odd == 1, first, second)
        return 0

    lax.fori_loop(0, seqs, one_sequence, 0)


def output_kernel(own_ref, other_ref, *refs):
    *w_refs, x_ref, y_ref = refs
    seqs, toks, depth = own_ref.shape
    n = len(w_refs) // 2
    y = x_ref[...].reshape(seqs * toks, x_ref.shape[2]).astype(F32)
    for o, ws in ((own_ref, w_refs[:n]), (other_ref, w_refs[n:])):
        w = jnp.concatenate([r[...] for r in ws], axis=0)
        y = y + dot(o[...].reshape(seqs * toks, depth), w)
    y_ref[...] = y.astype(BF16).reshape(y_ref.shape)


def solution(mesh):
    size = mesh.shape["tp"]
    swap = [(i, i ^ 1) for i in range(size)]
    rightward = [(i, (i + 2) % size) for i in range(size)]
    leftward = [(i, (i - 2) % size) for i in range(size)]

    def ring(w):
        from_left = lax.ppermute(w, "tp", rightward)
        from_right = lax.ppermute(w, "tp", leftward)
        cut = w.shape[0] // 2
        return [w, from_left, lax.ppermute(from_left[:cut], "tp", rightward), lax.ppermute(from_right[cut:], "tp", leftward), from_right]

    def local_step(hidden, lengths, rope_cos, rope_sin, cache_lat, cache_pe, norm_in, w_dq, norm_q, w_dkv, norm_kv, w_uq, w_uk, w_uv, w_out):
        seqs, toks, dim = hidden.shape
        q_rank = w_dq.shape[1]
        rank, heads, nope = w_uk.shape
        rope = cache_pe.shape[2]
        cache_len = cache_lat.shape[1]
        chips = size // 2
        head = nope + rope
        pairs = chips * heads // 2
        depth = pairs * 2 * nope
        chunk = size * toks
        per = BLOCK // rope
        groups = seqs // per
        cos_t, sin_t = rope_cos.transpose(0, 2, 1), rope_sin.transpose(0, 2, 1)
        pe_t = cache_pe.transpose(0, 2, 1)
        wkv_down = w_dkv.transpose(1, 0)

        wq = w_uq.transpose(1, 2, 0).reshape(heads * head, q_rank)
        weights = [wq[:, k * rank : (k + 1) * rank] for k in range(q_rank // rank)]
        weights += [w.transpose(1, 2, 0).reshape(heads * nope, rank) for w in (w_uk, w_uv)]
        weights = ring(jnp.concatenate(weights, axis=0))

        any_spec = pl.BlockSpec(memory_space=pl.ANY)
        vmem_spec = pl.BlockSpec(memory_space=pltpu.VMEM)
        c_all, p_all, cq_pair = pl.pallas_call(
            functools.partial(project_kernel, size),
            in_specs=[any_spec, vmem_spec, any_spec, vmem_spec, any_spec, vmem_spec, vmem_spec, vmem_spec],
            out_specs=[any_spec] * 3,
            out_shape=[
                jax.ShapeDtypeStruct((seqs, chips, 2, toks, rank), BF16),
                jax.ShapeDtypeStruct((groups, chips, 2, toks, BLOCK), BF16),
                jax.ShapeDtypeStruct((2, seqs, toks, q_rank), BF16),
            ],
            scratch_shapes=[
                pltpu.VMEM(hidden.shape, BF16),
                pltpu.VMEM(w_dq.shape, BF16),
                pltpu.VMEM(wkv_down.shape, BF16),
                pltpu.VMEM((groups, per * toks, dim), BF16),
                pltpu.VMEM((seqs, toks, rank), BF16),
                pltpu.VMEM((groups, toks, BLOCK), BF16),
                pltpu.VMEM((seqs, toks, q_rank), BF16),
                pltpu.SemaphoreType.DMA((groups + 2,)),
                pltpu.SemaphoreType.DMA((3, groups)),
                pltpu.SemaphoreType.DMA((8, groups, 2)),
                pltpu.SemaphoreType.DMA((8, groups, 2)),
            ],
            compiler_params=pltpu.CompilerParams(collective_id=0, has_side_effects=True, vmem_limit_bytes=40 * MIB),
            cost_estimate=pl.CostEstimate(flops=2 * seqs * toks * dim * (q_rank + rank + rope), bytes_accessed=12 * MIB, transcendentals=0),
            name="project",
        )(hidden, norm_in, w_dq, norm_q, wkv_down, norm_kv, cos_t, sin_t)

        w_out, c_all = lax.optimization_barrier((w_out, c_all))
        out_own = ring(w_out)
        out_other = [lax.ppermute(w, "tp", swap) for w in out_own]

        lat_new, pe_new = pl.pallas_call(
            cache_kernel,
            grid_spec=pltpu.PrefetchScalarGridSpec(
                num_scalar_prefetch=1,
                grid=(groups,),
                in_specs=[
                    pl.BlockSpec((per, chips, 2, toks, rank), lambda i, n: (i, 0, 0, 0, 0)),
                    pl.BlockSpec((1, chips, 2, toks, BLOCK), lambda i, n: (i, 0, 0, 0, 0)),
                    pl.BlockSpec((per, cache_len, rank), lambda i, n: (i, 0, 0)),
                    pl.BlockSpec((per, rope, cache_len), lambda i, n: (i, 0, 0)),
                ],
                out_specs=[
                    pl.BlockSpec((per, cache_len, rank), lambda i, n: (i, 0, 0)),
                    pl.BlockSpec((per, rope, cache_len), lambda i, n: (i, 0, 0)),
                ],
                scratch_shapes=[
                    pltpu.VMEM((rank // BLOCK, chunk + 2 * BLOCK, BLOCK), F32),
                    pltpu.VMEM((2 * cache_len - chunk, BLOCK), F32),
                ],
            ),
            out_shape=[jax.ShapeDtypeStruct(cache_lat.shape, BF16), jax.ShapeDtypeStruct(pe_t.shape, BF16)],
            cost_estimate=pl.CostEstimate(flops=4 * 10**9, bytes_accessed=20 * MIB, transcendentals=0),
            name="cache",
        )(lengths, c_all, p_all, cache_lat, pe_t)

        step = 2
        prefix = cache_len - chunk
        whole = lambda a: pl.BlockSpec(a.shape, lambda i, n: (0,) * a.ndim, pipeline_mode=pl.Buffered(1))
        o_shape = jax.ShapeDtypeStruct((seqs, toks, depth), BF16)
        own, send = pl.pallas_call(
            functools.partial(attend_kernel, (heads, nope, rope, q_rank, rank)),
            grid_spec=pltpu.PrefetchScalarGridSpec(
                num_scalar_prefetch=1,
                grid=(seqs // step,),
                in_specs=[whole(w) for w in weights]
                + [
                    pl.BlockSpec((2, step, toks, q_rank), lambda i, n: (0, i, 0, 0)),
                    pl.BlockSpec((step, rope // 2, chunk), lambda i, n: (i, 0, 0)),
                    pl.BlockSpec((step, rope // 2, chunk), lambda i, n: (i, 0, 0)),
                    pl.BlockSpec((step, chunk, rank), lambda i, n: (i, 0, 0)),
                    pl.BlockSpec((1, chunk, BLOCK), lambda i, n: (i * step // per, 0, 0)),
                    pl.BlockSpec((step, prefix, rank), lambda i, n: (i, 0, 0)),
                    pl.BlockSpec((per, rope, prefix), lambda i, n: (i * step // per, 0, 0)),
                ],
                out_specs=[
                    pl.BlockSpec((step, toks, depth), lambda i, n: (i, 0, 0)),
                    pl.BlockSpec((step, toks, depth), lambda i, n: (i, 0, 0)),
                ],
                scratch_shapes=[
                    pltpu.VMEM((2, heads * head, step * BLOCK), F32),
                    pltpu.VMEM((per, pairs, 2 * BLOCK, 2 * BLOCK), BF16),
                    pltpu.VMEM((cache_len, rank), BF16),
                    pltpu.VMEM((cache_len, BLOCK), BF16),
                    pltpu.VMEM((pairs // 2, cache_len, 2 * BLOCK), BF16),
                    pltpu.VMEM((pairs // 2, 2 * BLOCK, cache_len), BF16),
                    [pltpu.VMEM((cache_len, 2 * BLOCK), F32) for _ in range(3)],
                    [pltpu.VMEM((cache_len, 2 * BLOCK), BF16) for _ in range(2)],
                    pltpu.VMEM((pairs, BLOCK, BLOCK), BF16),
                ],
            ),
            out_shape=[o_shape, o_shape],
            compiler_params=pltpu.CompilerParams(vmem_limit_bytes=60 * MIB),
            cost_estimate=pl.CostEstimate(flops=40 * 10**9, bytes_accessed=30 * MIB, transcendentals=30 * 10**6),
            name="attend",
        )(
            lengths,
            *weights,
            cq_pair,
            cos_t,
            sin_t,
            c_all.reshape(seqs, chunk, rank),
            p_all.reshape(groups, chunk, BLOCK),
            cache_lat,
            pe_t,
        )

        other = lax.ppermute(send, "tp", swap)

        wide = 512
        held = lambda a: pl.BlockSpec(a.shape, lambda i: (0,) * a.ndim, pipeline_mode=pl.Buffered(1))
        y = pl.pallas_call(
            output_kernel,
            grid=(dim // wide,),
            in_specs=[held(own), held(other)]
            + [pl.BlockSpec((w.shape[0], wide), lambda i: (0, i)) for w in out_own + out_other]
            + [pl.BlockSpec((seqs, toks, wide), lambda i: (0, 0, i))],
            out_specs=pl.BlockSpec((seqs, toks, wide), lambda i: (0, 0, i)),
            out_shape=jax.ShapeDtypeStruct(hidden.shape, BF16),
            cost_estimate=pl.CostEstimate(flops=2 * seqs * toks * dim * dim, bytes_accessed=30 * MIB, transcendentals=0),
            name="output",
        )(own, other, *out_own, *out_other, hidden)
        return y, lat_new, pe_new.transpose(0, 2, 1)

    spec_tok = P("dp", "tp", None)
    spec_len = P("dp")
    spec_seq = P("dp", None, None)
    spec_vec = P(None)
    spec_mat = P(None, None)
    spec_head = P(None, "tp", None)
    spec_rows = P("tp", None)
    in_specs = (spec_tok, spec_len, spec_seq, spec_seq, spec_seq, spec_seq, spec_vec, spec_mat, spec_vec, spec_mat, spec_vec, spec_head, spec_head, spec_head, spec_rows)
    return jax.shard_map(local_step, mesh=mesh, in_specs=in_specs, out_specs=(spec_tok, spec_seq, spec_seq), check_vma=False)
```

```python
import functools

import jax
import jax.numpy as jnp
from jax import lax
from jax.experimental import pallas as pl
from jax.experimental.pallas import tpu as pltpu
from jax.sharding import PartitionSpec as P

BLOCK = 128
LOG2E = 1.4426950408889634
NEVER = -1e30
F32 = jnp.float32
BF16 = jnp.bfloat16
MESH = pl.DeviceIdType.MESH
MIB = 2**20


def dot(a, b):
    return lax.dot_general(a, b, (((1,), (0,)), ((), ())), preferred_element_type=F32)


def dot_t(a, b):
    return lax.dot_general(a, b, (((1,), (1,)), ((), ())), preferred_element_type=F32)


def unit(x):
    return x * lax.rsqrt(jnp.mean(x * x, axis=-1, keepdims=True) + 1e-6)


class Wire:
    def __init__(self, send_sem, recv_sem):
        self.sems = (send_sem, recv_sem)
        self.made = {}
        self.index = {}

    def add(self, name, src, dst, **peer):
        self.index[name] = len(self.index)
        self.made[name] = lambda: pltpu.make_async_remote_copy(
            src(), dst(), self.sems[0].at[self.index[name]], self.sems[1].at[self.index[name]], device_id=peer, device_id_type=MESH
        )

    def start(self, *names):
        for name in names:
            self.made[name]().start()

    def landed(self, *names):
        for name in names:
            self.made[name]().wait_recv()

    def sent(self, *names):
        for name in names:
            self.made[name]().wait_send()


def main_kernel(
    plan,
    len_ref,
    x_hbm,
    g1_ref,
    wdq_hbm,
    gq_ref,
    wdkv_hbm,
    gkv_ref,
    cos_ref,
    sin_ref,
    wq_hbm,
    wk_hbm,
    wv_hbm,
    wo_hbm,
    lat_hbm,
    pe_hbm,
    c_out,
    p_out,
    o_out,
    wo_out,
    x_buf,
    wdq,
    wdkv,
    a_buf,
    rows,
    rot,
    pe_buf,
    cq_buf,
    wq,
    wkv,
    kb,
    vb,
    qb,
    sb,
    mb,
    pb,
    lb,
    o_own,
    o_send,
    load_sem,
    send_sem,
    recv_sem,
):
    size, paired = plan
    me = lax.axis_index("tp")
    odd = lax.rem(me, 2)
    chip = me // 2
    right, left = lax.rem(me + 2, size), lax.rem(me + size - 2, size)
    onward = jnp.where(odd == 0, right, left)
    other = me + 1 - 2 * odd
    dp = lax.axis_index("dp")
    e = lax.rem(dp, 2) if paired else dp * 0
    partner = dp + 1 - 2 * e

    seqs, toks, dim = x_hbm.shape
    groups = rot.shape[0]
    per = seqs // groups
    rank = rows.shape[2]
    slots = size // 2
    chunk = size * toks
    prefix = rows.shape[1] - chunk
    heads = wq.shape[0] // slots
    head, q_rank = wq.shape[1:]
    rope = BLOCK // per
    half = rope // 2
    nope = head - rope
    quads = wq.shape[0] // 4
    duos = seqs // 2
    wide = 2 * BLOCK
    factor = LOG2E * head**-0.5

    loads = {}

    def load(name, src, dst):
        loads[name] = pltpu.make_async_copy(src, dst, load_sem.at[len(loads)])
        loads[name].start()

    def spot(slot, parity):
        return pl.ds(pl.multiple_of(prefix + slot * BLOCK + parity * toks, toks), toks)

    load("x0", x_hbm.at[pl.ds(0, per)], x_buf.at[pl.ds(0, per)])
    load("wdkv", wdkv_hbm, wdkv)
    load("wk", wk_hbm, wkv.at[pl.ds(0, heads), pl.ds(0, nope)])
    load("wv", wv_hbm, wkv.at[pl.ds(0, heads), pl.ds(nope, nope)])
    for g in range(1, groups):
        load(f"x{g}", x_hbm.at[pl.ds(g * per, per)], x_buf.at[pl.ds(g * per, per)])
    load("wdq", wdq_hbm, wdq)
    load("wq", wq_hbm, wq.at[pl.ds(0, heads)])
    load("pe", pe_hbm.at[:, :, pl.ds(0, prefix)], pe_buf)
    load("lat", lat_hbm.at[:, pl.ds(0, prefix)], rows.at[:, pl.ds(0, prefix)])

    barrier = pltpu.get_barrier_semaphore()
    for peer in (left, right, other):
        pl.semaphore_signal(barrier, inc=1, device_id={"tp": peer}, device_id_type=MESH)
    if paired:
        pl.semaphore_signal(barrier, inc=1, device_id={"dp": partner}, device_id_type=MESH)
    pl.semaphore_wait(barrier, 4 if paired else 3)

    wire = Wire(send_sem, recv_sem)

    def chain(name, here, there, places):
        near_left, near_right, opposite = places
        handed = jnp.where(odd == 0, near_left, near_right)
        wire.add(name + "R", lambda: here(0), lambda: there(near_left), tp=right)
        wire.add(name + "L", lambda: here(0), lambda: there(near_right), tp=left)
        wire.add(name + "O", lambda: there(handed), lambda: there(opposite), tp=onward)

    for g in range(groups):
        for name, ref in (("c", lambda slot, g=g: rows.at[pl.ds(g * per, per), spot(slot, odd)]), ("p", lambda slot, g=g: rot.at[g, spot(slot, odd)])):
            name = f"{name}{g}"
            chain(name, ref, ref, (1, 3, 2))
            for slot in range(slots):
                wire.add(f"{name}S{slot}", functools.partial(ref, slot), functools.partial(ref, slot), tp=other)
        cq_ref = lambda g=g: cq_buf.at[odd, pl.ds(g * per, per)]
        wire.add(f"q{g}S", cq_ref, cq_ref, tp=other)

    def cut(total, side, unit, part):
        if part == "mid":
            return pl.ds(side, total - 2 * side)
        flip = e if part == "mine" else 1 - e
        return pl.ds(pl.multiple_of(flip * (total - side), unit), side)

    def wq_at(part, slot):
        return wq.at[pl.ds(slot * heads, heads), :, cut(q_rank, q_rank // 3, BLOCK, part)]

    def wkv_at(part, slot):
        return wkv.at[pl.ds(slot * heads, heads), cut(2 * nope, 48, 16, part)]

    def wo_at(part, slot):
        return wo_out.at[odd, slot, cut(wo_hbm.shape[0], 80, 16, part)]

    def wo_own(part, slot):
        return wo_hbm.at[cut(wo_hbm.shape[0], 80, 16, part)]

    by_ring = ("mine", "mid") if paired else ("mine", "mid", "rest")
    for name, here, there in (("wq", wq_at, wq_at), ("wkv", wkv_at, wkv_at), ("wo", wo_own, wo_at)):
        for part in by_ring:
            chain(f"{name}.{part}", functools.partial(here, part), functools.partial(there, part), (1, 2, 3))
        if paired:
            for slot in (1, 2, 3):
                ref = functools.partial(there, "mine", slot)
                wire.add(f"{name}Z{slot}", ref, ref, dp=partner)
    late = ("mid",) if paired else ("mid", "rest")
    for slot in range(slots):
        mine = lambda slot=slot: wo_out.at[odd, slot]
        wire.add(f"woS{slot}", mine if slot else lambda: wo_hbm, mine, tp=other)
    for quad in range(quads):
        wire.add(f"o{quad}S", lambda quad=quad: o_send.at[quad], lambda quad=quad: o_out.at[1, quad], tp=other)

    def both(name, parts):
        return [f"{name}.{part}{way}" for part in parts for way in "RL"]

    def onwards(name, parts):
        return [f"{name}.{part}O" for part in parts]

    def across(name, *which):
        return [f"{name}Z{slot}" for slot in which] if paired else []

    loads["wk"].wait()
    loads["wv"].wait()
    wire.start(*both("wkv", ("mine",)))
    loads["wdkv"].wait()
    for g in range(groups):
        loads[f"x{g}"].wait()
    for g in range(groups):
        x = x_buf[g * per : (g + 1) * per].reshape(per * toks, dim).astype(F32)
        a = (unit(x) * g1_ref[...]).astype(BF16)
        a_buf[g] = a
        kv = dot_t(a, wdkv[...])
        rows[g * per : (g + 1) * per, spot(0, odd), :] = (unit(kv[:, :rank]) * gkv_ref[...]).astype(BF16).reshape(per, toks, rank)
        turned = []
        for s in range(per):
            lanes = pl.ds(pl.multiple_of(chip * BLOCK, BLOCK), BLOCK)
            cos_pair, sin_pair = cos_ref[g * per + s, :, lanes], sin_ref[g * per + s, :, lanes]
            cos = jnp.where(odd == 1, cos_pair[:, toks:], cos_pair[:, :toks])
            sin = jnp.where(odd == 1, sin_pair[:, toks:], sin_pair[:, :toks])
            table = jnp.concatenate([cos, cos, -sin, sin], axis=0).T
            p = kv[s * toks : (s + 1) * toks, rank:]
            swapped = jnp.concatenate([p[:, half:], p[:, :half]], axis=1)
            turned.append(p * table[:, :rope] + swapped * table[:, rope:])
        rot[g, spot(0, odd), :] = jnp.concatenate(turned, axis=1).astype(BF16)
        for way in ("R", "L", "S0"):
            wire.start(f"c{g}{way}", f"p{g}{way}")

    loads["wdq"].wait()
    for g in range(groups):
        h = dot(a_buf[g], wdq[...])
        cq_buf[odd, g * per : (g + 1) * per] = (unit(h) * gq_ref[...]).astype(BF16).reshape(per, toks, q_rank)
        wire.start(f"q{g}S")

    loads["pe"].wait()
    for g in range(groups):
        old = pe_buf[g * per : (g + 1) * per].reshape(per * rope, prefix).astype(F32)
        for b in range(prefix // BLOCK):
            rot[g, b * BLOCK : (b + 1) * BLOCK] = old[:, b * BLOCK : (b + 1) * BLOCK].T.astype(BF16)
    qb[...] = jnp.zeros_like(qb)

    for g in range(groups):
        wire.landed(f"c{g}R", f"p{g}R", f"c{g}L", f"p{g}L")
        wire.start(f"c{g}O", f"p{g}O", f"c{g}S1", f"p{g}S1", f"c{g}S3", f"p{g}S3")
    loads["wq"].wait()
    wire.start(*both("wq", ("mine",)), *both("wkv", late), *both("wq", late))
    wire.landed(*both("wkv", ("mine",)))
    wire.start(*across("wkv", 1, 2), *onwards("wkv", ("mine",)))

    def rest_of(g):
        wire.landed(f"c{g}O", f"p{g}O")
        wire.start(f"c{g}S2", f"p{g}S2")
        for slot in (0, 1, 3, 2):
            wire.landed(f"c{g}S{slot}", f"p{g}S{slot}")
        wire.landed(f"q{g}S")

    loads["lat"].wait()
    rest_of(0)

    row = lax.broadcasted_iota(jnp.int32, (BLOCK, wide), 0)
    lane = lax.rem(lax.broadcasted_iota(jnp.int32, (BLOCK, wide), 1), BLOCK)
    near = row <= lane
    lanes_chip = pl.ds(pl.multiple_of(chip * BLOCK, BLOCK), BLOCK)

    def place(n):
        return n // duos, lax.rem(n, duos)

    def query_stage(n):
        quad, duo = place(n)
        w = wq[pl.ds(quad * 4, 4)].reshape(4 * head, q_rank)
        cq = jnp.concatenate([cq_buf[parity, 2 * duo + u] for u in range(2) for parity in range(2)], axis=0)
        raw = dot_t(w, cq)
        for u in range(2):
            slot = 2 * lax.rem(duo, 2) + u
            cos, sin = cos_ref[2 * duo + u, :, lanes_chip], sin_ref[2 * duo + u, :, lanes_chip]
            for h in range(4):
                pair, side = h // 2, h % 2
                q = raw[h * head : (h + 1) * head, u * BLOCK : (u + 1) * BLOCK]
                cols = slice(side * BLOCK, (side + 1) * BLOCK)
                qb[u, pair, side * nope : (side + 1) * nope, cols] = q[:nope].astype(BF16)
                lo, hi = q[nope : nope + half], q[nope + half :]
                turned = jnp.concatenate([lo * cos - hi * sin, hi * cos + lo * sin], axis=0).astype(BF16)
                start = pl.multiple_of(BLOCK + slot * rope, rope)
                stale = pl.multiple_of(BLOCK + lax.rem(slot + 2, 4) * rope, rope)
                qb[u, pair, pl.ds(start, rope), cols] = turned
                qb[u, pair, pl.ds(stale, rope), cols] = jnp.zeros_like(turned)

    def key_stage(n, t):
        quad, duo = place(n)
        w = wkv[pl.ds(quad * 4, 4), :nope].reshape(4 * nope, rank)
        for u in range(2):
            kb[u, :t] = dot_t(rows[2 * duo + u, :t], w).astype(BF16)

    def value_stage(n, t):
        quad, duo = place(n)
        w = wkv[pl.ds(quad * 4, 4), nope:].reshape(4 * nope, rank)
        for u in range(2):
            vb[u, :, :t] = dot_t(w, rows[2 * duo + u, :t]).astype(BF16)

    def score_stage(n, t, u, pair):
        _, duo = place(n)
        length = len_ref[2 * duo + u]
        keys = jnp.concatenate([kb[u, :t, pair * BLOCK : (pair + 1) * BLOCK], rot[duo // 2, :t]], axis=1)
        value = dot(keys, qb[u, pair])
        most = None
        for b in range(t // BLOCK):
            part = value[b * BLOCK : (b + 1) * BLOCK]
            if BLOCK <= b * BLOCK < prefix:
                part = jnp.where(row < length - b * BLOCK, part, NEVER)
            if b * BLOCK == prefix:
                part = jnp.where(near, part, NEVER)
            sb[2 * u + pair][b * BLOCK : (b + 1) * BLOCK] = part
            part = jnp.max(part.reshape(BLOCK // 8, 8, wide), axis=0)
            most = part if most is None else jnp.maximum(most, part)
        mb[2 * u + pair] = jnp.broadcast_to(jnp.max(most, axis=0, keepdims=True), (8, wide))

    def soft_stage(t, u, pair):
        i = 2 * u + pair
        most = mb[i, :1]
        total = None
        for b in range(t // BLOCK):
            x = jnp.exp2((sb[i][b * BLOCK : (b + 1) * BLOCK] - most) * factor)
            part = jnp.sum(x.reshape(BLOCK // 8, 8, wide), axis=0)
            total = part if total is None else total + part
            pb[i][b * BLOCK : (b + 1) * BLOCK] = x.astype(BF16)
        lb[i] = total

    def mix_stage(n, t, u, pair):
        quad, duo = place(n)
        i = 2 * u + pair
        inv = 1.0 / jnp.sum(lb[i], axis=0, keepdims=True)
        o = dot(vb[u, pair * BLOCK : (pair + 1) * BLOCK, :t], pb[i][:t]) * inv
        o = jnp.concatenate([o[:nope, :BLOCK], o[nope:, BLOCK:]], axis=0).T.astype(BF16)
        first, second = o[:toks], o[toks:]
        cols = slice(pair * BLOCK, (pair + 1) * BLOCK)
        o_own[quad, 2 * duo + u, :, cols] = jnp.where(odd == 1, second, first)
        o_send[quad, 2 * duo + u, :, cols] = jnp.where(odd == 1, first, second)

    units = [(u, pair) for u in range(2) for pair in range(2)]
    total = quads * duos

    def each_chip(fn):
        for c in range(slots):
            pl.when(chip == c)(lambda c=c: fn(prefix + (c + 1) * BLOCK))

    def body(b, t):
        before, ahead, later = jnp.maximum(b - 1, 0), jnp.minimum(b + 1, total - 1), jnp.minimum(b + 2, total - 1)
        for u, pair in units:
            mix_stage(before, t, u, pair)
        value_stage(b, t)
        for u, pair in units:
            soft_stage(t, u, pair)
            score_stage(ahead, t, u, pair)
        key_stage(later, t)
        query_stage(later)

    def at(b, when):
        return pl.when(b == when)

    def step(b, _):
        @at(b, 0)
        def _():
            rest_of(1)

        @at(b, 2)
        def _():
            rest_of(2)
            pltpu.make_async_copy(rows.at[:, pl.ds(prefix, chunk)], c_out, load_sem.at[0]).start()
            pltpu.make_async_copy(rot.at[:, pl.ds(prefix, chunk)], p_out, load_sem.at[1]).start()

        @at(b, 3)
        def _():
            wire.landed(*both("wq", ("mine",)))
            wire.start(*across("wq", 1, 2), *onwards("wq", ("mine",)))

        @at(b, duos - 2)
        def _():
            wire.landed(*both("wkv", late), *both("wq", late))
            wire.start(*onwards("wkv", late), *onwards("wq", late))
            wire.start(*both("wo", ("mine",)), "woS0")
            wire.landed(*across("wkv", 1, 2), *across("wq", 1, 2))

        @at(b, 9)
        def _():
            wire.landed(*onwards("wkv", by_ring), *onwards("wq", by_ring))
            wire.start(*across("wkv", 3), *across("wq", 3))

        @at(b, 15)
        def _():
            wire.landed(*both("wo", ("mine",)))
            wire.start(*across("wo", 1, 2), *onwards("wo", ("mine",)), *both("wo", late))
            wire.landed(*across("wkv", 3), *across("wq", 3))

        @at(b, 25)
        def _():
            wire.landed(*onwards("wo", ("mine",)))
            wire.start(*across("wo", 3))

        @at(b, 27)
        def _():
            wire.landed(*both("wo", late))
            wire.start(*onwards("wo", late))

        for quad in range(quads - 1):
            at(b, (quad + 1) * duos + 1)(functools.partial(wire.start, f"o{quad}S"))

        each_chip(functools.partial(body, b))
        return 0

    def lead_in(t):
        key_stage(0, t)
        query_stage(0)

    def second(t):
        for u, pair in units:
            score_stage(0, t, u, pair)
        key_stage(1, t)
        query_stage(1)

    each_chip(lead_in)
    each_chip(second)
    lax.fori_loop(0, total, step, 0)

    def last(t):
        for u, pair in units:
            mix_stage(total - 1, t, u, pair)

    each_chip(last)
    wire.start(f"o{quads - 1}S")
    pltpu.make_async_copy(o_own, o_out.at[0], load_sem.at[2]).start()
    pltpu.make_async_copy(wo_hbm, wo_out.at[odd, 0], load_sem.at[3]).start()

    wire.landed(*across("wo", 1, 2))
    wire.start("woS1", "woS2")
    wire.landed(*onwards("wo", late), *across("wo", 3))
    wire.start("woS3")
    for slot in range(slots):
        wire.landed(f"woS{slot}")
    for quad in range(quads):
        wire.landed(f"o{quad}S")
    wire.sent(*wire.index)
    pltpu.make_async_copy(rows.at[:, pl.ds(prefix, chunk)], c_out, load_sem.at[0]).wait()
    pltpu.make_async_copy(rot.at[:, pl.ds(prefix, chunk)], p_out, load_sem.at[1]).wait()
    pltpu.make_async_copy(o_own, o_out.at[0], load_sem.at[2]).wait()
    pltpu.make_async_copy(wo_hbm, wo_out.at[odd, 0], load_sem.at[3]).wait()


def cache_kernel(len_ref, c_ref, p_ref, lat_ref, pe_ref, lat_out, pe_out, fresh, fresh_pe):
    step = pl.program_id(0)
    chip = lax.axis_index("tp") // 2
    per, slots, _, toks, rank = c_ref.shape
    rope = pe_ref.shape[1]
    cache_len = lat_ref.shape[1]
    chunk = slots * 2 * toks
    words = rank // BLOCK
    tile_row = lax.broadcasted_iota(jnp.int32, (16, BLOCK), 0)

    def slot_of(j):
        return lax.rem(chip - j + slots, slots)

    def one_sequence(s, _):
        length = len_ref[step * per + s]
        for j in range(slots):
            piece = c_ref[s, slot_of(j)].reshape(2 * toks, rank).astype(F32)
            for w in range(words):
                fresh[w, BLOCK + j * 2 * toks : BLOCK + (j + 1) * 2 * toks] = piece[:, w * BLOCK : (w + 1) * BLOCK]
        lat_out[s] = lat_ref[s]
        base = (length // 16) * 16
        skew = length - base

        def tile(k, partial):
            at = pl.multiple_of(base + k * 16, 16)
            for w in range(words):
                moved = fresh[w, pl.ds(BLOCK - skew + k * 16, 16), :].astype(BF16)
                cols = slice(w * BLOCK, (w + 1) * BLOCK)
                if partial:
                    local = tile_row + k * 16 - skew
                    moved = jnp.where((local >= 0) & (local < chunk), moved.astype(F32), lat_ref[s, pl.ds(at, 16), cols].astype(F32)).astype(BF16)
                lat_out[s, pl.ds(at, 16), cols] = moved

        for k in range(chunk // 16):
            tile(k, k == 0)
        pl.when(skew > 0)(functools.partial(tile, chunk // 16, True))
        return 0

    lax.fori_loop(0, per, one_sequence, 0)

    for j in range(slots):
        fresh_pe[cache_len - chunk + j * 2 * toks : cache_len - chunk + (j + 1) * 2 * toks] = p_ref[0, slot_of(j)].reshape(2 * toks, BLOCK).astype(F32)
    old = pe_ref[...].reshape(per * rope, cache_len).astype(F32)
    lane_seq = lax.broadcasted_iota(jnp.int32, (BLOCK, BLOCK), 1) // rope
    row = lax.broadcasted_iota(jnp.int32, (BLOCK, BLOCK), 0)
    for b in range(cache_len // BLOCK):
        value = old[:, b * BLOCK : (b + 1) * BLOCK].T
        for s in range(per):
            length = len_ref[step * per + s]
            moved = fresh_pe[pl.ds(b * BLOCK + cache_len - chunk - length, BLOCK), :]
            local = row + (b * BLOCK - length)
            value = jnp.where((lane_seq == s) & (local >= 0) & (local < chunk), moved, value)
        pe_out[:, :, b * BLOCK : (b + 1) * BLOCK] = value.T.astype(BF16).reshape(per, rope, BLOCK)


def output_kernel(o_ref, w_ref, x_ref, y_ref):
    odd = lax.rem(lax.axis_index("tp"), 2)
    _, quads, seqs, toks, depth = o_ref.shape
    slots, rows, wide = w_ref.shape[1:]
    y = x_ref[...].reshape(seqs * toks, wide).astype(F32)
    for side in range(2):
        w = w_ref[odd if side == 0 else 1 - odd].reshape(slots * rows, wide)
        for quad in range(quads):
            y = y + dot(o_ref[side, quad].reshape(seqs * toks, depth), w[quad * depth : (quad + 1) * depth])
    y_ref[...] = y.astype(BF16).reshape(y_ref.shape)


def solution(mesh):
    size = mesh.shape["tp"]
    paired = mesh.shape["dp"] % 2 == 0

    def local_step(hidden, lengths, rope_cos, rope_sin, cache_lat, cache_pe, norm_in, w_dq, norm_q, w_dkv, norm_kv, w_uq, w_uk, w_uv, w_out):
        seqs, toks, dim = hidden.shape
        q_rank = w_dq.shape[1]
        rank, heads, nope = w_uk.shape
        rope = cache_pe.shape[2]
        cache_len = cache_lat.shape[1]
        slots = size // 2
        head = nope + rope
        quads = slots * heads // 4
        chunk = size * toks
        prefix = cache_len - chunk
        per = BLOCK // rope
        groups = seqs // per
        wide = 2 * BLOCK
        cos_t, sin_t = rope_cos.transpose(0, 2, 1), rope_sin.transpose(0, 2, 1)
        pe_t = cache_pe.transpose(0, 2, 1)
        wdkv_t = w_dkv.transpose(1, 0)
        wq_t, wk_t, wv_t = (w.transpose(1, 2, 0) for w in (w_uq, w_uk, w_uv))

        any_spec = pl.BlockSpec(memory_space=pl.ANY)
        vmem_spec = pl.BlockSpec(memory_space=pltpu.VMEM)
        smem_spec = pl.BlockSpec(memory_space=pltpu.SMEM)
        c_all, p_all, o_all, wo_all = pl.pallas_call(
            functools.partial(main_kernel, (size, paired)),
            in_specs=[smem_spec, any_spec, vmem_spec, any_spec, vmem_spec, any_spec, vmem_spec, vmem_spec, vmem_spec] + [any_spec] * 6,
            out_specs=[any_spec] * 4,
            out_shape=[
                jax.ShapeDtypeStruct((seqs, chunk, rank), BF16),
                jax.ShapeDtypeStruct((groups, chunk, BLOCK), BF16),
                jax.ShapeDtypeStruct((2, quads, seqs, toks, 4 * nope), BF16),
                jax.ShapeDtypeStruct((2, slots) + w_out.shape, BF16),
            ],
            scratch_shapes=[
                pltpu.VMEM(hidden.shape, BF16),
                pltpu.VMEM(w_dq.shape, BF16),
                pltpu.VMEM(wdkv_t.shape, BF16),
                pltpu.VMEM((groups, per * toks, dim), BF16),
                pltpu.VMEM((seqs, cache_len, rank), BF16),
                pltpu.VMEM((groups, cache_len, BLOCK), BF16),
                pltpu.VMEM((seqs, rope, prefix), BF16),
                pltpu.VMEM((2, seqs, toks, q_rank), BF16),
                pltpu.VMEM((slots * heads, head, q_rank), BF16),
                pltpu.VMEM((slots * heads, 2 * nope, rank), BF16),
                pltpu.VMEM((2, cache_len, 4 * nope), BF16),
                pltpu.VMEM((2, 4 * nope, cache_len), BF16),
                pltpu.VMEM((2, 2, wide, wide), BF16),
                [pltpu.VMEM((cache_len, wide), F32) for _ in range(4)],
                pltpu.VMEM((4, 8, wide), F32),
                [pltpu.VMEM((cache_len, wide), BF16) for _ in range(4)],
                pltpu.VMEM((4, 8, wide), F32),
                pltpu.VMEM((quads, seqs, toks, 4 * nope), BF16),
                pltpu.VMEM((quads, seqs, toks, 4 * nope), BF16),
                pltpu.SemaphoreType.DMA((8 + groups,)),
                pltpu.SemaphoreType.DMA((128,)),
                pltpu.SemaphoreType.DMA((128,)),
            ],
            compiler_params=pltpu.CompilerParams(collective_id=0, has_side_effects=True, vmem_limit_bytes=63 * MIB),
            cost_estimate=pl.CostEstimate(flops=70 * 10**9, bytes_accessed=40 * MIB, transcendentals=30 * 10**6),
            name="main",
        )(lengths, hidden, norm_in, w_dq, norm_q, wdkv_t, norm_kv, cos_t, sin_t, wq_t, wk_t, wv_t, w_out, cache_lat, pe_t)

        c_all = c_all.reshape(seqs, slots, 2, toks, rank)
        p_all = p_all.reshape(groups, slots, 2, toks, BLOCK)
        lat_new, pe_new = pl.pallas_call(
            cache_kernel,
            grid_spec=pltpu.PrefetchScalarGridSpec(
                num_scalar_prefetch=1,
                grid=(groups,),
                in_specs=[
                    pl.BlockSpec((per, slots, 2, toks, rank), lambda i, n: (i, 0, 0, 0, 0)),
                    pl.BlockSpec((1, slots, 2, toks, BLOCK), lambda i, n: (i, 0, 0, 0, 0)),
                    pl.BlockSpec((per, cache_len, rank), lambda i, n: (i, 0, 0)),
                    pl.BlockSpec((per, rope, cache_len), lambda i, n: (i, 0, 0)),
                ],
                out_specs=[
                    pl.BlockSpec((per, cache_len, rank), lambda i, n: (i, 0, 0)),
                    pl.BlockSpec((per, rope, cache_len), lambda i, n: (i, 0, 0)),
                ],
                scratch_shapes=[
                    pltpu.VMEM((rank // BLOCK, chunk + 2 * BLOCK, BLOCK), F32),
                    pltpu.VMEM((2 * cache_len - chunk, BLOCK), F32),
                ],
            ),
            out_shape=[jax.ShapeDtypeStruct(cache_lat.shape, BF16), jax.ShapeDtypeStruct(pe_t.shape, BF16)],
            compiler_params=pltpu.CompilerParams(vmem_limit_bytes=63 * MIB),
            cost_estimate=pl.CostEstimate(flops=4 * 10**9, bytes_accessed=20 * MIB, transcendentals=0),
            name="cache",
        )(lengths, c_all, p_all, cache_lat, pe_t)

        part = 512
        y = pl.pallas_call(
            output_kernel,
            grid=(dim // part,),
            in_specs=[
                pl.BlockSpec(o_all.shape, lambda i: (0, 0, 0, 0, 0), pipeline_mode=pl.Buffered(1)),
                pl.BlockSpec(wo_all.shape[:3] + (part,), lambda i: (0, 0, 0, i)),
                pl.BlockSpec((seqs, toks, part), lambda i: (0, 0, i)),
            ],
            out_specs=pl.BlockSpec((seqs, toks, part), lambda i: (0, 0, i)),
            out_shape=jax.ShapeDtypeStruct(hidden.shape, BF16),
            compiler_params=pltpu.CompilerParams(vmem_limit_bytes=63 * MIB),
            cost_estimate=pl.CostEstimate(flops=2 * seqs * toks * dim * dim, bytes_accessed=30 * MIB, transcendentals=0),
            name="output",
        )(o_all, wo_all, hidden)
        return y, lat_new, pe_new.transpose(0, 2, 1)

    spec_tok = P("dp", "tp", None)
    spec_len = P("dp")
    spec_seq = P("dp", None, None)
    spec_vec = P(None)
    spec_mat = P(None, None)
    spec_head = P(None, "tp", None)
    spec_rows = P("tp", None)
    in_specs = (spec_tok, spec_len, spec_seq, spec_seq, spec_seq, spec_seq, spec_vec, spec_mat, spec_vec, spec_mat, spec_vec, spec_head, spec_head, spec_head, spec_rows)
    return jax.shard_map(local_step, mesh=mesh, in_specs=in_specs, out_specs=(spec_tok, spec_seq, spec_seq), check_vma=False)
```

```python
import functools

import jax
import jax.numpy as jnp
from jax import lax
from jax.experimental import pallas as pl
from jax.experimental.pallas import tpu as pltpu
from jax.sharding import PartitionSpec as P

BLOCK = 128
LOG2E = 1.4426950408889634
NEVER = -1e30
F32 = jnp.float32
BF16 = jnp.bfloat16
MESH = pl.DeviceIdType.MESH
MIB = 2**20


def dot(a, b):
    return lax.dot_general(a, b, (((1,), (0,)), ((), ())), preferred_element_type=F32)


def dot_t(a, b):
    return lax.dot_general(a, b, (((1,), (1,)), ((), ())), preferred_element_type=F32)


def unit(x):
    return x * lax.rsqrt(jnp.mean(x * x, axis=-1, keepdims=True) + 1e-6)


class Wire:
    def __init__(self, send_sem, recv_sem):
        self.sems = (send_sem, recv_sem)
        self.made = {}
        self.index = {}

    def add(self, name, src, dst, **peer):
        self.index[name] = len(self.index)
        self.made[name] = lambda: pltpu.make_async_remote_copy(
            src(), dst(), self.sems[0].at[self.index[name]], self.sems[1].at[self.index[name]], device_id=peer, device_id_type=MESH
        )

    def start(self, *names):
        for name in names:
            self.made[name]().start()

    def landed(self, *names):
        for name in names:
            self.made[name]().wait_recv()

    def sent(self, *names):
        for name in names:
            self.made[name]().wait_send()


def main_kernel(
    plan,
    len_ref,
    x_hbm,
    g1_ref,
    wdq_hbm,
    gq_ref,
    wdkv_hbm,
    gkv_ref,
    cos_hbm,
    sin_hbm,
    wq_hbm,
    wk_hbm,
    wv_hbm,
    wo_hbm,
    lat_hbm,
    pe_hbm,
    c_out,
    p_out,
    o_out,
    wo_out,
    x_buf,
    wdq,
    wdkv,
    a_buf,
    rows,
    rot,
    pe_buf,
    cos_ref,
    sin_ref,
    cq_buf,
    wq,
    wkv,
    kb,
    vb,
    qb,
    q_raw,
    sb,
    mb,
    pb,
    lb,
    o_own,
    o_send,
    load_sem,
    send_sem,
    recv_sem,
):
    size, paired = plan
    me = lax.axis_index("tp")
    odd = lax.rem(me, 2)
    chip = me // 2
    right, left = lax.rem(me + 2, size), lax.rem(me + size - 2, size)
    onward = jnp.where(odd == 0, right, left)
    other = me + 1 - 2 * odd
    dp = lax.axis_index("dp")
    e = lax.rem(dp, 2) if paired else dp * 0
    partner = dp + 1 - 2 * e

    seqs, toks, dim = x_hbm.shape
    groups = rot.shape[0]
    per = seqs // groups
    rank = rows.shape[2]
    slots = size // 2
    chunk = size * toks
    prefix = rows.shape[1] - chunk
    heads = wq.shape[0] // slots
    head, q_rank = wq.shape[1:]
    rope = BLOCK // per
    half = rope // 2
    nope = head - rope
    quads = wq.shape[0] // 4
    duos = seqs // 2
    wide = 2 * BLOCK
    factor = LOG2E * head**-0.5

    loads = {}

    def load(name, src, dst):
        loads[name] = pltpu.make_async_copy(src, dst, load_sem.at[len(loads)])
        loads[name].start()

    def spot(slot, parity):
        return pl.ds(pl.multiple_of(prefix + slot * BLOCK + parity * toks, toks), toks)

    barrier = pltpu.get_barrier_semaphore()
    for peer in (left, right, other):
        pl.semaphore_signal(barrier, inc=1, device_id={"tp": peer}, device_id_type=MESH)
    if paired:
        pl.semaphore_signal(barrier, inc=1, device_id={"dp": partner}, device_id_type=MESH)

    lanes_chip = pl.ds(pl.multiple_of(chip * BLOCK, BLOCK), BLOCK)
    load("wk", wk_hbm, wkv.at[pl.ds(0, heads), pl.ds(0, nope)])
    load("wv", wv_hbm, wkv.at[pl.ds(0, heads), pl.ds(nope, nope)])
    for g in range(groups):
        load(f"x{g}", x_hbm.at[pl.ds(g * per, per)], x_buf.at[pl.ds(g * per, per)])
        if g == 0:
            load("wdkv", wdkv_hbm, wdkv)
            load("cos", cos_hbm.at[:, :, lanes_chip], cos_ref)
            load("sin", sin_hbm.at[:, :, lanes_chip], sin_ref)
    load("wq", wq_hbm, wq.at[pl.ds(0, heads)])
    load("wdq", wdq_hbm, wdq)
    load("pe", pe_hbm.at[:, :, pl.ds(0, prefix)], pe_buf)
    load("lat", lat_hbm.at[:, pl.ds(0, prefix)], rows.at[:, pl.ds(0, prefix)])
    pl.semaphore_wait(barrier, 4 if paired else 3)

    wire = Wire(send_sem, recv_sem)

    def chain(name, here, there, places, via="split"):
        near_left, near_right, opposite = places
        handed = {"right": near_left, "left": near_right, "split": jnp.where(odd == 0, near_left, near_right)}[via]
        wire.add(name + "R", lambda: here(0), lambda: there(near_left), tp=right)
        wire.add(name + "L", lambda: here(0), lambda: there(near_right), tp=left)
        wire.add(name + "O", lambda: there(handed), lambda: there(opposite), tp={"right": right, "left": left, "split": onward}[via])

    for g in range(groups):
        for name, ref in (("c", lambda slot, g=g: rows.at[pl.ds(g * per, per), spot(slot, odd)]), ("p", lambda slot, g=g: rot.at[g, spot(slot, odd)])):
            name = f"{name}{g}"
            chain(name, ref, ref, (1, 3, 2), "left")
            for slot in range(slots):
                wire.add(f"{name}S{slot}", functools.partial(ref, slot), functools.partial(ref, slot), tp=other)
        cq_ref = lambda g=g: cq_buf.at[odd, pl.ds(g * per, per)]
        wire.add(f"q{g}S", cq_ref, cq_ref, tp=other)

    def cut(total, side, unit, part):
        if part == "mid":
            return pl.ds(side, total - 2 * side)
        flip = e if part == "mine" else 1 - e
        return pl.ds(pl.multiple_of(flip * (total - side), unit), side)

    def wq_at(part, slot):
        return wq.at[pl.ds(slot * heads, heads), :, cut(q_rank, q_rank // 3, BLOCK, part)]

    def wkv_at(part, slot):
        return wkv.at[pl.ds(slot * heads, heads), cut(2 * nope, 48, 16, part)]

    def wo_at(part, slot):
        return wo_out.at[odd, slot, cut(wo_hbm.shape[0], 80, 16, part)]

    def wo_own(part, slot):
        return wo_hbm.at[cut(wo_hbm.shape[0], 80, 16, part)]

    by_ring = ("mine", "mid") if paired else ("mine", "mid", "rest")
    for name, here, there in (("wq", wq_at, wq_at), ("wkv", wkv_at, wkv_at), ("wo", wo_own, wo_at)):
        for part in by_ring:
            chain(f"{name}.{part}", functools.partial(here, part), functools.partial(there, part), (1, 2, 3), "right" if part == "mine" and name != "wo" else "split")
        if paired:
            for slot in (1, 2, 3):
                ref = functools.partial(there, "mine", slot)
                wire.add(f"{name}Z{slot}", ref, ref, dp=partner)
    late = ("mid",) if paired else ("mid", "rest")
    for slot in range(slots):
        mine = lambda slot=slot: wo_out.at[odd, slot]
        wire.add(f"woS{slot}", mine if slot else lambda: wo_hbm, mine, tp=other)
    for quad in range(quads):
        wire.add(f"o{quad}S", lambda quad=quad: o_send.at[quad], lambda quad=quad: o_out.at[1, quad], tp=other)

    def both(name, parts):
        return [f"{name}.{part}{way}" for part in parts for way in "RL"]

    def onwards(name, parts):
        return [f"{name}.{part}O" for part in parts]

    def across(name, *which):
        return [f"{name}Z{slot}" for slot in which] if paired else []

    def ways(name, parts, which):
        return [f"{name}.{part}{way}" for part in parts for way in which]

    def norm(g):
        for r in range(0, per):
            x = x_buf[g * per + r].astype(F32)
            a_buf[g, r * toks : (r + 1) * toks] = (unit(x) * g1_ref[...]).astype(BF16)

    def latent(g):
        kv = dot_t(a_buf[g], wdkv[...])
        rows[g * per : (g + 1) * per, spot(0, odd), :] = (unit(kv[:, :rank]) * gkv_ref[...]).astype(BF16).reshape(per, toks, rank)
        turned = []
        for s in range(per):
            cos_pair, sin_pair = cos_ref[g * per + s], sin_ref[g * per + s]
            cos = jnp.where(odd == 1, cos_pair[:, toks:], cos_pair[:, :toks])
            sin = jnp.where(odd == 1, sin_pair[:, toks:], sin_pair[:, :toks])
            table = jnp.concatenate([cos, cos, -sin, sin], axis=0).T
            p = kv[s * toks : (s + 1) * toks, rank:]
            swapped = jnp.concatenate([p[:, half:], p[:, :half]], axis=1)
            turned.append(p * table[:, :rope] + swapped * table[:, rope:])
        rot[g, spot(0, odd), :] = jnp.concatenate(turned, axis=1).astype(BF16)

    def queries(g):
        h = jnp.concatenate([dot(a_buf[g], wdq[:, : 2 * rank]), dot(a_buf[g], wdq[:, 2 * rank :])], axis=1)
        cq_buf[odd, g * per : (g + 1) * per] = (unit(h) * gq_ref[...]).astype(BF16).reshape(per, toks, q_rank)

    loads["wk"].wait()
    loads["wv"].wait()
    wire.start(*both("wkv", ("mine",)))
    for name in ("x0", "wdkv", "cos", "sin"):
        loads[name].wait()
    norm(0)
    for g in range(groups):
        if g + 1 < groups:
            loads[f"x{g + 1}"].wait()
            norm(g + 1)
        latent(g)
        for way in ("R", "L", "S0"):
            wire.start(f"c{g}{way}", f"p{g}{way}")
    loads["wq"].wait()
    wire.start(*ways("wq", ("mine",), "R"), *ways("wkv", late, "R"), *ways("wq", late, "R"))

    def hand_on(g):
        wire.landed(f"c{g}R", f"p{g}R", f"c{g}L", f"p{g}L")
        wire.start(f"c{g}O", f"p{g}O", f"c{g}S1", f"p{g}S1", f"c{g}S3", f"p{g}S3")

    loads["wdq"].wait()
    queries(0)
    wire.start("q0S")
    hand_on(0)
    queries(1)
    wire.start("q1S")
    hand_on(1)
    wire.landed(*both("wkv", ("mine",)))
    wire.start(*across("wkv", 1, 2), *onwards("wkv", ("mine",)))
    for g in range(2, groups):
        queries(g)
        wire.start(f"q{g}S")

    loads["pe"].wait()
    for g in range(groups):
        old = pe_buf[g * per : (g + 1) * per].reshape(per * rope, prefix).astype(F32)
        for b in range(prefix // BLOCK):
            rot[g, b * BLOCK : (b + 1) * BLOCK] = old[:, b * BLOCK : (b + 1) * BLOCK].T.astype(BF16)
    qb[...] = jnp.zeros_like(qb)

    for g in range(2, groups):
        hand_on(g)
    wire.start(*ways("wq", ("mine",), "L"), *ways("wkv", late, "L"), *ways("wq", late, "L"), *ways("wo", ("mine",), "L"), "woS0")

    def rest_of(g):
        wire.landed(f"c{g}O", f"p{g}O")
        wire.start(f"c{g}S2", f"p{g}S2")
        for slot in (0, 1, 3, 2):
            wire.landed(f"c{g}S{slot}", f"p{g}S{slot}")
        wire.landed(f"q{g}S")

    loads["lat"].wait()
    rest_of(0)

    row = lax.broadcasted_iota(jnp.int32, (BLOCK, wide), 0)
    lane = lax.rem(lax.broadcasted_iota(jnp.int32, (BLOCK, wide), 1), BLOCK)
    near = row <= lane

    def place(n):
        return n // duos, lax.rem(n, duos)

    def query_dot(n):
        quad, duo = place(n)
        w = wq[pl.ds(quad * 4, 4)].reshape(4 * head, q_rank)
        cq = jnp.concatenate([cq_buf[parity, 2 * duo + u] for u in range(2) for parity in range(2)], axis=0)
        q_raw[...] = dot_t(w, cq)

    def query_stage(n):
        quad, duo = place(n)
        raw = q_raw
        for u in range(2):
            slot = 2 * lax.rem(duo, 2) + u
            cos, sin = cos_ref[2 * duo + u], sin_ref[2 * duo + u]
            for h in range(4):
                pair, side = h // 2, h % 2
                q = raw[h * head : (h + 1) * head, u * BLOCK : (u + 1) * BLOCK]
                cols = slice(side * BLOCK, (side + 1) * BLOCK)
                qb[u, pair, side * nope : (side + 1) * nope, cols] = q[:nope].astype(BF16)
                lo, hi = q[nope : nope + half], q[nope + half :]
                turned = jnp.concatenate([lo * cos - hi * sin, hi * cos + lo * sin], axis=0).astype(BF16)
                start = pl.multiple_of(BLOCK + slot * rope, rope)
                stale = pl.multiple_of(BLOCK + lax.rem(slot + 2, 4) * rope, rope)
                qb[u, pair, pl.ds(start, rope), cols] = turned
                qb[u, pair, pl.ds(stale, rope), cols] = jnp.zeros_like(turned)

    def key_stage(n, t, u):
        quad, duo = place(n)
        w = wkv[pl.ds(quad * 4, 4), :nope].reshape(4 * nope, rank)
        kb[u][:t] = dot_t(rows[2 * duo + u, :t], w).astype(BF16)

    def value_stage(n, t, u):
        quad, duo = place(n)
        w = wkv[pl.ds(quad * 4, 4), nope:].reshape(4 * nope, rank)
        vb[u][:, :t] = dot_t(w, rows[2 * duo + u, :t]).astype(BF16)

    def score_stage(n, t, u, pair):
        _, duo = place(n)
        length = len_ref[2 * duo + u]
        keys = jnp.concatenate([kb[u][:t, pair * BLOCK : (pair + 1) * BLOCK], rot[duo // 2, :t]], axis=1)
        value = dot(keys, qb[u, pair])
        most = None
        for b in range(t // BLOCK):
            part = value[b * BLOCK : (b + 1) * BLOCK]
            if BLOCK <= b * BLOCK < prefix:
                part = jnp.where(row < length - b * BLOCK, part, NEVER)
            if b * BLOCK == prefix:
                part = jnp.where(near, part, NEVER)
            sb[2 * u + pair][b * BLOCK : (b + 1) * BLOCK] = part
            part = jnp.max(part.reshape(BLOCK // 8, 8, wide), axis=0)
            most = part if most is None else jnp.maximum(most, part)
        mb[2 * u + pair] = jnp.broadcast_to(jnp.max(most, axis=0, keepdims=True), (8, wide))

    def soft_stage(t, u, pair):
        i = 2 * u + pair
        most = mb[i, :1]
        total = None
        for b in range(t // BLOCK):
            x = jnp.exp2((sb[i][b * BLOCK : (b + 1) * BLOCK] - most) * factor)
            part = jnp.sum(x.reshape(BLOCK // 8, 8, wide), axis=0)
            total = part if total is None else total + part
            pb[i][b * BLOCK : (b + 1) * BLOCK] = x.astype(BF16)
        lb[i] = total

    def mix_stage(n, t, u, pair):
        quad, duo = place(n)
        i = 2 * u + pair
        inv = 1.0 / jnp.sum(lb[i], axis=0, keepdims=True)
        o = dot(vb[u][pair * BLOCK : (pair + 1) * BLOCK, :t], pb[i][:t]) * inv
        o = jnp.concatenate([o[:nope, :BLOCK], o[nope:, BLOCK:]], axis=0).T.astype(BF16)
        first, second = o[:toks], o[toks:]
        cols = slice(pair * BLOCK, (pair + 1) * BLOCK)
        o_own[quad, 2 * duo + u, :, cols] = jnp.where(odd == 1, second, first)
        o_send[quad, 2 * duo + u, :, cols] = jnp.where(odd == 1, first, second)

    units = [(u, pair) for u in range(2) for pair in range(2)]
    total = quads * duos

    def each_chip(fn):
        for c in range(slots):
            pl.when(chip == c)(lambda c=c: fn(prefix + (c + 1) * BLOCK))

    def body(b, t):
        before, ahead, later = jnp.maximum(b - 1, 0), jnp.minimum(b + 1, total - 1), jnp.minimum(b + 2, total - 1)
        mix_stage(before, t, 0, 0)
        soft_stage(t, 0, 0)
        score_stage(ahead, t, 0, 0)
        mix_stage(before, t, 0, 1)
        value_stage(b, t, 0)
        soft_stage(t, 0, 1)
        score_stage(ahead, t, 0, 1)
        mix_stage(before, t, 1, 0)
        mix_stage(before, t, 1, 1)
        key_stage(later, t, 0)
        soft_stage(t, 1, 0)
        score_stage(ahead, t, 1, 0)
        value_stage(b, t, 1)
        soft_stage(t, 1, 1)
        score_stage(ahead, t, 1, 1)
        key_stage(later, t, 1)
        query_dot(later)
        query_stage(later)

    def at(b, when):
        return pl.when(b == when)

    def step(b, _):
        @at(b, 0)
        def _():
            rest_of(1)

        @at(b, 2)
        def _():
            rest_of(2)
            pltpu.make_async_copy(rows.at[:, pl.ds(prefix, chunk)], c_out, load_sem.at[0]).start()
            pltpu.make_async_copy(rot.at[:, pl.ds(prefix, chunk)], p_out, load_sem.at[1]).start()

        @at(b, 1)
        def _():
            wire.landed(*ways("wq", ("mine",), "R"))
            wire.start(*across("wq", 1), *onwards("wq", ("mine",)))

        @at(b, duos - 2)
        def _():
            wire.landed(*ways("wkv", late, "R"), *ways("wq", late, "R"), *across("wkv", 1), *across("wq", 1))
            wire.start(*ways("wo", ("mine",), "R"))

        @at(b, duos - 1)
        def _():
            wire.landed(*ways("wq", ("mine",), "L"))
            wire.start(*across("wq", 2))

        @at(b, 9)
        def _():
            wire.landed(*ways("wkv", late, "L"), *ways("wq", late, "L"), *across("wkv", 2), *across("wq", 2))
            wire.start(*onwards("wkv", late), *onwards("wq", late))

        @at(b, 14)
        def _():
            wire.landed(*onwards("wkv", by_ring), *onwards("wq", by_ring))
            wire.start(*across("wkv", 3), *across("wq", 3))
            wire.landed(*ways("wo", ("mine",), "L"))
            wire.start(*across("wo", 2), *ways("wo", late, "L"))

        @at(b, 16)
        def _():
            wire.landed(*across("wkv", 3), *across("wq", 3))
            wire.landed(*ways("wo", ("mine",), "R"))
            wire.start(*across("wo", 1), *onwards("wo", ("mine",)), *ways("wo", late, "R"))

        @at(b, 22)
        def _():
            wire.landed(*onwards("wo", ("mine",)))
            wire.start(*across("wo", 3))

        @at(b, 28)
        def _():
            wire.landed(*both("wo", late))
            wire.start(*onwards("wo", late))

        for quad in range(quads - 1):
            at(b, (quad + 1) * duos + 1)(functools.partial(wire.start, f"o{quad}S"))

        each_chip(functools.partial(body, b))
        return 0

    def lead_in(t):
        for u in range(2):
            key_stage(0, t, u)
        query_dot(0)
        query_stage(0)

    def second(t):
        for u, pair in units:
            score_stage(0, t, u, pair)
        for u in range(2):
            key_stage(1, t, u)
        query_dot(1)
        query_stage(1)

    each_chip(lead_in)
    each_chip(second)
    lax.fori_loop(0, total, step, 0)

    def last(t):
        for u, pair in units:
            mix_stage(total - 1, t, u, pair)

    each_chip(last)
    wire.start(f"o{quads - 1}S")
    pltpu.make_async_copy(o_own, o_out.at[0], load_sem.at[2]).start()

    wire.landed(*across("wo", 1, 2))
    wire.start("woS1", "woS2")
    wire.landed(*onwards("wo", late), *across("wo", 3))
    wire.start("woS3")
    for slot in range(slots):
        wire.landed(f"woS{slot}")
    for quad in range(quads):
        wire.landed(f"o{quad}S")
    wire.sent(*wire.index)
    pltpu.make_async_copy(rows.at[:, pl.ds(prefix, chunk)], c_out, load_sem.at[0]).wait()
    pltpu.make_async_copy(rot.at[:, pl.ds(prefix, chunk)], p_out, load_sem.at[1]).wait()
    pltpu.make_async_copy(o_own, o_out.at[0], load_sem.at[2]).wait()


def cache_kernel(len_ref, c_ref, p_ref, lat_ref, pe_ref, lat_out, pe_out, fresh, fresh_pe):
    step = pl.program_id(0)
    chip = lax.axis_index("tp") // 2
    per, slots, _, toks, rank = c_ref.shape
    rope = pe_ref.shape[1]
    cache_len = lat_ref.shape[1]
    chunk = slots * 2 * toks
    words = rank // BLOCK
    tile_row = lax.broadcasted_iota(jnp.int32, (16, BLOCK), 0)

    def slot_of(j):
        return lax.rem(chip - j + slots, slots)

    def one_sequence(s, _):
        length = len_ref[step * per + s]
        for j in range(slots):
            piece = c_ref[s, slot_of(j)].reshape(2 * toks, rank).astype(F32)
            for w in range(words):
                fresh[w, BLOCK + j * 2 * toks : BLOCK + (j + 1) * 2 * toks] = piece[:, w * BLOCK : (w + 1) * BLOCK]
        lat_out[s] = lat_ref[s]
        base = (length // 16) * 16
        skew = length - base

        def tile(k, partial):
            at = pl.multiple_of(base + k * 16, 16)
            for w in range(words):
                moved = fresh[w, pl.ds(BLOCK - skew + k * 16, 16), :].astype(BF16)
                cols = slice(w * BLOCK, (w + 1) * BLOCK)
                if partial:
                    local = tile_row + k * 16 - skew
                    moved = jnp.where((local >= 0) & (local < chunk), moved.astype(F32), lat_ref[s, pl.ds(at, 16), cols].astype(F32)).astype(BF16)
                lat_out[s, pl.ds(at, 16), cols] = moved

        for k in range(chunk // 16):
            tile(k, k == 0)
        pl.when(skew > 0)(functools.partial(tile, chunk // 16, True))
        return 0

    lax.fori_loop(0, per, one_sequence, 0)

    for j in range(slots):
        fresh_pe[cache_len - chunk + j * 2 * toks : cache_len - chunk + (j + 1) * 2 * toks] = p_ref[0, slot_of(j)].reshape(2 * toks, BLOCK).astype(F32)
    old = pe_ref[...].reshape(per * rope, cache_len).astype(F32)
    lane_seq = lax.broadcasted_iota(jnp.int32, (BLOCK, BLOCK), 1) // rope
    row = lax.broadcasted_iota(jnp.int32, (BLOCK, BLOCK), 0)
    for b in range(cache_len // BLOCK):
        value = old[:, b * BLOCK : (b + 1) * BLOCK].T
        for s in range(per):
            length = len_ref[step * per + s]
            moved = fresh_pe[pl.ds(b * BLOCK + cache_len - chunk - length, BLOCK), :]
            local = row + (b * BLOCK - length)
            value = jnp.where((lane_seq == s) & (local >= 0) & (local < chunk), moved, value)
        pe_out[:, :, b * BLOCK : (b + 1) * BLOCK] = value.T.astype(BF16).reshape(per, rope, BLOCK)


def output_kernel(o_ref, own_ref, w_ref, x_ref, y_ref):
    odd = lax.rem(lax.axis_index("tp"), 2)
    _, quads, seqs, toks, depth = o_ref.shape
    slots, rows, wide = w_ref.shape[1:]
    y = x_ref[...].reshape(seqs * toks, wide).astype(F32)
    for side in range(2):
        parity = odd if side == 0 else 1 - odd
        w = w_ref[parity].reshape(slots * rows, wide)
        if side == 0:
            w = jnp.concatenate([own_ref[...], w[rows:]], axis=0)
        for quad in range(quads):
            y = y + dot(o_ref[side, quad].reshape(seqs * toks, depth), w[quad * depth : (quad + 1) * depth])
    y_ref[...] = y.astype(BF16).reshape(y_ref.shape)


def solution(mesh):
    size = mesh.shape["tp"]
    paired = mesh.shape["dp"] % 2 == 0

    def local_step(hidden, lengths, rope_cos, rope_sin, cache_lat, cache_pe, norm_in, w_dq, norm_q, w_dkv, norm_kv, w_uq, w_uk, w_uv, w_out):
        seqs, toks, dim = hidden.shape
        q_rank = w_dq.shape[1]
        rank, heads, nope = w_uk.shape
        rope = cache_pe.shape[2]
        cache_len = cache_lat.shape[1]
        slots = size // 2
        head = nope + rope
        quads = slots * heads // 4
        chunk = size * toks
        prefix = cache_len - chunk
        per = BLOCK // rope
        groups = seqs // per
        wide = 2 * BLOCK
        cos_t, sin_t = rope_cos.transpose(0, 2, 1), rope_sin.transpose(0, 2, 1)
        pe_t = cache_pe.transpose(0, 2, 1)
        wdkv_t = w_dkv.transpose(1, 0)
        wq_t, wk_t, wv_t = (w.transpose(1, 2, 0) for w in (w_uq, w_uk, w_uv))

        any_spec = pl.BlockSpec(memory_space=pl.ANY)
        vmem_spec = pl.BlockSpec(memory_space=pltpu.VMEM)
        smem_spec = pl.BlockSpec(memory_space=pltpu.SMEM)
        c_all, p_all, o_all, wo_all = pl.pallas_call(
            functools.partial(main_kernel, (size, paired)),
            in_specs=[smem_spec, any_spec, vmem_spec, any_spec, vmem_spec, any_spec, vmem_spec] + [any_spec] * 8,
            out_specs=[any_spec] * 4,
            out_shape=[
                jax.ShapeDtypeStruct((seqs, chunk, rank), BF16),
                jax.ShapeDtypeStruct((groups, chunk, BLOCK), BF16),
                jax.ShapeDtypeStruct((2, quads, seqs, toks, 4 * nope), BF16),
                jax.ShapeDtypeStruct((2, slots) + w_out.shape, BF16),
            ],
            scratch_shapes=[
                pltpu.VMEM(hidden.shape, BF16),
                pltpu.VMEM(w_dq.shape, BF16),
                pltpu.VMEM(wdkv_t.shape, BF16),
                pltpu.VMEM((groups, per * toks, dim), BF16),
                pltpu.VMEM((seqs, cache_len, rank), BF16),
                pltpu.VMEM((groups, cache_len, BLOCK), BF16),
                pltpu.VMEM((seqs, rope, prefix), BF16),
                pltpu.VMEM((seqs, rope // 2, BLOCK), F32),
                pltpu.VMEM((seqs, rope // 2, BLOCK), F32),
                pltpu.VMEM((2, seqs, toks, q_rank), BF16),
                pltpu.VMEM((slots * heads, head, q_rank), BF16),
                pltpu.VMEM((slots * heads, 2 * nope, rank), BF16),
                [pltpu.VMEM((cache_len, 4 * nope), BF16) for _ in range(2)],
                [pltpu.VMEM((4 * nope, cache_len), BF16) for _ in range(2)],
                pltpu.VMEM((2, 2, wide, wide), BF16),
                pltpu.VMEM((4 * head, wide), F32),
                [pltpu.VMEM((cache_len, wide), F32) for _ in range(4)],
                pltpu.VMEM((4, 8, wide), F32),
                [pltpu.VMEM((cache_len, wide), BF16) for _ in range(4)],
                pltpu.VMEM((4, 8, wide), F32),
                pltpu.VMEM((quads, seqs, toks, 4 * nope), BF16),
                pltpu.VMEM((quads, seqs, toks, 4 * nope), BF16),
                pltpu.SemaphoreType.DMA((10 + groups,)),
                pltpu.SemaphoreType.DMA((128,)),
                pltpu.SemaphoreType.DMA((128,)),
            ],
            compiler_params=pltpu.CompilerParams(collective_id=0, has_side_effects=True, vmem_limit_bytes=63 * MIB),
            cost_estimate=pl.CostEstimate(flops=70 * 10**9, bytes_accessed=40 * MIB, transcendentals=30 * 10**6),
            name="main",
        )(lengths, hidden, norm_in, w_dq, norm_q, wdkv_t, norm_kv, cos_t, sin_t, wq_t, wk_t, wv_t, w_out, cache_lat, pe_t)

        c_all = c_all.reshape(seqs, slots, 2, toks, rank)
        p_all = p_all.reshape(groups, slots, 2, toks, BLOCK)
        lat_new, pe_new = pl.pallas_call(
            cache_kernel,
            grid_spec=pltpu.PrefetchScalarGridSpec(
                num_scalar_prefetch=1,
                grid=(groups,),
                in_specs=[
                    pl.BlockSpec((per, slots, 2, toks, rank), lambda i, n: (i, 0, 0, 0, 0)),
                    pl.BlockSpec((1, slots, 2, toks, BLOCK), lambda i, n: (i, 0, 0, 0, 0)),
                    pl.BlockSpec((per, cache_len, rank), lambda i, n: (i, 0, 0)),
                    pl.BlockSpec((per, rope, cache_len), lambda i, n: (i, 0, 0)),
                ],
                out_specs=[
                    pl.BlockSpec((per, cache_len, rank), lambda i, n: (i, 0, 0)),
                    pl.BlockSpec((per, rope, cache_len), lambda i, n: (i, 0, 0)),
                ],
                scratch_shapes=[
                    pltpu.VMEM((rank // BLOCK, chunk + 2 * BLOCK, BLOCK), F32),
                    pltpu.VMEM((2 * cache_len - chunk, BLOCK), F32),
                ],
            ),
            out_shape=[jax.ShapeDtypeStruct(cache_lat.shape, BF16), jax.ShapeDtypeStruct(pe_t.shape, BF16)],
            compiler_params=pltpu.CompilerParams(vmem_limit_bytes=63 * MIB),
            cost_estimate=pl.CostEstimate(flops=4 * 10**9, bytes_accessed=20 * MIB, transcendentals=0),
            name="cache",
        )(lengths, c_all, p_all, cache_lat, pe_t)

        part = 512
        y = pl.pallas_call(
            output_kernel,
            grid=(dim // part,),
            in_specs=[
                pl.BlockSpec(o_all.shape, lambda i: (0, 0, 0, 0, 0), pipeline_mode=pl.Buffered(1)),
                pl.BlockSpec((w_out.shape[0], part), lambda i: (0, i)),
                pl.BlockSpec(wo_all.shape[:3] + (part,), lambda i: (0, 0, 0, i)),
                pl.BlockSpec((seqs, toks, part), lambda i: (0, 0, i)),
            ],
            out_specs=pl.BlockSpec((seqs, toks, part), lambda i: (0, 0, i)),
            out_shape=jax.ShapeDtypeStruct(hidden.shape, BF16),
            compiler_params=pltpu.CompilerParams(vmem_limit_bytes=63 * MIB),
            cost_estimate=pl.CostEstimate(flops=2 * seqs * toks * dim * dim, bytes_accessed=30 * MIB, transcendentals=0),
            name="output",
        )(o_all, w_out, wo_all, hidden)
        return y, lat_new, pe_new.transpose(0, 2, 1)

    spec_tok = P("dp", "tp", None)
    spec_len = P("dp")
    spec_seq = P("dp", None, None)
    spec_vec = P(None)
    spec_mat = P(None, None)
    spec_head = P(None, "tp", None)
    spec_rows = P("tp", None)
    in_specs = (spec_tok, spec_len, spec_seq, spec_seq, spec_seq, spec_seq, spec_vec, spec_mat, spec_vec, spec_mat, spec_vec, spec_head, spec_head, spec_head, spec_rows)
    return jax.shard_map(local_step, mesh=mesh, in_specs=in_specs, out_specs=(spec_tok, spec_seq, spec_seq), check_vma=False)
```

```python
import functools

import jax
import jax.numpy as jnp
from jax import lax
from jax.experimental import pallas as pl
from jax.experimental.pallas import tpu as pltpu
from jax.sharding import PartitionSpec as P

BLOCK = 128
LOG2E = 1.4426950408889634
NEVER = -1e30
F32 = jnp.float32
BF16 = jnp.bfloat16
MESH = pl.DeviceIdType.MESH
MIB = 2**20


def dot(a, b):
    return lax.dot_general(a, b, (((1,), (0,)), ((), ())), preferred_element_type=F32)


def dot_t(a, b):
    return lax.dot_general(a, b, (((1,), (1,)), ((), ())), preferred_element_type=F32)


def unit(x):
    return x * lax.rsqrt(jnp.mean(x * x, axis=-1, keepdims=True) + 1e-6)


class Wire:
    def __init__(self, send_sem, recv_sem):
        self.sems = (send_sem, recv_sem)
        self.made = {}
        self.index = {}

    def add(self, name, src, dst, **peer):
        self.index[name] = len(self.index)
        self.made[name] = lambda: pltpu.make_async_remote_copy(
            src(), dst(), self.sems[0].at[self.index[name]], self.sems[1].at[self.index[name]], device_id=peer, device_id_type=MESH
        )

    def start(self, *names):
        for name in names:
            self.made[name]().start()

    def landed(self, *names):
        for name in names:
            self.made[name]().wait_recv()

    def sent(self, *names):
        for name in names:
            self.made[name]().wait_send()


def main_kernel(
    plan,
    len_ref,
    x_hbm,
    g1_ref,
    wdq_hbm,
    gq_ref,
    wdkv_hbm,
    gkv_ref,
    cos_hbm,
    sin_hbm,
    wq_hbm,
    wk_hbm,
    wv_hbm,
    wo_hbm,
    lat_hbm,
    pe_hbm,
    c_out,
    p_out,
    o_out,
    wo_out,
    x_buf,
    wdq,
    wdkv,
    a_buf,
    rows,
    rot,
    pe_buf,
    cos_ref,
    sin_ref,
    cq_buf,
    wq,
    wkv,
    kb,
    vb,
    qb,
    q_raw,
    sb,
    mb,
    pb,
    lb,
    o_own,
    o_send,
    load_sem,
    send_sem,
    recv_sem,
):
    size, paired = plan
    me = lax.axis_index("tp")
    odd = lax.rem(me, 2)
    chip = me // 2
    right, left = lax.rem(me + 2, size), lax.rem(me + size - 2, size)
    onward = jnp.where(odd == 0, right, left)
    other = me + 1 - 2 * odd
    dp = lax.axis_index("dp")
    e = lax.rem(dp, 2) if paired else dp * 0
    partner = dp + 1 - 2 * e

    seqs, toks, dim = x_hbm.shape
    groups = rot.shape[0]
    per = seqs // groups
    rank = rows.shape[2]
    slots = size // 2
    chunk = size * toks
    prefix = rows.shape[1] - chunk
    heads = wq.shape[0] // slots
    head, q_rank = wq.shape[1:]
    rope = BLOCK // per
    half = rope // 2
    nope = head - rope
    quads = wq.shape[0] // 4
    duos = seqs // 2
    wide = 2 * BLOCK
    factor = LOG2E * head**-0.5

    loads = {}

    def load(name, src, dst):
        loads[name] = pltpu.make_async_copy(src, dst, load_sem.at[len(loads)])
        loads[name].start()

    def spot(slot, parity):
        return pl.ds(pl.multiple_of(prefix + slot * BLOCK + parity * toks, toks), toks)

    barrier = pltpu.get_barrier_semaphore()
    for peer in (left, right, other):
        pl.semaphore_signal(barrier, inc=1, device_id={"tp": peer}, device_id_type=MESH)
    if paired:
        pl.semaphore_signal(barrier, inc=1, device_id={"dp": partner}, device_id_type=MESH)

    lanes_chip = pl.ds(pl.multiple_of(chip * BLOCK, BLOCK), BLOCK)
    load("wk", wk_hbm, wkv.at[pl.ds(0, heads), pl.ds(0, nope)])
    load("wv", wv_hbm, wkv.at[pl.ds(0, heads), pl.ds(nope, nope)])
    for g in range(groups):
        load(f"x{g}", x_hbm.at[pl.ds(g * per, per)], x_buf.at[pl.ds(g * per, per)])
        if g == 0:
            load("wdkv", wdkv_hbm, wdkv)
            load("cos", cos_hbm.at[:, :, lanes_chip], cos_ref)
            load("sin", sin_hbm.at[:, :, lanes_chip], sin_ref)
    load("wq", wq_hbm, wq.at[pl.ds(0, heads)])
    load("wdq", wdq_hbm, wdq)
    load("pe", pe_hbm.at[:, :, pl.ds(0, prefix)], pe_buf)
    load("lat", lat_hbm.at[:, pl.ds(0, prefix)], rows.at[:, pl.ds(0, prefix)])
    pl.semaphore_wait(barrier, 4 if paired else 3)

    wire = Wire(send_sem, recv_sem)

    def chain(name, here, there, places, via="split"):
        near_left, near_right, opposite = places
        handed = {"right": near_left, "left": near_right, "split": jnp.where(odd == 0, near_left, near_right)}[via]
        wire.add(name + "R", lambda: here(0), lambda: there(near_left), tp=right)
        wire.add(name + "L", lambda: here(0), lambda: there(near_right), tp=left)
        wire.add(name + "O", lambda: there(handed), lambda: there(opposite), tp={"right": right, "left": left, "split": onward}[via])

    for g in range(groups):
        for name, ref in (("c", lambda slot, g=g: rows.at[pl.ds(g * per, per), spot(slot, odd)]), ("p", lambda slot, g=g: rot.at[g, spot(slot, odd)])):
            name = f"{name}{g}"
            chain(name, ref, ref, (1, 3, 2), "left")
            for slot in range(slots):
                wire.add(f"{name}S{slot}", functools.partial(ref, slot), functools.partial(ref, slot), tp=other)
        cq_ref = lambda g=g: cq_buf.at[odd, pl.ds(g * per, per)]
        wire.add(f"q{g}S", cq_ref, cq_ref, tp=other)

    def cut(total, side, unit, part):
        if part == "mid":
            return pl.ds(side, total - 2 * side)
        flip = e if part == "mine" else 1 - e
        return pl.ds(pl.multiple_of(flip * (total - side), unit), side)

    def wq_at(part, slot):
        return wq.at[pl.ds(slot * heads, heads), :, cut(q_rank, q_rank // 3, BLOCK, part)]

    def wkv_at(part, slot):
        return wkv.at[pl.ds(slot * heads, heads), cut(2 * nope, 48, 16, part)]

    def wo_at(part, slot):
        return wo_out.at[odd, slot, cut(wo_hbm.shape[0], 80, 16, part)]

    def wo_own(part, slot):
        return wo_hbm.at[cut(wo_hbm.shape[0], 80, 16, part)]

    by_ring = ("mine", "mid") if paired else ("mine", "mid", "rest")
    for name, here, there in (("wq", wq_at, wq_at), ("wkv", wkv_at, wkv_at), ("wo", wo_own, wo_at)):
        for part in by_ring:
            chain(f"{name}.{part}", functools.partial(here, part), functools.partial(there, part), (1, 2, 3), "right" if part == "mine" and name != "wo" else "split")
        if paired:
            for slot in (1, 2, 3):
                ref = functools.partial(there, "mine", slot)
                wire.add(f"{name}Z{slot}", ref, ref, dp=partner)
    late = ("mid",) if paired else ("mid", "rest")
    for slot in range(slots):
        mine = lambda slot=slot: wo_out.at[odd, slot]
        wire.add(f"woS{slot}", mine if slot else lambda: wo_hbm, mine, tp=other)
    for quad in range(quads):
        wire.add(f"o{quad}S", lambda quad=quad: o_send.at[quad], lambda quad=quad: o_out.at[1, quad], tp=other)

    def both(name, parts):
        return [f"{name}.{part}{way}" for part in parts for way in "RL"]

    def onwards(name, parts):
        return [f"{name}.{part}O" for part in parts]

    def across(name, *which):
        return [f"{name}Z{slot}" for slot in which] if paired else []

    def ways(name, parts, which):
        return [f"{name}.{part}{way}" for part in parts for way in which]

    def norm(g):
        for r in range(0, per):
            x = x_buf[g * per + r].astype(F32)
            a_buf[g, r * toks : (r + 1) * toks] = (unit(x) * g1_ref[...]).astype(BF16)

    def latent(g):
        kv = dot_t(a_buf[g], wdkv[...])
        rows[g * per : (g + 1) * per, spot(0, odd), :] = (unit(kv[:, :rank]) * gkv_ref[...]).astype(BF16).reshape(per, toks, rank)
        turned = []
        for s in range(per):
            cos_pair, sin_pair = cos_ref[g * per + s], sin_ref[g * per + s]
            cos = jnp.where(odd == 1, cos_pair[:, toks:], cos_pair[:, :toks])
            sin = jnp.where(odd == 1, sin_pair[:, toks:], sin_pair[:, :toks])
            table = jnp.concatenate([cos, cos, -sin, sin], axis=0).T
            p = kv[s * toks : (s + 1) * toks, rank:]
            swapped = jnp.concatenate([p[:, half:], p[:, :half]], axis=1)
            turned.append(p * table[:, :rope] + swapped * table[:, rope:])
        rot[g, spot(0, odd), :] = jnp.concatenate(turned, axis=1).astype(BF16)

    def queries(g):
        h = jnp.concatenate([dot(a_buf[g], wdq[:, : 2 * rank]), dot(a_buf[g], wdq[:, 2 * rank :])], axis=1)
        cq_buf[odd, g * per : (g + 1) * per] = (unit(h) * gq_ref[...]).astype(BF16).reshape(per, toks, q_rank)

    loads["wk"].wait()
    loads["wv"].wait()
    wire.start(*both("wkv", ("mine",)))
    for name in ("x0", "wdkv", "cos", "sin"):
        loads[name].wait()
    norm(0)
    for g in range(groups):
        if g + 1 < groups:
            loads[f"x{g + 1}"].wait()
            norm(g + 1)
        latent(g)
        for way in ("R", "L", "S0"):
            wire.start(f"c{g}{way}", f"p{g}{way}")
    loads["wq"].wait()
    wire.start(*ways("wq", ("mine",), "R"), *ways("wkv", late, "R"), *ways("wq", late, "R"))

    def hand_on(g):
        wire.landed(f"c{g}R", f"p{g}R", f"c{g}L", f"p{g}L")
        wire.start(f"c{g}O", f"p{g}O", f"c{g}S1", f"p{g}S1", f"c{g}S3", f"p{g}S3")

    loads["wdq"].wait()
    queries(0)
    wire.start("q0S")
    hand_on(0)
    queries(1)
    wire.start("q1S")
    hand_on(1)
    wire.landed(*both("wkv", ("mine",)))
    wire.start(*across("wkv", 1, 2), *onwards("wkv", ("mine",)))
    for g in range(2, groups):
        queries(g)
        wire.start(f"q{g}S")

    loads["pe"].wait()
    for g in range(groups):
        old = pe_buf[g * per : (g + 1) * per].reshape(per * rope, prefix).astype(F32)
        for b in range(prefix // BLOCK):
            rot[g, b * BLOCK : (b + 1) * BLOCK] = old[:, b * BLOCK : (b + 1) * BLOCK].T.astype(BF16)
    qb[...] = jnp.zeros_like(qb)

    for g in range(2, groups):
        hand_on(g)
    wire.start(*ways("wq", ("mine",), "L"), *ways("wkv", late, "L"), *ways("wq", late, "L"), *ways("wo", ("mine",), "L"), "woS0")

    def rest_of(g):
        wire.landed(f"c{g}O", f"p{g}O")
        wire.start(f"c{g}S2", f"p{g}S2")
        for slot in (0, 1, 3, 2):
            wire.landed(f"c{g}S{slot}", f"p{g}S{slot}")
        wire.landed(f"q{g}S")

    loads["lat"].wait()
    rest_of(0)

    row = lax.broadcasted_iota(jnp.int32, (BLOCK, wide), 0)
    lane = lax.rem(lax.broadcasted_iota(jnp.int32, (BLOCK, wide), 1), BLOCK)
    near = row <= lane

    def place(n):
        return n // duos, lax.rem(n, duos)

    def query_dot(n):
        quad, duo = place(n)
        w = wq[pl.ds(quad * 4, 4)].reshape(4 * head, q_rank)
        cq = jnp.concatenate([cq_buf[parity, 2 * duo + u] for u in range(2) for parity in range(2)], axis=0)
        q_raw[...] = dot_t(w, cq)

    def query_stage(n):
        quad, duo = place(n)
        raw = q_raw
        for u in range(2):
            slot = 2 * lax.rem(duo, 2) + u
            cos, sin = cos_ref[2 * duo + u], sin_ref[2 * duo + u]
            for h in range(4):
                pair, side = h // 2, h % 2
                q = raw[h * head : (h + 1) * head, u * BLOCK : (u + 1) * BLOCK]
                cols = slice(side * BLOCK, (side + 1) * BLOCK)
                qb[u, pair, side * nope : (side + 1) * nope, cols] = q[:nope].astype(BF16)
                lo, hi = q[nope : nope + half], q[nope + half :]
                turned = jnp.concatenate([lo * cos - hi * sin, hi * cos + lo * sin], axis=0).astype(BF16)
                start = pl.multiple_of(BLOCK + slot * rope, rope)
                stale = pl.multiple_of(BLOCK + lax.rem(slot + 2, 4) * rope, rope)
                qb[u, pair, pl.ds(start, rope), cols] = turned
                qb[u, pair, pl.ds(stale, rope), cols] = jnp.zeros_like(turned)

    def key_stage(n, t, u):
        quad, duo = place(n)
        w = wkv[pl.ds(quad * 4, 4), :nope].reshape(4 * nope, rank)
        kb[u][:t] = dot_t(rows[2 * duo + u, :t], w).astype(BF16)

    def value_stage(n, t, u):
        quad, duo = place(n)
        w = wkv[pl.ds(quad * 4, 4), nope:].reshape(4 * nope, rank)
        vb[u][:, :t] = dot_t(w, rows[2 * duo + u, :t]).astype(BF16)

    def score_stage(n, t, u, pair):
        _, duo = place(n)
        length = len_ref[2 * duo + u]
        keys = jnp.concatenate([kb[u][:t, pair * BLOCK : (pair + 1) * BLOCK], rot[duo // 2, :t]], axis=1)
        value = dot(keys, qb[u, pair])
        most = None
        for b in range(t // BLOCK):
            part = value[b * BLOCK : (b + 1) * BLOCK]
            if BLOCK <= b * BLOCK < prefix:
                part = jnp.where(row < length - b * BLOCK, part, NEVER)
            if b * BLOCK == prefix:
                part = jnp.where(near, part, NEVER)
            sb[2 * u + pair][b * BLOCK : (b + 1) * BLOCK] = part
            part = jnp.max(part.reshape(BLOCK // 8, 8, wide), axis=0)
            most = part if most is None else jnp.maximum(most, part)
        mb[2 * u + pair] = jnp.broadcast_to(jnp.max(most, axis=0, keepdims=True), (8, wide))

    def soft_stage(t, u, pair):
        i = 2 * u + pair
        most = mb[i, :1]
        total = None
        for b in range(t // BLOCK):
            x = jnp.exp2((sb[i][b * BLOCK : (b + 1) * BLOCK] - most) * factor)
            part = jnp.sum(x.reshape(BLOCK // 8, 8, wide), axis=0)
            total = part if total is None else total + part
            pb[i][b * BLOCK : (b + 1) * BLOCK] = x.astype(BF16)
        lb[i] = total

    def mix_stage(n, t, u, pair):
        quad, duo = place(n)
        i = 2 * u + pair
        inv = 1.0 / jnp.sum(lb[i], axis=0, keepdims=True)
        o = dot(vb[u][pair * BLOCK : (pair + 1) * BLOCK, :t], pb[i][:t]) * inv
        o = jnp.concatenate([o[:nope, :BLOCK], o[nope:, BLOCK:]], axis=0).T.astype(BF16)
        first, second = o[:toks], o[toks:]
        cols = slice(pair * BLOCK, (pair + 1) * BLOCK)
        o_own[quad, 2 * duo + u, :, cols] = jnp.where(odd == 1, second, first)
        o_send[quad, 2 * duo + u, :, cols] = jnp.where(odd == 1, first, second)

    units = [(u, pair) for u in range(2) for pair in range(2)]
    total = quads * duos

    def each_chip(fn):
        for c in range(slots):
            pl.when(chip == c)(lambda c=c: fn(prefix + (c + 1) * BLOCK))

    def body(b, t):
        before, ahead, later = jnp.maximum(b - 1, 0), jnp.minimum(b + 1, total - 1), jnp.minimum(b + 2, total - 1)
        mix_stage(before, t, 0, 0)
        soft_stage(t, 0, 0)
        score_stage(ahead, t, 0, 0)
        mix_stage(before, t, 0, 1)
        value_stage(b, t, 0)
        soft_stage(t, 0, 1)
        score_stage(ahead, t, 0, 1)
        mix_stage(before, t, 1, 0)
        mix_stage(before, t, 1, 1)
        key_stage(later, t, 0)
        soft_stage(t, 1, 0)
        score_stage(ahead, t, 1, 0)
        value_stage(b, t, 1)
        soft_stage(t, 1, 1)
        score_stage(ahead, t, 1, 1)
        key_stage(later, t, 1)
        query_dot(later)
        query_stage(later)

    def at(b, when):
        return pl.when(b == when)

    def step(b, _):
        @at(b, 0)
        def _():
            rest_of(1)

        @at(b, 2)
        def _():
            rest_of(2)
            pltpu.make_async_copy(rows.at[:, pl.ds(prefix, chunk)], c_out, load_sem.at[0]).start()
            pltpu.make_async_copy(rot.at[:, pl.ds(prefix, chunk)], p_out, load_sem.at[1]).start()

        @at(b, 1)
        def _():
            wire.landed(*ways("wq", ("mine",), "R"))
            wire.start(*across("wq", 1), *onwards("wq", ("mine",)))

        @at(b, duos - 2)
        def _():
            wire.landed(*ways("wkv", late, "R"), *ways("wq", late, "R"), *across("wkv", 1), *across("wq", 1))
            wire.start(*ways("wo", ("mine",), "R"))

        @at(b, duos - 1)
        def _():
            wire.landed(*ways("wq", ("mine",), "L"))
            wire.start(*across("wq", 2))

        @at(b, 9)
        def _():
            wire.landed(*ways("wkv", late, "L"), *ways("wq", late, "L"), *across("wkv", 2), *across("wq", 2))
            wire.start(*onwards("wkv", late), *onwards("wq", late))

        @at(b, 14)
        def _():
            wire.landed(*onwards("wkv", by_ring), *onwards("wq", by_ring))
            wire.start(*across("wkv", 3), *across("wq", 3))
            wire.landed(*ways("wo", ("mine",), "L"))
            wire.start(*across("wo", 2), *ways("wo", late, "L"))

        @at(b, 16)
        def _():
            wire.landed(*across("wkv", 3), *across("wq", 3))
            wire.landed(*ways("wo", ("mine",), "R"))
            wire.start(*across("wo", 1), *onwards("wo", ("mine",)), *ways("wo", late, "R"))

        @at(b, 22)
        def _():
            wire.landed(*onwards("wo", ("mine",)))
            wire.start(*across("wo", 3))

        @at(b, 28)
        def _():
            wire.landed(*both("wo", late))
            wire.start(*onwards("wo", late))

        for quad in range(quads - 1):
            at(b, (quad + 1) * duos + 1)(functools.partial(wire.start, f"o{quad}S"))

        each_chip(functools.partial(body, b))
        return 0

    def lead_in(t):
        for u in range(2):
            key_stage(0, t, u)
        query_dot(0)
        query_stage(0)

    def second(t):
        for u, pair in units:
            score_stage(0, t, u, pair)
        for u in range(2):
            key_stage(1, t, u)
        query_dot(1)
        query_stage(1)

    each_chip(lead_in)
    each_chip(second)
    lax.fori_loop(0, total, step, 0)

    def last(t):
        for u, pair in units:
            mix_stage(total - 1, t, u, pair)

    each_chip(last)
    wire.start(f"o{quads - 1}S")
    pltpu.make_async_copy(o_own, o_out.at[0], load_sem.at[2]).start()

    wire.landed(*across("wo", 1, 2))
    wire.start("woS1", "woS2")
    wire.landed(*onwards("wo", late), *across("wo", 3))
    wire.start("woS3")
    for slot in range(slots):
        wire.landed(f"woS{slot}")
    for quad in range(quads):
        wire.landed(f"o{quad}S")
    wire.sent(*wire.index)
    pltpu.make_async_copy(rows.at[:, pl.ds(prefix, chunk)], c_out, load_sem.at[0]).wait()
    pltpu.make_async_copy(rot.at[:, pl.ds(prefix, chunk)], p_out, load_sem.at[1]).wait()
    pltpu.make_async_copy(o_own, o_out.at[0], load_sem.at[2]).wait()


def finish_kernel(tiles, len_ref, o_ref, own_ref, w_ref, x_ref, c_ref, p_ref, lat_ref, pe_ref, y_ref, lat_out, pe_out, fresh):
    step = pl.program_id(0)
    me = lax.axis_index("tp")
    odd, chip = lax.rem(me, 2), me // 2
    _, quads, seqs, toks, depth = o_ref.shape
    slots, w_rows, wide = w_ref.shape[1:]
    rank = lat_ref.shape[2]
    rope, cache_len = pe_ref.shape[1:]
    chunk = slots * 2 * toks
    words = rank // BLOCK
    length = len_ref[step]

    def slot_of(j):
        return lax.rem(chip - j + slots, slots)

    def output():
        y = x_ref[...].reshape(seqs * toks, wide).astype(F32)
        for side in range(2):
            w = w_ref[odd if side == 0 else 1 - odd].reshape(slots * w_rows, wide)
            if side == 0:
                w = jnp.concatenate([own_ref[...], w[w_rows:]], axis=0)
            for quad in range(quads):
                y = y + dot(o_ref[side, quad].reshape(seqs * toks, depth), w[quad * depth : (quad + 1) * depth])
        y_ref[...] = y.astype(BF16).reshape(y_ref.shape)

    def cache():
        for j in range(slots):
            piece = c_ref[0, slot_of(j)].reshape(2 * toks, rank).astype(F32)
            for w in range(words):
                fresh[w, BLOCK + j * 2 * toks : BLOCK + (j + 1) * 2 * toks] = piece[:, w * BLOCK : (w + 1) * BLOCK]
        lat_out[...] = lat_ref[...]
        base = (length // 16) * 16
        skew = length - base
        tile_row = lax.broadcasted_iota(jnp.int32, (16, BLOCK), 0)
        for k in range(chunk // 16 + 1):
            at = pl.multiple_of(jnp.minimum(base + k * 16, cache_len - 16), 16)
            for w in range(words):
                cols = slice(w * BLOCK, (w + 1) * BLOCK)
                moved = fresh[w, pl.ds(BLOCK - skew + k * 16, 16), :].astype(BF16)
                if k == 0 or k == chunk // 16:
                    local = tile_row + (at - length)
                    shown = (local >= 0) & (local < chunk) if k == 0 else (local < chunk)
                    if k == 0:
                        rest = lat_ref[0, pl.ds(at, 16), cols]
                    else:
                        shown = shown & (skew > 0)
                        rest = lat_out[0, pl.ds(at, 16), cols]
                    moved = jnp.where(shown, moved.astype(F32), rest.astype(F32)).astype(BF16)
                lat_out[0, pl.ds(at, 16), cols] = moved

        turned = jnp.concatenate([p_ref[0, slot_of(j)].reshape(2 * toks, BLOCK).astype(F32).T for j in range(slots)], axis=1)
        group = lax.rem(step, BLOCK // rope)
        mine = turned[:rope]
        for g in range(1, BLOCK // rope):
            mine = jnp.where(group == g, turned[g * rope : (g + 1) * rope], mine)
        mine = jnp.concatenate([mine, jnp.zeros((rope, cache_len - chunk), F32)], axis=1)
        mine = pltpu.roll(mine, length, axis=1)
        spot = lax.broadcasted_iota(jnp.int32, (rope, cache_len), 1) - length
        pe_out[0] = jnp.where((spot >= 0) & (spot < chunk), mine, pe_ref[0].astype(F32)).astype(BF16)

    @pl.when(step < tiles)
    def _():
        output()
        cache()

    @pl.when(step >= tiles)
    def _():
        cache()


def solution(mesh):
    size = mesh.shape["tp"]
    paired = mesh.shape["dp"] % 2 == 0

    def local_step(hidden, lengths, rope_cos, rope_sin, cache_lat, cache_pe, norm_in, w_dq, norm_q, w_dkv, norm_kv, w_uq, w_uk, w_uv, w_out):
        seqs, toks, dim = hidden.shape
        q_rank = w_dq.shape[1]
        rank, heads, nope = w_uk.shape
        rope = cache_pe.shape[2]
        cache_len = cache_lat.shape[1]
        slots = size // 2
        head = nope + rope
        quads = slots * heads // 4
        chunk = size * toks
        prefix = cache_len - chunk
        per = BLOCK // rope
        groups = seqs // per
        wide = 2 * BLOCK
        cos_t, sin_t = rope_cos.transpose(0, 2, 1), rope_sin.transpose(0, 2, 1)
        pe_t = cache_pe.transpose(0, 2, 1)
        wdkv_t = w_dkv.transpose(1, 0)
        wq_t, wk_t, wv_t = (w.transpose(1, 2, 0) for w in (w_uq, w_uk, w_uv))

        any_spec = pl.BlockSpec(memory_space=pl.ANY)
        vmem_spec = pl.BlockSpec(memory_space=pltpu.VMEM)
        smem_spec = pl.BlockSpec(memory_space=pltpu.SMEM)
        c_all, p_all, o_all, wo_all = pl.pallas_call(
            functools.partial(main_kernel, (size, paired)),
            in_specs=[smem_spec, any_spec, vmem_spec, any_spec, vmem_spec, any_spec, vmem_spec] + [any_spec] * 8,
            out_specs=[any_spec] * 4,
            out_shape=[
                jax.ShapeDtypeStruct((seqs, chunk, rank), BF16),
                jax.ShapeDtypeStruct((groups, chunk, BLOCK), BF16),
                jax.ShapeDtypeStruct((2, quads, seqs, toks, 4 * nope), BF16),
                jax.ShapeDtypeStruct((2, slots) + w_out.shape, BF16),
            ],
            scratch_shapes=[
                pltpu.VMEM(hidden.shape, BF16),
                pltpu.VMEM(w_dq.shape, BF16),
                pltpu.VMEM(wdkv_t.shape, BF16),
                pltpu.VMEM((groups, per * toks, dim), BF16),
                pltpu.VMEM((seqs, cache_len, rank), BF16),
                pltpu.VMEM((groups, cache_len, BLOCK), BF16),
                pltpu.VMEM((seqs, rope, prefix), BF16),
                pltpu.VMEM((seqs, rope // 2, BLOCK), F32),
                pltpu.VMEM((seqs, rope // 2, BLOCK), F32),
                pltpu.VMEM((2, seqs, toks, q_rank), BF16),
                pltpu.VMEM((slots * heads, head, q_rank), BF16),
                pltpu.VMEM((slots * heads, 2 * nope, rank), BF16),
                [pltpu.VMEM((cache_len, 4 * nope), BF16) for _ in range(2)],
                [pltpu.VMEM((4 * nope, cache_len), BF16) for _ in range(2)],
                pltpu.VMEM((2, 2, wide, wide), BF16),
                pltpu.VMEM((4 * head, wide), F32),
                [pltpu.VMEM((cache_len, wide), F32) for _ in range(4)],
                pltpu.VMEM((4, 8, wide), F32),
                [pltpu.VMEM((cache_len, wide), BF16) for _ in range(4)],
                pltpu.VMEM((4, 8, wide), F32),
                pltpu.VMEM((quads, seqs, toks, 4 * nope), BF16),
                pltpu.VMEM((quads, seqs, toks, 4 * nope), BF16),
                pltpu.SemaphoreType.DMA((10 + groups,)),
                pltpu.SemaphoreType.DMA((128,)),
                pltpu.SemaphoreType.DMA((128,)),
            ],
            compiler_params=pltpu.CompilerParams(collective_id=0, has_side_effects=True, vmem_limit_bytes=63 * MIB),
            cost_estimate=pl.CostEstimate(flops=70 * 10**9, bytes_accessed=40 * MIB, transcendentals=30 * 10**6),
            name="main",
        )(lengths, hidden, norm_in, w_dq, norm_q, wdkv_t, norm_kv, cos_t, sin_t, wq_t, wk_t, wv_t, w_out, cache_lat, pe_t)

        part = wide
        tiles = dim // part
        tile = lambda i: jnp.minimum(i, tiles - 1)
        y, lat_new, pe_new = pl.pallas_call(
            functools.partial(finish_kernel, tiles),
            grid_spec=pltpu.PrefetchScalarGridSpec(
                num_scalar_prefetch=1,
                grid=(seqs,),
                in_specs=[
                    pl.BlockSpec(o_all.shape, lambda i, n: (0, 0, 0, 0, 0), pipeline_mode=pl.Buffered(1)),
                    pl.BlockSpec((w_out.shape[0], part), lambda i, n: (0, tile(i))),
                    pl.BlockSpec(wo_all.shape[:3] + (part,), lambda i, n: (0, 0, 0, tile(i))),
                    pl.BlockSpec((seqs, toks, part), lambda i, n: (0, 0, tile(i))),
                    pl.BlockSpec((1, slots, 2, toks, rank), lambda i, n: (i, 0, 0, 0, 0)),
                    pl.BlockSpec((1, slots, 2, toks, BLOCK), lambda i, n: (i // per, 0, 0, 0, 0)),
                    pl.BlockSpec((1, cache_len, rank), lambda i, n: (i, 0, 0)),
                    pl.BlockSpec((1, rope, cache_len), lambda i, n: (i, 0, 0)),
                ],
                out_specs=[
                    pl.BlockSpec((seqs, toks, part), lambda i, n: (0, 0, tile(i))),
                    pl.BlockSpec((1, cache_len, rank), lambda i, n: (i, 0, 0)),
                    pl.BlockSpec((1, rope, cache_len), lambda i, n: (i, 0, 0)),
                ],
                scratch_shapes=[pltpu.VMEM((rank // BLOCK, chunk + 2 * BLOCK, BLOCK), F32)],
            ),
            out_shape=[
                jax.ShapeDtypeStruct(hidden.shape, BF16),
                jax.ShapeDtypeStruct(cache_lat.shape, BF16),
                jax.ShapeDtypeStruct(pe_t.shape, BF16),
            ],
            compiler_params=pltpu.CompilerParams(vmem_limit_bytes=63 * MIB),
            cost_estimate=pl.CostEstimate(flops=2 * seqs * toks * dim * dim, bytes_accessed=50 * MIB, transcendentals=0),
            name="finish",
        )(
            lengths,
            o_all,
            w_out,
            wo_all,
            hidden,
            c_all.reshape(seqs, slots, 2, toks, rank),
            p_all.reshape(groups, slots, 2, toks, BLOCK),
            cache_lat,
            pe_t,
        )
        return y, lat_new, pe_new.transpose(0, 2, 1)

    spec_tok = P("dp", "tp", None)
    spec_len = P("dp")
    spec_seq = P("dp", None, None)
    spec_vec = P(None)
    spec_mat = P(None, None)
    spec_head = P(None, "tp", None)
    spec_rows = P("tp", None)
    in_specs = (spec_tok, spec_len, spec_seq, spec_seq, spec_seq, spec_seq, spec_vec, spec_mat, spec_vec, spec_mat, spec_vec, spec_head, spec_head, spec_head, spec_rows)
    return jax.shard_map(local_step, mesh=mesh, in_specs=in_specs, out_specs=(spec_tok, spec_seq, spec_seq), check_vma=False)
```

```python
import functools

import jax
import jax.numpy as jnp
from jax import lax
from jax.experimental import pallas as pl
from jax.experimental.pallas import tpu as pltpu
from jax.sharding import PartitionSpec as P

BLOCK = 128
LOG2E = 1.4426950408889634
NEVER = -1e30
WO_SIDE = 80
F32 = jnp.float32
BF16 = jnp.bfloat16
MESH = pl.DeviceIdType.MESH
MIB = 2**20


def dot(a, b):
    return lax.dot_general(a, b, (((1,), (0,)), ((), ())), preferred_element_type=F32)


def dot_t(a, b):
    return lax.dot_general(a, b, (((1,), (1,)), ((), ())), preferred_element_type=F32)


def unit(x):
    return x * lax.rsqrt(jnp.mean(x * x, axis=-1, keepdims=True) + 1e-6)


class Wire:
    def __init__(self, send_sem, recv_sem):
        self.sems = (send_sem, recv_sem)
        self.made = {}
        self.index = {}

    def add(self, name, src, dst, **peer):
        self.index[name] = len(self.index)
        self.made[name] = lambda: pltpu.make_async_remote_copy(
            src(), dst(), self.sems[0].at[self.index[name]], self.sems[1].at[self.index[name]], device_id=peer, device_id_type=MESH
        )

    def start(self, *names):
        for name in names:
            self.made[name]().start()

    def landed(self, *names):
        for name in names:
            self.made[name]().wait_recv()

    def sent(self, *names):
        for name in names:
            self.made[name]().wait_send()


def main_kernel(
    plan,
    len_ref,
    x_hbm,
    g1_ref,
    wdq_hbm,
    gq_ref,
    wdkv_hbm,
    gkv_ref,
    cos_hbm,
    sin_hbm,
    wq_hbm,
    wk_hbm,
    wv_hbm,
    wo_hbm,
    lat_hbm,
    pe_hbm,
    c_out,
    p_out,
    o_out,
    wo_out,
    x_buf,
    wdq,
    wdkv,
    a_buf,
    rows,
    rot,
    pe_buf,
    cos_ref,
    sin_ref,
    cq_buf,
    wq,
    wkv,
    kb,
    vb,
    qb,
    q_raw,
    sb,
    mb,
    pb,
    lb,
    o_own,
    o_send,
    wo_buf,
    load_sem,
    send_sem,
    recv_sem,
):
    size, paired = plan
    me = lax.axis_index("tp")
    odd = lax.rem(me, 2)
    chip = me // 2
    right, left = lax.rem(me + 2, size), lax.rem(me + size - 2, size)
    onward = jnp.where(odd == 0, right, left)
    other = me + 1 - 2 * odd
    dp = lax.axis_index("dp")
    e = lax.rem(dp, 2) if paired else dp * 0
    partner = dp + 1 - 2 * e

    seqs, toks, dim = x_hbm.shape
    groups = rot.shape[0]
    per = seqs // groups
    rank = rows.shape[2]
    slots = size // 2
    chunk = size * toks
    prefix = rows.shape[1] - chunk
    heads = wq.shape[0] // slots
    head, q_rank = wq.shape[1:]
    rope = BLOCK // per
    half = rope // 2
    nope = head - rope
    quads = wq.shape[0] // 4
    duos = seqs // 2
    wide = 2 * BLOCK
    factor = LOG2E * head**-0.5

    loads = {}

    def load(name, src, dst):
        loads[name] = pltpu.make_async_copy(src, dst, load_sem.at[len(loads)])
        loads[name].start()

    def spot(slot, parity):
        return pl.ds(pl.multiple_of(prefix + slot * BLOCK + parity * toks, toks), toks)

    barrier = pltpu.get_barrier_semaphore()
    for peer in (left, right, other):
        pl.semaphore_signal(barrier, inc=1, device_id={"tp": peer}, device_id_type=MESH)
    if paired:
        pl.semaphore_signal(barrier, inc=1, device_id={"dp": partner}, device_id_type=MESH)

    lanes_chip = pl.ds(pl.multiple_of(chip * BLOCK, BLOCK), BLOCK)
    load("wk", wk_hbm, wkv.at[pl.ds(0, heads), pl.ds(0, nope)])
    load("wv", wv_hbm, wkv.at[pl.ds(0, heads), pl.ds(nope, nope)])
    for g in range(groups):
        load(f"x{g}", x_hbm.at[pl.ds(g * per, per)], x_buf.at[pl.ds(g * per, per)])
        if g == 0:
            load("wdkv", wdkv_hbm, wdkv)
            load("cos", cos_hbm.at[:, :, lanes_chip], cos_ref)
            load("sin", sin_hbm.at[:, :, lanes_chip], sin_ref)
    load("wq", wq_hbm, wq.at[pl.ds(0, heads)])
    load("wdq", wdq_hbm, wdq)
    load("pe", pe_hbm.at[:, :, pl.ds(0, prefix)], pe_buf)
    load("lat", lat_hbm.at[:, pl.ds(0, prefix)], rows.at[:, pl.ds(0, prefix)])
    pl.semaphore_wait(barrier, 4 if paired else 3)

    wire = Wire(send_sem, recv_sem)

    def chain(name, here, there, places, via="split"):
        near_left, near_right, opposite = places
        handed = {"right": near_left, "left": near_right, "split": jnp.where(odd == 0, near_left, near_right)}[via]
        wire.add(name + "R", lambda: here(0), lambda: there(near_left), tp=right)
        wire.add(name + "L", lambda: here(0), lambda: there(near_right), tp=left)
        wire.add(name + "O", lambda: there(handed), lambda: there(opposite), tp={"right": right, "left": left, "split": onward}[via])

    for g in range(groups):
        for name, ref in (("c", lambda slot, g=g: rows.at[pl.ds(g * per, per), spot(slot, odd)]), ("p", lambda slot, g=g: rot.at[g, spot(slot, odd)])):
            name = f"{name}{g}"
            chain(name, ref, ref, (1, 3, 2), "left")
            for slot in range(slots):
                wire.add(f"{name}S{slot}", functools.partial(ref, slot), functools.partial(ref, slot), tp=other)
        cq_ref = lambda g=g: cq_buf.at[odd, pl.ds(g * per, per)]
        wire.add(f"q{g}S", cq_ref, cq_ref, tp=other)

    def cut(total, side, unit, part):
        if part == "mid":
            return pl.ds(side, total - 2 * side)
        flip = e if part == "mine" else 1 - e
        return pl.ds(pl.multiple_of(flip * (total - side), unit), side)

    def wq_at(part, slot):
        return wq.at[pl.ds(slot * heads, heads), :, cut(q_rank, q_rank // 3, BLOCK, part)]

    def wk_at(part, slot):
        return wkv.at[pl.ds(slot * heads, heads), pl.ds(0, nope), cut(rank, rank // 2, BLOCK, part)]

    def wv_at(part, slot):
        return wkv.at[pl.ds(slot * heads, heads), pl.ds(nope, nope), cut(rank, rank // 2, BLOCK, part)]

    def wo_at(part, slot):
        return wo_out.at[odd, slot, cut(wo_hbm.shape[0], WO_SIDE, 16, part)]

    def own(ref, total, side, unit, rows=False):
        return lambda part, slot: ref.at[cut(total, side, unit, part)] if rows else ref.at[:, :, cut(total, side, unit, part)]

    halves = ("mine",) if paired else ("mine", "rest")
    thirds = ("mine", "mid") if paired else ("mine", "mid", "rest")
    for name, here, there, parts in (
        ("wq", own(wq_hbm, q_rank, q_rank // 3, BLOCK), wq_at, thirds),
        ("wk", own(wk_hbm, rank, rank // 2, BLOCK), wk_at, halves),
        ("wv", own(wv_hbm, rank, rank // 2, BLOCK), wv_at, halves),
        ("wo", own(wo_hbm, wo_hbm.shape[0], WO_SIDE, 16, True), wo_at, thirds),
    ):
        for part in parts:
            via = "right" if part == "mine" and name != "wo" else "split"
            chain(f"{name}.{part}", functools.partial(here, part), functools.partial(there, part), (1, 2, 3), via)
        if paired:
            for slot in (1, 2, 3):
                ref = functools.partial(there, "mine", slot)
                wire.add(f"{name}Z{slot}", ref, ref, dp=partner)
    for slot in range(slots):
        ref = lambda slot=slot: wo_out.at[odd, slot]
        if slot < slots - 1:
            wire.add(f"woS{slot}", ref if slot else lambda: wo_hbm, ref, tp=other)
    for part in ("mine", "mid", "rest"):
        ref = functools.partial(wo_at, part, slots - 1)
        wire.add(f"woS.{part}", ref, ref, tp=other)
    for quad in range(quads):
        wire.add(f"o{quad}S", lambda quad=quad: o_send.at[quad], lambda quad=quad: o_out.at[odd, quad], tp=other)

    more = {"wq": thirds[1:], "wo": thirds[1:], "wk": halves[1:], "wv": halves[1:]}
    small = ("wk", "wv", "wq")

    def names(kinds, which, parts):
        out = []
        for kind in kinds:
            for part in {"first": ("mine",), "more": more[kind], "all": ("mine",) + tuple(more[kind])}[parts]:
                out += [f"{kind}.{part}{way}" for way in which]
        return out

    def across(slot, *kinds):
        return [f"{kind}Z{slot}" for kind in kinds] if paired else []

    def norm(g):
        for r in range(0, per):
            x = x_buf[g * per + r].astype(F32)
            a_buf[g, r * toks : (r + 1) * toks] = (unit(x) * g1_ref[...]).astype(BF16)

    def latent(g):
        kv = dot_t(a_buf[g], wdkv[...])
        rows[g * per : (g + 1) * per, spot(0, odd), :] = (unit(kv[:, :rank]) * gkv_ref[...]).astype(BF16).reshape(per, toks, rank)
        turned = []
        for s in range(per):
            cos_pair, sin_pair = cos_ref[g * per + s], sin_ref[g * per + s]
            cos = jnp.where(odd == 1, cos_pair[:, toks:], cos_pair[:, :toks])
            sin = jnp.where(odd == 1, sin_pair[:, toks:], sin_pair[:, :toks])
            table = jnp.concatenate([cos, cos, -sin, sin], axis=0).T
            p = kv[s * toks : (s + 1) * toks, rank:]
            swapped = jnp.concatenate([p[:, half:], p[:, :half]], axis=1)
            turned.append(p * table[:, :rope] + swapped * table[:, rope:])
        rot[g, spot(0, odd), :] = jnp.concatenate(turned, axis=1).astype(BF16)

    def queries(g):
        h = jnp.concatenate([dot(a_buf[g], wdq[:, : 2 * rank]), dot(a_buf[g], wdq[:, 2 * rank :])], axis=1)
        cq_buf[odd, g * per : (g + 1) * per] = (unit(h) * gq_ref[...]).astype(BF16).reshape(per, toks, q_rank)

    wire.start(*names(("wk", "wv"), "RL", "first"))
    with jax.named_scope('p_kv'):
        for name in ("x0", "wdkv", "cos", "sin"):
            loads[name].wait()
        norm(0)
        for g in range(groups):
            if g + 1 < groups:
                loads[f"x{g + 1}"].wait()
                norm(g + 1)
            latent(g)
            for way in ("R", "L", "S0"):
                wire.start(f"c{g}{way}", f"p{g}{way}")
    wire.start(*names(("wq",), "R", "first"), *names(small, "R", "more"))

    def hand_on(g):
        wire.landed(f"c{g}L", f"p{g}L", f"c{g}R", f"p{g}R")
        wire.start(f"c{g}O", f"p{g}O", f"c{g}S3", f"p{g}S3", f"c{g}S1", f"p{g}S1")

    with jax.named_scope('p_cq'):
        loads["wdq"].wait()
        for g in range(groups):
            queries(g)
            wire.start(f"q{g}S")
            hand_on(g)
            if g == 1:
                wire.landed(*names(("wk", "wv"), "RL", "first"))
                wire.start(*across(1, "wk", "wv"), *across(2, "wk", "wv"))
    wire.start(*names(("wq",), "L", "first"), *names(small, "L", "more"), *names(("wo",), "L", "first"), "woS0")

    loads["pe"].wait()
    for g in range(groups):
        old = pe_buf[g * per : (g + 1) * per].reshape(per * rope, prefix).astype(F32)
        for b in range(prefix // BLOCK):
            rot[g, b * BLOCK : (b + 1) * BLOCK] = old[:, b * BLOCK : (b + 1) * BLOCK].T.astype(BF16)
    qb[...] = jnp.zeros_like(qb)

    def rest_of(g):
        wire.landed(f"c{g}O", f"p{g}O")
        wire.start(f"c{g}S2", f"p{g}S2")
        for slot in (0, 1, 3, 2):
            wire.landed(f"c{g}S{slot}", f"p{g}S{slot}")
        wire.landed(f"q{g}S")

    with jax.named_scope('p_rest0'):
        for name in ("wk", "wv", "wq", "lat"):
            loads[name].wait()
        rest_of(0)

    row = lax.broadcasted_iota(jnp.int32, (BLOCK, wide), 0)
    lane = lax.rem(lax.broadcasted_iota(jnp.int32, (BLOCK, wide), 1), BLOCK)
    near = row <= lane

    def place(n):
        return n // duos, lax.rem(n, duos)

    def query_dot(n):
        quad, duo = place(n)
        w = wq[pl.ds(quad * 4, 4)].reshape(4 * head, q_rank)
        cq = jnp.concatenate([cq_buf[parity, 2 * duo + u] for u in range(2) for parity in range(2)], axis=0)
        q_raw[...] = dot_t(w, cq)

    def query_stage(n):
        quad, duo = place(n)
        raw = q_raw
        for u in range(2):
            slot = 2 * lax.rem(duo, 2) + u
            cos, sin = cos_ref[2 * duo + u], sin_ref[2 * duo + u]
            for h in range(4):
                pair, side = h // 2, h % 2
                q = raw[h * head : (h + 1) * head, u * BLOCK : (u + 1) * BLOCK]
                cols = slice(side * BLOCK, (side + 1) * BLOCK)
                qb[u, pair, side * nope : (side + 1) * nope, cols] = q[:nope].astype(BF16)
                lo, hi = q[nope : nope + half], q[nope + half :]
                turned = jnp.concatenate([lo * cos - hi * sin, hi * cos + lo * sin], axis=0).astype(BF16)
                start = pl.multiple_of(BLOCK + slot * rope, rope)
                stale = pl.multiple_of(BLOCK + lax.rem(slot + 2, 4) * rope, rope)
                qb[u, pair, pl.ds(start, rope), cols] = turned
                qb[u, pair, pl.ds(stale, rope), cols] = jnp.zeros_like(turned)

    def key_stage(n, t, u):
        quad, duo = place(n)
        w = wkv[pl.ds(quad * 4, 4), :nope].reshape(4 * nope, rank)
        kb[u][:t] = dot_t(rows[2 * duo + u, :t], w).astype(BF16)

    def value_stage(n, t, u):
        quad, duo = place(n)
        w = wkv[pl.ds(quad * 4, 4), nope:].reshape(4 * nope, rank)
        vb[u][:, :t] = dot_t(w, rows[2 * duo + u, :t]).astype(BF16)

    def score_stage(n, t, u, pair):
        _, duo = place(n)
        length = len_ref[2 * duo + u]
        keys = jnp.concatenate([kb[u][:t, pair * BLOCK : (pair + 1) * BLOCK], rot[duo // 2, :t]], axis=1)
        value = dot(keys, qb[u, pair])
        most = None
        for b in range(t // BLOCK):
            part = value[b * BLOCK : (b + 1) * BLOCK]
            if BLOCK <= b * BLOCK < prefix:
                part = jnp.where(row < length - b * BLOCK, part, NEVER)
            if b * BLOCK == prefix:
                part = jnp.where(near, part, NEVER)
            sb[2 * u + pair][b * BLOCK : (b + 1) * BLOCK] = part
            part = jnp.max(part.reshape(BLOCK // 8, 8, wide), axis=0)
            most = part if most is None else jnp.maximum(most, part)
        mb[2 * u + pair] = jnp.broadcast_to(jnp.max(most, axis=0, keepdims=True), (8, wide))

    def soft_stage(t, u, pair):
        i = 2 * u + pair
        most = mb[i, :1]
        total = None
        for b in range(t // BLOCK):
            x = jnp.exp2((sb[i][b * BLOCK : (b + 1) * BLOCK] - most) * factor)
            part = jnp.sum(x.reshape(BLOCK // 8, 8, wide), axis=0)
            total = part if total is None else total + part
            pb[i][b * BLOCK : (b + 1) * BLOCK] = x.astype(BF16)
        lb[i] = total

    def mix_stage(n, t, u, pair):
        quad, duo = place(n)
        i = 2 * u + pair
        inv = 1.0 / jnp.sum(lb[i], axis=0, keepdims=True)
        o = dot(vb[u][pair * BLOCK : (pair + 1) * BLOCK, :t], pb[i][:t]) * inv
        o = jnp.concatenate([o[:nope, :BLOCK], o[nope:, BLOCK:]], axis=0).T.astype(BF16)
        first, second = o[:toks], o[toks:]
        cols = slice(pair * BLOCK, (pair + 1) * BLOCK)
        o_own[quad, 2 * duo + u, :, cols] = jnp.where(odd == 1, second, first)
        o_send[quad, 2 * duo + u, :, cols] = jnp.where(odd == 1, first, second)

    units = [(u, pair) for u in range(2) for pair in range(2)]
    total = quads * duos

    def each_chip(fn):
        for c in range(slots):
            pl.when(chip == c)(lambda c=c: fn(prefix + (c + 1) * BLOCK))

    def body(b, t):
        before, ahead, later = jnp.maximum(b - 1, 0), jnp.minimum(b + 1, total - 1), jnp.minimum(b + 2, total - 1)
        mix_stage(before, t, 0, 0)
        soft_stage(t, 0, 0)
        score_stage(ahead, t, 0, 0)
        mix_stage(before, t, 0, 1)
        value_stage(b, t, 0)
        soft_stage(t, 0, 1)
        score_stage(ahead, t, 0, 1)
        mix_stage(before, t, 1, 0)
        mix_stage(before, t, 1, 1)
        key_stage(later, t, 0)
        soft_stage(t, 1, 0)
        score_stage(ahead, t, 1, 0)
        value_stage(b, t, 1)
        soft_stage(t, 1, 1)
        score_stage(ahead, t, 1, 1)
        key_stage(later, t, 1)
        query_dot(later)
        query_stage(later)

    def at(b, when):
        return pl.when(b == when)

    agenda = [
        (0, None, names(("wq",), "R", "first"), across(1, "wq") + names(small, "O", "first")),
        (2, None, names(small, "R", "more"), []),
        (2, 0, [], names(small, "O", "more")),
        (2, None, [], names(("wo",), "R", "first")),
        (4, None, across(1, *small), []),
        (4, None, names(("wq",), "L", "first"), across(2, "wq")),
        (6, None, names(small, "O", "first"), across(3, *small)),
        (7, 1, names(small, "L", "more"), names(small, "O", "more")),
        (9, 0, names(small, "L", "more"), []),
        (9, None, across(2, *small), []),
        (12, None, names(("wo",), "L", "first"), []),
        (12, 1, [], names(("wo",), "O", "first")),
        (12, None, [], names(("wo",), "L", "more") + across(2, "wo")),
        (13, None, names(("wo",), "R", "first"), []),
        (13, 0, [], names(("wo",), "O", "first")),
        (13, None, [], names(("wo",), "R", "more") + across(1, "wo")),
        (14, None, names(small, "O", "more") + across(3, *small), []),
        (20, None, names(("wo",), "O", "first"), across(3, "wo") + ["woS.mine"]),
        (24, 0, names(("wo",), "L", "more") + across(2, "wo"), ["woS2"]),
        (24, 1, names(("wo",), "R", "more") + across(1, "wo"), ["woS1"]),
        (26, 0, names(("wo",), "R", "more") + across(1, "wo"), names(("wo",), "O", "more") + ["woS1"]),
        (26, 1, names(("wo",), "L", "more") + across(2, "wo"), names(("wo",), "O", "more") + ["woS2"]),
    ]

    def step(b, _):
        @at(b, 0)
        def _():
            with jax.named_scope('ev_k1'):
                rest_of(1)

        @at(b, 2)
        def _():
            with jax.named_scope('ev_k2'):
                rest_of(2)
            pltpu.make_async_copy(rows.at[:, pl.ds(prefix, chunk)], c_out, load_sem.at[0]).start()
            pltpu.make_async_copy(rot.at[:, pl.ds(prefix, chunk)], p_out, load_sem.at[1]).start()

        for when, parity, waits, starts in agenda:

            @at(b, when)
            def _():
                if parity is None:
                    with jax.named_scope(f"ev_{when}"):
                        wire.landed(*waits)
                    wire.start(*starts)
                else:

                    @pl.when(odd == parity)
                    def _():
                        with jax.named_scope(f"ev_{when}p{parity}"):
                            wire.landed(*waits)
                        wire.start(*starts)

        bounce = pltpu.make_async_copy(wo_hbm, wo_buf, load_sem.at[3])

        @at(b, 1)
        def _():
            bounce.start()

        @at(b, 5)
        def _():
            bounce.wait()
            pltpu.make_async_copy(wo_buf, wo_out.at[odd, 0], load_sem.at[4]).start()

        for quad in range(quads - 1):
            at(b, (quad + 1) * duos + 1)(functools.partial(wire.start, f"o{quad}S"))

        with jax.named_scope('body'):
            each_chip(functools.partial(body, b))
        return 0

    def lead_in(t):
        for u in range(2):
            key_stage(0, t, u)
        query_dot(0)
        query_stage(0)

    def second(t):
        for u, pair in units:
            score_stage(0, t, u, pair)
        for u in range(2):
            key_stage(1, t, u)
        query_dot(1)
        query_stage(1)

    with jax.named_scope('p_lead'):
        each_chip(lead_in)
        each_chip(second)
    lax.fori_loop(0, total, step, 0)

    def last(t):
        for u, pair in units:
            mix_stage(total - 1, t, u, pair)

    with jax.named_scope('p_last'):
        each_chip(last)
        wire.start(f"o{quads - 1}S")
        pltpu.make_async_copy(o_own, o_out.at[odd], load_sem.at[2]).start()
    with jax.named_scope('f_land'):
        if paired:
            wire.landed(*across(3, "wo"))
            wire.start("woS.rest")
        wire.landed(*names(("wo",), "O", "more"))
        wire.start("woS.mid")
        if not paired:
            wire.start("woS.rest")
        for slot in range(slots - 1):
            wire.landed(f"woS{slot}")
        for part in ("mine", "rest", "mid"):
            wire.landed(f"woS.{part}")
        for quad in range(quads):
            wire.landed(f"o{quad}S")
    with jax.named_scope('f_sent'):
        wire.sent(*wire.index)
        pltpu.make_async_copy(rows.at[:, pl.ds(prefix, chunk)], c_out, load_sem.at[0]).wait()
        pltpu.make_async_copy(rot.at[:, pl.ds(prefix, chunk)], p_out, load_sem.at[1]).wait()
        pltpu.make_async_copy(o_own, o_out.at[odd], load_sem.at[2]).wait()
        pltpu.make_async_copy(wo_buf, wo_out.at[odd, 0], load_sem.at[4]).wait()


def finish_kernel(len_ref, o_ref, w_ref, x_hbm, c_ref, p_ref, lat_ref, pe_ref, y_hbm, lat_out, pe_out, fresh, acc, x_buf, y_buf, sems):
    step = pl.program_id(0)
    chip = lax.axis_index("tp") // 2
    seqs, toks, depth = o_ref.shape[2:]
    terms = x_hbm.shape[2] // depth
    slots = c_ref.shape[1]
    rank = lat_ref.shape[2]
    rope, cache_len = pe_ref.shape[1:]
    chunk = slots * 2 * toks
    words = rank // BLOCK
    length = len_ref[step]
    dim = x_hbm.shape[2]
    part = 2 * depth
    load_x = pltpu.make_async_copy(x_hbm, x_buf, sems.at[0])

    def store_y(s):
        return pltpu.make_async_copy(y_buf.at[s], y_hbm.at[s], sems.at[1 + s])

    def slot_of(j):
        return lax.rem(chip - j + slots, slots)

    def project(kind):
        o = o_ref[0, 0].reshape(seqs * toks, depth)
        for n in range(0, dim, part):
            cols = slice(n, n + part)
            y = dot(o, w_ref[0, :, cols])
            if kind != "first":
                y = acc[:, cols] + y
            if kind == "last":
                y = y + x_buf[:, :, cols].reshape(seqs * toks, part).astype(F32)
                y_buf[:, :, cols] = y.astype(BF16).reshape(seqs, toks, part)
            else:
                acc[:, cols] = y

    def cache():
        for j in range(slots):
            piece = c_ref[0, slot_of(j)].reshape(2 * toks, rank).astype(F32)
            for w in range(words):
                fresh[w, BLOCK + j * 2 * toks : BLOCK + (j + 1) * 2 * toks] = piece[:, w * BLOCK : (w + 1) * BLOCK]
        lat_out[...] = lat_ref[...]
        base = (length // 16) * 16
        skew = length - base
        tile_row = lax.broadcasted_iota(jnp.int32, (16, BLOCK), 0)
        for k in range(chunk // 16 + 1):
            at = pl.multiple_of(jnp.minimum(base + k * 16, cache_len - 16), 16)
            for w in range(words):
                cols = slice(w * BLOCK, (w + 1) * BLOCK)
                moved = fresh[w, pl.ds(BLOCK - skew + k * 16, 16), :].astype(BF16)
                if k == 0 or k == chunk // 16:
                    local = tile_row + (at - length)
                    shown = (local >= 0) & (local < chunk) if k == 0 else (local < chunk)
                    if k == 0:
                        rest = lat_ref[0, pl.ds(at, 16), cols]
                    else:
                        shown = shown & (skew > 0)
                        rest = lat_out[0, pl.ds(at, 16), cols]
                    moved = jnp.where(shown, moved.astype(F32), rest.astype(F32)).astype(BF16)
                lat_out[0, pl.ds(at, 16), cols] = moved

        turned = jnp.concatenate([p_ref[0, slot_of(j)].reshape(2 * toks, BLOCK).astype(F32).T for j in range(slots)], axis=1)
        group = lax.rem(step, BLOCK // rope)
        mine = turned[:rope]
        for g in range(1, BLOCK // rope):
            mine = jnp.where(group == g, turned[g * rope : (g + 1) * rope], mine)
        mine = jnp.concatenate([mine, jnp.zeros((rope, cache_len - chunk), F32)], axis=1)
        mine = pltpu.roll(mine, length, axis=1)
        spot = lax.broadcasted_iota(jnp.int32, (rope, cache_len), 1) - length
        pe_out[0] = jnp.where((spot >= 0) & (spot < chunk), mine, pe_ref[0].astype(F32)).astype(BF16)

    @pl.when(step == 0)
    def _():
        load_x.start()
        project("first")
        cache()

    @pl.when((step > 0) & (step < terms - 1))
    def _():
        project("middle")
        cache()

    @pl.when(step == terms - 1)
    def _():
        load_x.wait()
        project("last")
        cache()
        for s in range(seqs):
            store_y(s).start()

    @pl.when(step >= terms)
    def _():
        cache()

    @pl.when(step == pl.num_programs(0) - 1)
    def _():
        for s in range(seqs):
            store_y(s).wait()


def solution(mesh):
    size = mesh.shape["tp"]
    paired = mesh.shape["dp"] % 2 == 0

    def local_step(hidden, lengths, rope_cos, rope_sin, cache_lat, cache_pe, norm_in, w_dq, norm_q, w_dkv, norm_kv, w_uq, w_uk, w_uv, w_out):
        seqs, toks, dim = hidden.shape
        q_rank = w_dq.shape[1]
        rank, heads, nope = w_uk.shape
        rope = cache_pe.shape[2]
        cache_len = cache_lat.shape[1]
        slots = size // 2
        head = nope + rope
        quads = slots * heads // 4
        chunk = size * toks
        prefix = cache_len - chunk
        per = BLOCK // rope
        groups = seqs // per
        wide = 2 * BLOCK
        cos_t, sin_t = rope_cos.transpose(0, 2, 1), rope_sin.transpose(0, 2, 1)
        pe_t = cache_pe.transpose(0, 2, 1)
        wdkv_t = w_dkv.transpose(1, 0)
        wq_t, wk_t, wv_t = (w.transpose(1, 2, 0) for w in (w_uq, w_uk, w_uv))

        any_spec = pl.BlockSpec(memory_space=pl.ANY)
        vmem_spec = pl.BlockSpec(memory_space=pltpu.VMEM)
        smem_spec = pl.BlockSpec(memory_space=pltpu.SMEM)
        c_all, p_all, o_all, wo_all = pl.pallas_call(
            functools.partial(main_kernel, (size, paired)),
            in_specs=[smem_spec, any_spec, vmem_spec, any_spec, vmem_spec, any_spec, vmem_spec] + [any_spec] * 8,
            out_specs=[any_spec] * 4,
            out_shape=[
                jax.ShapeDtypeStruct((seqs, chunk, rank), BF16),
                jax.ShapeDtypeStruct((groups, chunk, BLOCK), BF16),
                jax.ShapeDtypeStruct((2, quads, seqs, toks, 4 * nope), BF16),
                jax.ShapeDtypeStruct((2, slots) + w_out.shape, BF16),
            ],
            scratch_shapes=[
                pltpu.VMEM(hidden.shape, BF16),
                pltpu.VMEM(w_dq.shape, BF16),
                pltpu.VMEM(wdkv_t.shape, BF16),
                pltpu.VMEM((groups, per * toks, dim), BF16),
                pltpu.VMEM((seqs, cache_len, rank), BF16),
                pltpu.VMEM((groups, cache_len, BLOCK), BF16),
                pltpu.VMEM((seqs, rope, prefix), BF16),
                pltpu.VMEM((seqs, rope // 2, BLOCK), F32),
                pltpu.VMEM((seqs, rope // 2, BLOCK), F32),
                pltpu.VMEM((2, seqs, toks, q_rank), BF16),
                pltpu.VMEM((slots * heads, head, q_rank), BF16),
                pltpu.VMEM((slots * heads, 2 * nope, rank), BF16),
                [pltpu.VMEM((cache_len, 4 * nope), BF16) for _ in range(2)],
                [pltpu.VMEM((4 * nope, cache_len), BF16) for _ in range(2)],
                pltpu.VMEM((2, 2, wide, wide), BF16),
                pltpu.VMEM((4 * head, wide), F32),
                [pltpu.VMEM((cache_len, wide), F32) for _ in range(4)],
                pltpu.VMEM((4, 8, wide), F32),
                [pltpu.VMEM((cache_len, wide), BF16) for _ in range(4)],
                pltpu.VMEM((4, 8, wide), F32),
                pltpu.VMEM((quads, seqs, toks, 4 * nope), BF16),
                pltpu.VMEM((quads, seqs, toks, 4 * nope), BF16),
                pltpu.VMEM(w_out.shape, BF16),
                pltpu.SemaphoreType.DMA((10 + groups,)),
                pltpu.SemaphoreType.DMA((128,)),
                pltpu.SemaphoreType.DMA((128,)),
            ],
            compiler_params=pltpu.CompilerParams(collective_id=0, has_side_effects=True, vmem_limit_bytes=63 * MIB),
            cost_estimate=pl.CostEstimate(flops=70 * 10**9, bytes_accessed=40 * MIB, transcendentals=30 * 10**6),
            name="main",
        )(lengths, hidden, norm_in, w_dq, norm_q, wdkv_t, norm_kv, cos_t, sin_t, wq_t, wk_t, wv_t, w_out, cache_lat, pe_t)

        depth = 4 * nope
        term = lambda i: jnp.minimum(i, 2 * quads - 1)
        y, lat_new, pe_new = pl.pallas_call(
            finish_kernel,
            grid_spec=pltpu.PrefetchScalarGridSpec(
                num_scalar_prefetch=1,
                grid=(seqs,),
                in_specs=[
                    pl.BlockSpec((1, 1, seqs, toks, depth), lambda i, n: (term(i) // quads, lax.rem(term(i), quads), 0, 0, 0)),
                    pl.BlockSpec((1, depth, dim), lambda i, n: (term(i) // quads, lax.rem(term(i), quads), 0)),
                    any_spec,
                    pl.BlockSpec((1, slots, 2, toks, rank), lambda i, n: (i, 0, 0, 0, 0)),
                    pl.BlockSpec((1, slots, 2, toks, BLOCK), lambda i, n: (i // per, 0, 0, 0, 0)),
                    pl.BlockSpec((1, cache_len, rank), lambda i, n: (i, 0, 0)),
                    pl.BlockSpec((1, rope, cache_len), lambda i, n: (i, 0, 0)),
                ],
                out_specs=[
                    any_spec,
                    pl.BlockSpec((1, cache_len, rank), lambda i, n: (i, 0, 0)),
                    pl.BlockSpec((1, rope, cache_len), lambda i, n: (i, 0, 0)),
                ],
                scratch_shapes=[
                    pltpu.VMEM((rank // BLOCK, chunk + 2 * BLOCK, BLOCK), F32),
                    pltpu.VMEM((seqs * toks, dim), F32),
                    pltpu.VMEM(hidden.shape, BF16),
                    pltpu.VMEM(hidden.shape, BF16),
                    pltpu.SemaphoreType.DMA((1 + seqs,)),
                ],
            ),
            out_shape=[
                jax.ShapeDtypeStruct(hidden.shape, BF16),
                jax.ShapeDtypeStruct(cache_lat.shape, BF16),
                jax.ShapeDtypeStruct(pe_t.shape, BF16),
            ],
            compiler_params=pltpu.CompilerParams(vmem_limit_bytes=63 * MIB),
            cost_estimate=pl.CostEstimate(flops=2 * seqs * toks * dim * dim, bytes_accessed=50 * MIB, transcendentals=0),
            name="finish",
        )(
            lengths,
            o_all,
            wo_all.reshape(2, slots * w_out.shape[0], dim),
            hidden,
            c_all.reshape(seqs, slots, 2, toks, rank),
            p_all.reshape(groups, slots, 2, toks, BLOCK),
            cache_lat,
            pe_t,
        )
        return y, lat_new, pe_new.transpose(0, 2, 1)

    spec_tok = P("dp", "tp", None)
    spec_len = P("dp")
    spec_seq = P("dp", None, None)
    spec_vec = P(None)
    spec_mat = P(None, None)
    spec_head = P(None, "tp", None)
    spec_rows = P("tp", None)
    in_specs = (spec_tok, spec_len, spec_seq, spec_seq, spec_seq, spec_seq, spec_vec, spec_mat, spec_vec, spec_mat, spec_vec, spec_head, spec_head, spec_head, spec_rows)
    return jax.shard_map(local_step, mesh=mesh, in_specs=in_specs, out_specs=(spec_tok, spec_seq, spec_seq), check_vma=False)
```

```python
import functools

import jax
import jax.numpy as jnp
from jax import lax
from jax.experimental import pallas as pl
from jax.experimental.pallas import tpu as pltpu
from jax.sharding import PartitionSpec as P

BLOCK = 128
LOG2E = 1.4426950408889634
NEVER = -1e30
NORM_ROWS = 16
F32 = jnp.float32
BF16 = jnp.bfloat16
MESH = pl.DeviceIdType.MESH
MIB = 2**20


def dot(a, b):
    return lax.dot_general(a, b, (((1,), (0,)), ((), ())), preferred_element_type=F32)


def dot_t(a, b):
    return lax.dot_general(a, b, (((1,), (1,)), ((), ())), preferred_element_type=F32)


def unit(x):
    return x * lax.rsqrt(jnp.mean(x * x, axis=-1, keepdims=True) + 1e-6)


class Wire:
    def __init__(self, send_sem, recv_sem):
        self.sems = (send_sem, recv_sem)
        self.made = {}
        self.index = {}

    def add(self, name, src, dst, **peer):
        self.index[name] = len(self.index)
        self.made[name] = lambda: pltpu.make_async_remote_copy(
            src(), dst(), self.sems[0].at[self.index[name]], self.sems[1].at[self.index[name]], device_id=peer, device_id_type=MESH
        )

    def start(self, *names):
        for name in names:
            self.made[name]().start()

    def landed(self, *names):
        for name in names:
            self.made[name]().wait_recv()

    def sent(self, *names):
        for name in names:
            self.made[name]().wait_send()


def main_kernel(
    plan,
    len_ref,
    x_hbm,
    g1_ref,
    wdq_hbm,
    gq_ref,
    wdkv_hbm,
    gkv_ref,
    cos_hbm,
    sin_hbm,
    wq_hbm,
    wk_hbm,
    wv_hbm,
    wo_hbm,
    lat_hbm,
    pe_hbm,
    c_out,
    p_out,
    o_out,
    wo_out,
    x_buf,
    wdq,
    wdkv,
    a_buf,
    rows,
    rot,
    pe_buf,
    cos_ref,
    sin_ref,
    cq_buf,
    wq,
    wkv,
    kb,
    vb,
    qb,
    q_raw,
    sb,
    mb,
    pb,
    lb,
    o_own,
    o_send,
    wo_buf,
    load_sem,
    send_sem,
    recv_sem,
):
    size, stride, paired = plan
    me = lax.axis_index("tp")
    odd = lax.rem(me, 2)
    chip = me // 2
    right, left = lax.rem(me + 2, size), lax.rem(me + size - 2, size)
    onward = jnp.where(odd == 0, right, left)
    other = me + 1 - 2 * odd
    dp = lax.axis_index("dp")
    flip = {"a": lax.rem(dp, 2), "b": lax.rem(dp // stride, 2)}
    partner = {"a": dp + 1 - 2 * flip["a"], "b": dp + stride * (1 - 2 * flip["b"])}

    seqs, toks, dim = x_hbm.shape
    groups = rot.shape[0]
    per = seqs // groups
    rank = rows.shape[2]
    slots = size // 2
    chunk = size * toks
    prefix = rows.shape[1] - chunk
    heads = wq.shape[0] // slots
    head, q_rank = wq.shape[1:]
    rope = BLOCK // per
    half = rope // 2
    nope = head - rope
    quads = wq.shape[0] // 4
    duos = seqs // 2
    wide = 2 * BLOCK
    factor = LOG2E * head**-0.5

    loads = {}

    def load(name, src, dst):
        loads[name] = pltpu.make_async_copy(src, dst, load_sem.at[len(loads)])
        loads[name].start()

    def spot(slot, parity):
        return pl.ds(pl.multiple_of(prefix + slot * BLOCK + parity * toks, toks), toks)

    barrier = pltpu.get_barrier_semaphore()
    for peer in (left, right, other):
        pl.semaphore_signal(barrier, inc=1, device_id={"tp": peer}, device_id_type=MESH)
    for side in "ab":
        if paired[side]:
            pl.semaphore_signal(barrier, inc=1, device_id={"dp": partner[side]}, device_id_type=MESH)

    lanes_chip = pl.ds(pl.multiple_of(chip * BLOCK, BLOCK), BLOCK)
    load("wk", wk_hbm, wkv.at[pl.ds(0, heads), pl.ds(0, nope)])
    load("wv", wv_hbm, wkv.at[pl.ds(0, heads), pl.ds(nope, nope)])
    for g in range(groups):
        load(f"x{g}", x_hbm.at[pl.ds(g * per, per)], x_buf.at[pl.ds(g * per, per)])
        if g == 0:
            load("wdkv", wdkv_hbm, wdkv)
            load("cos", cos_hbm.at[:, :, lanes_chip], cos_ref)
            load("sin", sin_hbm.at[:, :, lanes_chip], sin_ref)
    load("wq", wq_hbm, wq.at[pl.ds(0, heads)])
    load("wdq", wdq_hbm, wdq)
    load("pe", pe_hbm.at[:, :, pl.ds(0, prefix)], pe_buf)
    load("lat", lat_hbm.at[:, pl.ds(0, prefix)], rows.at[:, pl.ds(0, prefix)])
    wire = Wire(send_sem, recv_sem)

    def chain(name, here, there, places, via="split"):
        near_left, near_right, opposite = places
        handed = {"right": near_left, "left": near_right, "split": jnp.where(odd == 0, near_left, near_right)}[via]
        wire.add(name + "R", lambda: here(0), lambda: there(near_left), tp=right)
        wire.add(name + "L", lambda: here(0), lambda: there(near_right), tp=left)
        wire.add(name + "O", lambda: there(handed), lambda: there(opposite), tp={"right": right, "left": left, "split": onward}[via])

    for g in range(groups):
        for name, ref in (("c", lambda slot, g=g: rows.at[pl.ds(g * per, per), spot(slot, odd)]), ("p", lambda slot, g=g: rot.at[g, spot(slot, odd)])):
            name = f"{name}{g}"
            chain(name, ref, ref, (1, 3, 2), "left")
            for slot in range(slots):
                wire.add(f"{name}S{slot}", functools.partial(ref, slot), functools.partial(ref, slot), tp=other)
        cq_ref = lambda g=g: cq_buf.at[odd, pl.ds(g * per, per)]
        wire.add(f"q{g}S", cq_ref, cq_ref, tp=other)

    def cut(side, low, high, unit, mine):
        half_size = (high - low) // 2
        which = flip[side] if mine else 1 - flip[side]
        return pl.ds(pl.multiple_of(low + which * half_size, unit), half_size)

    q_cut = head * 2 // 3
    o_cut = wo_hbm.shape[0] // 2
    pieces = {
        "wq.a": (lambda r: wq_hbm.at[:, r], lambda place, r: wq.at[pl.ds(place * heads, heads), r], ("a", 0, q_cut, 16)),
        "wq.b": (lambda r: wq_hbm.at[:, r], lambda place, r: wq.at[pl.ds(place * heads, heads), r], ("b", q_cut, head, 16)),
        "wk.a": (lambda r: wk_hbm.at[:, :, r], lambda place, r: wkv.at[pl.ds(place * heads, heads), pl.ds(0, nope), r], ("a", 0, rank, BLOCK)),
        "wv.b": (lambda r: wv_hbm.at[:, :, r], lambda place, r: wkv.at[pl.ds(place * heads, heads), pl.ds(nope, nope), r], ("b", 0, rank, BLOCK)),
        "wo.a": (lambda r: wo_hbm.at[r], lambda place, r: wo_out.at[odd, place, r], ("a", 0, o_cut, 16)),
        "wo.b": (lambda r: wo_hbm.at[r], lambda place, r: wo_out.at[odd, place, r], ("b", o_cut, 2 * o_cut, 16)),
    }
    for piece, (source, target, bounds) in pieces.items():
        side = bounds[0]
        via = "split" if piece.startswith("wo") else "right"
        for mine in (True,) if paired[side] else (True, False):
            here = lambda place, source=source, bounds=bounds, mine=mine: source(cut(*bounds, mine))
            there = lambda place, target=target, bounds=bounds, mine=mine: target(place, cut(*bounds, mine))
            chain(piece + ("" if mine else "~"), here, there, (1, 2, 3), via)
        if paired[side]:
            for place in (1, 2, 3):
                ref = lambda place=place, target=target, bounds=bounds: target(place, cut(*bounds, True))
                wire.add(f"{piece}X{place}", ref, ref, dp=partner[side])
    for place in range(slots):
        ref = lambda place=place: wo_out.at[odd, place]
        wire.add(f"woS{place}", ref if place else lambda: wo_hbm, ref, tp=other)
    for quad in range(quads):
        wire.add(f"o{quad}S", lambda quad=quad: o_send.at[quad], lambda quad=quad: o_out.at[odd, quad], tp=other)

    small = ("wk.a", "wv.b", "wq.a", "wq.b")

    def ring(which, *kinds):
        return [f"{kind}{half_name}{way}" for kind in kinds for half_name in ("", "~")[: 1 if paired[kind[-1]] else 2] for way in which]

    def across(place, *kinds):
        return [f"{kind}X{place}" for kind in kinds if paired[kind[-1]]]

    def norm(g):
        for r in range(per):
            for at in range(0, toks, NORM_ROWS):
                x = x_buf[g * per + r, at : at + NORM_ROWS].astype(F32)
                a_buf[g, r * toks + at : r * toks + at + NORM_ROWS] = (unit(x) * g1_ref[...]).astype(BF16)

    def latent(g):
        kv = dot_t(a_buf[g], wdkv[...])
        rows[g * per : (g + 1) * per, spot(0, odd), :] = (unit(kv[:, :rank]) * gkv_ref[...]).astype(BF16).reshape(per, toks, rank)
        turned = []
        for s in range(per):
            cos_pair, sin_pair = cos_ref[g * per + s], sin_ref[g * per + s]
            cos = jnp.where(odd == 1, cos_pair[:, toks:], cos_pair[:, :toks])
            sin = jnp.where(odd == 1, sin_pair[:, toks:], sin_pair[:, :toks])
            table = jnp.concatenate([cos, cos, -sin, sin], axis=0).T
            p = kv[s * toks : (s + 1) * toks, rank:]
            swapped = jnp.concatenate([p[:, half:], p[:, :half]], axis=1)
            turned.append(p * table[:, :rope] + swapped * table[:, rope:])
        rot[g, spot(0, odd), :] = jnp.concatenate(turned, axis=1).astype(BF16)

    def queries(g):
        h = jnp.concatenate([dot(a_buf[g], wdq[:, : 2 * rank]), dot(a_buf[g], wdq[:, 2 * rank :])], axis=1)
        cq_buf[odd, g * per : (g + 1) * per] = (unit(h) * gq_ref[...]).astype(BF16).reshape(per, toks, q_rank)

    with jax.named_scope('p_norm0'):
        loads["x0"].wait()
        norm(0)
        pl.semaphore_wait(barrier, 3 + paired["a"] + paired["b"])
    wire.start(*ring("R", "wk.a", "wv.b"))
    with jax.named_scope('p_kv'):
        for name in ("wdkv", "cos", "sin"):
            loads[name].wait()
        for g in range(groups):
            if g + 1 < groups:
                loads[f"x{g + 1}"].wait()
                norm(g + 1)
            latent(g)
            for way in ("R", "L", "S0"):
                wire.start(f"c{g}{way}", f"p{g}{way}")
    wire.start(*ring("R", "wq.a", "wq.b"))

    def hand_on(g):
        wire.landed(f"c{g}L", f"p{g}L", f"c{g}R", f"p{g}R")
        wire.start(f"c{g}O", f"p{g}O", f"c{g}S3", f"p{g}S3", f"c{g}S1", f"p{g}S1")

    with jax.named_scope('p_cq'):
        loads["wdq"].wait()
        for g in range(groups):
            queries(g)
            wire.start(f"q{g}S")
            hand_on(g)
    wire.start(*ring("L", *small, "wo.b", "wo.a"), "woS0")
    wire.landed(*ring("R", "wk.a", "wv.b"))
    wire.start(*across(1, "wk.a", "wv.b"), *ring("O", "wk.a", "wv.b"))

    loads["pe"].wait()
    for g in range(groups):
        old = pe_buf[g * per : (g + 1) * per].reshape(per * rope, prefix).astype(F32)
        for b in range(prefix // BLOCK):
            rot[g, b * BLOCK : (b + 1) * BLOCK] = old[:, b * BLOCK : (b + 1) * BLOCK].T.astype(BF16)
    qb[...] = jnp.zeros_like(qb)

    def rest_of(g):
        wire.landed(f"c{g}O", f"p{g}O")
        wire.start(f"c{g}S2", f"p{g}S2")
        for slot in (0, 1, 3, 2):
            wire.landed(f"c{g}S{slot}", f"p{g}S{slot}")
        wire.landed(f"q{g}S")

    with jax.named_scope('p_rest0'):
        for name in ("wk", "wv", "wq", "lat"):
            loads[name].wait()
        rest_of(0)

    row = lax.broadcasted_iota(jnp.int32, (BLOCK, wide), 0)
    lane = lax.rem(lax.broadcasted_iota(jnp.int32, (BLOCK, wide), 1), BLOCK)
    near = row <= lane

    def place(n):
        return n // duos, lax.rem(n, duos)

    def query_dot(n):
        quad, duo = place(n)
        w = wq[pl.ds(quad * 4, 4)].reshape(4 * head, q_rank)
        cq = jnp.concatenate([cq_buf[parity, 2 * duo + u] for u in range(2) for parity in range(2)], axis=0)
        q_raw[...] = dot_t(w, cq)

    def query_stage(n):
        quad, duo = place(n)
        raw = q_raw
        for u in range(2):
            slot = 2 * lax.rem(duo, 2) + u
            cos, sin = cos_ref[2 * duo + u], sin_ref[2 * duo + u]
            for h in range(4):
                pair, side = h // 2, h % 2
                q = raw[h * head : (h + 1) * head, u * BLOCK : (u + 1) * BLOCK]
                cols = slice(side * BLOCK, (side + 1) * BLOCK)
                qb[u, pair, side * nope : (side + 1) * nope, cols] = q[:nope].astype(BF16)
                lo, hi = q[nope : nope + half], q[nope + half :]
                turned = jnp.concatenate([lo * cos - hi * sin, hi * cos + lo * sin], axis=0).astype(BF16)
                start = pl.multiple_of(BLOCK + slot * rope, rope)
                stale = pl.multiple_of(BLOCK + lax.rem(slot + 2, 4) * rope, rope)
                qb[u, pair, pl.ds(start, rope), cols] = turned
                qb[u, pair, pl.ds(stale, rope), cols] = jnp.zeros_like(turned)

    def key_stage(n, t, u):
        quad, duo = place(n)
        w = wkv[pl.ds(quad * 4, 4), :nope].reshape(4 * nope, rank)
        kb[u][:t] = dot_t(rows[2 * duo + u, :t], w).astype(BF16)

    def value_stage(n, t, u):
        quad, duo = place(n)
        w = wkv[pl.ds(quad * 4, 4), nope:].reshape(4 * nope, rank)
        vb[u][:, :t] = dot_t(w, rows[2 * duo + u, :t]).astype(BF16)

    def score_stage(n, t, u, pair):
        _, duo = place(n)
        length = len_ref[2 * duo + u]
        keys = jnp.concatenate([kb[u][:t, pair * BLOCK : (pair + 1) * BLOCK], rot[duo // 2, :t]], axis=1)
        value = dot(keys, qb[u, pair])
        most = None
        for b in range(t // BLOCK):
            part = value[b * BLOCK : (b + 1) * BLOCK]
            if BLOCK <= b * BLOCK < prefix:
                part = jnp.where(row < length - b * BLOCK, part, NEVER)
            if b * BLOCK == prefix:
                part = jnp.where(near, part, NEVER)
            sb[2 * u + pair][b * BLOCK : (b + 1) * BLOCK] = part
            part = jnp.max(part.reshape(BLOCK // 8, 8, wide), axis=0)
            most = part if most is None else jnp.maximum(most, part)
        mb[2 * u + pair] = jnp.broadcast_to(jnp.max(most, axis=0, keepdims=True), (8, wide))

    def soft_stage(t, u, pair):
        i = 2 * u + pair
        most = mb[i, :1]
        total = None
        for b in range(t // BLOCK):
            x = jnp.exp2((sb[i][b * BLOCK : (b + 1) * BLOCK] - most) * factor)
            part = jnp.sum(x.reshape(BLOCK // 8, 8, wide), axis=0)
            total = part if total is None else total + part
            pb[i][b * BLOCK : (b + 1) * BLOCK] = x.astype(BF16)
        lb[i] = total

    def mix_stage(n, t, u, pair):
        quad, duo = place(n)
        i = 2 * u + pair
        inv = 1.0 / jnp.sum(lb[i], axis=0, keepdims=True)
        o = dot(vb[u][pair * BLOCK : (pair + 1) * BLOCK, :t], pb[i][:t]) * inv
        o = jnp.concatenate([o[:nope, :BLOCK], o[nope:, BLOCK:]], axis=0).T.astype(BF16)
        first, second = o[:toks], o[toks:]
        cols = slice(pair * BLOCK, (pair + 1) * BLOCK)
        o_own[quad, 2 * duo + u, :, cols] = jnp.where(odd == 1, second, first)
        o_send[quad, 2 * duo + u, :, cols] = jnp.where(odd == 1, first, second)

    units = [(u, pair) for u in range(2) for pair in range(2)]
    total = quads * duos

    def each_chip(fn):
        for c in range(slots):
            pl.when(chip == c)(lambda c=c: fn(prefix + (c + 1) * BLOCK))

    def body(b, t):
        before, ahead, later = jnp.maximum(b - 1, 0), jnp.minimum(b + 1, total - 1), jnp.minimum(b + 2, total - 1)
        mix_stage(before, t, 0, 0)
        soft_stage(t, 0, 0)
        score_stage(ahead, t, 0, 0)
        mix_stage(before, t, 0, 1)
        value_stage(b, t, 0)
        soft_stage(t, 0, 1)
        score_stage(ahead, t, 0, 1)
        mix_stage(before, t, 1, 0)
        mix_stage(before, t, 1, 1)
        key_stage(later, t, 0)
        soft_stage(t, 1, 0)
        score_stage(ahead, t, 1, 0)
        value_stage(b, t, 1)
        soft_stage(t, 1, 1)
        score_stage(ahead, t, 1, 1)
        key_stage(later, t, 1)
        query_dot(later)
        query_stage(later)

    def at(b, when):
        return pl.when(b == when)

    agenda = [
        (0, None, ring("R", "wq.a"), across(1, "wq.a") + ring("O", "wq.a")),
        (1, None, ring("R", "wq.b"), across(1, "wq.b") + ring("O", "wq.b") + ring("R", "wo.a", "wo.b")),
        (2, None, ring("L", "wk.a", "wv.b"), across(2, "wk.a", "wv.b")),
        (4, None, across(1, *small), []),
        (5, None, ring("L", "wq.a"), across(2, "wq.a")),
        (5, None, ring("O", "wk.a", "wq.a"), across(3, "wk.a", "wq.a")),
        (6, None, ring("L", "wq.b"), across(2, "wq.b")),
        (6, None, ring("O", "wv.b", "wq.b"), across(3, "wv.b", "wq.b")),
        (10, None, across(2, *small), []),
        (12, None, ring("R", "wo.a"), across(1, "wo.a")),
        (12, None, ring("L", "wo.b"), across(2, "wo.b")),
        (12, 0, [], ring("O", "wo.a")),
        (12, 1, [], ring("O", "wo.b")),
        (15, None, across(3, *small), []),
        (17, None, ring("L", "wo.a"), across(2, "wo.a")),
        (17, None, ring("R", "wo.b"), across(1, "wo.b")),
        (17, 0, [], ring("O", "wo.b")),
        (17, 1, [], ring("O", "wo.a")),
        (19, 0, ring("O", "wo.a"), across(3, "wo.a")),
        (19, 1, ring("O", "wo.b"), across(3, "wo.b")),
        (22, 0, ring("O", "wo.b"), across(3, "wo.b")),
        (22, 1, ring("O", "wo.a"), across(3, "wo.a")),
        (24, None, across(1, "wo.a", "wo.b") + across(2, "wo.a", "wo.b"), ["woS1", "woS2"]),
        (29, None, across(3, "wo.a", "wo.b"), ["woS3"]),
    ]

    def step(b, _):
        @at(b, 0)
        def _():
            with jax.named_scope('ev_k1'):
                rest_of(1)

        @at(b, 2)
        def _():
            with jax.named_scope('ev_k2'):
                rest_of(2)
            pltpu.make_async_copy(rows.at[:, pl.ds(prefix, chunk)], c_out, load_sem.at[0]).start()
            pltpu.make_async_copy(rot.at[:, pl.ds(prefix, chunk)], p_out, load_sem.at[1]).start()

        for when, parity, waits, starts in agenda:

            @at(b, when)
            def _():
                if parity is None:
                    with jax.named_scope(f"ev_{when}"):
                        wire.landed(*waits)
                    wire.start(*starts)
                else:

                    @pl.when(odd == parity)
                    def _():
                        with jax.named_scope(f"ev_{when}p{parity}"):
                            wire.landed(*waits)
                        wire.start(*starts)

        bounce = pltpu.make_async_copy(wo_hbm, wo_buf, load_sem.at[3])

        @at(b, 1)
        def _():
            bounce.start()

        @at(b, 5)
        def _():
            bounce.wait()
            pltpu.make_async_copy(wo_buf, wo_out.at[odd, 0], load_sem.at[4]).start()

        for quad in range(quads - 1):
            at(b, (quad + 1) * duos + 1)(functools.partial(wire.start, f"o{quad}S"))

        with jax.named_scope('body'):
            each_chip(functools.partial(body, b))
        return 0

    def lead_in(t):
        for u in range(2):
            key_stage(0, t, u)
        query_dot(0)
        query_stage(0)

    def second(t):
        for u, pair in units:
            score_stage(0, t, u, pair)
        for u in range(2):
            key_stage(1, t, u)
        query_dot(1)
        query_stage(1)

    with jax.named_scope('p_lead'):
        each_chip(lead_in)
        each_chip(second)
    lax.fori_loop(0, total, step, 0)

    def last(t):
        for u, pair in units:
            mix_stage(total - 1, t, u, pair)

    with jax.named_scope('p_last'):
        each_chip(last)
        wire.start(f"o{quads - 1}S")
        pltpu.make_async_copy(o_own, o_out.at[odd], load_sem.at[2]).start()
    with jax.named_scope('f_land'):
        for place in range(slots):
            wire.landed(f"woS{place}")
        for quad in range(quads):
            wire.landed(f"o{quad}S")
    with jax.named_scope('f_sent'):
        wire.sent(*wire.index)
        pltpu.make_async_copy(rows.at[:, pl.ds(prefix, chunk)], c_out, load_sem.at[0]).wait()
        pltpu.make_async_copy(rot.at[:, pl.ds(prefix, chunk)], p_out, load_sem.at[1]).wait()
        pltpu.make_async_copy(o_own, o_out.at[odd], load_sem.at[2]).wait()
        pltpu.make_async_copy(wo_buf, wo_out.at[odd, 0], load_sem.at[4]).wait()


def finish_kernel(
    len_ref, o_hbm, w_hbm, x_hbm, c_hbm, p_hbm, lat_hbm, pe_hbm, y_hbm, lat_out, pe_out, fresh, acc, x_buf, y_buf, o_buf, w_buf, c_buf, p_buf, lat_buf, pe_buf, lat_new, pe_new, load_sem, store_sem, sems
):
    chip = lax.axis_index("tp") // 2
    quads, seqs, toks, depth = o_hbm.shape[1:]
    terms = 2 * quads
    slots = c_hbm.shape[1]
    rank = lat_hbm.shape[2]
    rope, cache_len = pe_hbm.shape[1:]
    chunk = slots * 2 * toks
    words = rank // BLOCK
    dim = x_hbm.shape[2]
    part = 2 * depth
    ring = w_buf.shape[0]

    def loads(k, with_term):
        slot = lax.rem(k, ring)
        out = [
            pltpu.make_async_copy(c_hbm.at[k], c_buf.at[slot], load_sem.at[0, slot]),
            pltpu.make_async_copy(lat_hbm.at[k], lat_buf.at[slot], load_sem.at[1, slot]),
        ]
        if with_term:
            side, quad = k // quads, lax.rem(k, quads)
            out.append(pltpu.make_async_copy(o_hbm.at[side, quad], o_buf.at[slot], load_sem.at[2, slot]))
            out.append(pltpu.make_async_copy(w_hbm.at[side, pl.ds(pl.multiple_of(quad * depth, depth), depth)], w_buf.at[slot], load_sem.at[3, slot]))
        return out

    def store(k):
        slot = lax.rem(k, ring)
        return pltpu.make_async_copy(lat_new.at[slot], lat_out.at[k], store_sem.at[slot])

    load_x = pltpu.make_async_copy(x_hbm, x_buf, sems.at[0])
    load_p = pltpu.make_async_copy(p_hbm, p_buf, sems.at[1])
    load_pe = pltpu.make_async_copy(pe_hbm, pe_buf, sems.at[2])
    store_y = pltpu.make_async_copy(y_buf, y_hbm, sems.at[3])
    store_pe = pltpu.make_async_copy(pe_new, pe_out, sems.at[4])

    def slot_of(j):
        return lax.rem(chip - j + slots, slots)

    def project(k, kind):
        slot = lax.rem(k, ring)
        o = o_buf[slot].reshape(seqs * toks, depth)
        for n in range(0, dim, part):
            cols = slice(n, n + part)
            y = dot(o, w_buf[slot, :, cols])
            if kind != "first":
                y = acc[:, cols] + y
            if kind == "last":
                y = y + x_buf[:, :, cols].reshape(seqs * toks, part).astype(F32)
                y_buf[:, :, cols] = y.astype(BF16).reshape(seqs, toks, part)
            else:
                acc[:, cols] = y

    def cache(k):
        at_slot = lax.rem(k, ring)
        length = len_ref[k]
        for j in range(slots):
            piece = c_buf[at_slot, slot_of(j)].reshape(2 * toks, rank).astype(F32)
            for w in range(words):
                fresh[w, BLOCK + j * 2 * toks : BLOCK + (j + 1) * 2 * toks] = piece[:, w * BLOCK : (w + 1) * BLOCK]
        lat_new[at_slot] = lat_buf[at_slot]
        base = (length // 16) * 16
        skew = length - base
        tile_row = lax.broadcasted_iota(jnp.int32, (16, BLOCK), 0)
        for i in range(chunk // 16 + 1):
            at = pl.multiple_of(jnp.minimum(base + i * 16, cache_len - 16), 16)
            for w in range(words):
                cols = slice(w * BLOCK, (w + 1) * BLOCK)
                moved = fresh[w, pl.ds(BLOCK - skew + i * 16, 16), :].astype(BF16)
                if i == 0 or i == chunk // 16:
                    local = tile_row + (at - length)
                    shown = (local >= 0) & (local < chunk) if i == 0 else (local < chunk)
                    if i == 0:
                        rest = lat_buf[at_slot, pl.ds(at, 16), cols]
                    else:
                        shown = shown & (skew > 0)
                        rest = lat_new[at_slot, pl.ds(at, 16), cols]
                    moved = jnp.where(shown, moved.astype(F32), rest.astype(F32)).astype(BF16)
                lat_new[at_slot, pl.ds(at, 16), cols] = moved

        turned = jnp.concatenate([p_buf[k // (BLOCK // rope), slot_of(j)].reshape(2 * toks, BLOCK).astype(F32).T for j in range(slots)], axis=1)
        group = lax.rem(k, BLOCK // rope)
        mine = turned[:rope]
        for g in range(1, BLOCK // rope):
            mine = jnp.where(group == g, turned[g * rope : (g + 1) * rope], mine)
        mine = jnp.concatenate([mine, jnp.zeros((rope, cache_len - chunk), F32)], axis=1)
        mine = pltpu.roll(mine, length, axis=1)
        spot = lax.broadcasted_iota(jnp.int32, (rope, cache_len), 1) - length
        pe_new[k] = jnp.where((spot >= 0) & (spot < chunk), mine, pe_buf[k].astype(F32)).astype(BF16)

    def begin(k, with_term):
        for load in loads(k, with_term):
            load.start()

    def arrived(k, with_term):
        for load in loads(k, with_term):
            load.wait()

    def work(k, kind):
        if kind != "none":
            project(k, kind)
        cache(k)
        store(k).start()

    def more(k):
        pl.when(k < terms)(lambda: begin(k, True))
        pl.when((k >= terms) & (k < seqs))(lambda: begin(k, False))

    begin(0, True)
    load_p.start()
    load_pe.start()
    begin(1, True)
    begin(2, True)
    load_x.start()
    load_p.wait()
    load_pe.wait()
    arrived(0, True)
    more(ring - 1)
    with jax.named_scope('g_first'):
        work(0, "first")

    def middle(k, _):
        with jax.named_scope('g_wait'):
            arrived(k, True)
        more(k + ring - 1)

        @pl.when(k >= ring)
        def _():
            store(k - ring).wait()

        with jax.named_scope('g_work'):
            work(k, "middle")
        return 0

    lax.fori_loop(1, terms - 1, middle, 0)
    last = terms - 1
    arrived(last, True)
    more(last + ring - 1)
    store(last - ring).wait()
    load_x.wait()
    with jax.named_scope('g_last'):
        work(last, "last")
    store_y.start()

    def tail(k, _):
        arrived(k, False)
        store(k - ring).wait()
        with jax.named_scope('g_tail'):
            work(k, "none")
        return 0

    lax.fori_loop(terms, seqs, tail, 0)
    store_pe.start()
    for k in range(ring):
        store(seqs - ring + k).wait()
    store_pe.wait()
    store_y.wait()


def solution(mesh):
    size = mesh.shape["tp"]
    count = mesh.shape["dp"]
    stride = 2 ** (count.bit_length() // 2)
    paired = {"a": count % 2 == 0, "b": count % (2 * stride) == 0}

    def local_step(hidden, lengths, rope_cos, rope_sin, cache_lat, cache_pe, norm_in, w_dq, norm_q, w_dkv, norm_kv, w_uq, w_uk, w_uv, w_out):
        seqs, toks, dim = hidden.shape
        q_rank = w_dq.shape[1]
        rank, heads, nope = w_uk.shape
        rope = cache_pe.shape[2]
        cache_len = cache_lat.shape[1]
        slots = size // 2
        head = nope + rope
        quads = slots * heads // 4
        chunk = size * toks
        prefix = cache_len - chunk
        per = BLOCK // rope
        groups = seqs // per
        wide = 2 * BLOCK
        cos_t, sin_t = rope_cos.transpose(0, 2, 1), rope_sin.transpose(0, 2, 1)
        pe_t = cache_pe.transpose(0, 2, 1)
        wdkv_t = w_dkv.transpose(1, 0)
        wq_t, wk_t, wv_t = (w.transpose(1, 2, 0) for w in (w_uq, w_uk, w_uv))

        any_spec = pl.BlockSpec(memory_space=pl.ANY)
        vmem_spec = pl.BlockSpec(memory_space=pltpu.VMEM)
        smem_spec = pl.BlockSpec(memory_space=pltpu.SMEM)
        c_all, p_all, o_all, wo_all = pl.pallas_call(
            functools.partial(main_kernel, (size, stride, paired)),
            in_specs=[smem_spec, any_spec, vmem_spec, any_spec, vmem_spec, any_spec, vmem_spec] + [any_spec] * 8,
            out_specs=[any_spec] * 4,
            out_shape=[
                jax.ShapeDtypeStruct((seqs, chunk, rank), BF16),
                jax.ShapeDtypeStruct((groups, chunk, BLOCK), BF16),
                jax.ShapeDtypeStruct((2, quads, seqs, toks, 4 * nope), BF16),
                jax.ShapeDtypeStruct((2, slots) + w_out.shape, BF16),
            ],
            scratch_shapes=[
                pltpu.VMEM(hidden.shape, BF16),
                pltpu.VMEM(w_dq.shape, BF16),
                pltpu.VMEM(wdkv_t.shape, BF16),
                pltpu.VMEM((groups, per * toks, dim), BF16),
                pltpu.VMEM((seqs, cache_len, rank), BF16),
                pltpu.VMEM((groups, cache_len, BLOCK), BF16),
                pltpu.VMEM((seqs, rope, prefix), BF16),
                pltpu.VMEM((seqs, rope // 2, BLOCK), F32),
                pltpu.VMEM((seqs, rope // 2, BLOCK), F32),
                pltpu.VMEM((2, seqs, toks, q_rank), BF16),
                pltpu.VMEM((slots * heads, head, q_rank), BF16),
                pltpu.VMEM((slots * heads, 2 * nope, rank), BF16),
                [pltpu.VMEM((cache_len, 4 * nope), BF16) for _ in range(2)],
                [pltpu.VMEM((4 * nope, cache_len), BF16) for _ in range(2)],
                pltpu.VMEM((2, 2, wide, wide), BF16),
                pltpu.VMEM((4 * head, wide), F32),
                [pltpu.VMEM((cache_len, wide), F32) for _ in range(4)],
                pltpu.VMEM((4, 8, wide), F32),
                [pltpu.VMEM((cache_len, wide), BF16) for _ in range(4)],
                pltpu.VMEM((4, 8, wide), F32),
                pltpu.VMEM((quads, seqs, toks, 4 * nope), BF16),
                pltpu.VMEM((quads, seqs, toks, 4 * nope), BF16),
                pltpu.VMEM(w_out.shape, BF16),
                pltpu.SemaphoreType.DMA((10 + groups,)),
                pltpu.SemaphoreType.DMA((128,)),
                pltpu.SemaphoreType.DMA((128,)),
            ],
            compiler_params=pltpu.CompilerParams(collective_id=0, has_side_effects=True, vmem_limit_bytes=63 * MIB),
            cost_estimate=pl.CostEstimate(flops=70 * 10**9, bytes_accessed=40 * MIB, transcendentals=30 * 10**6),
            name="main",
        )(lengths, hidden, norm_in, w_dq, norm_q, wdkv_t, norm_kv, cos_t, sin_t, wq_t, wk_t, wv_t, w_out, cache_lat, pe_t)

        depth = 4 * nope
        ahead = 4
        y, lat_new, pe_new = pl.pallas_call(
            finish_kernel,
            in_specs=[smem_spec] + [any_spec] * 7,
            out_specs=[any_spec] * 3,
            scratch_shapes=[
                pltpu.VMEM((rank // BLOCK, chunk + 2 * BLOCK, BLOCK), F32),
                pltpu.VMEM((seqs * toks, dim), F32),
                pltpu.VMEM(hidden.shape, BF16),
                pltpu.VMEM(hidden.shape, BF16),
                pltpu.VMEM((ahead, seqs, toks, depth), BF16),
                pltpu.VMEM((ahead, depth, dim), BF16),
                pltpu.VMEM((ahead, slots, 2, toks, rank), BF16),
                pltpu.VMEM((groups, slots, 2, toks, BLOCK), BF16),
                pltpu.VMEM((ahead, cache_len, rank), BF16),
                pltpu.VMEM(pe_t.shape, BF16),
                pltpu.VMEM((ahead, cache_len, rank), BF16),
                pltpu.VMEM(pe_t.shape, BF16),
                pltpu.SemaphoreType.DMA((4, ahead)),
                pltpu.SemaphoreType.DMA((ahead,)),
                pltpu.SemaphoreType.DMA((5,)),
            ],
            out_shape=[
                jax.ShapeDtypeStruct(hidden.shape, BF16),
                jax.ShapeDtypeStruct(cache_lat.shape, BF16),
                jax.ShapeDtypeStruct(pe_t.shape, BF16),
            ],
            compiler_params=pltpu.CompilerParams(vmem_limit_bytes=63 * MIB),
            cost_estimate=pl.CostEstimate(flops=2 * seqs * toks * dim * dim, bytes_accessed=50 * MIB, transcendentals=0),
            name="finish",
        )(
            lengths,
            o_all,
            wo_all.reshape(2, slots * w_out.shape[0], dim),
            hidden,
            c_all.reshape(seqs, slots, 2, toks, rank),
            p_all.reshape(groups, slots, 2, toks, BLOCK),
            cache_lat,
            pe_t,
        )
        return y, lat_new, pe_new.transpose(0, 2, 1)

    spec_tok = P("dp", "tp", None)
    spec_len = P("dp")
    spec_seq = P("dp", None, None)
    spec_vec = P(None)
    spec_mat = P(None, None)
    spec_head = P(None, "tp", None)
    spec_rows = P("tp", None)
    in_specs = (spec_tok, spec_len, spec_seq, spec_seq, spec_seq, spec_seq, spec_vec, spec_mat, spec_vec, spec_mat, spec_vec, spec_head, spec_head, spec_head, spec_rows)
    return jax.shard_map(local_step, mesh=mesh, in_specs=in_specs, out_specs=(spec_tok, spec_seq, spec_seq), check_vma=False)
```

```python
import functools

import jax
import jax.numpy as jnp
from jax import lax
from jax.experimental import pallas as pl
from jax.experimental.pallas import tpu as pltpu
from jax.sharding import PartitionSpec as P

BLOCK = 128
LOG2E = 1.4426950408889634
NEVER = -1e30
NORM_ROWS = 16
F32 = jnp.float32
BF16 = jnp.bfloat16
MESH = pl.DeviceIdType.MESH
MIB = 2**20


def dot(a, b):
    return lax.dot_general(a, b, (((1,), (0,)), ((), ())), preferred_element_type=F32)


def dot_t(a, b):
    return lax.dot_general(a, b, (((1,), (1,)), ((), ())), preferred_element_type=F32)


def unit(x):
    return x * lax.rsqrt(jnp.mean(x * x, axis=-1, keepdims=True) + 1e-6)


class Wire:
    def __init__(self, send_sem, recv_sem):
        self.sems = (send_sem, recv_sem)
        self.made = {}
        self.index = {}

    def add(self, name, src, dst, **peer):
        self.index[name] = len(self.index)
        self.made[name] = lambda: pltpu.make_async_remote_copy(
            src(), dst(), self.sems[0].at[self.index[name]], self.sems[1].at[self.index[name]], device_id=peer, device_id_type=MESH
        )

    def start(self, *names):
        for name in names:
            self.made[name]().start()

    def landed(self, *names):
        for name in names:
            self.made[name]().wait_recv()

    def sent(self, *names):
        for name in names:
            self.made[name]().wait_send()


def main_kernel(
    plan,
    len_ref,
    x_hbm,
    g1_ref,
    wdq_hbm,
    gq_ref,
    wdkv_hbm,
    gkv_ref,
    cos_hbm,
    sin_hbm,
    wq_hbm,
    wk_hbm,
    wv_hbm,
    wo_hbm,
    lat_hbm,
    pe_hbm,
    c_out,
    p_out,
    o_out,
    wo_out,
    x_buf,
    wdq,
    wdkv,
    a_buf,
    rows,
    rot,
    pe_buf,
    cos_ref,
    sin_ref,
    cq_buf,
    wq,
    wkv,
    kb,
    vb,
    qb,
    q_raw,
    sb,
    mb,
    pb,
    lb,
    o_own,
    o_send,
    wo_buf,
    load_sem,
    send_sem,
    recv_sem,
):
    size, stride, paired = plan
    me = lax.axis_index("tp")
    odd = lax.rem(me, 2)
    chip = me // 2
    right, left = lax.rem(me + 2, size), lax.rem(me + size - 2, size)
    onward = jnp.where(odd == 0, right, left)
    other = me + 1 - 2 * odd
    dp = lax.axis_index("dp")
    flip = {"a": lax.rem(dp, 2), "b": lax.rem(dp // stride, 2)}
    partner = {"a": dp + 1 - 2 * flip["a"], "b": dp + stride * (1 - 2 * flip["b"])}

    seqs, toks, dim = x_hbm.shape
    groups = rot.shape[0]
    per = seqs // groups
    rank = rows.shape[2]
    slots = size // 2
    chunk = size * toks
    prefix = rows.shape[1] - chunk
    heads = wq.shape[0] // slots
    head, q_rank = wq.shape[1:]
    rope = BLOCK // per
    half = rope // 2
    nope = head - rope
    quads = wq.shape[0] // 4
    duos = seqs // 2
    wide = 2 * BLOCK
    factor = LOG2E * head**-0.5

    loads = {}

    def load(name, src, dst):
        loads[name] = pltpu.make_async_copy(src, dst, load_sem.at[len(loads)])
        loads[name].start()

    def spot(slot, parity):
        return pl.ds(pl.multiple_of(prefix + slot * BLOCK + parity * toks, toks), toks)

    barrier = pltpu.get_barrier_semaphore()
    for peer in (left, right, other):
        pl.semaphore_signal(barrier, inc=1, device_id={"tp": peer}, device_id_type=MESH)
    for side in "ab":
        if paired[side]:
            pl.semaphore_signal(barrier, inc=1, device_id={"dp": partner[side]}, device_id_type=MESH)

    lanes_chip = pl.ds(pl.multiple_of(chip * BLOCK, BLOCK), BLOCK)
    def load_x(g):
        load(f"x{g}", x_hbm.at[pl.ds(g * per, per)], x_buf.at[pl.ds(g * per, per)])

    load_x(0)
    load("wdkv", wdkv_hbm, wdkv)
    load("cos", cos_hbm.at[:, :, lanes_chip], cos_ref)
    load("sin", sin_hbm.at[:, :, lanes_chip], sin_ref)

    wire = Wire(send_sem, recv_sem)

    def chain(name, here, there, places, via="split"):
        near_left, near_right, opposite = places
        handed = {"right": near_left, "left": near_right, "split": jnp.where(odd == 0, near_left, near_right)}[via]
        wire.add(name + "R", lambda: here(0), lambda: there(near_left), tp=right)
        wire.add(name + "L", lambda: here(0), lambda: there(near_right), tp=left)
        wire.add(name + "O", lambda: there(handed), lambda: there(opposite), tp={"right": right, "left": left, "split": onward}[via])

    for g in range(groups):
        for name, ref in (("c", lambda slot, g=g: rows.at[pl.ds(g * per, per), spot(slot, odd)]), ("p", lambda slot, g=g: rot.at[g, spot(slot, odd)])):
            name = f"{name}{g}"
            chain(name, ref, ref, (1, 3, 2), "left")
            for slot in range(slots):
                wire.add(f"{name}S{slot}", functools.partial(ref, slot), functools.partial(ref, slot), tp=other)
        cq_ref = lambda g=g: cq_buf.at[odd, pl.ds(g * per, per)]
        wire.add(f"q{g}S", cq_ref, cq_ref, tp=other)

    def cut(side, low, high, unit, mine):
        half_size = (high - low) // 2
        which = flip[side] if mine else 1 - flip[side]
        return pl.ds(pl.multiple_of(low + which * half_size, unit), half_size)

    q_cut = head * 2 // 3
    o_cut = wo_hbm.shape[0] // 2
    pieces = {
        "wq.a": (lambda r: wq_hbm.at[:, r], lambda place, r: wq.at[pl.ds(place * heads, heads), r], ("a", 0, q_cut, 16)),
        "wq.b": (lambda r: wq_hbm.at[:, r], lambda place, r: wq.at[pl.ds(place * heads, heads), r], ("b", q_cut, head, 16)),
        "wk.a": (lambda r: wk_hbm.at[:, :, r], lambda place, r: wkv.at[pl.ds(place * heads, heads), pl.ds(0, nope), r], ("a", 0, rank, BLOCK)),
        "wv.b": (lambda r: wv_hbm.at[:, :, r], lambda place, r: wkv.at[pl.ds(place * heads, heads), pl.ds(nope, nope), r], ("b", 0, rank, BLOCK)),
        "wo.a": (lambda r: wo_hbm.at[r], lambda place, r: wo_out.at[odd, place, r], ("a", 0, o_cut, 16)),
        "wo.b": (lambda r: wo_hbm.at[r], lambda place, r: wo_out.at[odd, place, r], ("b", o_cut, 2 * o_cut, 16)),
    }
    for piece, (source, target, bounds) in pieces.items():
        side = bounds[0]
        via = "split" if piece.startswith("wo") else "right"
        for mine in (True,) if paired[side] else (True, False):
            here = lambda place, source=source, bounds=bounds, mine=mine: source(cut(*bounds, mine))
            there = lambda place, target=target, bounds=bounds, mine=mine: target(place, cut(*bounds, mine))
            chain(piece + ("" if mine else "~"), here, there, (1, 2, 3), via)
        if paired[side]:
            for place in (1, 2, 3):
                ref = lambda place=place, target=target, bounds=bounds: target(place, cut(*bounds, True))
                wire.add(f"{piece}X{place}", ref, ref, dp=partner[side])
    for place in range(slots - 1):
        ref = lambda place=place: wo_out.at[odd, place]
        wire.add(f"woS{place}", ref if place else lambda: wo_hbm, ref, tp=other)
    for piece in ("wo.a", "wo.b"):
        for mine in (True, False):
            ref = lambda piece=piece, mine=mine: pieces[piece][1](slots - 1, cut(*pieces[piece][2], mine))
            wire.add(f"{piece}S" + ("" if mine else "~"), ref, ref, tp=other)
    for quad in range(quads):
        wire.add(f"o{quad}S", lambda quad=quad: o_send.at[quad], lambda quad=quad: o_out.at[odd, quad], tp=other)

    small = ("wk.a", "wv.b", "wq.a", "wq.b")

    def ring(which, *kinds):
        return [f"{kind}{half_name}{way}" for kind in kinds for half_name in ("", "~")[: 1 if paired[kind[-1]] else 2] for way in which]

    def across(place, *kinds):
        return [f"{kind}X{place}" for kind in kinds if paired[kind[-1]]]

    def norm(g):
        for r in range(per):
            for at in range(0, toks, NORM_ROWS):
                x = x_buf[g * per + r, at : at + NORM_ROWS].astype(F32)
                a_buf[g, r * toks + at : r * toks + at + NORM_ROWS] = (unit(x) * g1_ref[...]).astype(BF16)

    def latent(g):
        kv = dot_t(a_buf[g], wdkv[...])
        rows[g * per : (g + 1) * per, spot(0, odd), :] = (unit(kv[:, :rank]) * gkv_ref[...]).astype(BF16).reshape(per, toks, rank)
        turned = []
        for s in range(per):
            cos_pair, sin_pair = cos_ref[g * per + s], sin_ref[g * per + s]
            cos = jnp.where(odd == 1, cos_pair[:, toks:], cos_pair[:, :toks])
            sin = jnp.where(odd == 1, sin_pair[:, toks:], sin_pair[:, :toks])
            table = jnp.concatenate([cos, cos, -sin, sin], axis=0).T
            p = kv[s * toks : (s + 1) * toks, rank:]
            swapped = jnp.concatenate([p[:, half:], p[:, :half]], axis=1)
            turned.append(p * table[:, :rope] + swapped * table[:, rope:])
        rot[g, spot(0, odd), :] = jnp.concatenate(turned, axis=1).astype(BF16)

    def queries(g):
        h = jnp.concatenate([dot(a_buf[g], wdq[:, : 2 * rank]), dot(a_buf[g], wdq[:, 2 * rank :])], axis=1)
        cq_buf[odd, g * per : (g + 1) * per] = (unit(h) * gq_ref[...]).astype(BF16).reshape(per, toks, q_rank)

    with jax.named_scope('p_norm0'):
        loads["x0"].wait()
        for g in range(1, groups):
            load_x(g)
        norm(0)
    for name in ("wdkv", "cos", "sin"):
        loads[name].wait()
    load("wdq", wdq_hbm, wdq)
    load("wk", wk_hbm, wkv.at[pl.ds(0, heads), pl.ds(0, nope)])
    load("wv", wv_hbm, wkv.at[pl.ds(0, heads), pl.ds(nope, nope)])
    load("wq", wq_hbm, wq.at[pl.ds(0, heads)])
    load("pe", pe_hbm.at[:, :, pl.ds(0, prefix)], pe_buf)
    load("lat", lat_hbm.at[:, pl.ds(0, prefix)], rows.at[:, pl.ds(0, prefix)])
    with jax.named_scope('p_bar'):
        pl.semaphore_wait(barrier, 3 + paired["a"] + paired["b"])
    with jax.named_scope('p_kv'):
        for g in range(groups):
            latent(g)
            for way in ("R", "L", "S0"):
                wire.start(f"c{g}{way}", f"p{g}{way}")
            if g + 1 < groups:
                loads[f"x{g + 1}"].wait()
                norm(g + 1)
    wire.start(*ring("R", *small))

    def hand_on(g):
        wire.landed(f"c{g}L", f"p{g}L", f"c{g}R", f"p{g}R")
        wire.start(f"c{g}O", f"p{g}O", f"c{g}S3", f"p{g}S3", f"c{g}S1", f"p{g}S1")

    with jax.named_scope('p_cq'):
        loads["wdq"].wait()
        for g in range(groups):
            queries(g)
            wire.start(f"q{g}S")
            hand_on(g)
    wire.start(*ring("L", *small, "wo.b", "wo.a"), "woS0")

    loads["pe"].wait()
    for g in range(groups):
        old = pe_buf[g * per : (g + 1) * per].reshape(per * rope, prefix).astype(F32)
        for b in range(prefix // BLOCK):
            rot[g, b * BLOCK : (b + 1) * BLOCK] = old[:, b * BLOCK : (b + 1) * BLOCK].T.astype(BF16)
    qb[...] = jnp.zeros_like(qb)

    def rest_of(g):
        wire.landed(f"c{g}O", f"p{g}O")
        wire.start(f"c{g}S2", f"p{g}S2")
        for slot in (0, 1, 3, 2):
            wire.landed(f"c{g}S{slot}", f"p{g}S{slot}")
        wire.landed(f"q{g}S")

    with jax.named_scope('p_rest0'):
        for name in ("wk", "wv", "wq", "lat"):
            loads[name].wait()
        rest_of(0)
        wire.landed(*ring("R", "wk.a", "wv.b"))
        wire.start(*across(1, "wk.a", "wv.b"), *ring("O", "wk.a", "wv.b"))

    row = lax.broadcasted_iota(jnp.int32, (BLOCK, wide), 0)
    lane = lax.rem(lax.broadcasted_iota(jnp.int32, (BLOCK, wide), 1), BLOCK)
    near = row <= lane

    def place(n):
        return n // duos, lax.rem(n, duos)

    def query_dot(n):
        quad, duo = place(n)
        w = wq[pl.ds(quad * 4, 4)].reshape(4 * head, q_rank)
        cq = jnp.concatenate([cq_buf[parity, 2 * duo + u] for u in range(2) for parity in range(2)], axis=0)
        q_raw[...] = dot_t(w, cq)

    def query_stage(n):
        quad, duo = place(n)
        raw = q_raw
        for u in range(2):
            slot = 2 * lax.rem(duo, 2) + u
            cos, sin = cos_ref[2 * duo + u], sin_ref[2 * duo + u]
            for h in range(4):
                pair, side = h // 2, h % 2
                q = raw[h * head : (h + 1) * head, u * BLOCK : (u + 1) * BLOCK]
                cols = slice(side * BLOCK, (side + 1) * BLOCK)
                qb[u, pair, side * nope : (side + 1) * nope, cols] = q[:nope].astype(BF16)
                lo, hi = q[nope : nope + half], q[nope + half :]
                turned = jnp.concatenate([lo * cos - hi * sin, hi * cos + lo * sin], axis=0).astype(BF16)
                start = pl.multiple_of(BLOCK + slot * rope, rope)
                stale = pl.multiple_of(BLOCK + lax.rem(slot + 2, 4) * rope, rope)
                qb[u, pair, pl.ds(start, rope), cols] = turned
                qb[u, pair, pl.ds(stale, rope), cols] = jnp.zeros_like(turned)

    def key_stage(n, t, u):
        quad, duo = place(n)
        w = wkv[pl.ds(quad * 4, 4), :nope].reshape(4 * nope, rank)
        kb[u][:t] = dot_t(rows[2 * duo + u, :t], w).astype(BF16)

    def value_stage(n, t, u):
        quad, duo = place(n)
        w = wkv[pl.ds(quad * 4, 4), nope:].reshape(4 * nope, rank)
        vb[u][:, :t] = dot_t(w, rows[2 * duo + u, :t]).astype(BF16)

    def score_stage(n, t, u, pair):
        _, duo = place(n)
        length = len_ref[2 * duo + u]
        keys = jnp.concatenate([kb[u][:t, pair * BLOCK : (pair + 1) * BLOCK], rot[duo // 2, :t]], axis=1)
        value = dot(keys, qb[u, pair])
        most = None
        for b in range(t // BLOCK):
            part = value[b * BLOCK : (b + 1) * BLOCK]
            if BLOCK <= b * BLOCK < prefix:
                part = jnp.where(row < length - b * BLOCK, part, NEVER)
            if b * BLOCK == prefix:
                part = jnp.where(near, part, NEVER)
            sb[2 * u + pair][b * BLOCK : (b + 1) * BLOCK] = part
            part = jnp.max(part.reshape(BLOCK // 8, 8, wide), axis=0)
            most = part if most is None else jnp.maximum(most, part)
        mb[2 * u + pair] = jnp.broadcast_to(jnp.max(most, axis=0, keepdims=True), (8, wide))

    def soft_stage(t, u, pair):
        i = 2 * u + pair
        most = mb[i, :1]
        total = None
        for b in range(t // BLOCK):
            x = jnp.exp2((sb[i][b * BLOCK : (b + 1) * BLOCK] - most) * factor)
            part = jnp.sum(x.reshape(BLOCK // 8, 8, wide), axis=0)
            total = part if total is None else total + part
            pb[i][b * BLOCK : (b + 1) * BLOCK] = x.astype(BF16)
        lb[i] = total

    def mix_stage(n, t, u, pair):
        quad, duo = place(n)
        i = 2 * u + pair
        inv = 1.0 / jnp.sum(lb[i], axis=0, keepdims=True)
        o = dot(vb[u][pair * BLOCK : (pair + 1) * BLOCK, :t], pb[i][:t]) * inv
        o = jnp.concatenate([o[:nope, :BLOCK], o[nope:, BLOCK:]], axis=0).T.astype(BF16)
        first, second = o[:toks], o[toks:]
        cols = slice(pair * BLOCK, (pair + 1) * BLOCK)
        o_own[quad, 2 * duo + u, :, cols] = jnp.where(odd == 1, second, first)
        o_send[quad, 2 * duo + u, :, cols] = jnp.where(odd == 1, first, second)

    units = [(u, pair) for u in range(2) for pair in range(2)]
    total = quads * duos

    def each_chip(fn):
        for c in range(slots):
            pl.when(chip == c)(lambda c=c: fn(prefix + (c + 1) * BLOCK))

    def body(b, t):
        before, ahead, later = jnp.maximum(b - 1, 0), jnp.minimum(b + 1, total - 1), jnp.minimum(b + 2, total - 1)
        mix_stage(before, t, 0, 0)
        mix_stage(before, t, 0, 1)
        mix_stage(before, t, 1, 0)
        mix_stage(before, t, 1, 1)
        soft_stage(t, 0, 0)
        score_stage(ahead, t, 0, 0)
        value_stage(b, t, 0)
        soft_stage(t, 0, 1)
        score_stage(ahead, t, 0, 1)
        key_stage(later, t, 0)
        soft_stage(t, 1, 0)
        score_stage(ahead, t, 1, 0)
        value_stage(b, t, 1)
        soft_stage(t, 1, 1)
        score_stage(ahead, t, 1, 1)
        query_dot(later)
        query_stage(later)
        key_stage(later, t, 1)

    def at(b, when):
        return pl.when(b == when)

    agenda = {
        1: [(None, ring("R", "wq.a"), across(1, "wq.a") + ring("O", "wq.a"))],
        2: [(None, ring("R", "wq.b"), across(1, "wq.b") + ring("O", "wq.b") + ring("R", "wo.a", "wo.b"))],
        3: [(None, ring("L", "wk.a", "wv.b"), across(2, "wk.a", "wv.b"))],
        4: [(None, across(1, *small), [])],
        5: [(None, ring("L", "wq.a"), across(2, "wq.a"))],
        6: [(None, ring("O", "wk.a", "wq.a"), across(3, "wk.a", "wq.a"))],
        7: [(None, ring("L", "wq.b"), across(2, "wq.b"))],
        8: [(None, ring("O", "wv.b", "wq.b"), across(3, "wv.b", "wq.b"))],
        10: [(None, across(2, *small), [])],
        12: [(None, ring("L", "wo.b"), across(2, "wo.b")), (1, [], ring("O", "wo.b"))],
        13: [(None, ring("R", "wo.a"), across(1, "wo.a")), (0, [], ring("O", "wo.a"))],
        15: [(None, across(3, *small), [])],
        17: [(None, ring("L", "wo.a"), across(2, "wo.a")), (1, [], ring("O", "wo.a"))],
        18: [(None, ring("R", "wo.b"), across(1, "wo.b")), (0, [], ring("O", "wo.b"))],
        20: [(0, ring("O", "wo.a"), across(3, "wo.a") + ["wo.aS"]), (1, ring("O", "wo.b"), across(3, "wo.b") + ["wo.bS"])],
        22: [(0, ring("O", "wo.b"), across(3, "wo.b") + ["wo.bS"]), (1, ring("O", "wo.a"), across(3, "wo.a") + ["wo.aS"])],
        25: [(None, across(1, "wo.a", "wo.b") + across(2, "wo.a", "wo.b"), ["woS1", "woS2"])],
    }
    for quad in range(quads - 1):
        agenda.setdefault((quad + 1) * duos + 1, []).append((None, [], [f"o{quad}S"]))

    def run_agenda(when):
        for parity, waits, starts in agenda[when]:

            def item(waits=waits, starts=starts):
                with jax.named_scope(f"ev_{when}"):
                    wire.landed(*waits)
                wire.start(*starts)

            if parity is None:
                item()
            else:
                pl.when(odd == parity)(item)

    bounce = pltpu.make_async_copy(wo_hbm, wo_buf, load_sem.at[3])
    span = 8

    def step(b, _):
        for first in range(0, total, span):

            @pl.when(b // span == first // span)
            def _():
                if first == 0:

                    @at(b, 0)
                    def _():
                        with jax.named_scope('ev_k1'):
                            rest_of(1)

                    @at(b, 2)
                    def _():
                        with jax.named_scope('ev_k2'):
                            rest_of(2)
                        pltpu.make_async_copy(rows.at[:, pl.ds(prefix, chunk)], c_out, load_sem.at[0]).start()
                        pltpu.make_async_copy(rot.at[:, pl.ds(prefix, chunk)], p_out, load_sem.at[1]).start()
                        bounce.start()

                    @at(b, 6)
                    def _():
                        bounce.wait()
                        pltpu.make_async_copy(wo_buf, wo_out.at[odd, 0], load_sem.at[4]).start()

                for when in sorted(agenda):
                    if first <= when < first + span:
                        at(b, when)(functools.partial(run_agenda, when))

        with jax.named_scope('body'):
            each_chip(functools.partial(body, b))
        return 0

    def lead_in(t):
        for u in range(2):
            key_stage(0, t, u)
        query_dot(0)
        query_stage(0)

    def second(t):
        for u, pair in units:
            score_stage(0, t, u, pair)
        for u in range(2):
            key_stage(1, t, u)
        query_dot(1)
        query_stage(1)

    with jax.named_scope('p_lead'):
        each_chip(lead_in)
        each_chip(second)
    lax.fori_loop(0, total, step, 0)

    def last(t):
        for u, pair in units:
            mix_stage(total - 1, t, u, pair)

    with jax.named_scope('p_last'):
        each_chip(last)
        wire.start(f"o{quads - 1}S")
        pltpu.make_async_copy(o_own, o_out.at[odd], load_sem.at[2]).start()
    with jax.named_scope('f_land'):
        for piece in ("wo.a", "wo.b"):
            wire.landed(*across(3, piece))
            wire.start(f"{piece}S~")
        for place in range(slots - 1):
            wire.landed(f"woS{place}")
        wire.landed("wo.aS", "wo.bS", "wo.aS~", "wo.bS~")
        for quad in range(quads):
            wire.landed(f"o{quad}S")
    with jax.named_scope('f_sent'):
        wire.sent(*wire.index)
        pltpu.make_async_copy(rows.at[:, pl.ds(prefix, chunk)], c_out, load_sem.at[0]).wait()
        pltpu.make_async_copy(rot.at[:, pl.ds(prefix, chunk)], p_out, load_sem.at[1]).wait()
        pltpu.make_async_copy(o_own, o_out.at[odd], load_sem.at[2]).wait()
        pltpu.make_async_copy(wo_buf, wo_out.at[odd, 0], load_sem.at[4]).wait()


def finish_kernel(
    len_ref, o_hbm, w_hbm, x_hbm, c_hbm, p_hbm, lat_hbm, pe_hbm, y_hbm, lat_out, pe_out, fresh, acc, x_buf, y_buf, o_buf, w_buf, c_buf, p_buf, lat_buf, pe_buf, lat_new, pe_new, load_sem, store_sem, sems
):
    chip = lax.axis_index("tp") // 2
    quads, seqs, toks, depth = o_hbm.shape[1:]
    terms = 2 * quads
    slots = c_hbm.shape[1]
    rank = lat_hbm.shape[2]
    rope, cache_len = pe_hbm.shape[1:]
    chunk = slots * 2 * toks
    words = rank // BLOCK
    dim = x_hbm.shape[2]
    part = 2 * depth
    ring = w_buf.shape[0]

    def loads(k, with_term):
        slot = lax.rem(k, ring)
        out = [
            pltpu.make_async_copy(c_hbm.at[k], c_buf.at[slot], load_sem.at[0, slot]),
            pltpu.make_async_copy(lat_hbm.at[k], lat_buf.at[slot], load_sem.at[1, slot]),
        ]
        if with_term:
            side, quad = k // quads, lax.rem(k, quads)
            out.append(pltpu.make_async_copy(o_hbm.at[side, quad], o_buf.at[slot], load_sem.at[2, slot]))
            out.append(pltpu.make_async_copy(w_hbm.at[side, pl.ds(pl.multiple_of(quad * depth, depth), depth)], w_buf.at[slot], load_sem.at[3, slot]))
        return out

    def store(k):
        slot = lax.rem(k, ring)
        return pltpu.make_async_copy(lat_new.at[slot], lat_out.at[k], store_sem.at[slot])

    load_x = pltpu.make_async_copy(x_hbm, x_buf, sems.at[0])
    load_p = pltpu.make_async_copy(p_hbm, p_buf, sems.at[1])
    load_pe = pltpu.make_async_copy(pe_hbm, pe_buf, sems.at[2])
    store_pe = pltpu.make_async_copy(pe_new, pe_out, sems.at[3])

    def store_y(n):
        cols = pl.ds(n * part, part)
        return pltpu.make_async_copy(y_buf.at[:, :, cols], y_hbm.at[:, :, cols], sems.at[4 + n])


    def slot_of(j):
        return lax.rem(chip - j + slots, slots)

    def project(k, kind):
        slot = lax.rem(k, ring)
        o = o_buf[slot].reshape(seqs * toks, depth)
        for n in range(0, dim, part):
            cols = slice(n, n + part)
            y = dot(o, w_buf[slot, :, cols])
            if kind != "first":
                y = acc[:, cols] + y
            if kind == "last":
                y = y + x_buf[:, :, cols].reshape(seqs * toks, part).astype(F32)
                y_buf[:, :, cols] = y.astype(BF16).reshape(seqs, toks, part)
                store_y(n // part).start()
            else:
                acc[:, cols] = y

    def cache(k):
        at_slot = lax.rem(k, ring)
        length = len_ref[k]
        for j in range(slots):
            piece = c_buf[at_slot, slot_of(j)].reshape(2 * toks, rank).astype(F32)
            for w in range(words):
                fresh[w, BLOCK + j * 2 * toks : BLOCK + (j + 1) * 2 * toks] = piece[:, w * BLOCK : (w + 1) * BLOCK]
        lat_new[at_slot] = lat_buf[at_slot]
        base = (length // 16) * 16
        skew = length - base
        tile_row = lax.broadcasted_iota(jnp.int32, (16, BLOCK), 0)
        for i in range(chunk // 16 + 1):
            at = pl.multiple_of(jnp.minimum(base + i * 16, cache_len - 16), 16)
            for w in range(words):
                cols = slice(w * BLOCK, (w + 1) * BLOCK)
                moved = fresh[w, pl.ds(BLOCK - skew + i * 16, 16), :].astype(BF16)
                if i == 0 or i == chunk // 16:
                    local = tile_row + (at - length)
                    shown = (local >= 0) & (local < chunk) if i == 0 else (local < chunk)
                    if i == 0:
                        rest = lat_buf[at_slot, pl.ds(at, 16), cols]
                    else:
                        shown = shown & (skew > 0)
                        rest = lat_new[at_slot, pl.ds(at, 16), cols]
                    moved = jnp.where(shown, moved.astype(F32), rest.astype(F32)).astype(BF16)
                lat_new[at_slot, pl.ds(at, 16), cols] = moved

        turned = jnp.concatenate([p_buf[k // (BLOCK // rope), slot_of(j)].reshape(2 * toks, BLOCK).astype(F32).T for j in range(slots)], axis=1)
        group = lax.rem(k, BLOCK // rope)
        mine = turned[:rope]
        for g in range(1, BLOCK // rope):
            mine = jnp.where(group == g, turned[g * rope : (g + 1) * rope], mine)
        mine = jnp.concatenate([mine, jnp.zeros((rope, cache_len - chunk), F32)], axis=1)
        mine = pltpu.roll(mine, length, axis=1)
        spot = lax.broadcasted_iota(jnp.int32, (rope, cache_len), 1) - length
        pe_new[k] = jnp.where((spot >= 0) & (spot < chunk), mine, pe_buf[k].astype(F32)).astype(BF16)

    def begin(k, with_term):
        for load in loads(k, with_term):
            load.start()

    def arrived(k, with_term):
        for load in loads(k, with_term):
            load.wait()

    def work(k, kind):
        if kind != "none":
            project(k, kind)
        cache(k)
        store(k).start()

    def more(k):
        pl.when(k < terms)(lambda: begin(k, True))
        pl.when((k >= terms) & (k < seqs))(lambda: begin(k, False))

    begin(0, True)
    load_p.start()
    load_pe.start()
    arrived(0, True)
    for k in range(1, ring):
        begin(k, True)
    load_p.wait()
    load_pe.wait()
    with jax.named_scope('g_first'):
        work(0, "first")
    load_x.start()

    def middle(k, _):
        with jax.named_scope('g_wait'):
            arrived(k, True)
        more(k + ring - 1)

        @pl.when(k >= ring)
        def _():
            store(k - ring).wait()

        with jax.named_scope('g_work'):
            work(k, "middle")
        return 0

    lax.fori_loop(1, terms - 1, middle, 0)
    last = terms - 1
    arrived(last, True)
    more(last + ring - 1)
    store(last - ring).wait()
    load_x.wait()
    with jax.named_scope('g_last'):
        work(last, "last")

    def tail(k, _):
        arrived(k, False)
        store(k - ring).wait()
        with jax.named_scope('g_tail'):
            work(k, "none")
        return 0

    lax.fori_loop(terms, seqs, tail, 0)
    store_pe.start()
    for k in range(ring):
        store(seqs - ring + k).wait()
    store_pe.wait()
    for n in range(dim // part):
        store_y(n).wait()


def solution(mesh):
    size = mesh.shape["tp"]
    count = mesh.shape["dp"]
    stride = 2 ** (count.bit_length() // 2)
    paired = {"a": count % 2 == 0, "b": count % (2 * stride) == 0}

    def local_step(hidden, lengths, rope_cos, rope_sin, cache_lat, cache_pe, norm_in, w_dq, norm_q, w_dkv, norm_kv, w_uq, w_uk, w_uv, w_out):
        seqs, toks, dim = hidden.shape
        q_rank = w_dq.shape[1]
        rank, heads, nope = w_uk.shape
        rope = cache_pe.shape[2]
        cache_len = cache_lat.shape[1]
        slots = size // 2
        head = nope + rope
        quads = slots * heads // 4
        chunk = size * toks
        prefix = cache_len - chunk
        per = BLOCK // rope
        groups = seqs // per
        wide = 2 * BLOCK
        cos_t, sin_t = rope_cos.transpose(0, 2, 1), rope_sin.transpose(0, 2, 1)
        pe_t = cache_pe.transpose(0, 2, 1)
        wdkv_t = w_dkv.transpose(1, 0)
        wq_t, wk_t, wv_t = (w.transpose(1, 2, 0) for w in (w_uq, w_uk, w_uv))

        copies = 15 * groups + 36 + slots + 3 + quads
        any_spec = pl.BlockSpec(memory_space=pl.ANY)
        vmem_spec = pl.BlockSpec(memory_space=pltpu.VMEM)
        smem_spec = pl.BlockSpec(memory_space=pltpu.SMEM)
        c_all, p_all, o_all, wo_all = pl.pallas_call(
            functools.partial(main_kernel, (size, stride, paired)),
            in_specs=[smem_spec, any_spec, vmem_spec, any_spec, vmem_spec, any_spec, vmem_spec] + [any_spec] * 8,
            out_specs=[any_spec] * 4,
            out_shape=[
                jax.ShapeDtypeStruct((seqs, chunk, rank), BF16),
                jax.ShapeDtypeStruct((groups, chunk, BLOCK), BF16),
                jax.ShapeDtypeStruct((2, quads, seqs, toks, 4 * nope), BF16),
                jax.ShapeDtypeStruct((2, slots) + w_out.shape, BF16),
            ],
            scratch_shapes=[
                pltpu.VMEM(hidden.shape, BF16),
                pltpu.VMEM(w_dq.shape, BF16),
                pltpu.VMEM(wdkv_t.shape, BF16),
                pltpu.VMEM((groups, per * toks, dim), BF16),
                pltpu.VMEM((seqs, cache_len, rank), BF16),
                pltpu.VMEM((groups, cache_len, BLOCK), BF16),
                pltpu.VMEM((seqs, rope, prefix), BF16),
                pltpu.VMEM((seqs, rope // 2, BLOCK), F32),
                pltpu.VMEM((seqs, rope // 2, BLOCK), F32),
                pltpu.VMEM((2, seqs, toks, q_rank), BF16),
                pltpu.VMEM((slots * heads, head, q_rank), BF16),
                pltpu.VMEM((slots * heads, 2 * nope, rank), BF16),
                [pltpu.VMEM((cache_len, 4 * nope), BF16) for _ in range(2)],
                [pltpu.VMEM((4 * nope, cache_len), BF16) for _ in range(2)],
                pltpu.VMEM((2, 2, wide, wide), BF16),
                pltpu.VMEM((4 * head, wide), F32),
                [pltpu.VMEM((cache_len, wide), F32) for _ in range(4)],
                pltpu.VMEM((4, 8, wide), F32),
                [pltpu.VMEM((cache_len, wide), BF16) for _ in range(4)],
                pltpu.VMEM((4, 8, wide), F32),
                pltpu.VMEM((quads, seqs, toks, 4 * nope), BF16),
                pltpu.VMEM((quads, seqs, toks, 4 * nope), BF16),
                pltpu.VMEM(w_out.shape, BF16),
                pltpu.SemaphoreType.DMA((9 + groups,)),
                pltpu.SemaphoreType.DMA((copies,)),
                pltpu.SemaphoreType.DMA((copies,)),
            ],
            compiler_params=pltpu.CompilerParams(collective_id=0, has_side_effects=True, vmem_limit_bytes=63 * MIB),
            cost_estimate=pl.CostEstimate(flops=70 * 10**9, bytes_accessed=40 * MIB, transcendentals=30 * 10**6),
            name="main",
        )(lengths, hidden, norm_in, w_dq, norm_q, wdkv_t, norm_kv, cos_t, sin_t, wq_t, wk_t, wv_t, w_out, cache_lat, pe_t)

        depth = 4 * nope
        ahead = 4
        y, lat_new, pe_new = pl.pallas_call(
            finish_kernel,
            in_specs=[smem_spec] + [any_spec] * 7,
            out_specs=[any_spec] * 3,
            scratch_shapes=[
                pltpu.VMEM((rank // BLOCK, chunk + 2 * BLOCK, BLOCK), F32),
                pltpu.VMEM((seqs * toks, dim), F32),
                pltpu.VMEM(hidden.shape, BF16),
                pltpu.VMEM(hidden.shape, BF16),
                pltpu.VMEM((ahead, seqs, toks, depth), BF16),
                pltpu.VMEM((ahead, depth, dim), BF16),
                pltpu.VMEM((ahead, slots, 2, toks, rank), BF16),
                pltpu.VMEM((groups, slots, 2, toks, BLOCK), BF16),
                pltpu.VMEM((ahead, cache_len, rank), BF16),
                pltpu.VMEM(pe_t.shape, BF16),
                pltpu.VMEM((ahead, cache_len, rank), BF16),
                pltpu.VMEM(pe_t.shape, BF16),
                pltpu.SemaphoreType.DMA((4, ahead)),
                pltpu.SemaphoreType.DMA((ahead,)),
                pltpu.SemaphoreType.DMA((4 + dim // (2 * depth),)),
            ],
            out_shape=[
                jax.ShapeDtypeStruct(hidden.shape, BF16),
                jax.ShapeDtypeStruct(cache_lat.shape, BF16),
                jax.ShapeDtypeStruct(pe_t.shape, BF16),
            ],
            compiler_params=pltpu.CompilerParams(vmem_limit_bytes=63 * MIB),
            cost_estimate=pl.CostEstimate(flops=2 * seqs * toks * dim * dim, bytes_accessed=50 * MIB, transcendentals=0),
            name="finish",
        )(
            lengths,
            o_all,
            wo_all.reshape(2, slots * w_out.shape[0], dim),
            hidden,
            c_all.reshape(seqs, slots, 2, toks, rank),
            p_all.reshape(groups, slots, 2, toks, BLOCK),
            cache_lat,
            pe_t,
        )
        return y, lat_new, pe_new.transpose(0, 2, 1)

    spec_tok = P("dp", "tp", None)
    spec_len = P("dp")
    spec_seq = P("dp", None, None)
    spec_vec = P(None)
    spec_mat = P(None, None)
    spec_head = P(None, "tp", None)
    spec_rows = P("tp", None)
    in_specs = (spec_tok, spec_len, spec_seq, spec_seq, spec_seq, spec_seq, spec_vec, spec_mat, spec_vec, spec_mat, spec_vec, spec_head, spec_head, spec_head, spec_rows)
    return jax.shard_map(local_step, mesh=mesh, in_specs=in_specs, out_specs=(spec_tok, spec_seq, spec_seq), check_vma=False)
```

```python
import functools

import jax
import jax.numpy as jnp
from jax import lax
from jax.experimental import pallas as pl
from jax.experimental.pallas import tpu as pltpu
from jax.sharding import PartitionSpec as P

BLOCK = 128
LOG2E = 1.4426950408889634
NEVER = -1e30
NORM_ROWS = 16
F32 = jnp.float32
BF16 = jnp.bfloat16
MESH = pl.DeviceIdType.MESH
MIB = 2**20


def dot(a, b):
    return lax.dot_general(a, b, (((1,), (0,)), ((), ())), preferred_element_type=F32)


def dot_t(a, b):
    return lax.dot_general(a, b, (((1,), (1,)), ((), ())), preferred_element_type=F32)


def unit(x):
    return x * lax.rsqrt(jnp.mean(x * x, axis=-1, keepdims=True) + 1e-6)


class Wire:
    def __init__(self, send_sem, recv_sem):
        self.sems = (send_sem, recv_sem)
        self.made = {}
        self.index = {}

    def add(self, name, src, dst, **peer):
        self.index[name] = len(self.index)
        self.made[name] = lambda: pltpu.make_async_remote_copy(
            src(), dst(), self.sems[0].at[self.index[name]], self.sems[1].at[self.index[name]], device_id=peer, device_id_type=MESH
        )

    def start(self, *names):
        for name in names:
            self.made[name]().start()

    def landed(self, *names):
        for name in names:
            self.made[name]().wait_recv()

    def sent(self, *names):
        for name in names:
            self.made[name]().wait_send()


def main_kernel(
    plan,
    len_ref,
    x_hbm,
    g1_ref,
    wdq_hbm,
    gq_ref,
    wdkv_hbm,
    gkv_ref,
    cos_hbm,
    sin_hbm,
    wq_hbm,
    wk_hbm,
    wv_hbm,
    wo_hbm,
    lat_hbm,
    pe_hbm,
    c_out,
    p_out,
    o_out,
    wo_out,
    x_buf,
    wdq,
    wdkv,
    a_buf,
    rows,
    rot,
    pe_buf,
    cos_ref,
    sin_ref,
    cq_buf,
    wq,
    wkv,
    kb,
    vb,
    qb,
    q_raw,
    sb,
    mb,
    pb,
    lb,
    o_own,
    o_send,
    wo_buf,
    load_sem,
    send_sem,
    recv_sem,
):
    size, stride, paired = plan
    me = lax.axis_index("tp")
    odd = lax.rem(me, 2)
    chip = me // 2
    right, left = lax.rem(me + 2, size), lax.rem(me + size - 2, size)
    onward = jnp.where(odd == 0, right, left)
    other = me + 1 - 2 * odd
    dp = lax.axis_index("dp")
    flip = {"a": lax.rem(dp, 2), "b": lax.rem(dp // stride, 2)}
    partner = {"a": dp + 1 - 2 * flip["a"], "b": dp + stride * (1 - 2 * flip["b"])}

    seqs, toks, dim = x_hbm.shape
    groups = rot.shape[0]
    per = seqs // groups
    rank = rows.shape[2]
    slots = size // 2
    chunk = size * toks
    prefix = rows.shape[1] - chunk
    heads = wq.shape[0] // slots
    head, q_rank = wq.shape[1:]
    rope = BLOCK // per
    half = rope // 2
    nope = head - rope
    quads = wq.shape[0] // 4
    duos = seqs // 2
    wide = 2 * BLOCK
    factor = LOG2E * head**-0.5

    loads = {}

    def load(name, src, dst):
        loads[name] = pltpu.make_async_copy(src, dst, load_sem.at[len(loads)])
        loads[name].start()

    def spot(slot, parity):
        return pl.ds(pl.multiple_of(prefix + slot * BLOCK + parity * toks, toks), toks)

    barrier = pltpu.get_barrier_semaphore()
    for peer in (left, right, other):
        pl.semaphore_signal(barrier, inc=1, device_id={"tp": peer}, device_id_type=MESH)
    for side in "ab":
        if paired[side]:
            pl.semaphore_signal(barrier, inc=1, device_id={"dp": partner[side]}, device_id_type=MESH)

    lanes_chip = pl.ds(pl.multiple_of(chip * BLOCK, BLOCK), BLOCK)
    def load_x(g):
        load(f"x{g}", x_hbm.at[pl.ds(g * per, per)], x_buf.at[pl.ds(g * per, per)])

    load_x(0)
    load("wdkv", wdkv_hbm, wdkv)
    load("cos", cos_hbm.at[:, :, lanes_chip], cos_ref)
    load("sin", sin_hbm.at[:, :, lanes_chip], sin_ref)

    wire = Wire(send_sem, recv_sem)

    def chain(name, here, there, places, via="split"):
        near_left, near_right, opposite = places
        handed = {"right": near_left, "left": near_right, "split": jnp.where(odd == 0, near_left, near_right)}[via]
        wire.add(name + "R", lambda: here(0), lambda: there(near_left), tp=right)
        wire.add(name + "L", lambda: here(0), lambda: there(near_right), tp=left)
        wire.add(name + "O", lambda: there(handed), lambda: there(opposite), tp={"right": right, "left": left, "split": onward}[via])

    for g in range(groups):
        for name, ref in (("c", lambda slot, g=g: rows.at[pl.ds(g * per, per), spot(slot, odd)]), ("p", lambda slot, g=g: rot.at[g, spot(slot, odd)])):
            name = f"{name}{g}"
            chain(name, ref, ref, (1, 3, 2), "left")
            for slot in range(slots):
                wire.add(f"{name}S{slot}", functools.partial(ref, slot), functools.partial(ref, slot), tp=other)
        cq_ref = lambda g=g: cq_buf.at[odd, pl.ds(g * per, per)]
        wire.add(f"q{g}S", cq_ref, cq_ref, tp=other)

    def cut(side, low, high, unit, mine):
        half_size = (high - low) // 2
        which = flip[side] if mine else 1 - flip[side]
        return pl.ds(pl.multiple_of(low + which * half_size, unit), half_size)

    q_cut = head * 2 // 3
    o_cut = wo_hbm.shape[0] * 2 // 5
    pieces = {
        "wq.a": (lambda r: wq_hbm.at[:, r], lambda place, r: wq.at[pl.ds(place * heads, heads), r], ("a", 0, q_cut, 16)),
        "wq.b": (lambda r: wq_hbm.at[:, r], lambda place, r: wq.at[pl.ds(place * heads, heads), r], ("b", q_cut, head, 16)),
        "wk.a": (lambda r: wk_hbm.at[:, :, r], lambda place, r: wkv.at[pl.ds(place * heads, heads), pl.ds(0, nope), r], ("a", 0, rank, BLOCK)),
        "wv.b": (lambda r: wv_hbm.at[:, :, r], lambda place, r: wkv.at[pl.ds(place * heads, heads), pl.ds(nope, nope), r], ("b", 0, rank, BLOCK)),
        "wo.a": (lambda r: wo_hbm.at[r], lambda place, r: wo_out.at[odd, place, r], ("a", 0, o_cut, 16)),
        "wo.b": (lambda r: wo_hbm.at[r], lambda place, r: wo_out.at[odd, place, r], ("b", o_cut, 2 * o_cut, 16)),
    }
    left_over = pl.ds(2 * o_cut, wo_hbm.shape[0] - 2 * o_cut)
    chain("wo.m", lambda place: wo_hbm.at[left_over], lambda place: wo_out.at[odd, place, left_over], (1, 2, 3))
    for piece, (source, target, bounds) in pieces.items():
        side = bounds[0]
        via = "split" if piece.startswith("wo") else "right"
        for mine in (True,) if paired[side] else (True, False):
            here = lambda place, source=source, bounds=bounds, mine=mine: source(cut(*bounds, mine))
            there = lambda place, target=target, bounds=bounds, mine=mine: target(place, cut(*bounds, mine))
            chain(piece + ("" if mine else "~"), here, there, (1, 2, 3), via)
        if paired[side]:
            for place in (1, 2, 3):
                ref = lambda place=place, target=target, bounds=bounds: target(place, cut(*bounds, True))
                wire.add(f"{piece}X{place}", ref, ref, dp=partner[side])
    for place in range(slots - 1):
        ref = lambda place=place: wo_out.at[odd, place]
        wire.add(f"woS{place}", ref if place else lambda: wo_hbm, ref, tp=other)
    for piece in ("wo.a", "wo.b"):
        for mine in (True, False):
            ref = lambda piece=piece, mine=mine: pieces[piece][1](slots - 1, cut(*pieces[piece][2], mine))
            wire.add(f"{piece}S" + ("" if mine else "~"), ref, ref, tp=other)
    ref = lambda: wo_out.at[odd, slots - 1, left_over]
    wire.add("wo.mS", ref, ref, tp=other)
    for quad in range(quads):
        wire.add(f"o{quad}S", lambda quad=quad: o_send.at[quad], lambda quad=quad: o_out.at[odd, quad], tp=other)

    small = ("wk.a", "wv.b", "wq.a", "wq.b")

    def ring(which, *kinds):
        return [f"{kind}{half_name}{way}" for kind in kinds for half_name in ("", "~")[: 1 if paired[kind[-1]] else 2] for way in which]

    def across(place, *kinds):
        return [f"{kind}X{place}" for kind in kinds if paired[kind[-1]]]

    def norm(g):
        for r in range(per):
            for at in range(0, toks, NORM_ROWS):
                x = x_buf[g * per + r, at : at + NORM_ROWS].astype(F32)
                a_buf[g, r * toks + at : r * toks + at + NORM_ROWS] = (unit(x) * g1_ref[...]).astype(BF16)

    def latent(g):
        kv = dot_t(a_buf[g], wdkv[...])
        rows[g * per : (g + 1) * per, spot(0, odd), :] = (unit(kv[:, :rank]) * gkv_ref[...]).astype(BF16).reshape(per, toks, rank)
        turned = []
        for s in range(per):
            cos_pair, sin_pair = cos_ref[g * per + s], sin_ref[g * per + s]
            cos = jnp.where(odd == 1, cos_pair[:, toks:], cos_pair[:, :toks])
            sin = jnp.where(odd == 1, sin_pair[:, toks:], sin_pair[:, :toks])
            table = jnp.concatenate([cos, cos, -sin, sin], axis=0).T
            p = kv[s * toks : (s + 1) * toks, rank:]
            swapped = jnp.concatenate([p[:, half:], p[:, :half]], axis=1)
            turned.append(p * table[:, :rope] + swapped * table[:, rope:])
        rot[g, spot(0, odd), :] = jnp.concatenate(turned, axis=1).astype(BF16)

    def queries(g):
        h = jnp.concatenate([dot(a_buf[g], wdq[:, : 2 * rank]), dot(a_buf[g], wdq[:, 2 * rank :])], axis=1)
        cq_buf[odd, g * per : (g + 1) * per] = (unit(h) * gq_ref[...]).astype(BF16).reshape(per, toks, q_rank)

    with jax.named_scope('p_norm0'):
        loads["x0"].wait()
        for g in range(1, groups):
            load_x(g)
        norm(0)
    for name in ("wdkv", "cos", "sin"):
        loads[name].wait()
    load("wdq", wdq_hbm, wdq)
    load("wk", wk_hbm, wkv.at[pl.ds(0, heads), pl.ds(0, nope)])
    load("wv", wv_hbm, wkv.at[pl.ds(0, heads), pl.ds(nope, nope)])
    load("wq", wq_hbm, wq.at[pl.ds(0, heads)])
    load("pe", pe_hbm.at[:, :, pl.ds(0, prefix)], pe_buf)
    load("lat", lat_hbm.at[:, pl.ds(0, prefix)], rows.at[:, pl.ds(0, prefix)])
    with jax.named_scope('p_bar'):
        pl.semaphore_wait(barrier, 3 + paired["a"] + paired["b"])
    with jax.named_scope('p_kv'):
        for g in range(groups):
            latent(g)
            for way in ("R", "L", "S0"):
                wire.start(f"c{g}{way}", f"p{g}{way}")
            if g + 1 < groups:
                loads[f"x{g + 1}"].wait()
                norm(g + 1)
    wire.start(*ring("R", *small))

    def hand_on(g):
        wire.landed(f"c{g}L", f"p{g}L", f"c{g}R", f"p{g}R")
        wire.start(f"c{g}O", f"p{g}O", f"c{g}S3", f"p{g}S3", f"c{g}S1", f"p{g}S1")

    with jax.named_scope('p_cq'):
        loads["wdq"].wait()
        for g in range(groups):
            queries(g)
            wire.start(f"q{g}S")
            hand_on(g)
    wire.start(*ring("L", *small, "wo.b", "wo.a"), "wo.mL", "woS0")

    loads["pe"].wait()
    for g in range(groups):
        old = pe_buf[g * per : (g + 1) * per].reshape(per * rope, prefix).astype(F32)
        for b in range(prefix // BLOCK):
            rot[g, b * BLOCK : (b + 1) * BLOCK] = old[:, b * BLOCK : (b + 1) * BLOCK].T.astype(BF16)
    qb[...] = jnp.zeros_like(qb)

    def rest_of(g):
        wire.landed(f"c{g}O", f"p{g}O")
        wire.start(f"c{g}S2", f"p{g}S2")
        for slot in (0, 1, 3, 2):
            wire.landed(f"c{g}S{slot}", f"p{g}S{slot}")
        if g:
            wire.landed(f"q{g}S")

    with jax.named_scope('p_rest0'):
        for name in ("wk", "wv", "wq", "lat"):
            loads[name].wait()
    row = lax.broadcasted_iota(jnp.int32, (BLOCK, wide), 0)
    lane = lax.rem(lax.broadcasted_iota(jnp.int32, (BLOCK, wide), 1), BLOCK)
    near = row <= lane

    def place(n):
        return n // duos, lax.rem(n, duos)

    def query_dot(n):
        quad, duo = place(n)
        w = wq[pl.ds(quad * 4, 4)].reshape(4 * head, q_rank)
        cq = jnp.concatenate([cq_buf[parity, 2 * duo + u] for u in range(2) for parity in range(2)], axis=0)
        q_raw[...] = dot_t(w, cq)

    def query_stage(n):
        quad, duo = place(n)
        raw = q_raw
        for u in range(2):
            slot = 2 * lax.rem(duo, 2) + u
            cos, sin = cos_ref[2 * duo + u], sin_ref[2 * duo + u]
            for h in range(4):
                pair, side = h // 2, h % 2
                q = raw[h * head : (h + 1) * head, u * BLOCK : (u + 1) * BLOCK]
                cols = slice(side * BLOCK, (side + 1) * BLOCK)
                qb[u, pair, side * nope : (side + 1) * nope, cols] = q[:nope].astype(BF16)
                lo, hi = q[nope : nope + half], q[nope + half :]
                turned = jnp.concatenate([lo * cos - hi * sin, hi * cos + lo * sin], axis=0).astype(BF16)
                start = pl.multiple_of(BLOCK + slot * rope, rope)
                stale = pl.multiple_of(BLOCK + lax.rem(slot + 2, 4) * rope, rope)
                qb[u, pair, pl.ds(start, rope), cols] = turned
                qb[u, pair, pl.ds(stale, rope), cols] = jnp.zeros_like(turned)

    def key_stage(n, t, u):
        quad, duo = place(n)
        w = wkv[pl.ds(quad * 4, 4), :nope].reshape(4 * nope, rank)
        kb[u][:t] = dot_t(rows[2 * duo + u, :t], w).astype(BF16)

    def value_stage(n, t, u):
        quad, duo = place(n)
        w = wkv[pl.ds(quad * 4, 4), nope:].reshape(4 * nope, rank)
        vb[u][:, :t] = dot_t(w, rows[2 * duo + u, :t]).astype(BF16)

    def score_stage(n, t, u, pair):
        _, duo = place(n)
        length = len_ref[2 * duo + u]
        keys = jnp.concatenate([kb[u][:t, pair * BLOCK : (pair + 1) * BLOCK], rot[duo // 2, :t]], axis=1)
        value = dot(keys, qb[u, pair])
        most = None
        for b in range(t // BLOCK):
            part = value[b * BLOCK : (b + 1) * BLOCK]
            if BLOCK <= b * BLOCK < prefix:
                part = jnp.where(row < length - b * BLOCK, part, NEVER)
            if b * BLOCK == prefix:
                part = jnp.where(near, part, NEVER)
            sb[2 * u + pair][b * BLOCK : (b + 1) * BLOCK] = part
            part = jnp.max(part.reshape(BLOCK // 8, 8, wide), axis=0)
            most = part if most is None else jnp.maximum(most, part)
        mb[2 * u + pair] = jnp.broadcast_to(jnp.max(most, axis=0, keepdims=True), (8, wide))

    def soft_stage(t, u, pair):
        i = 2 * u + pair
        most = mb[i, :1]
        total = None
        for b in range(t // BLOCK):
            x = jnp.exp2((sb[i][b * BLOCK : (b + 1) * BLOCK] - most) * factor)
            part = jnp.sum(x.reshape(BLOCK // 8, 8, wide), axis=0)
            total = part if total is None else total + part
            pb[i][b * BLOCK : (b + 1) * BLOCK] = x.astype(BF16)
        lb[i] = total

    def mix_stage(n, t, u, pair):
        quad, duo = place(n)
        i = 2 * u + pair
        inv = 1.0 / jnp.sum(lb[i], axis=0, keepdims=True)
        o = dot(vb[u][pair * BLOCK : (pair + 1) * BLOCK, :t], pb[i][:t]) * inv
        o = jnp.concatenate([o[:nope, :BLOCK], o[nope:, BLOCK:]], axis=0).T.astype(BF16)
        first, second = o[:toks], o[toks:]
        cols = slice(pair * BLOCK, (pair + 1) * BLOCK)
        o_own[quad, 2 * duo + u, :, cols] = jnp.where(odd == 1, second, first)
        o_send[quad, 2 * duo + u, :, cols] = jnp.where(odd == 1, first, second)

    units = [(u, pair) for u in range(2) for pair in range(2)]
    total = quads * duos

    def each_chip(fn):
        for c in range(slots):
            pl.when(chip == c)(lambda c=c: fn(prefix + (c + 1) * BLOCK))

    def body(b, t):
        before, ahead, later = jnp.maximum(b - 1, 0), jnp.minimum(b + 1, total - 1), jnp.minimum(b + 2, total - 1)
        mix_stage(before, t, 0, 0)
        mix_stage(before, t, 0, 1)
        mix_stage(before, t, 1, 0)
        mix_stage(before, t, 1, 1)
        soft_stage(t, 0, 0)
        score_stage(ahead, t, 0, 0)
        value_stage(b, t, 0)
        soft_stage(t, 0, 1)
        score_stage(ahead, t, 0, 1)
        key_stage(later, t, 0)
        soft_stage(t, 1, 0)
        score_stage(ahead, t, 1, 0)
        value_stage(b, t, 1)
        soft_stage(t, 1, 1)
        score_stage(ahead, t, 1, 1)
        query_dot(later)
        query_stage(later)
        key_stage(later, t, 1)

    def at(b, when):
        return pl.when(b == when)

    agenda = {
        1: [(None, ring("R", "wq.a"), across(1, "wq.a") + ring("O", "wq.a"))],
        2: [(None, ring("R", "wq.b"), across(1, "wq.b") + ring("O", "wq.b") + ring("R", "wo.a", "wo.b") + ["wo.mR"])],
        3: [(None, ring("L", "wk.a", "wv.b"), across(2, "wk.a", "wv.b"))],
        4: [(None, across(1, *small), [])],
        5: [(None, ring("L", "wq.a"), across(2, "wq.a"))],
        6: [(None, ring("O", "wk.a", "wq.a"), across(3, "wk.a", "wq.a"))],
        7: [(None, ring("L", "wq.b"), across(2, "wq.b"))],
        8: [(None, ring("O", "wv.b", "wq.b"), across(3, "wv.b", "wq.b"))],
        10: [(None, across(2, *small), [])],
        11: [(None, ring("L", "wo.b"), across(2, "wo.b")), (1, [], ring("O", "wo.b"))],
        12: [(None, ring("R", "wo.a"), across(1, "wo.a")), (0, [], ring("O", "wo.a"))],
        15: [(None, across(3, *small), []), (None, ring("L", "wo.a"), across(2, "wo.a")), (1, [], ring("O", "wo.a"))],
        16: [(None, ring("R", "wo.b"), across(1, "wo.b")), (0, [], ring("O", "wo.b"))],
        19: [(0, ["wo.mR"], ["wo.mO"]), (1, ["wo.mL"], ["wo.mO"])],
        22: [(0, ring("O", "wo.a"), across(3, "wo.a") + ["wo.aS"]), (1, ring("O", "wo.b"), across(3, "wo.b") + ["wo.bS"])],
        23: [
            (0, ["wo.mL"], []),
            (1, ["wo.mR"], []),
            (None, across(1, "wo.a", "wo.b") + across(2, "wo.a", "wo.b"), ["woS1", "woS2"]),
        ],
        24: [(0, ring("O", "wo.b"), across(3, "wo.b") + ["wo.bS"]), (1, ring("O", "wo.a"), across(3, "wo.a") + ["wo.aS"])],
        29: [(None, ["wo.mO"], ["wo.mS"]), (None, across(3, "wo.a"), ["wo.aS~"])],
    }
    for quad in range(quads - 1):
        agenda.setdefault((quad + 1) * duos + 1, []).append((None, [], [f"o{quad}S"]))

    def run_agenda(when):
        for parity, waits, starts in agenda[when]:

            def item(waits=waits, starts=starts):
                with jax.named_scope(f"ev_{when}"):
                    wire.landed(*waits)
                wire.start(*starts)

            if parity is None:
                item()
            else:
                pl.when(odd == parity)(item)

    bounce = pltpu.make_async_copy(wo_hbm, wo_buf, load_sem.at[3])
    span = 8

    def step(b, _):
        for first in range(0, total, span):

            @pl.when(b // span == first // span)
            def _():
                if first == 0:

                    @at(b, 0)
                    def _():
                        with jax.named_scope('ev_k1'):
                            rest_of(1)

                    @at(b, 2)
                    def _():
                        with jax.named_scope('ev_k2'):
                            rest_of(2)
                        pltpu.make_async_copy(rows.at[:, pl.ds(prefix, chunk)], c_out, load_sem.at[0]).start()
                        pltpu.make_async_copy(rot.at[:, pl.ds(prefix, chunk)], p_out, load_sem.at[1]).start()
                        bounce.start()

                    @at(b, 6)
                    def _():
                        bounce.wait()
                        pltpu.make_async_copy(wo_buf, wo_out.at[odd, 0], load_sem.at[4]).start()

                for when in sorted(agenda):
                    if first <= when < first + span:
                        at(b, when)(functools.partial(run_agenda, when))

        with jax.named_scope('body'):
            each_chip(functools.partial(body, b))
        return 0

    def lead_in(t):
        for u in range(2):
            key_stage(0, t, u)
        for u, pair in units:
            score_stage(0, t, u, pair)
        for u in range(2):
            key_stage(1, t, u)
        query_dot(1)
        query_stage(1)

    wire.landed("q0S")
    query_dot(0)
    query_stage(0)
    rest_of(0)
    wire.landed(*ring("R", "wk.a", "wv.b"))
    wire.start(*across(1, "wk.a", "wv.b"), *ring("O", "wk.a", "wv.b"))
    with jax.named_scope('p_lead'):
        each_chip(lead_in)
    lax.fori_loop(0, total, step, 0)

    def last(t):
        for u, pair in units:
            mix_stage(total - 1, t, u, pair)

    with jax.named_scope('p_last'):
        each_chip(last)
        wire.start(f"o{quads - 1}S")
        pltpu.make_async_copy(o_own, o_out.at[odd], load_sem.at[2]).start()
    with jax.named_scope('f_land'):
        wire.landed(*across(3, "wo.b"))
        wire.start("wo.bS~")
        for place in range(slots - 1):
            wire.landed(f"woS{place}")
        wire.landed("wo.aS", "wo.bS", "wo.mS", "wo.aS~", "wo.bS~")
        for quad in range(quads):
            wire.landed(f"o{quad}S")
    with jax.named_scope('f_sent'):
        wire.sent(*wire.index)
        pltpu.make_async_copy(rows.at[:, pl.ds(prefix, chunk)], c_out, load_sem.at[0]).wait()
        pltpu.make_async_copy(rot.at[:, pl.ds(prefix, chunk)], p_out, load_sem.at[1]).wait()
        pltpu.make_async_copy(o_own, o_out.at[odd], load_sem.at[2]).wait()
        pltpu.make_async_copy(wo_buf, wo_out.at[odd, 0], load_sem.at[4]).wait()


def finish_kernel(
    len_ref, o_hbm, w_hbm, x_hbm, c_hbm, p_hbm, lat_hbm, pe_hbm, y_hbm, lat_out, pe_out, fresh, acc, x_buf, y_buf, o_buf, w_buf, c_buf, p_buf, lat_buf, pe_buf, lat_new, pe_new, load_sem, store_sem, sems
):
    chip = lax.axis_index("tp") // 2
    quads, seqs, toks, depth = o_hbm.shape[1:]
    terms = 2 * quads
    slots = c_hbm.shape[1]
    rank = lat_hbm.shape[2]
    rope, cache_len = pe_hbm.shape[1:]
    chunk = slots * 2 * toks
    words = rank // BLOCK
    dim = x_hbm.shape[2]
    part = 2 * depth
    ring = w_buf.shape[0]

    def loads(k, with_term):
        slot = lax.rem(k, ring)
        out = [
            pltpu.make_async_copy(c_hbm.at[k], c_buf.at[slot], load_sem.at[0, slot]),
            pltpu.make_async_copy(lat_hbm.at[k], lat_buf.at[slot], load_sem.at[1, slot]),
        ]
        if with_term:
            side, quad = k // quads, lax.rem(k, quads)
            out.append(pltpu.make_async_copy(o_hbm.at[side, quad], o_buf.at[slot], load_sem.at[2, slot]))
            out.append(pltpu.make_async_copy(w_hbm.at[side, pl.ds(pl.multiple_of(quad * depth, depth), depth)], w_buf.at[slot], load_sem.at[3, slot]))
        return out

    def store(k):
        slot = lax.rem(k, ring)
        return pltpu.make_async_copy(lat_new.at[slot], lat_out.at[k], store_sem.at[slot])

    load_x = pltpu.make_async_copy(x_hbm, x_buf, sems.at[0])
    load_p = pltpu.make_async_copy(p_hbm, p_buf, sems.at[1])
    load_pe = pltpu.make_async_copy(pe_hbm, pe_buf, sems.at[2])
    store_pe = pltpu.make_async_copy(pe_new, pe_out, sems.at[3])

    def store_y(n):
        cols = pl.ds(n * part, part)
        return pltpu.make_async_copy(y_buf.at[:, :, cols], y_hbm.at[:, :, cols], sems.at[4 + n])


    def slot_of(j):
        return lax.rem(chip - j + slots, slots)

    def project(k, kind):
        slot = lax.rem(k, ring)
        o = o_buf[slot].reshape(seqs * toks, depth)
        for n in range(0, dim, part):
            cols = slice(n, n + part)
            y = dot(o, w_buf[slot, :, cols])
            if kind != "first":
                y = acc[:, cols] + y
            if kind == "last":
                y = y + x_buf[:, :, cols].reshape(seqs * toks, part).astype(F32)
                y_buf[:, :, cols] = y.astype(BF16).reshape(seqs, toks, part)
                store_y(n // part).start()
            else:
                acc[:, cols] = y

    def cache(k):
        at_slot = lax.rem(k, ring)
        length = len_ref[k]
        for j in range(slots):
            piece = c_buf[at_slot, slot_of(j)].reshape(2 * toks, rank).astype(F32)
            for w in range(words):
                fresh[w, BLOCK + j * 2 * toks : BLOCK + (j + 1) * 2 * toks] = piece[:, w * BLOCK : (w + 1) * BLOCK]
        lat_new[at_slot] = lat_buf[at_slot]
        base = (length // 16) * 16
        skew = length - base
        tile_row = lax.broadcasted_iota(jnp.int32, (16, BLOCK), 0)
        for i in range(chunk // 16 + 1):
            at = pl.multiple_of(jnp.minimum(base + i * 16, cache_len - 16), 16)
            for w in range(words):
                cols = slice(w * BLOCK, (w + 1) * BLOCK)
                moved = fresh[w, pl.ds(BLOCK - skew + i * 16, 16), :].astype(BF16)
                if i == 0 or i == chunk // 16:
                    local = tile_row + (at - length)
                    shown = (local >= 0) & (local < chunk) if i == 0 else (local < chunk)
                    if i == 0:
                        rest = lat_buf[at_slot, pl.ds(at, 16), cols]
                    else:
                        shown = shown & (skew > 0)
                        rest = lat_new[at_slot, pl.ds(at, 16), cols]
                    moved = jnp.where(shown, moved.astype(F32), rest.astype(F32)).astype(BF16)
                lat_new[at_slot, pl.ds(at, 16), cols] = moved

        turned = jnp.concatenate([p_buf[k // (BLOCK // rope), slot_of(j)].reshape(2 * toks, BLOCK).astype(F32).T for j in range(slots)], axis=1)
        group = lax.rem(k, BLOCK // rope)
        mine = turned[:rope]
        for g in range(1, BLOCK // rope):
            mine = jnp.where(group == g, turned[g * rope : (g + 1) * rope], mine)
        mine = jnp.concatenate([mine, jnp.zeros((rope, cache_len - chunk), F32)], axis=1)
        mine = pltpu.roll(mine, length, axis=1)
        spot = lax.broadcasted_iota(jnp.int32, (rope, cache_len), 1) - length
        pe_new[k] = jnp.where((spot >= 0) & (spot < chunk), mine, pe_buf[k].astype(F32)).astype(BF16)

    def begin(k, with_term):
        for load in loads(k, with_term):
            load.start()

    def arrived(k, with_term):
        for load in loads(k, with_term):
            load.wait()

    def work(k, kind):
        if kind != "none":
            project(k, kind)
        cache(k)
        store(k).start()

    def more(k):
        pl.when(k < terms)(lambda: begin(k, True))
        pl.when((k >= terms) & (k < seqs))(lambda: begin(k, False))

    first = loads(0, True)
    for load in first[2:] + first[:2]:
        load.start()
    load_p.start()
    load_pe.start()
    for load in first[2:]:
        load.wait()
    begin(1, True)
    begin(2, True)
    project(0, "first")
    for load in first[:2] + [load_p, load_pe]:
        load.wait()
    begin(3, True)
    cache(0)
    store(0).start()
    load_x.start()

    def middle(k, _):
        with jax.named_scope('g_wait'):
            arrived(k, True)
        more(k + ring - 1)

        @pl.when(k >= ring)
        def _():
            store(k - ring).wait()

        with jax.named_scope('g_work'):
            work(k, "middle")
        return 0

    lax.fori_loop(1, terms - 1, middle, 0)
    last = terms - 1
    arrived(last, True)
    more(last + ring - 1)
    store(last - ring).wait()
    load_x.wait()
    with jax.named_scope('g_last'):
        work(last, "last")

    def tail(k, _):
        arrived(k, False)
        store(k - ring).wait()
        with jax.named_scope('g_tail'):
            work(k, "none")
        return 0

    lax.fori_loop(terms, seqs, tail, 0)
    store_pe.start()
    for k in range(ring):
        store(seqs - ring + k).wait()
    store_pe.wait()
    for n in range(dim // part):
        store_y(n).wait()


def solution(mesh):
    size = mesh.shape["tp"]
    count = mesh.shape["dp"]
    stride = 2 ** (count.bit_length() // 2)
    paired = {"a": count % 2 == 0, "b": count % (2 * stride) == 0}

    def local_step(hidden, lengths, rope_cos, rope_sin, cache_lat, cache_pe, norm_in, w_dq, norm_q, w_dkv, norm_kv, w_uq, w_uk, w_uv, w_out):
        seqs, toks, dim = hidden.shape
        q_rank = w_dq.shape[1]
        rank, heads, nope = w_uk.shape
        rope = cache_pe.shape[2]
        cache_len = cache_lat.shape[1]
        slots = size // 2
        head = nope + rope
        quads = slots * heads // 4
        chunk = size * toks
        prefix = cache_len - chunk
        per = BLOCK // rope
        groups = seqs // per
        wide = 2 * BLOCK
        cos_t, sin_t = rope_cos.transpose(0, 2, 1), rope_sin.transpose(0, 2, 1)
        pe_t = cache_pe.transpose(0, 2, 1)
        wdkv_t = w_dkv.transpose(1, 0)
        wq_t, wk_t, wv_t = (w.transpose(1, 2, 0) for w in (w_uq, w_uk, w_uv))

        copies = 15 * groups + 36 + 3 + slots + 4 + quads
        any_spec = pl.BlockSpec(memory_space=pl.ANY)
        vmem_spec = pl.BlockSpec(memory_space=pltpu.VMEM)
        smem_spec = pl.BlockSpec(memory_space=pltpu.SMEM)
        c_all, p_all, o_all, wo_all = pl.pallas_call(
            functools.partial(main_kernel, (size, stride, paired)),
            in_specs=[smem_spec, any_spec, vmem_spec, any_spec, vmem_spec, any_spec, vmem_spec] + [any_spec] * 8,
            out_specs=[any_spec] * 4,
            out_shape=[
                jax.ShapeDtypeStruct((seqs, chunk, rank), BF16),
                jax.ShapeDtypeStruct((groups, chunk, BLOCK), BF16),
                jax.ShapeDtypeStruct((2, quads, seqs, toks, 4 * nope), BF16),
                jax.ShapeDtypeStruct((2, slots) + w_out.shape, BF16),
            ],
            scratch_shapes=[
                pltpu.VMEM(hidden.shape, BF16),
                pltpu.VMEM(w_dq.shape, BF16),
                pltpu.VMEM(wdkv_t.shape, BF16),
                pltpu.VMEM((groups, per * toks, dim), BF16),
                pltpu.VMEM((seqs, cache_len, rank), BF16),
                pltpu.VMEM((groups, cache_len, BLOCK), BF16),
                pltpu.VMEM((seqs, rope, prefix), BF16),
                pltpu.VMEM((seqs, rope // 2, BLOCK), F32),
                pltpu.VMEM((seqs, rope // 2, BLOCK), F32),
                pltpu.VMEM((2, seqs, toks, q_rank), BF16),
                pltpu.VMEM((slots * heads, head, q_rank), BF16),
                pltpu.VMEM((slots * heads, 2 * nope, rank), BF16),
                [pltpu.VMEM((cache_len, 4 * nope), BF16) for _ in range(2)],
                [pltpu.VMEM((4 * nope, cache_len), BF16) for _ in range(2)],
                pltpu.VMEM((2, 2, wide, wide), BF16),
                pltpu.VMEM((4 * head, wide), F32),
                [pltpu.VMEM((cache_len, wide), F32) for _ in range(4)],
                pltpu.VMEM((4, 8, wide), F32),
                [pltpu.VMEM((cache_len, wide), BF16) for _ in range(4)],
                pltpu.VMEM((4, 8, wide), F32),
                pltpu.VMEM((quads, seqs, toks, 4 * nope), BF16),
                pltpu.VMEM((quads, seqs, toks, 4 * nope), BF16),
                pltpu.VMEM(w_out.shape, BF16),
                pltpu.SemaphoreType.DMA((9 + groups,)),
                pltpu.SemaphoreType.DMA((copies,)),
                pltpu.SemaphoreType.DMA((copies,)),
            ],
            compiler_params=pltpu.CompilerParams(collective_id=0, has_side_effects=True, vmem_limit_bytes=63 * MIB),
            cost_estimate=pl.CostEstimate(flops=70 * 10**9, bytes_accessed=40 * MIB, transcendentals=30 * 10**6),
            name="main",
        )(lengths, hidden, norm_in, w_dq, norm_q, wdkv_t, norm_kv, cos_t, sin_t, wq_t, wk_t, wv_t, w_out, cache_lat, pe_t)

        depth = 4 * nope
        ahead = 4
        y, lat_new, pe_new = pl.pallas_call(
            finish_kernel,
            in_specs=[smem_spec] + [any_spec] * 7,
            out_specs=[any_spec] * 3,
            scratch_shapes=[
                pltpu.VMEM((rank // BLOCK, chunk + 2 * BLOCK, BLOCK), F32),
                pltpu.VMEM((seqs * toks, dim), F32),
                pltpu.VMEM(hidden.shape, BF16),
                pltpu.VMEM(hidden.shape, BF16),
                pltpu.VMEM((ahead, seqs, toks, depth), BF16),
                pltpu.VMEM((ahead, depth, dim), BF16),
                pltpu.VMEM((ahead, slots, 2, toks, rank), BF16),
                pltpu.VMEM((groups, slots, 2, toks, BLOCK), BF16),
                pltpu.VMEM((ahead, cache_len, rank), BF16),
                pltpu.VMEM(pe_t.shape, BF16),
                pltpu.VMEM((ahead, cache_len, rank), BF16),
                pltpu.VMEM(pe_t.shape, BF16),
                pltpu.SemaphoreType.DMA((4, ahead)),
                pltpu.SemaphoreType.DMA((ahead,)),
                pltpu.SemaphoreType.DMA((4 + dim // (2 * depth),)),
            ],
            out_shape=[
                jax.ShapeDtypeStruct(hidden.shape, BF16),
                jax.ShapeDtypeStruct(cache_lat.shape, BF16),
                jax.ShapeDtypeStruct(pe_t.shape, BF16),
            ],
            compiler_params=pltpu.CompilerParams(vmem_limit_bytes=63 * MIB),
            cost_estimate=pl.CostEstimate(flops=2 * seqs * toks * dim * dim, bytes_accessed=50 * MIB, transcendentals=0),
            name="finish",
        )(
            lengths,
            o_all,
            wo_all.reshape(2, slots * w_out.shape[0], dim),
            hidden,
            c_all.reshape(seqs, slots, 2, toks, rank),
            p_all.reshape(groups, slots, 2, toks, BLOCK),
            cache_lat,
            pe_t,
        )
        return y, lat_new, pe_new.transpose(0, 2, 1)

    spec_tok = P("dp", "tp", None)
    spec_len = P("dp")
    spec_seq = P("dp", None, None)
    spec_vec = P(None)
    spec_mat = P(None, None)
    spec_head = P(None, "tp", None)
    spec_rows = P("tp", None)
    in_specs = (spec_tok, spec_len, spec_seq, spec_seq, spec_seq, spec_seq, spec_vec, spec_mat, spec_vec, spec_mat, spec_vec, spec_head, spec_head, spec_head, spec_rows)
    return jax.shard_map(local_step, mesh=mesh, in_specs=in_specs, out_specs=(spec_tok, spec_seq, spec_seq), check_vma=False)
```

```python
import functools

import jax
import jax.numpy as jnp
from jax import lax
from jax.experimental import pallas as pl
from jax.experimental.pallas import tpu as pltpu
from jax.sharding import PartitionSpec as P

BLOCK = 128
LOG2E = 1.4426950408889634
NEVER = -1e30
NORM_ROWS = 16
F32 = jnp.float32
BF16 = jnp.bfloat16
MESH = pl.DeviceIdType.MESH
MIB = 2**20


def dot(a, b):
    return lax.dot_general(a, b, (((1,), (0,)), ((), ())), preferred_element_type=F32)


def dot_t(a, b):
    return lax.dot_general(a, b, (((1,), (1,)), ((), ())), preferred_element_type=F32)


def unit(x):
    return x * lax.rsqrt(jnp.mean(x * x, axis=-1, keepdims=True) + 1e-6)


class Wire:
    def __init__(self, send_sem, recv_sem):
        self.sems = (send_sem, recv_sem)
        self.made = {}
        self.index = {}

    def add(self, name, src, dst, **peer):
        self.index[name] = len(self.index)
        self.made[name] = lambda: pltpu.make_async_remote_copy(
            src(), dst(), self.sems[0].at[self.index[name]], self.sems[1].at[self.index[name]], device_id=peer, device_id_type=MESH
        )

    def start(self, *names):
        for name in names:
            self.made[name]().start()

    def landed(self, *names):
        for name in names:
            self.made[name]().wait_recv()

    def sent(self, *names):
        for name in names:
            self.made[name]().wait_send()


def main_kernel(
    plan,
    len_hbm,
    x_hbm,
    g1_hbm,
    wdq_hbm,
    gq_hbm,
    wdkv_hbm,
    gkv_hbm,
    cos_hbm,
    sin_hbm,
    wq_hbm,
    wk_hbm,
    wv_hbm,
    wo_hbm,
    lat_hbm,
    pe_hbm,
    c_out,
    p_out,
    o_out,
    wo_out,
    x_buf,
    wdq,
    wdkv,
    a_buf,
    rows,
    rot,
    pe_buf,
    cos_ref,
    sin_ref,
    cq_buf,
    wq,
    wkv,
    kb,
    vb,
    qb,
    q_raw,
    sb,
    mb,
    pb,
    lb,
    o_own,
    o_send,
    wo_buf,
    len_ref,
    g1_ref,
    gq_ref,
    gkv_ref,
    load_sem,
    send_sem,
    recv_sem,
):
    size, stride, paired = plan
    me = lax.axis_index("tp")
    odd = lax.rem(me, 2)
    chip = me // 2
    right, left = lax.rem(me + 2, size), lax.rem(me + size - 2, size)
    onward = jnp.where(odd == 0, right, left)
    other = me + 1 - 2 * odd
    dp = lax.axis_index("dp")
    flip = {"a": lax.rem(dp, 2), "b": lax.rem(dp // stride, 2)}
    partner = {"a": dp + 1 - 2 * flip["a"], "b": dp + stride * (1 - 2 * flip["b"])}

    seqs, toks, dim = x_hbm.shape
    groups = rot.shape[0]
    per = seqs // groups
    rank = rows.shape[2]
    slots = size // 2
    chunk = size * toks
    prefix = rows.shape[1] - chunk
    heads = wq.shape[0] // slots
    head, q_rank = wq.shape[1:]
    rope = BLOCK // per
    half = rope // 2
    nope = head - rope
    quads = wq.shape[0] // 4
    duos = seqs // 2
    wide = 2 * BLOCK
    factor = LOG2E * head**-0.5

    loads = {}

    def load(name, src, dst):
        loads[name] = pltpu.make_async_copy(src, dst, load_sem.at[len(loads)])
        loads[name].start()

    def spot(slot, parity):
        return pl.ds(pl.multiple_of(prefix + slot * BLOCK + parity * toks, toks), toks)

    barrier = pltpu.get_barrier_semaphore()
    for peer in (left, right, other):
        pl.semaphore_signal(barrier, inc=1, device_id={"tp": peer}, device_id_type=MESH)
    for side in "ab":
        if paired[side]:
            pl.semaphore_signal(barrier, inc=1, device_id={"dp": partner[side]}, device_id_type=MESH)

    lanes_chip = pl.ds(pl.multiple_of(chip * BLOCK, BLOCK), BLOCK)
    def load_x(g):
        load(f"x{g}", x_hbm.at[pl.ds(g * per, per)], x_buf.at[pl.ds(g * per, per)])

    load("g1", g1_hbm, g1_ref)
    load_x(0)
    load("wdkv", wdkv_hbm, wdkv)
    load("gkv", gkv_hbm, gkv_ref)
    load("gq", gq_hbm, gq_ref)
    load("len", len_hbm, len_ref)
    load("cos", cos_hbm.at[:, :, lanes_chip], cos_ref)
    load("sin", sin_hbm.at[:, :, lanes_chip], sin_ref)

    wire = Wire(send_sem, recv_sem)

    def chain(name, here, there, places, via="split", whole=True):
        near_left, near_right, opposite = places
        handed = {"right": near_left, "left": near_right, "split": jnp.where(odd == 0, near_left, near_right)}[via]
        if whole:
            wire.add(name + "R", lambda: here(0), lambda: there(near_left), tp=right)
        wire.add(name + "L", lambda: here(0), lambda: there(near_right), tp=left)
        wire.add(name + "O", lambda: there(handed), lambda: there(opposite), tp={"right": right, "left": left, "split": onward}[via])

    for g in range(groups):
        for name, ref in (("c", lambda slot, g=g: rows.at[pl.ds(g * per, per), spot(slot, odd)]), ("p", lambda slot, g=g: rot.at[g, spot(slot, odd)])):
            name = f"{name}{g}"
            chain(name, ref, ref, (1, 3, 2), "left")
            for slot in range(slots):
                wire.add(f"{name}S{slot}", functools.partial(ref, slot), functools.partial(ref, slot), tp=other)
        cq_ref = lambda g=g: cq_buf.at[odd, pl.ds(g * per, per)]
        wire.add(f"q{g}S", cq_ref, cq_ref, tp=other)

    def cut(side, low, high, unit, mine):
        half_size = (high - low) // 2
        which = flip[side] if mine else 1 - flip[side]
        return pl.ds(pl.multiple_of(low + which * half_size, unit), half_size)

    q_cut = head * 2 // 3
    o_cut = wo_hbm.shape[0] * 2 // 5
    lots = {"R": (0, 3), "r": (3, heads - 3)}
    everyone = (0, heads)

    def lot_of(place, lot):
        return pl.ds(place * heads + lot[0], lot[1])

    pieces = {
        "wq.a": (lambda r, lot: wq_hbm.at[pl.ds(*lot), r], lambda place, r, lot: wq.at[lot_of(place, lot), r], ("a", 0, q_cut, 16)),
        "wq.b": (lambda r, lot: wq_hbm.at[pl.ds(*lot), r], lambda place, r, lot: wq.at[lot_of(place, lot), r], ("b", q_cut, head, 16)),
        "wk.a": (
            lambda r, lot: wk_hbm.at[pl.ds(*lot), :, r],
            lambda place, r, lot: wkv.at[lot_of(place, lot), pl.ds(0, nope), r],
            ("a", 0, rank, BLOCK),
        ),
        "wv.b": (
            lambda r, lot: wv_hbm.at[pl.ds(*lot), :, r],
            lambda place, r, lot: wkv.at[lot_of(place, lot), pl.ds(nope, nope), r],
            ("b", 0, rank, BLOCK),
        ),
        "wo.a": (lambda r, lot: wo_hbm.at[r], lambda place, r, lot: wo_out.at[odd, place, r], ("a", 0, o_cut, 16)),
        "wo.b": (lambda r, lot: wo_hbm.at[r], lambda place, r, lot: wo_out.at[odd, place, r], ("b", o_cut, 2 * o_cut, 16)),
    }
    left_over = pl.ds(2 * o_cut, wo_hbm.shape[0] - 2 * o_cut)
    chain("wo.m", lambda place: wo_hbm.at[left_over], lambda place: wo_out.at[odd, place, left_over], (1, 2, 3))
    for piece, (source, target, bounds) in pieces.items():
        side = bounds[0]
        large = piece.startswith("wo")
        for mine in (True,) if paired[side] else (True, False):
            here = lambda place, lot=everyone, source=source, bounds=bounds, mine=mine: source(cut(*bounds, mine), lot)
            there = lambda place, lot=everyone, target=target, bounds=bounds, mine=mine: target(place, cut(*bounds, mine), lot)
            name = piece + ("" if mine else "~")
            chain(name, here, there, (1, 2, 3), "split" if large else "right", large)
            if not large:
                for way, lot in lots.items():
                    wire.add(name + way, functools.partial(here, 0, lot), functools.partial(there, 1, lot), tp=right)
        if paired[side]:
            for place, tag, lot in ((1, "", everyone),) if large else ((1, "", lots["R"]), (1, "r", lots["r"])):
                ref = lambda place=place, lot=lot, target=target, bounds=bounds: target(place, cut(*bounds, True), lot)
                wire.add(f"{piece}X{place}{tag}", ref, ref, dp=partner[side])
            for place in (2, 3):
                ref = lambda place=place, target=target, bounds=bounds: target(place, cut(*bounds, True), everyone)
                wire.add(f"{piece}X{place}", ref, ref, dp=partner[side])
    for place in range(slots - 1):
        ref = lambda place=place: wo_out.at[odd, place]
        wire.add(f"woS{place}", ref if place else lambda: wo_hbm, ref, tp=other)
    for piece in ("wo.a", "wo.b"):
        for mine in (True, False):
            ref = lambda piece=piece, mine=mine: pieces[piece][1](slots - 1, cut(*pieces[piece][2], mine), everyone)
            wire.add(f"{piece}S" + ("" if mine else "~"), ref, ref, tp=other)
    ref = lambda: wo_out.at[odd, slots - 1, left_over]
    wire.add("wo.mS", ref, ref, tp=other)
    for quad in range(quads - 1):
        wire.add(f"o{quad}S", lambda quad=quad: o_send.at[quad], lambda quad=quad: o_out.at[odd, quad], tp=other)
    cut_o = seqs - 4
    for name, part in (("o.a", pl.ds(0, cut_o)), ("o.b", pl.ds(cut_o, seqs - cut_o))):
        wire.add(name + "S", lambda part=part: o_send.at[quads - 1, part], lambda part=part: o_out.at[odd, quads - 1, part], tp=other)

    small = ("wk.a", "wv.b", "wq.a", "wq.b")

    def ring(which, *kinds):
        return [f"{kind}{half_name}{way}" for kind in kinds for half_name in ("", "~")[: 1 if paired[kind[-1]] else 2] for way in which]

    def across(place, *kinds):
        return [f"{kind}X{place}" for kind in kinds if paired[kind[-1]]]

    def norm(g):
        for r in range(per):
            for at in range(0, toks, NORM_ROWS):
                x = x_buf[g * per + r, at : at + NORM_ROWS].astype(F32)
                a_buf[g, r * toks + at : r * toks + at + NORM_ROWS] = (unit(x) * g1_ref[...]).astype(BF16)

    def latent(g):
        kv = dot_t(a_buf[g], wdkv[...])
        rows[g * per : (g + 1) * per, spot(0, odd), :] = (unit(kv[:, :rank]) * gkv_ref[...]).astype(BF16).reshape(per, toks, rank)
        turned = []
        for s in range(per):
            cos_pair, sin_pair = cos_ref[g * per + s], sin_ref[g * per + s]
            cos = jnp.where(odd == 1, cos_pair[:, toks:], cos_pair[:, :toks])
            sin = jnp.where(odd == 1, sin_pair[:, toks:], sin_pair[:, :toks])
            table = jnp.concatenate([cos, cos, -sin, sin], axis=0).T
            p = kv[s * toks : (s + 1) * toks, rank:]
            swapped = jnp.concatenate([p[:, half:], p[:, :half]], axis=1)
            turned.append(p * table[:, :rope] + swapped * table[:, rope:])
        rot[g, spot(0, odd), :] = jnp.concatenate(turned, axis=1).astype(BF16)

    def queries(g):
        h = jnp.concatenate([dot(a_buf[g], wdq[:, : 2 * rank]), dot(a_buf[g], wdq[:, 2 * rank :])], axis=1)
        cq_buf[odd, g * per : (g + 1) * per] = (unit(h) * gq_ref[...]).astype(BF16).reshape(per, toks, q_rank)

    loads["g1"].wait()
    with jax.named_scope('p_norm0'):
        loads["x0"].wait()
        for g in range(1, groups):
            load_x(g)
        norm(0)
    for name in ("wdkv", "cos", "sin", "gkv", "gq", "len"):
        loads[name].wait()
    load("wdq", wdq_hbm, wdq)
    load("wk", wk_hbm, wkv.at[pl.ds(0, heads), pl.ds(0, nope)])
    load("wv", wv_hbm, wkv.at[pl.ds(0, heads), pl.ds(nope, nope)])
    load("wq", wq_hbm, wq.at[pl.ds(0, heads)])
    load("pe", pe_hbm.at[:, :, pl.ds(0, prefix)], pe_buf)
    load("lat", lat_hbm.at[:, pl.ds(0, prefix)], rows.at[:, pl.ds(0, prefix)])
    with jax.named_scope('p_bar'):
        pl.semaphore_wait(barrier, 3 + paired["a"] + paired["b"])
    with jax.named_scope('p_kv'):
        for g in range(groups):
            latent(g)
            for way in ("R", "L", "S0"):
                wire.start(f"c{g}{way}", f"p{g}{way}")
            if g + 1 < groups:
                loads[f"x{g + 1}"].wait()
                norm(g + 1)
    wire.start(*ring("R", *small), *ring("r", *small))

    def hand_on(g):
        wire.landed(f"c{g}L", f"p{g}L", f"c{g}R", f"p{g}R")
        wire.start(f"c{g}O", f"p{g}O", f"c{g}S3", f"p{g}S3", f"c{g}S1", f"p{g}S1")

    with jax.named_scope('p_cq'):
        loads["wdq"].wait()
        for g in range(groups):
            queries(g)
            wire.start(f"q{g}S")
            hand_on(g)
    wire.start(*ring("L", *small, "wo.b", "wo.a"), "wo.mL", "woS0")

    loads["pe"].wait()
    for g in range(groups):
        old = pe_buf[g * per : (g + 1) * per].reshape(per * rope, prefix).astype(F32)
        for b in range(prefix // BLOCK):
            rot[g, b * BLOCK : (b + 1) * BLOCK] = old[:, b * BLOCK : (b + 1) * BLOCK].T.astype(BF16)
    qb[...] = jnp.zeros_like(qb)

    def rest_of(g):
        wire.landed(f"c{g}O", f"p{g}O")
        wire.start(f"c{g}S2", f"p{g}S2")
        for slot in (0, 1, 3, 2):
            wire.landed(f"c{g}S{slot}", f"p{g}S{slot}")
        if g:
            wire.landed(f"q{g}S")

    with jax.named_scope('p_rest0'):
        for name in ("wk", "wv", "wq", "lat"):
            loads[name].wait()
    row = lax.broadcasted_iota(jnp.int32, (BLOCK, wide), 0)
    lane = lax.rem(lax.broadcasted_iota(jnp.int32, (BLOCK, wide), 1), BLOCK)
    near = row <= lane

    def place(n):
        return n // duos, lax.rem(n, duos)

    def query_dot(n):
        quad, duo = place(n)
        w = wq[pl.ds(quad * 4, 4)].reshape(4 * head, q_rank)
        cq = jnp.concatenate([cq_buf[parity, 2 * duo + u] for u in range(2) for parity in range(2)], axis=0)
        q_raw[...] = dot_t(w, cq)

    def query_stage(n):
        quad, duo = place(n)
        raw = q_raw
        for u in range(2):
            slot = 2 * lax.rem(duo, 2) + u
            cos, sin = cos_ref[2 * duo + u], sin_ref[2 * duo + u]
            for h in range(4):
                pair, side = h // 2, h % 2
                q = raw[h * head : (h + 1) * head, u * BLOCK : (u + 1) * BLOCK]
                cols = slice(side * BLOCK, (side + 1) * BLOCK)
                qb[u, pair, side * nope : (side + 1) * nope, cols] = q[:nope].astype(BF16)
                lo, hi = q[nope : nope + half], q[nope + half :]
                turned = jnp.concatenate([lo * cos - hi * sin, hi * cos + lo * sin], axis=0).astype(BF16)
                start = pl.multiple_of(BLOCK + slot * rope, rope)
                stale = pl.multiple_of(BLOCK + lax.rem(slot + 2, 4) * rope, rope)
                qb[u, pair, pl.ds(start, rope), cols] = turned
                qb[u, pair, pl.ds(stale, rope), cols] = jnp.zeros_like(turned)

    def key_stage(n, t, u):
        quad, duo = place(n)
        w = wkv[pl.ds(quad * 4, 4), :nope].reshape(4 * nope, rank)
        kb[u][:t] = dot_t(rows[2 * duo + u, :t], w).astype(BF16)

    def value_stage(n, t, u):
        quad, duo = place(n)
        w = wkv[pl.ds(quad * 4, 4), nope:].reshape(4 * nope, rank)
        vb[u][:, :t] = dot_t(w, rows[2 * duo + u, :t]).astype(BF16)

    def score_stage(n, t, u, pair):
        _, duo = place(n)
        length = len_ref[2 * duo + u]
        keys = jnp.concatenate([kb[u][:t, pair * BLOCK : (pair + 1) * BLOCK], rot[duo // 2, :t]], axis=1)
        value = dot(keys, qb[u, pair])
        most = None
        for b in range(t // BLOCK):
            part = value[b * BLOCK : (b + 1) * BLOCK]
            if BLOCK <= b * BLOCK < prefix:
                part = jnp.where(row < length - b * BLOCK, part, NEVER)
            if b * BLOCK == prefix:
                part = jnp.where(near, part, NEVER)
            sb[2 * u + pair][b * BLOCK : (b + 1) * BLOCK] = part
            part = jnp.max(part.reshape(BLOCK // 8, 8, wide), axis=0)
            most = part if most is None else jnp.maximum(most, part)
        mb[2 * u + pair] = jnp.broadcast_to(jnp.max(most, axis=0, keepdims=True), (8, wide))

    def soft_stage(t, u, pair):
        i = 2 * u + pair
        most = mb[i, :1]
        total = None
        for b in range(t // BLOCK):
            x = jnp.exp2((sb[i][b * BLOCK : (b + 1) * BLOCK] - most) * factor)
            part = jnp.sum(x.reshape(BLOCK // 8, 8, wide), axis=0)
            total = part if total is None else total + part
            pb[i][b * BLOCK : (b + 1) * BLOCK] = x.astype(BF16)
        lb[i] = total

    def mix_stage(n, t, u, pair):
        quad, duo = place(n)
        i = 2 * u + pair
        inv = 1.0 / jnp.sum(lb[i], axis=0, keepdims=True)
        o = dot(vb[u][pair * BLOCK : (pair + 1) * BLOCK, :t], pb[i][:t]) * inv
        o = jnp.concatenate([o[:nope, :BLOCK], o[nope:, BLOCK:]], axis=0).T.astype(BF16)
        first, second = o[:toks], o[toks:]
        cols = slice(pair * BLOCK, (pair + 1) * BLOCK)
        o_own[quad, 2 * duo + u, :, cols] = jnp.where(odd == 1, second, first)
        o_send[quad, 2 * duo + u, :, cols] = jnp.where(odd == 1, first, second)

    units = [(u, pair) for u in range(2) for pair in range(2)]
    total = quads * duos

    def each_chip(fn):
        for c in range(slots):
            pl.when(chip == c)(lambda c=c: fn(prefix + (c + 1) * BLOCK))

    def body(b, t):
        before, ahead, later = jnp.maximum(b - 1, 0), jnp.minimum(b + 1, total - 1), jnp.minimum(b + 2, total - 1)
        mix_stage(before, t, 0, 0)
        mix_stage(before, t, 0, 1)
        mix_stage(before, t, 1, 0)
        mix_stage(before, t, 1, 1)
        soft_stage(t, 0, 0)
        score_stage(ahead, t, 0, 0)
        value_stage(b, t, 0)
        soft_stage(t, 0, 1)
        score_stage(ahead, t, 0, 1)
        key_stage(later, t, 0)
        soft_stage(t, 1, 0)
        score_stage(ahead, t, 1, 0)
        value_stage(b, t, 1)
        soft_stage(t, 1, 1)
        score_stage(ahead, t, 1, 1)
        query_dot(later)
        query_stage(later)
        key_stage(later, t, 1)

    def at(b, when):
        return pl.when(b == when)

    agenda = {
        0: [(None, ring("R", "wq.a", "wq.b"), across(1, "wq.a", "wq.b"))],
        2: [(None, ring("r", *small), across("1r", *small) + ring("O", *small) + ring("R", "wo.a", "wo.b") + ["wo.mR"])],
        3: [(None, ring("L", "wk.a", "wv.b"), across(2, "wk.a", "wv.b"))],
        4: [(None, across(1, *small), [])],
        5: [(None, ring("L", "wq.a"), across(2, "wq.a"))],
        7: [(None, ring("L", "wq.b"), across(2, "wq.b"))],
        9: [(None, ring("O", *small), across(3, *small))],
        10: [(None, across("1r", *small) + across(2, *small), [])],
        11: [(None, ring("L", "wo.b"), across(2, "wo.b")), (1, [], ring("O", "wo.b"))],
        12: [(None, ring("R", "wo.a"), across(1, "wo.a")), (0, [], ring("O", "wo.a"))],
        15: [(None, across(3, *small), []), (None, ring("L", "wo.a"), across(2, "wo.a")), (1, [], ring("O", "wo.a"))],
        16: [(None, ring("R", "wo.b"), across(1, "wo.b")), (0, [], ring("O", "wo.b"))],
        19: [(0, ["wo.mR"], ["wo.mO"]), (1, ["wo.mL"], ["wo.mO"])],
        22: [(0, ring("O", "wo.a"), across(3, "wo.a") + ["wo.aS"]), (1, ring("O", "wo.b"), across(3, "wo.b") + ["wo.bS"])],
        23: [
            (0, ["wo.mL"], []),
            (1, ["wo.mR"], []),
            (None, across(1, "wo.a", "wo.b") + across(2, "wo.a", "wo.b"), ["woS1", "woS2"]),
        ],
        24: [(0, ring("O", "wo.b"), across(3, "wo.b") + ["wo.bS"]), (1, ring("O", "wo.a"), across(3, "wo.a") + ["wo.aS"])],
        29: [(None, ["wo.mO"], ["wo.mS"]), (None, across(3, "wo.a", "wo.b"), ["wo.aS~", "wo.bS~", "o.aS"])],
    }
    for quad in range(quads - 1):
        agenda.setdefault((quad + 1) * duos + 1, []).append((None, [], [f"o{quad}S"]))

    def run_agenda(when):
        for parity, waits, starts in agenda[when]:

            def item(waits=waits, starts=starts):
                with jax.named_scope(f"ev_{when}"):
                    wire.landed(*waits)
                wire.start(*starts)

            if parity is None:
                item()
            else:
                pl.when(odd == parity)(item)

    bounce = pltpu.make_async_copy(wo_hbm, wo_buf, load_sem.at[3])
    span = 8

    def step(b, _):
        for first in range(0, total, span):

            @pl.when(b // span == first // span)
            def _():
                for when in sorted(agenda):
                    if first <= when < first + span:
                        at(b, when)(functools.partial(run_agenda, when))
                if first == 0:

                    @at(b, 0)
                    def _():
                        with jax.named_scope('ev_k1'):
                            rest_of(1)

                    @at(b, 2)
                    def _():
                        with jax.named_scope('ev_k2'):
                            rest_of(2)
                        pltpu.make_async_copy(rows.at[:, pl.ds(prefix, chunk)], c_out, load_sem.at[0]).start()
                        pltpu.make_async_copy(rot.at[:, pl.ds(prefix, chunk)], p_out, load_sem.at[1]).start()
                        bounce.start()

                    @at(b, 6)
                    def _():
                        bounce.wait()
                        pltpu.make_async_copy(wo_buf, wo_out.at[odd, 0], load_sem.at[4]).start()

        with jax.named_scope('body'):
            each_chip(functools.partial(body, b))
        return 0

    def lead_in(t):
        for u in range(2):
            key_stage(0, t, u)
        for u, pair in units:
            score_stage(0, t, u, pair)
        for u in range(2):
            key_stage(1, t, u)
        query_dot(1)
        query_stage(1)

    wire.landed("q0S")
    query_dot(0)
    query_stage(0)
    rest_of(0)
    wire.landed(*ring("R", "wk.a", "wv.b"))
    wire.start(*across(1, "wk.a", "wv.b"))
    with jax.named_scope('p_lead'):
        each_chip(lead_in)
    lax.fori_loop(0, total, step, 0)

    def last(t):
        for u, pair in units:
            mix_stage(total - 1, t, u, pair)

    with jax.named_scope('p_last'):
        each_chip(last)
        wire.start("o.bS")
        pltpu.make_async_copy(o_own, o_out.at[odd], load_sem.at[2]).start()
    with jax.named_scope('f_land'):
        for place in range(slots - 1):
            wire.landed(f"woS{place}")
        wire.landed("wo.aS", "wo.bS", "wo.mS", "wo.aS~", "wo.bS~")
        for quad in range(quads - 1):
            wire.landed(f"o{quad}S")
        wire.landed("o.aS", "o.bS")
    with jax.named_scope('f_sent'):
        wire.sent(*wire.index)
        pltpu.make_async_copy(rows.at[:, pl.ds(prefix, chunk)], c_out, load_sem.at[0]).wait()
        pltpu.make_async_copy(rot.at[:, pl.ds(prefix, chunk)], p_out, load_sem.at[1]).wait()
        pltpu.make_async_copy(o_own, o_out.at[odd], load_sem.at[2]).wait()
        pltpu.make_async_copy(wo_buf, wo_out.at[odd, 0], load_sem.at[4]).wait()


def finish_kernel(
    len_ref, o_hbm, w_hbm, x_hbm, c_hbm, p_hbm, lat_hbm, pe_hbm, y_hbm, lat_out, pe_out, fresh, acc, x_buf, y_buf, o_buf, w_buf, c_buf, p_buf, lat_buf, pe_buf, lat_new, pe_new, load_sem, store_sem, sems
):
    chip = lax.axis_index("tp") // 2
    quads, seqs, toks, depth = o_hbm.shape[1:]
    terms = 2 * quads
    slots = c_hbm.shape[1]
    rank = lat_hbm.shape[2]
    rope, cache_len = pe_hbm.shape[1:]
    chunk = slots * 2 * toks
    words = rank // BLOCK
    dim = x_hbm.shape[2]
    part = 2 * depth
    ring = w_buf.shape[0]

    def loads(k, with_term):
        slot = lax.rem(k, ring)
        out = [
            pltpu.make_async_copy(c_hbm.at[k], c_buf.at[slot], load_sem.at[0, slot]),
            pltpu.make_async_copy(lat_hbm.at[k], lat_buf.at[slot], load_sem.at[1, slot]),
        ]
        if with_term:
            side, quad = k // quads, lax.rem(k, quads)
            out.append(pltpu.make_async_copy(o_hbm.at[side, quad], o_buf.at[slot], load_sem.at[2, slot]))
            out.append(pltpu.make_async_copy(w_hbm.at[side, pl.ds(pl.multiple_of(quad * depth, depth), depth)], w_buf.at[slot], load_sem.at[3, slot]))
        return out

    def store(k):
        slot = lax.rem(k, ring)
        return pltpu.make_async_copy(lat_new.at[slot], lat_out.at[k], store_sem.at[slot])

    load_x = pltpu.make_async_copy(x_hbm, x_buf, sems.at[0])
    load_p = pltpu.make_async_copy(p_hbm, p_buf, sems.at[1])
    load_pe = pltpu.make_async_copy(pe_hbm, pe_buf, sems.at[2])
    store_pe = pltpu.make_async_copy(pe_new, pe_out, sems.at[3])

    def store_y(n):
        cols = pl.ds(n * part, part)
        return pltpu.make_async_copy(y_buf.at[:, :, cols], y_hbm.at[:, :, cols], sems.at[4 + n])


    def slot_of(j):
        return lax.rem(chip - j + slots, slots)

    def project(k, kind):
        slot = lax.rem(k, ring)
        o = o_buf[slot].reshape(seqs * toks, depth)
        for n in range(0, dim, part):
            cols = slice(n, n + part)
            y = dot(o, w_buf[slot, :, cols])
            if kind != "first":
                y = acc[:, cols] + y
            if kind == "last":
                y = y + x_buf[:, :, cols].reshape(seqs * toks, part).astype(F32)
                y_buf[:, :, cols] = y.astype(BF16).reshape(seqs, toks, part)
                store_y(n // part).start()
            else:
                acc[:, cols] = y

    def cache(k):
        at_slot = lax.rem(k, ring)
        length = len_ref[k]
        for j in range(slots):
            piece = c_buf[at_slot, slot_of(j)].reshape(2 * toks, rank).astype(F32)
            for w in range(words):
                fresh[w, BLOCK + j * 2 * toks : BLOCK + (j + 1) * 2 * toks] = piece[:, w * BLOCK : (w + 1) * BLOCK]
        lat_new[at_slot] = lat_buf[at_slot]
        base = (length // 16) * 16
        skew = length - base
        tile_row = lax.broadcasted_iota(jnp.int32, (16, BLOCK), 0)
        for i in range(chunk // 16 + 1):
            at = pl.multiple_of(jnp.minimum(base + i * 16, cache_len - 16), 16)
            for w in range(words):
                cols = slice(w * BLOCK, (w + 1) * BLOCK)
                moved = fresh[w, pl.ds(BLOCK - skew + i * 16, 16), :].astype(BF16)
                if i == 0 or i == chunk // 16:
                    local = tile_row + (at - length)
                    shown = (local >= 0) & (local < chunk) if i == 0 else (local < chunk)
                    if i == 0:
                        rest = lat_buf[at_slot, pl.ds(at, 16), cols]
                    else:
                        shown = shown & (skew > 0)
                        rest = lat_new[at_slot, pl.ds(at, 16), cols]
                    moved = jnp.where(shown, moved.astype(F32), rest.astype(F32)).astype(BF16)
                lat_new[at_slot, pl.ds(at, 16), cols] = moved

        turned = jnp.concatenate([p_buf[k // (BLOCK // rope), slot_of(j)].reshape(2 * toks, BLOCK).astype(F32).T for j in range(slots)], axis=1)
        group = lax.rem(k, BLOCK // rope)
        mine = turned[:rope]
        for g in range(1, BLOCK // rope):
            mine = jnp.where(group == g, turned[g * rope : (g + 1) * rope], mine)
        mine = jnp.concatenate([mine, jnp.zeros((rope, cache_len - chunk), F32)], axis=1)
        mine = pltpu.roll(mine, length, axis=1)
        spot = lax.broadcasted_iota(jnp.int32, (rope, cache_len), 1) - length
        pe_new[k] = jnp.where((spot >= 0) & (spot < chunk), mine, pe_buf[k].astype(F32)).astype(BF16)

    def begin(k, with_term):
        for load in loads(k, with_term):
            load.start()

    def arrived(k, with_term):
        for load in loads(k, with_term):
            load.wait()

    def work(k, kind):
        if kind != "none":
            project(k, kind)
        cache(k)
        store(k).start()

    def more(k):
        pl.when(k < terms)(lambda: begin(k, True))
        pl.when((k >= terms) & (k < seqs))(lambda: begin(k, False))

    first = loads(0, True)
    for load in first[2:] + first[:2]:
        load.start()
    load_p.start()
    load_pe.start()
    for load in first[2:]:
        load.wait()
    begin(1, True)
    begin(2, True)
    project(0, "first")
    for load in first[:2] + [load_p, load_pe]:
        load.wait()
    begin(3, True)
    cache(0)
    store(0).start()
    load_x.start()

    def middle(k, _):
        with jax.named_scope('g_wait'):
            arrived(k, True)
        more(k + ring - 1)

        @pl.when(k >= ring)
        def _():
            store(k - ring).wait()

        with jax.named_scope('g_work'):
            work(k, "middle")
        return 0

    lax.fori_loop(1, terms - 1, middle, 0)
    last = terms - 1
    arrived(last, True)
    more(last + ring - 1)
    store(last - ring).wait()
    load_x.wait()
    with jax.named_scope('g_last'):
        work(last, "last")

    def tail(k, _):
        arrived(k, False)
        store(k - ring).wait()
        with jax.named_scope('g_tail'):
            work(k, "none")
        return 0

    lax.fori_loop(terms, seqs, tail, 0)
    store_pe.start()
    for k in range(ring):
        store(seqs - ring + k).wait()
    store_pe.wait()
    for n in range(dim // part):
        store_y(n).wait()


def solution(mesh):
    size = mesh.shape["tp"]
    count = mesh.shape["dp"]
    stride = 2 ** (count.bit_length() // 2)
    paired = {"a": count % 2 == 0, "b": count % (2 * stride) == 0}

    def local_step(hidden, lengths, rope_cos, rope_sin, cache_lat, cache_pe, norm_in, w_dq, norm_q, w_dkv, norm_kv, w_uq, w_uk, w_uv, w_out):
        seqs, toks, dim = hidden.shape
        q_rank = w_dq.shape[1]
        rank, heads, nope = w_uk.shape
        rope = cache_pe.shape[2]
        cache_len = cache_lat.shape[1]
        slots = size // 2
        head = nope + rope
        quads = slots * heads // 4
        chunk = size * toks
        prefix = cache_len - chunk
        per = BLOCK // rope
        groups = seqs // per
        wide = 2 * BLOCK
        cos_t, sin_t = rope_cos.transpose(0, 2, 1), rope_sin.transpose(0, 2, 1)
        pe_t = cache_pe.transpose(0, 2, 1)
        wdkv_t = w_dkv.transpose(1, 0)
        wq_t, wk_t, wv_t = (w.transpose(1, 2, 0) for w in (w_uq, w_uk, w_uv))

        copies = 15 * groups + 36 + 8 + 3 + slots + 4 + quads + 1
        any_spec = pl.BlockSpec(memory_space=pl.ANY)
        smem_spec = pl.BlockSpec(memory_space=pltpu.SMEM)
        c_all, p_all, o_all, wo_all = pl.pallas_call(
            functools.partial(main_kernel, (size, stride, paired)),
            in_specs=[any_spec] * 15,
            out_specs=[any_spec] * 4,
            out_shape=[
                jax.ShapeDtypeStruct((seqs, chunk, rank), BF16),
                jax.ShapeDtypeStruct((groups, chunk, BLOCK), BF16),
                jax.ShapeDtypeStruct((2, quads, seqs, toks, 4 * nope), BF16),
                jax.ShapeDtypeStruct((2, slots) + w_out.shape, BF16),
            ],
            scratch_shapes=[
                pltpu.VMEM(hidden.shape, BF16),
                pltpu.VMEM(w_dq.shape, BF16),
                pltpu.VMEM(wdkv_t.shape, BF16),
                pltpu.VMEM((groups, per * toks, dim), BF16),
                pltpu.VMEM((seqs, cache_len, rank), BF16),
                pltpu.VMEM((groups, cache_len, BLOCK), BF16),
                pltpu.VMEM((seqs, rope, prefix), BF16),
                pltpu.VMEM((seqs, rope // 2, BLOCK), F32),
                pltpu.VMEM((seqs, rope // 2, BLOCK), F32),
                pltpu.VMEM((2, seqs, toks, q_rank), BF16),
                pltpu.VMEM((slots * heads, head, q_rank), BF16),
                pltpu.VMEM((slots * heads, 2 * nope, rank), BF16),
                [pltpu.VMEM((cache_len, 4 * nope), BF16) for _ in range(2)],
                [pltpu.VMEM((4 * nope, cache_len), BF16) for _ in range(2)],
                pltpu.VMEM((2, 2, wide, wide), BF16),
                pltpu.VMEM((4 * head, wide), F32),
                [pltpu.VMEM((cache_len, wide), F32) for _ in range(4)],
                pltpu.VMEM((4, 8, wide), F32),
                [pltpu.VMEM((cache_len, wide), BF16) for _ in range(4)],
                pltpu.VMEM((4, 8, wide), F32),
                pltpu.VMEM((quads, seqs, toks, 4 * nope), BF16),
                pltpu.VMEM((quads, seqs, toks, 4 * nope), BF16),
                pltpu.VMEM(w_out.shape, BF16),
                pltpu.SMEM(lengths.shape, jnp.int32),
                pltpu.VMEM(norm_in.shape, F32),
                pltpu.VMEM(norm_q.shape, F32),
                pltpu.VMEM(norm_kv.shape, F32),
                pltpu.SemaphoreType.DMA((13 + groups,)),
                pltpu.SemaphoreType.DMA((copies,)),
                pltpu.SemaphoreType.DMA((copies,)),
            ],
            compiler_params=pltpu.CompilerParams(collective_id=0, has_side_effects=True, vmem_limit_bytes=63 * MIB),
            cost_estimate=pl.CostEstimate(flops=70 * 10**9, bytes_accessed=40 * MIB, transcendentals=30 * 10**6),
            name="main",
        )(lengths, hidden, norm_in, w_dq, norm_q, wdkv_t, norm_kv, cos_t, sin_t, wq_t, wk_t, wv_t, w_out, cache_lat, pe_t)

        depth = 4 * nope
        ahead = 4
        y, lat_new, pe_new = pl.pallas_call(
            finish_kernel,
            in_specs=[smem_spec] + [any_spec] * 7,
            out_specs=[any_spec] * 3,
            scratch_shapes=[
                pltpu.VMEM((rank // BLOCK, chunk + 2 * BLOCK, BLOCK), F32),
                pltpu.VMEM((seqs * toks, dim), F32),
                pltpu.VMEM(hidden.shape, BF16),
                pltpu.VMEM(hidden.shape, BF16),
                pltpu.VMEM((ahead, seqs, toks, depth), BF16),
                pltpu.VMEM((ahead, depth, dim), BF16),
                pltpu.VMEM((ahead, slots, 2, toks, rank), BF16),
                pltpu.VMEM((groups, slots, 2, toks, BLOCK), BF16),
                pltpu.VMEM((ahead, cache_len, rank), BF16),
                pltpu.VMEM(pe_t.shape, BF16),
                pltpu.VMEM((ahead, cache_len, rank), BF16),
                pltpu.VMEM(pe_t.shape, BF16),
                pltpu.SemaphoreType.DMA((4, ahead)),
                pltpu.SemaphoreType.DMA((ahead,)),
                pltpu.SemaphoreType.DMA((4 + dim // (2 * depth),)),
            ],
            out_shape=[
                jax.ShapeDtypeStruct(hidden.shape, BF16),
                jax.ShapeDtypeStruct(cache_lat.shape, BF16),
                jax.ShapeDtypeStruct(pe_t.shape, BF16),
            ],
            compiler_params=pltpu.CompilerParams(vmem_limit_bytes=63 * MIB),
            cost_estimate=pl.CostEstimate(flops=2 * seqs * toks * dim * dim, bytes_accessed=50 * MIB, transcendentals=0),
            name="finish",
        )(
            lengths,
            o_all,
            wo_all.reshape(2, slots * w_out.shape[0], dim),
            hidden,
            c_all.reshape(seqs, slots, 2, toks, rank),
            p_all.reshape(groups, slots, 2, toks, BLOCK),
            cache_lat,
            pe_t,
        )
        return y, lat_new, pe_new.transpose(0, 2, 1)

    spec_tok = P("dp", "tp", None)
    spec_len = P("dp")
    spec_seq = P("dp", None, None)
    spec_vec = P(None)
    spec_mat = P(None, None)
    spec_head = P(None, "tp", None)
    spec_rows = P("tp", None)
    in_specs = (spec_tok, spec_len, spec_seq, spec_seq, spec_seq, spec_seq, spec_vec, spec_mat, spec_vec, spec_mat, spec_vec, spec_head, spec_head, spec_head, spec_rows)
    return jax.shard_map(local_step, mesh=mesh, in_specs=in_specs, out_specs=(spec_tok, spec_seq, spec_seq), check_vma=False)
```

```python
import functools

import jax
import jax.numpy as jnp
from jax import lax
from jax.experimental import pallas as pl
from jax.experimental.pallas import tpu as pltpu
from jax.sharding import PartitionSpec as P

BLOCK = 128
LOG2E = 1.4426950408889634
NEVER = -1e30
NORM_ROWS = 16
F32 = jnp.float32
BF16 = jnp.bfloat16
MESH = pl.DeviceIdType.MESH
MIB = 2**20


def dot(a, b):
    return lax.dot_general(a, b, (((1,), (0,)), ((), ())), preferred_element_type=F32)


def dot_t(a, b):
    return lax.dot_general(a, b, (((1,), (1,)), ((), ())), preferred_element_type=F32)


def unit(x):
    return x * lax.rsqrt(jnp.mean(x * x, axis=-1, keepdims=True) + 1e-6)


class Wire:
    def __init__(self, send_sem, recv_sem):
        self.sems = (send_sem, recv_sem)
        self.made = {}
        self.pools = {}
        self.inboxes = {}

    def add(self, name, pool, src, dst, inbox=None, **peer):
        send = self.pools.setdefault(pool, len(self.pools))
        recv = self.inboxes.setdefault(inbox or name, len(self.inboxes))
        self.made[name] = lambda: pltpu.make_async_remote_copy(
            src(), dst(), self.sems[0].at[send], self.sems[1].at[recv], device_id=peer, device_id_type=MESH
        )

    def start(self, *names):
        for name in names:
            self.made[name]().start()

    def landed(self, *names):
        for name in names:
            self.made[name]().wait_recv()

    def all_landed(self, inbox, whole, **peer):
        copy = pltpu.make_async_remote_copy(whole, whole, self.sems[0].at[0], self.sems[1].at[self.inboxes[inbox]], device_id=peer, device_id_type=MESH)
        copy.wait_recv()

    def all_sent(self, pool, whole, **peer):
        copy = pltpu.make_async_remote_copy(whole, whole, self.sems[0].at[self.pools[pool]], self.sems[1].at[0], device_id=peer, device_id_type=MESH)
        copy.wait_send()


def main_kernel(
    plan,
    len_hbm,
    x_hbm,
    g1_hbm,
    wdq_hbm,
    gq_hbm,
    wdkv_hbm,
    gkv_hbm,
    cos_hbm,
    sin_hbm,
    wq_hbm,
    wk_hbm,
    wv_hbm,
    wo_hbm,
    lat_hbm,
    pe_hbm,
    c_out,
    p_out,
    o_out,
    wo_out,
    x_buf,
    wdq,
    wdkv,
    a_buf,
    rows,
    rot,
    pe_buf,
    cos_ref,
    sin_ref,
    cq_buf,
    wq,
    wkv,
    kb,
    vb,
    qb,
    q_raw,
    sb,
    mb,
    pb,
    lb,
    o_own,
    o_send,
    wo_buf,
    len_ref,
    g1_ref,
    gq_ref,
    gkv_ref,
    load_sem,
    send_sem,
    recv_sem,
):
    size, stride, paired = plan
    me = lax.axis_index("tp")
    odd = lax.rem(me, 2)
    chip = me // 2
    right, left = lax.rem(me + 2, size), lax.rem(me + size - 2, size)
    onward = jnp.where(odd == 0, right, left)
    other = me + 1 - 2 * odd
    dp = lax.axis_index("dp")
    flip = {"a": lax.rem(dp, 2), "b": lax.rem(dp // stride, 2)}
    partner = {"a": dp + 1 - 2 * flip["a"], "b": dp + stride * (1 - 2 * flip["b"])}

    seqs, toks, dim = x_hbm.shape
    groups = rot.shape[0]
    per = seqs // groups
    rank = rows.shape[2]
    slots = size // 2
    chunk = size * toks
    prefix = rows.shape[1] - chunk
    heads = wq.shape[0] // slots
    head, q_rank = wq.shape[1:]
    rope = BLOCK // per
    half = rope // 2
    nope = head - rope
    quads = wq.shape[0] // 4
    duos = seqs // 2
    wide = 2 * BLOCK
    factor = LOG2E * head**-0.5

    loads = {}

    def load(name, src, dst):
        loads[name] = pltpu.make_async_copy(src, dst, load_sem.at[len(loads)])
        loads[name].start()

    def spot(slot, parity):
        return pl.ds(pl.multiple_of(prefix + slot * BLOCK + parity * toks, toks), toks)

    barrier = pltpu.get_barrier_semaphore()
    for peer in (left, right, other):
        pl.semaphore_signal(barrier, inc=1, device_id={"tp": peer}, device_id_type=MESH)
    for side in "ab":
        if paired[side]:
            pl.semaphore_signal(barrier, inc=1, device_id={"dp": partner[side]}, device_id_type=MESH)

    lanes_chip = pl.ds(pl.multiple_of(chip * BLOCK, BLOCK), BLOCK)
    def load_x(g):
        load(f"x{g}", x_hbm.at[pl.ds(g * per, per)], x_buf.at[pl.ds(g * per, per)])

    load("g1", g1_hbm, g1_ref)
    load_x(0)
    load("wdkv", wdkv_hbm, wdkv)
    load("gkv", gkv_hbm, gkv_ref)
    load("gq", gq_hbm, gq_ref)
    load("len", len_hbm, len_ref)
    load("cos", cos_hbm.at[:, :, lanes_chip], cos_ref)
    load("sin", sin_hbm.at[:, :, lanes_chip], sin_ref)

    wire = Wire(send_sem, recv_sem)

    def chain(name, here, there, places, via="split", whole=True):
        near_left, near_right, opposite = places
        handed = {"right": near_left, "left": near_right, "split": jnp.where(odd == 0, near_left, near_right)}[via]
        pool = name[0] if name[1].isdigit() else name[:4]
        if whole:
            wire.add(name + "R", pool, lambda: here(0), lambda: there(near_left), tp=right)
        wire.add(name + "L", pool, lambda: here(0), lambda: there(near_right), tp=left)
        wire.add(name + "O", pool, lambda: there(handed), lambda: there(opposite), tp={"right": right, "left": left, "split": onward}[via])

    for g in range(groups):
        for name, ref in (("c", lambda slot, g=g: rows.at[pl.ds(g * per, per), spot(slot, odd)]), ("p", lambda slot, g=g: rot.at[g, spot(slot, odd)])):
            name = f"{name}{g}"
            chain(name, ref, ref, (1, 3, 2), "left")
            for slot in range(slots):
                wire.add(f"{name}S{slot}", name[0], functools.partial(ref, slot), functools.partial(ref, slot), f"{name}S", tp=other)
        cq_ref = lambda g=g: cq_buf.at[odd, pl.ds(g * per, per)]
        wire.add(f"q{g}S", "q", cq_ref, cq_ref, tp=other)

    def cut(side, low, high, unit, mine):
        half_size = (high - low) // 2
        which = flip[side] if mine else 1 - flip[side]
        return pl.ds(pl.multiple_of(low + which * half_size, unit), half_size)

    q_cut = head * 2 // 3
    o_cut = wo_hbm.shape[0] * 2 // 5
    lots = {"R": (0, 3), "r": (3, heads - 3)}
    everyone = (0, heads)

    def lot_of(place, lot):
        return pl.ds(place * heads + lot[0], lot[1])

    pieces = {
        "wq.a": (lambda r, lot: wq_hbm.at[pl.ds(*lot), r], lambda place, r, lot: wq.at[lot_of(place, lot), r], ("a", 0, q_cut, 16)),
        "wq.b": (lambda r, lot: wq_hbm.at[pl.ds(*lot), r], lambda place, r, lot: wq.at[lot_of(place, lot), r], ("b", q_cut, head, 16)),
        "wk.a": (
            lambda r, lot: wk_hbm.at[pl.ds(*lot), :, r],
            lambda place, r, lot: wkv.at[lot_of(place, lot), pl.ds(0, nope), r],
            ("a", 0, rank, BLOCK),
        ),
        "wv.b": (
            lambda r, lot: wv_hbm.at[pl.ds(*lot), :, r],
            lambda place, r, lot: wkv.at[lot_of(place, lot), pl.ds(nope, nope), r],
            ("b", 0, rank, BLOCK),
        ),
        "wo.a": (lambda r, lot: wo_hbm.at[r], lambda place, r, lot: wo_out.at[odd, place, r], ("a", 0, o_cut, 16)),
        "wo.b": (lambda r, lot: wo_hbm.at[r], lambda place, r, lot: wo_out.at[odd, place, r], ("b", o_cut, 2 * o_cut, 16)),
    }
    left_over = pl.ds(2 * o_cut, wo_hbm.shape[0] - 2 * o_cut)
    chain("wo.m", lambda place: wo_hbm.at[left_over], lambda place: wo_out.at[odd, place, left_over], (1, 2, 3))
    for piece, (source, target, bounds) in pieces.items():
        side = bounds[0]
        large = piece.startswith("wo")
        for mine in (True,) if paired[side] else (True, False):
            here = lambda place, lot=everyone, source=source, bounds=bounds, mine=mine: source(cut(*bounds, mine), lot)
            there = lambda place, lot=everyone, target=target, bounds=bounds, mine=mine: target(place, cut(*bounds, mine), lot)
            name = piece + ("" if mine else "~")
            chain(name, here, there, (1, 2, 3), "split" if large else "right", large)
            if not large:
                for way, lot in lots.items():
                    wire.add(name + way, piece, functools.partial(here, 0, lot), functools.partial(there, 1, lot), tp=right)
        if paired[side]:
            for place, tag, lot in ((1, "", everyone),) if large else ((1, "", lots["R"]), (1, "r", lots["r"])):
                ref = lambda place=place, lot=lot, target=target, bounds=bounds: target(place, cut(*bounds, True), lot)
                wire.add(f"{piece}X{place}{tag}", piece, ref, ref, dp=partner[side])
            for place in (2, 3):
                ref = lambda place=place, target=target, bounds=bounds: target(place, cut(*bounds, True), everyone)
                wire.add(f"{piece}X{place}", piece, ref, ref, dp=partner[side])
    for place in range(slots - 1):
        ref = lambda place=place: wo_out.at[odd, place]
        wire.add(f"woS{place}", "woS", ref if place else lambda: wo_hbm, ref, tp=other)
    for piece in ("wo.a", "wo.b"):
        for mine in (True, False):
            ref = lambda piece=piece, mine=mine: pieces[piece][1](slots - 1, cut(*pieces[piece][2], mine), everyone)
            wire.add(f"{piece}S" + ("" if mine else "~"), "woS", ref, ref, tp=other)
    ref = lambda: wo_out.at[odd, slots - 1, left_over]
    wire.add("wo.mS", "woS", ref, ref, tp=other)
    for quad in range(quads - 1):
        wire.add(f"o{quad}S", "o", lambda quad=quad: o_send.at[quad], lambda quad=quad: o_out.at[odd, quad], tp=other)
    cut_o = seqs - 4
    for name, part in (("o.a", pl.ds(0, cut_o)), ("o.b", pl.ds(cut_o, seqs - cut_o))):
        wire.add(name + "S", "o", lambda part=part: o_send.at[quads - 1, part], lambda part=part: o_out.at[odd, quads - 1, part], tp=other)

    small = ("wk.a", "wv.b", "wq.a", "wq.b")

    def ring(which, *kinds):
        return [f"{kind}{half_name}{way}" for kind in kinds for half_name in ("", "~")[: 1 if paired[kind[-1]] else 2] for way in which]

    def across(place, *kinds):
        return [f"{kind}X{place}" for kind in kinds if paired[kind[-1]]]

    def norm(g):
        for r in range(per):
            for at in range(0, toks, NORM_ROWS):
                x = x_buf[g * per + r, at : at + NORM_ROWS].astype(F32)
                a_buf[g, r * toks + at : r * toks + at + NORM_ROWS] = (unit(x) * g1_ref[...]).astype(BF16)

    def latent(g):
        kv = dot_t(a_buf[g], wdkv[...])
        rows[g * per : (g + 1) * per, spot(0, odd), :] = (unit(kv[:, :rank]) * gkv_ref[...]).astype(BF16).reshape(per, toks, rank)
        turned = []
        for s in range(per):
            cos_pair, sin_pair = cos_ref[g * per + s], sin_ref[g * per + s]
            cos = jnp.where(odd == 1, cos_pair[:, toks:], cos_pair[:, :toks])
            sin = jnp.where(odd == 1, sin_pair[:, toks:], sin_pair[:, :toks])
            table = jnp.concatenate([cos, cos, -sin, sin], axis=0).T
            p = kv[s * toks : (s + 1) * toks, rank:]
            swapped = jnp.concatenate([p[:, half:], p[:, :half]], axis=1)
            turned.append(p * table[:, :rope] + swapped * table[:, rope:])
        rot[g, spot(0, odd), :] = jnp.concatenate(turned, axis=1).astype(BF16)

    def queries(g):
        h = jnp.concatenate([dot(a_buf[g], wdq[:, : 2 * rank]), dot(a_buf[g], wdq[:, 2 * rank :])], axis=1)
        cq_buf[odd, g * per : (g + 1) * per] = (unit(h) * gq_ref[...]).astype(BF16).reshape(per, toks, q_rank)

    loads["g1"].wait()
    with jax.named_scope('p_norm0'):
        loads["x0"].wait()
        for g in range(1, groups):
            load_x(g)
        norm(0)
    for name in ("wdkv", "cos", "sin", "gkv", "gq", "len"):
        loads[name].wait()
    load("wdq", wdq_hbm, wdq)
    load("wk", wk_hbm, wkv.at[pl.ds(0, heads), pl.ds(0, nope)])
    load("wv", wv_hbm, wkv.at[pl.ds(0, heads), pl.ds(nope, nope)])
    load("wq", wq_hbm, wq.at[pl.ds(0, heads)])
    load("pe", pe_hbm.at[:, :, pl.ds(0, prefix)], pe_buf)
    load("lat", lat_hbm.at[:, pl.ds(0, prefix)], rows.at[:, pl.ds(0, prefix)])
    with jax.named_scope('p_bar'):
        pl.semaphore_wait(barrier, 3 + paired["a"] + paired["b"])
    with jax.named_scope('p_kv'):
        for g in range(groups):
            latent(g)
            for way in ("R", "L", "S0"):
                wire.start(f"c{g}{way}", f"p{g}{way}")
            if g + 1 < groups:
                loads[f"x{g + 1}"].wait()
                norm(g + 1)
    wire.start(*ring("R", *small), *ring("r", *small))

    def hand_on(g):
        wire.landed(f"c{g}L", f"p{g}L", f"c{g}R", f"p{g}R")
        wire.start(f"c{g}O", f"p{g}O", f"c{g}S3", f"p{g}S3", f"c{g}S1", f"p{g}S1")

    with jax.named_scope('p_cq'):
        loads["wdq"].wait()
        for g in range(groups):
            queries(g)
            wire.start(f"q{g}S")
            hand_on(g)
    wire.start(*ring("L", *small, "wo.b", "wo.a"), "wo.mL", "woS0")

    loads["pe"].wait()
    for g in range(groups):
        old = pe_buf[g * per : (g + 1) * per].reshape(per * rope, prefix).astype(F32)
        for b in range(prefix // BLOCK):
            rot[g, b * BLOCK : (b + 1) * BLOCK] = old[:, b * BLOCK : (b + 1) * BLOCK].T.astype(BF16)
    qb[...] = jnp.zeros_like(qb)

    def rest_of(g):
        wire.landed(f"c{g}O", f"p{g}O")
        wire.start(f"c{g}S2", f"p{g}S2")
        wire.all_landed(f"c{g}S", rows.at[pl.ds(0, per), pl.ds(0, slots * toks)], tp=other)
        wire.all_landed(f"p{g}S", rot.at[0, pl.ds(0, slots * toks)], tp=other)
        if g:
            wire.landed(f"q{g}S")

    with jax.named_scope('p_rest0'):
        for name in ("wk", "wv", "wq", "lat"):
            loads[name].wait()
    row = lax.broadcasted_iota(jnp.int32, (BLOCK, wide), 0)
    lane = lax.rem(lax.broadcasted_iota(jnp.int32, (BLOCK, wide), 1), BLOCK)
    near = row <= lane

    def place(n):
        return n // duos, lax.rem(n, duos)

    def query_dot(n):
        quad, duo = place(n)
        w = wq[pl.ds(quad * 4, 4)].reshape(4 * head, q_rank)
        cq = jnp.concatenate([cq_buf[parity, 2 * duo + u] for u in range(2) for parity in range(2)], axis=0)
        q_raw[...] = dot_t(w, cq)

    def query_stage(n):
        quad, duo = place(n)
        raw = q_raw
        for u in range(2):
            slot = 2 * lax.rem(duo, 2) + u
            cos, sin = cos_ref[2 * duo + u], sin_ref[2 * duo + u]
            for h in range(4):
                pair, side = h // 2, h % 2
                q = raw[h * head : (h + 1) * head, u * BLOCK : (u + 1) * BLOCK]
                cols = slice(side * BLOCK, (side + 1) * BLOCK)
                qb[u, pair, side * nope : (side + 1) * nope, cols] = q[:nope].astype(BF16)
                lo, hi = q[nope : nope + half], q[nope + half :]
                turned = jnp.concatenate([lo * cos - hi * sin, hi * cos + lo * sin], axis=0).astype(BF16)
                start = pl.multiple_of(BLOCK + slot * rope, rope)
                stale = pl.multiple_of(BLOCK + lax.rem(slot + 2, 4) * rope, rope)
                qb[u, pair, pl.ds(start, rope), cols] = turned
                qb[u, pair, pl.ds(stale, rope), cols] = jnp.zeros_like(turned)

    def key_stage(n, t, u):
        quad, duo = place(n)
        w = wkv[pl.ds(quad * 4, 4), :nope].reshape(4 * nope, rank)
        kb[u][:t] = dot_t(rows[2 * duo + u, :t], w).astype(BF16)

    def value_stage(n, t, u):
        quad, duo = place(n)
        w = wkv[pl.ds(quad * 4, 4), nope:].reshape(4 * nope, rank)
        vb[u][:, :t] = dot_t(w, rows[2 * duo + u, :t]).astype(BF16)

    def score_stage(n, t, u, pair):
        _, duo = place(n)
        length = len_ref[2 * duo + u]
        keys = jnp.concatenate([kb[u][:t, pair * BLOCK : (pair + 1) * BLOCK], rot[duo // 2, :t]], axis=1)
        value = dot(keys, qb[u, pair])
        most = None
        for b in range(t // BLOCK):
            part = value[b * BLOCK : (b + 1) * BLOCK]
            if BLOCK <= b * BLOCK < prefix:
                part = jnp.where(row < length - b * BLOCK, part, NEVER)
            if b * BLOCK == prefix:
                part = jnp.where(near, part, NEVER)
            sb[2 * u + pair][b * BLOCK : (b + 1) * BLOCK] = part
            part = jnp.max(part.reshape(BLOCK // 8, 8, wide), axis=0)
            most = part if most is None else jnp.maximum(most, part)
        mb[2 * u + pair] = jnp.broadcast_to(jnp.max(most, axis=0, keepdims=True), (8, wide))

    def soft_stage(t, u, pair):
        i = 2 * u + pair
        most = mb[i, :1]
        total = None
        for b in range(t // BLOCK):
            x = jnp.exp2((sb[i][b * BLOCK : (b + 1) * BLOCK] - most) * factor)
            part = jnp.sum(x.reshape(BLOCK // 8, 8, wide), axis=0)
            total = part if total is None else total + part
            pb[i][b * BLOCK : (b + 1) * BLOCK] = x.astype(BF16)
        lb[i] = total

    def mix_stage(n, t, u, pair):
        quad, duo = place(n)
        i = 2 * u + pair
        inv = 1.0 / jnp.sum(lb[i], axis=0, keepdims=True)
        o = dot(vb[u][pair * BLOCK : (pair + 1) * BLOCK, :t], pb[i][:t]) * inv
        o = jnp.concatenate([o[:nope, :BLOCK], o[nope:, BLOCK:]], axis=0).T.astype(BF16)
        first, second = o[:toks], o[toks:]
        cols = slice(pair * BLOCK, (pair + 1) * BLOCK)
        o_own[quad, 2 * duo + u, :, cols] = jnp.where(odd == 1, second, first)
        o_send[quad, 2 * duo + u, :, cols] = jnp.where(odd == 1, first, second)

    units = [(u, pair) for u in range(2) for pair in range(2)]
    total = quads * duos

    def each_chip(fn):
        for c in range(slots):
            pl.when(chip == c)(lambda c=c: fn(prefix + (c + 1) * BLOCK))

    def body(b, t):
        before, ahead, later = jnp.maximum(b - 1, 0), jnp.minimum(b + 1, total - 1), jnp.minimum(b + 2, total - 1)
        mix_stage(before, t, 0, 0)
        mix_stage(before, t, 0, 1)
        mix_stage(before, t, 1, 0)
        mix_stage(before, t, 1, 1)
        soft_stage(t, 0, 0)
        score_stage(ahead, t, 0, 0)
        value_stage(b, t, 0)
        soft_stage(t, 0, 1)
        score_stage(ahead, t, 0, 1)
        key_stage(later, t, 0)
        soft_stage(t, 1, 0)
        score_stage(ahead, t, 1, 0)
        value_stage(b, t, 1)
        soft_stage(t, 1, 1)
        score_stage(ahead, t, 1, 1)
        query_dot(later)
        query_stage(later)
        key_stage(later, t, 1)

    def at(b, when):
        return pl.when(b == when)

    agenda = {
        0: [(None, ring("R", "wq.a", "wq.b"), across(1, "wq.a", "wq.b"))],
        2: [(None, ring("r", *small), across("1r", *small) + ring("O", *small) + ring("R", "wo.a", "wo.b") + ["wo.mR"])],
        3: [(None, ring("L", "wk.a", "wv.b"), across(2, "wk.a", "wv.b"))],
        4: [(None, across(1, *small), [])],
        5: [(None, ring("L", "wq.a"), across(2, "wq.a"))],
        7: [(None, ring("L", "wq.b"), across(2, "wq.b"))],
        9: [(None, ring("O", *small), across(3, *small))],
        10: [(None, across("1r", *small) + across(2, *small), [])],
        11: [(None, ring("L", "wo.b"), across(2, "wo.b")), (1, [], ring("O", "wo.b"))],
        12: [(None, ring("R", "wo.a"), across(1, "wo.a")), (0, [], ring("O", "wo.a"))],
        15: [(None, across(3, *small), []), (None, ring("L", "wo.a"), across(2, "wo.a")), (1, [], ring("O", "wo.a"))],
        16: [(None, ring("R", "wo.b"), across(1, "wo.b")), (0, [], ring("O", "wo.b"))],
        19: [(0, ["wo.mR"], ["wo.mO"]), (1, ["wo.mL"], ["wo.mO"])],
        22: [(0, ring("O", "wo.a"), across(3, "wo.a") + ["wo.aS"]), (1, ring("O", "wo.b"), across(3, "wo.b") + ["wo.bS"])],
        23: [
            (0, ["wo.mL"], []),
            (1, ["wo.mR"], []),
            (None, across(1, "wo.a", "wo.b") + across(2, "wo.a", "wo.b"), ["woS1", "woS2"]),
        ],
        24: [(0, ring("O", "wo.b"), across(3, "wo.b") + ["wo.bS"]), (1, ring("O", "wo.a"), across(3, "wo.a") + ["wo.aS"])],
        29: [(None, ["wo.mO"], ["wo.mS"]), (None, across(3, "wo.a", "wo.b"), ["wo.aS~", "wo.bS~", "o.aS"])],
    }
    for quad in range(quads - 1):
        agenda.setdefault((quad + 1) * duos + 1, []).append((None, [], [f"o{quad}S"]))

    def run_agenda(when):
        for parity, waits, starts in agenda[when]:

            def item(waits=waits, starts=starts):
                with jax.named_scope(f"ev_{when}"):
                    wire.landed(*waits)
                wire.start(*starts)

            if parity is None:
                item()
            else:
                pl.when(odd == parity)(item)

    bounce = pltpu.make_async_copy(wo_hbm, wo_buf, load_sem.at[3])
    span = 8

    def step(b, _):
        for first in range(0, total, span):

            @pl.when(b // span == first // span)
            def _():
                for when in sorted(agenda):
                    if first <= when < first + span:
                        at(b, when)(functools.partial(run_agenda, when))
                if first == 0:

                    @at(b, 0)
                    def _():
                        with jax.named_scope('ev_k1'):
                            rest_of(1)

                    @at(b, 2)
                    def _():
                        with jax.named_scope('ev_k2'):
                            rest_of(2)
                        pltpu.make_async_copy(rows.at[:, pl.ds(prefix, chunk)], c_out, load_sem.at[0]).start()
                        pltpu.make_async_copy(rot.at[:, pl.ds(prefix, chunk)], p_out, load_sem.at[1]).start()
                        bounce.start()

                    @at(b, 6)
                    def _():
                        bounce.wait()
                        pltpu.make_async_copy(wo_buf, wo_out.at[odd, 0], load_sem.at[4]).start()

        with jax.named_scope('body'):
            each_chip(functools.partial(body, b))
        return 0

    def lead_in(t):
        for u in range(2):
            key_stage(0, t, u)
        for u, pair in units:
            score_stage(0, t, u, pair)
        for u in range(2):
            key_stage(1, t, u)
        query_dot(1)
        query_stage(1)

    wire.landed("q0S")
    query_dot(0)
    query_stage(0)
    rest_of(0)
    wire.landed(*ring("R", "wk.a", "wv.b"))
    wire.start(*across(1, "wk.a", "wv.b"))
    with jax.named_scope('p_lead'):
        each_chip(lead_in)
    lax.fori_loop(0, total, step, 0)

    def last(t):
        for u, pair in units:
            mix_stage(total - 1, t, u, pair)

    with jax.named_scope('p_last'):
        each_chip(last)
        wire.start("o.bS")
        pltpu.make_async_copy(o_own, o_out.at[odd], load_sem.at[2]).start()
    with jax.named_scope('f_land'):
        for place in range(slots - 1):
            wire.landed(f"woS{place}")
        wire.landed("wo.aS", "wo.bS", "wo.mS", "wo.aS~", "wo.bS~")
        for quad in range(quads - 1):
            wire.landed(f"o{quad}S")
        wire.landed("o.aS", "o.bS")
    with jax.named_scope('f_sent'):
        wire.all_sent("c", rows.at[pl.ds(0, per * groups // 2), pl.ds(0, 14 * toks)], tp=other)
        wire.all_sent("p", rot.at[pl.ds(0, groups), pl.ds(0, 7 * toks)], tp=other)
        wire.all_sent("q", cq_buf.at[odd], tp=other)
        wire.all_sent("wq.a", wq.at[pl.ds(0, 3 * heads), pl.ds(0, q_cut)], tp=other)
        wire.all_sent("wq.b", wq.at[pl.ds(0, 3 * heads), pl.ds(0, head - q_cut)], tp=other)
        wire.all_sent("wk.a", wkv.at[pl.ds(0, 3 * heads), pl.ds(0, nope)], tp=other)
        wire.all_sent("wv.b", wkv.at[pl.ds(0, 3 * heads), pl.ds(0, nope)], tp=other)
        wire.all_sent("wo.a", wo_out.at[0, pl.ds(0, 3), pl.ds(0, o_cut)], tp=other)
        wire.all_sent("wo.b", wo_out.at[0, pl.ds(0, 3), pl.ds(0, o_cut)], tp=other)
        wire.all_sent("wo.m", wo_out.at[0, pl.ds(0, 3), left_over], tp=other)
        wire.all_sent("woS", wo_out.at[0], tp=other)
        wire.all_sent("o", o_send, tp=other)
        pltpu.make_async_copy(rows.at[:, pl.ds(prefix, chunk)], c_out, load_sem.at[0]).wait()
        pltpu.make_async_copy(rot.at[:, pl.ds(prefix, chunk)], p_out, load_sem.at[1]).wait()
        pltpu.make_async_copy(o_own, o_out.at[odd], load_sem.at[2]).wait()
        pltpu.make_async_copy(wo_buf, wo_out.at[odd, 0], load_sem.at[4]).wait()


def finish_kernel(
    len_ref, o_hbm, w_hbm, x_hbm, c_hbm, p_hbm, lat_hbm, pe_hbm, y_hbm, lat_out, pe_out, fresh, acc, x_buf, y_buf, o_buf, w_buf, c_buf, p_buf, lat_buf, pe_buf, lat_new, pe_new, load_sem, store_sem, sems
):
    chip = lax.axis_index("tp") // 2
    quads, seqs, toks, depth = o_hbm.shape[1:]
    terms = 2 * quads
    slots = c_hbm.shape[1]
    rank = lat_hbm.shape[2]
    rope, cache_len = pe_hbm.shape[1:]
    chunk = slots * 2 * toks
    words = rank // BLOCK
    dim = x_hbm.shape[2]
    part = 2 * depth
    ring = w_buf.shape[0]

    def loads(k, with_term):
        slot = lax.rem(k, ring)
        out = [
            pltpu.make_async_copy(c_hbm.at[k], c_buf.at[slot], load_sem.at[0, slot]),
            pltpu.make_async_copy(lat_hbm.at[k], lat_buf.at[slot], load_sem.at[1, slot]),
        ]
        if with_term:
            side, quad = k // quads, lax.rem(k, quads)
            out.append(pltpu.make_async_copy(o_hbm.at[side, quad], o_buf.at[slot], load_sem.at[2, slot]))
            out.append(pltpu.make_async_copy(w_hbm.at[side, pl.ds(pl.multiple_of(quad * depth, depth), depth)], w_buf.at[slot], load_sem.at[3, slot]))
        return out

    def store(k):
        slot = lax.rem(k, ring)
        return pltpu.make_async_copy(lat_new.at[slot], lat_out.at[k], store_sem.at[slot])

    load_x = pltpu.make_async_copy(x_hbm, x_buf, sems.at[0])
    load_p = pltpu.make_async_copy(p_hbm, p_buf, sems.at[1])
    load_pe = pltpu.make_async_copy(pe_hbm, pe_buf, sems.at[2])
    store_pe = pltpu.make_async_copy(pe_new, pe_out, sems.at[3])

    def store_y(n):
        cols = pl.ds(n * part, part)
        return pltpu.make_async_copy(y_buf.at[:, :, cols], y_hbm.at[:, :, cols], sems.at[4 + n])


    def slot_of(j):
        return lax.rem(chip - j + slots, slots)

    def project(k, kind):
        slot = lax.rem(k, ring)
        o = o_buf[slot].reshape(seqs * toks, depth)
        for n in range(0, dim, part):
            cols = slice(n, n + part)
            y = dot(o, w_buf[slot, :, cols])
            if kind != "first":
                y = acc[:, cols] + y
            if kind == "last":
                y = y + x_buf[:, :, cols].reshape(seqs * toks, part).astype(F32)
                y_buf[:, :, cols] = y.astype(BF16).reshape(seqs, toks, part)
                store_y(n // part).start()
            else:
                acc[:, cols] = y

    def cache(k):
        at_slot = lax.rem(k, ring)
        length = len_ref[k]
        for j in range(slots):
            piece = c_buf[at_slot, slot_of(j)].reshape(2 * toks, rank).astype(F32)
            for w in range(words):
                fresh[w, BLOCK + j * 2 * toks : BLOCK + (j + 1) * 2 * toks] = piece[:, w * BLOCK : (w + 1) * BLOCK]
        lat_new[at_slot] = lat_buf[at_slot]
        base = (length // 16) * 16
        skew = length - base
        tile_row = lax.broadcasted_iota(jnp.int32, (16, BLOCK), 0)
        for i in range(chunk // 16 + 1):
            at = pl.multiple_of(jnp.minimum(base + i * 16, cache_len - 16), 16)
            for w in range(words):
                cols = slice(w * BLOCK, (w + 1) * BLOCK)
                moved = fresh[w, pl.ds(BLOCK - skew + i * 16, 16), :].astype(BF16)
                if i == 0 or i == chunk // 16:
                    local = tile_row + (at - length)
                    shown = (local >= 0) & (local < chunk) if i == 0 else (local < chunk)
                    if i == 0:
                        rest = lat_buf[at_slot, pl.ds(at, 16), cols]
                    else:
                        shown = shown & (skew > 0)
                        rest = lat_new[at_slot, pl.ds(at, 16), cols]
                    moved = jnp.where(shown, moved.astype(F32), rest.astype(F32)).astype(BF16)
                lat_new[at_slot, pl.ds(at, 16), cols] = moved

        turned = jnp.concatenate([p_buf[k // (BLOCK // rope), slot_of(j)].reshape(2 * toks, BLOCK).astype(F32).T for j in range(slots)], axis=1)
        group = lax.rem(k, BLOCK // rope)
        mine = turned[:rope]
        for g in range(1, BLOCK // rope):
            mine = jnp.where(group == g, turned[g * rope : (g + 1) * rope], mine)
        mine = jnp.concatenate([mine, jnp.zeros((rope, cache_len - chunk), F32)], axis=1)
        mine = pltpu.roll(mine, length, axis=1)
        spot = lax.broadcasted_iota(jnp.int32, (rope, cache_len), 1) - length
        pe_new[k] = jnp.where((spot >= 0) & (spot < chunk), mine, pe_buf[k].astype(F32)).astype(BF16)

    def begin(k, with_term):
        for load in loads(k, with_term):
            load.start()

    def arrived(k, with_term):
        for load in loads(k, with_term):
            load.wait()

    def work(k, kind):
        if kind != "none":
            project(k, kind)
        cache(k)
        store(k).start()

    def more(k):
        pl.when(k < terms)(lambda: begin(k, True))
        pl.when((k >= terms) & (k < seqs))(lambda: begin(k, False))

    first = loads(0, True)
    for load in first[2:] + first[:2]:
        load.start()
    load_p.start()
    load_pe.start()
    for load in first[2:]:
        load.wait()
    begin(1, True)
    begin(2, True)
    project(0, "first")
    for load in first[:2] + [load_p, load_pe]:
        load.wait()
    begin(3, True)
    cache(0)
    store(0).start()
    load_x.start()

    def middle(k, _):
        with jax.named_scope('g_wait'):
            arrived(k, True)
        more(k + ring - 1)

        @pl.when(k >= ring)
        def _():
            store(k - ring).wait()

        with jax.named_scope('g_work'):
            work(k, "middle")
        return 0

    lax.fori_loop(1, terms - 1, middle, 0)
    last = terms - 1
    arrived(last, True)
    more(last + ring - 1)
    store(last - ring).wait()
    load_x.wait()
    with jax.named_scope('g_last'):
        work(last, "last")

    def tail(k, _):
        arrived(k, False)
        store(k - ring).wait()
        with jax.named_scope('g_tail'):
            work(k, "none")
        return 0

    lax.fori_loop(terms, seqs, tail, 0)
    store_pe.start()
    for k in range(ring):
        store(seqs - ring + k).wait()
    store_pe.wait()
    for n in range(dim // part):
        store_y(n).wait()


def solution(mesh):
    size = mesh.shape["tp"]
    count = mesh.shape["dp"]
    stride = 2 ** (count.bit_length() // 2)
    paired = {"a": count % 2 == 0, "b": count % (2 * stride) == 0}

    def local_step(hidden, lengths, rope_cos, rope_sin, cache_lat, cache_pe, norm_in, w_dq, norm_q, w_dkv, norm_kv, w_uq, w_uk, w_uv, w_out):
        seqs, toks, dim = hidden.shape
        q_rank = w_dq.shape[1]
        rank, heads, nope = w_uk.shape
        rope = cache_pe.shape[2]
        cache_len = cache_lat.shape[1]
        slots = size // 2
        head = nope + rope
        quads = slots * heads // 4
        chunk = size * toks
        prefix = cache_len - chunk
        per = BLOCK // rope
        groups = seqs // per
        wide = 2 * BLOCK
        cos_t, sin_t = rope_cos.transpose(0, 2, 1), rope_sin.transpose(0, 2, 1)
        pe_t = cache_pe.transpose(0, 2, 1)
        wdkv_t = w_dkv.transpose(1, 0)
        wq_t, wk_t, wv_t = (w.transpose(1, 2, 0) for w in (w_uq, w_uk, w_uv))

        inboxes = 9 * groups + 36 + 8 + 3 + slots + 4 + quads + 1
        any_spec = pl.BlockSpec(memory_space=pl.ANY)
        smem_spec = pl.BlockSpec(memory_space=pltpu.SMEM)
        c_all, p_all, o_all, wo_all = pl.pallas_call(
            functools.partial(main_kernel, (size, stride, paired)),
            in_specs=[any_spec] * 15,
            out_specs=[any_spec] * 4,
            out_shape=[
                jax.ShapeDtypeStruct((seqs, chunk, rank), BF16),
                jax.ShapeDtypeStruct((groups, chunk, BLOCK), BF16),
                jax.ShapeDtypeStruct((2, quads, seqs, toks, 4 * nope), BF16),
                jax.ShapeDtypeStruct((2, slots) + w_out.shape, BF16),
            ],
            scratch_shapes=[
                pltpu.VMEM(hidden.shape, BF16),
                pltpu.VMEM(w_dq.shape, BF16),
                pltpu.VMEM(wdkv_t.shape, BF16),
                pltpu.VMEM((groups, per * toks, dim), BF16),
                pltpu.VMEM((seqs, cache_len, rank), BF16),
                pltpu.VMEM((groups, cache_len, BLOCK), BF16),
                pltpu.VMEM((seqs, rope, prefix), BF16),
                pltpu.VMEM((seqs, rope // 2, BLOCK), F32),
                pltpu.VMEM((seqs, rope // 2, BLOCK), F32),
                pltpu.VMEM((2, seqs, toks, q_rank), BF16),
                pltpu.VMEM((slots * heads, head, q_rank), BF16),
                pltpu.VMEM((slots * heads, 2 * nope, rank), BF16),
                [pltpu.VMEM((cache_len, 4 * nope), BF16) for _ in range(2)],
                [pltpu.VMEM((4 * nope, cache_len), BF16) for _ in range(2)],
                pltpu.VMEM((2, 2, wide, wide), BF16),
                pltpu.VMEM((4 * head, wide), F32),
                [pltpu.VMEM((cache_len, wide), F32) for _ in range(4)],
                pltpu.VMEM((4, 8, wide), F32),
                [pltpu.VMEM((cache_len, wide), BF16) for _ in range(4)],
                pltpu.VMEM((4, 8, wide), F32),
                pltpu.VMEM((quads, seqs, toks, 4 * nope), BF16),
                pltpu.VMEM((quads, seqs, toks, 4 * nope), BF16),
                pltpu.VMEM(w_out.shape, BF16),
                pltpu.SMEM(lengths.shape, jnp.int32),
                pltpu.VMEM(norm_in.shape, F32),
                pltpu.VMEM(norm_q.shape, F32),
                pltpu.VMEM(norm_kv.shape, F32),
                pltpu.SemaphoreType.DMA((13 + groups,)),
                pltpu.SemaphoreType.DMA((12,)),
                pltpu.SemaphoreType.DMA((inboxes,)),
            ],
            compiler_params=pltpu.CompilerParams(collective_id=0, has_side_effects=True, vmem_limit_bytes=63 * MIB),
            cost_estimate=pl.CostEstimate(flops=70 * 10**9, bytes_accessed=40 * MIB, transcendentals=30 * 10**6),
            name="main",
        )(lengths, hidden, norm_in, w_dq, norm_q, wdkv_t, norm_kv, cos_t, sin_t, wq_t, wk_t, wv_t, w_out, cache_lat, pe_t)

        depth = 4 * nope
        ahead = 4
        y, lat_new, pe_new = pl.pallas_call(
            finish_kernel,
            in_specs=[smem_spec] + [any_spec] * 7,
            out_specs=[any_spec] * 3,
            scratch_shapes=[
                pltpu.VMEM((rank // BLOCK, chunk + 2 * BLOCK, BLOCK), F32),
                pltpu.VMEM((seqs * toks, dim), F32),
                pltpu.VMEM(hidden.shape, BF16),
                pltpu.VMEM(hidden.shape, BF16),
                pltpu.VMEM((ahead, seqs, toks, depth), BF16),
                pltpu.VMEM((ahead, depth, dim), BF16),
                pltpu.VMEM((ahead, slots, 2, toks, rank), BF16),
                pltpu.VMEM((groups, slots, 2, toks, BLOCK), BF16),
                pltpu.VMEM((ahead, cache_len, rank), BF16),
                pltpu.VMEM(pe_t.shape, BF16),
                pltpu.VMEM((ahead, cache_len, rank), BF16),
                pltpu.VMEM(pe_t.shape, BF16),
                pltpu.SemaphoreType.DMA((4, ahead)),
                pltpu.SemaphoreType.DMA((ahead,)),
                pltpu.SemaphoreType.DMA((4 + dim // (2 * depth),)),
            ],
            out_shape=[
                jax.ShapeDtypeStruct(hidden.shape, BF16),
                jax.ShapeDtypeStruct(cache_lat.shape, BF16),
                jax.ShapeDtypeStruct(pe_t.shape, BF16),
            ],
            compiler_params=pltpu.CompilerParams(vmem_limit_bytes=63 * MIB),
            cost_estimate=pl.CostEstimate(flops=2 * seqs * toks * dim * dim, bytes_accessed=50 * MIB, transcendentals=0),
            name="finish",
        )(
            lengths,
            o_all,
            wo_all.reshape(2, slots * w_out.shape[0], dim),
            hidden,
            c_all.reshape(seqs, slots, 2, toks, rank),
            p_all.reshape(groups, slots, 2, toks, BLOCK),
            cache_lat,
            pe_t,
        )
        return y, lat_new, pe_new.transpose(0, 2, 1)

    spec_tok = P("dp", "tp", None)
    spec_len = P("dp")
    spec_seq = P("dp", None, None)
    spec_vec = P(None)
    spec_mat = P(None, None)
    spec_head = P(None, "tp", None)
    spec_rows = P("tp", None)
    in_specs = (spec_tok, spec_len, spec_seq, spec_seq, spec_seq, spec_seq, spec_vec, spec_mat, spec_vec, spec_mat, spec_vec, spec_head, spec_head, spec_head, spec_rows)
    return jax.shard_map(local_step, mesh=mesh, in_specs=in_specs, out_specs=(spec_tok, spec_seq, spec_seq), check_vma=False)
```

```python
import functools

import jax
import jax.numpy as jnp
from jax import lax
from jax.experimental import pallas as pl
from jax.experimental.pallas import tpu as pltpu
from jax.sharding import PartitionSpec as P

BLOCK = 128
LOG2E = 1.4426950408889634
NEVER = -1e30
NORM_ROWS = 16
F32 = jnp.float32
BF16 = jnp.bfloat16
MESH = pl.DeviceIdType.MESH
MIB = 2**20


def dot(a, b):
    return lax.dot_general(a, b, (((1,), (0,)), ((), ())), preferred_element_type=F32)


def dot_t(a, b):
    return lax.dot_general(a, b, (((1,), (1,)), ((), ())), preferred_element_type=F32)


def unit(x):
    return x * lax.rsqrt(jnp.mean(x * x, axis=-1, keepdims=True) + 1e-6)


class Wire:
    def __init__(self, send_sem, recv_sem):
        self.sems = (send_sem, recv_sem)
        self.made = {}
        self.pools = {}
        self.inboxes = {}

    def add(self, name, pool, src, dst, inbox=None, **peer):
        send = self.pools.setdefault(pool, len(self.pools))
        recv = self.inboxes.setdefault(inbox or name, len(self.inboxes))
        self.made[name] = lambda: pltpu.make_async_remote_copy(
            src(), dst(), self.sems[0].at[send], self.sems[1].at[recv], device_id=peer, device_id_type=MESH
        )

    def start(self, *names):
        for name in names:
            self.made[name]().start()

    def landed(self, *names):
        for name in names:
            self.made[name]().wait_recv()

    def all_landed(self, inbox, whole, **peer):
        copy = pltpu.make_async_remote_copy(whole, whole, self.sems[0].at[0], self.sems[1].at[self.inboxes[inbox]], device_id=peer, device_id_type=MESH)
        copy.wait_recv()

    def all_sent(self, pool, whole, **peer):
        copy = pltpu.make_async_remote_copy(whole, whole, self.sems[0].at[self.pools[pool]], self.sems[1].at[0], device_id=peer, device_id_type=MESH)
        copy.wait_send()


def main_kernel(
    plan,
    len_hbm,
    x_hbm,
    g1_hbm,
    wdq_hbm,
    gq_hbm,
    wdkv_hbm,
    gkv_hbm,
    cos_hbm,
    sin_hbm,
    wq_hbm,
    wk_hbm,
    wv_hbm,
    wo_hbm,
    lat_hbm,
    pe_hbm,
    c_out,
    p_out,
    o_out,
    wo_out,
    x_buf,
    wdq,
    wdkv,
    a_buf,
    rows,
    rot,
    pe_buf,
    cos_ref,
    sin_ref,
    cq_buf,
    wq,
    wkv,
    kb,
    vb,
    qb,
    q_raw,
    sb,
    mb,
    pb,
    lb,
    o_own,
    o_send,
    wo_buf,
    len_ref,
    g1_ref,
    gq_ref,
    gkv_ref,
    load_sem,
    send_sem,
    recv_sem,
):
    size, stride, paired = plan
    me = lax.axis_index("tp")
    odd = lax.rem(me, 2)
    chip = me // 2
    right, left = lax.rem(me + 2, size), lax.rem(me + size - 2, size)
    onward = jnp.where(odd == 0, right, left)
    other = me + 1 - 2 * odd
    dp = lax.axis_index("dp")
    flip = {"a": lax.rem(dp, 2), "b": lax.rem(dp // stride, 2)}
    partner = {"a": dp + 1 - 2 * flip["a"], "b": dp + stride * (1 - 2 * flip["b"])}

    seqs, toks, dim = x_hbm.shape
    groups = rot.shape[0]
    per = seqs // groups
    rank = rows.shape[2]
    slots = size // 2
    chunk = size * toks
    prefix = rows.shape[1] - chunk
    heads = wq.shape[0] // slots
    head, q_rank = wq.shape[1:]
    rope = BLOCK // per
    half = rope // 2
    nope = head - rope
    quads = wq.shape[0] // 4
    duos = seqs // 2
    wide = 2 * BLOCK
    factor = LOG2E * head**-0.5

    loads = {}

    def load(name, src, dst):
        loads[name] = pltpu.make_async_copy(src, dst, load_sem.at[len(loads)])
        loads[name].start()

    def spot(slot, parity):
        return pl.ds(pl.multiple_of(prefix + slot * BLOCK + parity * toks, toks), toks)

    barrier = pltpu.get_barrier_semaphore()
    for peer in (left, right, other):
        pl.semaphore_signal(barrier, inc=1, device_id={"tp": peer}, device_id_type=MESH)
    for side in "ab":
        if paired[side]:
            pl.semaphore_signal(barrier, inc=1, device_id={"dp": partner[side]}, device_id_type=MESH)

    lanes_chip = pl.ds(pl.multiple_of(chip * BLOCK, BLOCK), BLOCK)
    def load_x(g):
        load(f"x{g}", x_hbm.at[pl.ds(g * per, per)], x_buf.at[pl.ds(g * per, per)])

    load("g1", g1_hbm, g1_ref)
    load_x(0)
    load("wdkv", wdkv_hbm, wdkv)
    load("gkv", gkv_hbm, gkv_ref)
    load("gq", gq_hbm, gq_ref)
    load("len", len_hbm, len_ref)
    load("cos", cos_hbm.at[:, :, lanes_chip], cos_ref)
    load("sin", sin_hbm.at[:, :, lanes_chip], sin_ref)

    wire = Wire(send_sem, recv_sem)

    def chain(name, here, there, places, via="split", whole=True):
        near_left, near_right, opposite = places
        handed = {"right": near_left, "left": near_right, "split": jnp.where(odd == 0, near_left, near_right)}[via]
        pool = name[0] if name[1].isdigit() else name[:4]
        if whole:
            wire.add(name + "R", pool, lambda: here(0), lambda: there(near_left), tp=right)
        wire.add(name + "L", pool, lambda: here(0), lambda: there(near_right), tp=left)
        wire.add(name + "O", pool, lambda: there(handed), lambda: there(opposite), tp={"right": right, "left": left, "split": onward}[via])

    for g in range(groups):
        for name, ref in (("c", lambda slot, g=g: rows.at[pl.ds(g * per, per), spot(slot, odd)]), ("p", lambda slot, g=g: rot.at[g, spot(slot, odd)])):
            name = f"{name}{g}"
            chain(name, ref, ref, (1, 3, 2), "left")
            for slot in range(slots):
                wire.add(f"{name}S{slot}", name[0], functools.partial(ref, slot), functools.partial(ref, slot), f"{name}S", tp=other)
        cq_ref = lambda g=g: cq_buf.at[odd, pl.ds(g * per, per)]
        wire.add(f"q{g}S", "q", cq_ref, cq_ref, tp=other)

    def cut(side, low, high, unit, mine):
        half_size = (high - low) // 2
        which = flip[side] if mine else 1 - flip[side]
        return pl.ds(pl.multiple_of(low + which * half_size, unit), half_size)

    q_cut = head * 2 // 3
    o_cut = wo_hbm.shape[0] * 2 // 5
    lots = {"R": (0, 3), "r": (3, heads - 3)}
    everyone = (0, heads)

    def lot_of(place, lot):
        return pl.ds(place * heads + lot[0], lot[1])

    pieces = {
        "wq.a": (lambda r, lot: wq_hbm.at[pl.ds(*lot), r], lambda place, r, lot: wq.at[lot_of(place, lot), r], ("a", 0, q_cut, 16)),
        "wq.b": (lambda r, lot: wq_hbm.at[pl.ds(*lot), r], lambda place, r, lot: wq.at[lot_of(place, lot), r], ("b", q_cut, head, 16)),
        "wk.a": (
            lambda r, lot: wk_hbm.at[pl.ds(*lot), :, r],
            lambda place, r, lot: wkv.at[lot_of(place, lot), pl.ds(0, nope), r],
            ("a", 0, rank, BLOCK),
        ),
        "wv.b": (
            lambda r, lot: wv_hbm.at[pl.ds(*lot), :, r],
            lambda place, r, lot: wkv.at[lot_of(place, lot), pl.ds(nope, nope), r],
            ("b", 0, rank, BLOCK),
        ),
        "wo.a": (lambda r, lot: wo_hbm.at[r], lambda place, r, lot: wo_out.at[odd, place, r], ("a", 0, o_cut, 16)),
        "wo.b": (lambda r, lot: wo_hbm.at[r], lambda place, r, lot: wo_out.at[odd, place, r], ("b", o_cut, 2 * o_cut, 16)),
    }
    left_over = pl.ds(2 * o_cut, wo_hbm.shape[0] - 2 * o_cut)
    chain("wo.m", lambda place: wo_hbm.at[left_over], lambda place: wo_out.at[odd, place, left_over], (1, 2, 3))
    for piece, (source, target, bounds) in pieces.items():
        side = bounds[0]
        large = piece.startswith("wo")
        for mine in (True,) if paired[side] else (True, False):
            here = lambda place, lot=everyone, source=source, bounds=bounds, mine=mine: source(cut(*bounds, mine), lot)
            there = lambda place, lot=everyone, target=target, bounds=bounds, mine=mine: target(place, cut(*bounds, mine), lot)
            name = piece + ("" if mine else "~")
            chain(name, here, there, (1, 2, 3), "split" if large else "right", large)
            if not large:
                for way, lot in lots.items():
                    wire.add(name + way, piece, functools.partial(here, 0, lot), functools.partial(there, 1, lot), tp=right)
        if paired[side]:
            for place, tag, lot in ((1, "", everyone),) if large else ((1, "", lots["R"]), (1, "r", lots["r"])):
                ref = lambda place=place, lot=lot, target=target, bounds=bounds: target(place, cut(*bounds, True), lot)
                wire.add(f"{piece}X{place}{tag}", piece, ref, ref, dp=partner[side])
            for place in (2, 3):
                ref = lambda place=place, target=target, bounds=bounds: target(place, cut(*bounds, True), everyone)
                wire.add(f"{piece}X{place}", piece, ref, ref, dp=partner[side])
    for place in range(slots - 1):
        ref = lambda place=place: wo_out.at[odd, place]
        wire.add(f"woS{place}", "woS", ref if place else lambda: wo_hbm, ref, tp=other)
    for piece in ("wo.a", "wo.b"):
        for mine in (True, False):
            ref = lambda piece=piece, mine=mine: pieces[piece][1](slots - 1, cut(*pieces[piece][2], mine), everyone)
            wire.add(f"{piece}S" + ("" if mine else "~"), "woS", ref, ref, tp=other)
    ref = lambda: wo_out.at[odd, slots - 1, left_over]
    wire.add("wo.mS", "woS", ref, ref, tp=other)
    for quad in range(quads - 1):
        wire.add(f"o{quad}S", "o", lambda quad=quad: o_send.at[quad], lambda quad=quad: o_out.at[odd, quad], tp=other)
    cut_o = seqs - 4
    for name, part in (("o.a", pl.ds(0, cut_o)), ("o.b", pl.ds(cut_o, seqs - cut_o))):
        wire.add(name + "S", "o", lambda part=part: o_send.at[quads - 1, part], lambda part=part: o_out.at[odd, quads - 1, part], tp=other)

    small = ("wk.a", "wv.b", "wq.a", "wq.b")

    def ring(which, *kinds):
        return [f"{kind}{half_name}{way}" for kind in kinds for half_name in ("", "~")[: 1 if paired[kind[-1]] else 2] for way in which]

    def across(place, *kinds):
        return [f"{kind}X{place}" for kind in kinds if paired[kind[-1]]]

    def norm(g):
        for r in range(per):
            for at in range(0, toks, NORM_ROWS):
                x = x_buf[g * per + r, at : at + NORM_ROWS].astype(F32)
                a_buf[g, r * toks + at : r * toks + at + NORM_ROWS] = (unit(x) * g1_ref[...]).astype(BF16)

    def latent(g):
        kv = dot_t(a_buf[g], wdkv[...])
        rows[g * per : (g + 1) * per, spot(0, odd), :] = (unit(kv[:, :rank]) * gkv_ref[...]).astype(BF16).reshape(per, toks, rank)
        turned = []
        for s in range(per):
            cos_pair, sin_pair = cos_ref[g * per + s], sin_ref[g * per + s]
            cos = jnp.where(odd == 1, cos_pair[:, toks:], cos_pair[:, :toks])
            sin = jnp.where(odd == 1, sin_pair[:, toks:], sin_pair[:, :toks])
            table = jnp.concatenate([cos, cos, -sin, sin], axis=0).T
            p = kv[s * toks : (s + 1) * toks, rank:]
            swapped = jnp.concatenate([p[:, half:], p[:, :half]], axis=1)
            turned.append(p * table[:, :rope] + swapped * table[:, rope:])
        rot[g, spot(0, odd), :] = jnp.concatenate(turned, axis=1).astype(BF16)

    def queries(g):
        h = jnp.concatenate([dot(a_buf[g], wdq[:, : 2 * rank]), dot(a_buf[g], wdq[:, 2 * rank :])], axis=1)
        cq_buf[odd, g * per : (g + 1) * per] = (unit(h) * gq_ref[...]).astype(BF16).reshape(per, toks, q_rank)

    loads["g1"].wait()
    with jax.named_scope('p_norm0'):
        loads["x0"].wait()
        for g in range(1, groups):
            load_x(g)
        norm(0)
    for name in ("wdkv", "cos", "sin", "gkv", "gq", "len"):
        loads[name].wait()
    load("wdq", wdq_hbm, wdq)
    load("wk", wk_hbm, wkv.at[pl.ds(0, heads), pl.ds(0, nope)])
    load("wv", wv_hbm, wkv.at[pl.ds(0, heads), pl.ds(nope, nope)])
    load("wq", wq_hbm, wq.at[pl.ds(0, heads)])
    load("pe", pe_hbm.at[:, :, pl.ds(0, prefix)], pe_buf)
    load("lat", lat_hbm.at[:, pl.ds(0, prefix)], rows.at[:, pl.ds(0, prefix)])
    with jax.named_scope('p_bar'):
        pl.semaphore_wait(barrier, 3 + paired["a"] + paired["b"])
    with jax.named_scope('p_kv'):
        for g in range(groups):
            latent(g)
            for way in ("R", "L", "S0"):
                wire.start(f"c{g}{way}", f"p{g}{way}")
            if g + 1 < groups:
                loads[f"x{g + 1}"].wait()
                norm(g + 1)
    wire.start(*ring("R", *small), *ring("r", *small))

    def hand_on(g):
        wire.landed(f"c{g}L", f"p{g}L", f"c{g}R", f"p{g}R")
        wire.start(f"c{g}O", f"p{g}O", f"c{g}S3", f"p{g}S3", f"c{g}S1", f"p{g}S1")

    with jax.named_scope('p_cq'):
        loads["wdq"].wait()
        for g in range(groups):
            queries(g)
            wire.start(f"q{g}S")
            hand_on(g)
    wire.start(*ring("L", *small, "wo.b", "wo.a"), "wo.mL", "woS0")

    loads["pe"].wait()
    for g in range(groups):
        old = pe_buf[g * per : (g + 1) * per].reshape(per * rope, prefix).astype(F32)
        for b in range(prefix // BLOCK):
            rot[g, b * BLOCK : (b + 1) * BLOCK] = old[:, b * BLOCK : (b + 1) * BLOCK].T.astype(BF16)
    qb[...] = jnp.zeros_like(qb)

    def rest_of(g):
        wire.landed(f"c{g}O", f"p{g}O")
        wire.start(f"c{g}S2", f"p{g}S2")
        wire.all_landed(f"c{g}S", rows.at[pl.ds(0, per), pl.ds(0, slots * toks)], tp=other)
        wire.all_landed(f"p{g}S", rot.at[0, pl.ds(0, slots * toks)], tp=other)
        if g:
            wire.landed(f"q{g}S")

    with jax.named_scope('p_rest0'):
        for name in ("wk", "wv", "wq", "lat"):
            loads[name].wait()
    row = lax.broadcasted_iota(jnp.int32, (BLOCK, wide), 0)
    lane = lax.rem(lax.broadcasted_iota(jnp.int32, (BLOCK, wide), 1), BLOCK)
    near = row <= lane

    def place(n):
        return n // duos, lax.rem(n, duos)

    def query_dot(n):
        quad, duo = place(n)
        w = wq[pl.ds(quad * 4, 4)].reshape(4 * head, q_rank)
        cq = jnp.concatenate([cq_buf[parity, 2 * duo + u] for u in range(2) for parity in range(2)], axis=0)
        q_raw[...] = dot_t(w, cq)

    def query_stage(n):
        quad, duo = place(n)
        raw = q_raw
        for u in range(2):
            slot = 2 * lax.rem(duo, 2) + u
            cos, sin = cos_ref[2 * duo + u], sin_ref[2 * duo + u]
            for h in range(4):
                pair, side = h // 2, h % 2
                q = raw[h * head : (h + 1) * head, u * BLOCK : (u + 1) * BLOCK]
                cols = slice(side * BLOCK, (side + 1) * BLOCK)
                qb[u, pair, side * nope : (side + 1) * nope, cols] = q[:nope].astype(BF16)
                lo, hi = q[nope : nope + half], q[nope + half :]
                turned = jnp.concatenate([lo * cos - hi * sin, hi * cos + lo * sin], axis=0).astype(BF16)
                start = pl.multiple_of(BLOCK + slot * rope, rope)
                stale = pl.multiple_of(BLOCK + lax.rem(slot + 2, 4) * rope, rope)
                qb[u, pair, pl.ds(start, rope), cols] = turned
                qb[u, pair, pl.ds(stale, rope), cols] = jnp.zeros_like(turned)

    def key_stage(n, t, u):
        quad, duo = place(n)
        w = wkv[pl.ds(quad * 4, 4), :nope].reshape(4 * nope, rank)
        kb[u][:t] = dot_t(rows[2 * duo + u, :t], w).astype(BF16)

    def value_stage(n, t, u):
        quad, duo = place(n)
        w = wkv[pl.ds(quad * 4, 4), nope:].reshape(4 * nope, rank)
        vb[u][:, :t] = dot_t(w, rows[2 * duo + u, :t]).astype(BF16)

    def score_stage(n, t, u, pair):
        _, duo = place(n)
        length = len_ref[2 * duo + u]
        keys = jnp.concatenate([kb[u][:t, pair * BLOCK : (pair + 1) * BLOCK], rot[duo // 2, :t]], axis=1)
        value = dot(keys, qb[u, pair])
        most = None
        for b in range(t // BLOCK):
            part = value[b * BLOCK : (b + 1) * BLOCK]
            if BLOCK <= b * BLOCK < prefix:
                part = jnp.where(row < length - b * BLOCK, part, NEVER)
            if b * BLOCK == prefix:
                part = jnp.where(near, part, NEVER)
            sb[2 * u + pair][b * BLOCK : (b + 1) * BLOCK] = part
            part = jnp.max(part.reshape(BLOCK // 8, 8, wide), axis=0)
            most = part if most is None else jnp.maximum(most, part)
        mb[2 * u + pair] = jnp.broadcast_to(jnp.max(most, axis=0, keepdims=True), (8, wide))

    def soft_stage(t, u, pair):
        i = 2 * u + pair
        most = mb[i, :1]
        total = None
        for b in range(t // BLOCK):
            x = jnp.exp2((sb[i][b * BLOCK : (b + 1) * BLOCK] - most) * factor)
            part = jnp.sum(x.reshape(BLOCK // 8, 8, wide), axis=0)
            total = part if total is None else total + part
            pb[i][b * BLOCK : (b + 1) * BLOCK] = x.astype(BF16)
        lb[i] = total

    def mix_stage(n, t, u, pair):
        quad, duo = place(n)
        i = 2 * u + pair
        inv = 1.0 / jnp.sum(lb[i], axis=0, keepdims=True)
        o = dot(vb[u][pair * BLOCK : (pair + 1) * BLOCK, :t], pb[i][:t]) * inv
        o = jnp.concatenate([o[:nope, :BLOCK], o[nope:, BLOCK:]], axis=0).T.astype(BF16)
        first, second = o[:toks], o[toks:]
        cols = slice(pair * BLOCK, (pair + 1) * BLOCK)
        o_own[quad, 2 * duo + u, :, cols] = jnp.where(odd == 1, second, first)
        o_send[quad, 2 * duo + u, :, cols] = jnp.where(odd == 1, first, second)

    units = [(u, pair) for u in range(2) for pair in range(2)]
    total = quads * duos

    def each_chip(fn):
        for c in range(slots):
            pl.when(chip == c)(lambda c=c: fn(prefix + (c + 1) * BLOCK))

    def body(b, t):
        before, ahead, later = jnp.maximum(b - 1, 0), jnp.minimum(b + 1, total - 1), jnp.minimum(b + 2, total - 1)
        mix_stage(before, t, 0, 0)
        mix_stage(before, t, 0, 1)
        mix_stage(before, t, 1, 0)
        mix_stage(before, t, 1, 1)
        soft_stage(t, 0, 0)
        score_stage(ahead, t, 0, 0)
        value_stage(b, t, 0)
        soft_stage(t, 0, 1)
        score_stage(ahead, t, 0, 1)
        key_stage(later, t, 0)
        soft_stage(t, 1, 0)
        score_stage(ahead, t, 1, 0)
        value_stage(b, t, 1)
        soft_stage(t, 1, 1)
        score_stage(ahead, t, 1, 1)
        query_dot(later)
        query_stage(later)
        key_stage(later, t, 1)

    def front(b, t):
        before, ahead = jnp.maximum(b - 1, 0), b + 1
        for u, pair in units:
            mix_stage(before, t, u, pair)
        for u in range(2):
            soft_stage(t, u, 0)
            score_stage(ahead, t, u, 0)
            value_stage(b, t, u)
            soft_stage(t, u, 1)
            score_stage(ahead, t, u, 1)

    def back(b, t):
        for u in range(2):
            key_stage(b + 2, t, u)
        query_dot(b + 2)
        query_stage(b + 2)

    def at(b, when):
        return pl.when(b == when)

    agenda = {
        0: [(None, ring("R", "wq.a", "wq.b"), across(1, "wq.a", "wq.b"))],
        2: [(None, ring("r", *small), across("1r", *small) + ring("O", *small) + ring("R", "wo.a", "wo.b") + ["wo.mR"])],
        3: [(None, ring("L", "wk.a", "wv.b"), across(2, "wk.a", "wv.b"))],
        4: [(None, across(1, *small), [])],
        5: [(None, ring("L", "wq.a"), across(2, "wq.a"))],
        7: [(None, ring("L", "wq.b"), across(2, "wq.b"))],
        9: [(None, ring("O", *small), across(3, *small))],
        10: [(None, across("1r", *small) + across(2, *small), [])],
        11: [(None, ring("L", "wo.b"), across(2, "wo.b")), (1, [], ring("O", "wo.b"))],
        13: [(None, ring("R", "wo.a"), across(1, "wo.a")), (0, [], ring("O", "wo.a"))],
        15: [(None, across(3, *small), []), (None, ring("L", "wo.a"), across(2, "wo.a")), (1, [], ring("O", "wo.a"))],
        16: [(None, ring("R", "wo.b"), across(1, "wo.b")), (0, [], ring("O", "wo.b"))],
        20: [(0, ["wo.mR"], ["wo.mO"]), (1, ["wo.mL"], ["wo.mO"])],
        22: [(0, ring("O", "wo.a"), across(3, "wo.a") + ["wo.aS"]), (1, ring("O", "wo.b"), across(3, "wo.b") + ["wo.bS"])],
        23: [
            (0, ["wo.mL"], []),
            (1, ["wo.mR"], []),
            (None, across(1, "wo.a", "wo.b") + across(2, "wo.a", "wo.b"), ["woS1", "woS2"]),
        ],
        24: [(0, ring("O", "wo.b"), across(3, "wo.b") + ["wo.bS"]), (1, ring("O", "wo.a"), across(3, "wo.a") + ["wo.aS"])],
        29: [(None, ["wo.mO"], ["wo.mS"]), (None, across(3, "wo.a", "wo.b"), ["wo.aS~", "wo.bS~", "o.aS"])],
    }
    for quad in range(quads - 1):
        agenda.setdefault((quad + 1) * duos + 1, []).append((None, [], [f"o{quad}S"]))

    def run_agenda(when):
        for parity, waits, starts in agenda[when]:

            def item(waits=waits, starts=starts):
                with jax.named_scope(f"ev_{when}"):
                    wire.landed(*waits)
                wire.start(*starts)

            if parity is None:
                item()
            else:
                pl.when(odd == parity)(item)

    bounce = pltpu.make_async_copy(wo_hbm, wo_buf, load_sem.at[3])
    span = 8

    def step(b, _):
        for first in range(0, total, span):

            @pl.when(b // span == first // span)
            def _():
                for when in sorted(agenda):
                    if first <= when < first + span:
                        at(b, when)(functools.partial(run_agenda, when))
                if first == 0:

                    @at(b, 4)
                    def _():
                        pltpu.make_async_copy(rows.at[:, pl.ds(prefix, chunk)], c_out, load_sem.at[0]).start()
                        pltpu.make_async_copy(rot.at[:, pl.ds(prefix, chunk)], p_out, load_sem.at[1]).start()
                        bounce.start()

                    @at(b, 6)
                    def _():
                        bounce.wait()
                        pltpu.make_async_copy(wo_buf, wo_out.at[odd, 0], load_sem.at[4]).start()

        split = (b == 0) | (b == 2)

        @pl.when(split)
        def _():
            with jax.named_scope('front'):
                each_chip(functools.partial(front, b))
            at(b, 0)(lambda: rest_of(1))
            at(b, 2)(lambda: rest_of(2))
            with jax.named_scope('back'):
                each_chip(functools.partial(back, b))

        @pl.when(jnp.logical_not(split))
        def _():
            with jax.named_scope('body'):
                each_chip(functools.partial(body, b))

        return 0

    def lead_in(t):
        for u in range(2):
            key_stage(0, t, u)
        for u, pair in units:
            score_stage(0, t, u, pair)
        for u in range(2):
            key_stage(1, t, u)
        query_dot(1)
        query_stage(1)

    wire.landed("q0S")
    query_dot(0)
    query_stage(0)
    rest_of(0)
    wire.landed(*ring("R", "wk.a", "wv.b"))
    wire.start(*across(1, "wk.a", "wv.b"))
    with jax.named_scope('p_lead'):
        each_chip(lead_in)
    lax.fori_loop(0, total, step, 0)

    def last(t):
        for u, pair in units:
            mix_stage(total - 1, t, u, pair)

    with jax.named_scope('p_last'):
        each_chip(last)
        wire.start("o.bS")
        pltpu.make_async_copy(o_own, o_out.at[odd], load_sem.at[2]).start()
    with jax.named_scope('f_land'):
        for place in range(slots - 1):
            wire.landed(f"woS{place}")
        wire.landed("wo.aS", "wo.bS", "wo.mS", "wo.aS~", "wo.bS~")
        for quad in range(quads - 1):
            wire.landed(f"o{quad}S")
        wire.landed("o.aS", "o.bS")
    with jax.named_scope('f_sent'):
        wire.all_sent("c", rows.at[pl.ds(0, per * groups // 2), pl.ds(0, 14 * toks)], tp=other)
        wire.all_sent("p", rot.at[pl.ds(0, groups), pl.ds(0, 7 * toks)], tp=other)
        wire.all_sent("q", cq_buf.at[odd], tp=other)
        wire.all_sent("wq.a", wq.at[pl.ds(0, 3 * heads), pl.ds(0, q_cut)], tp=other)
        wire.all_sent("wq.b", wq.at[pl.ds(0, 3 * heads), pl.ds(0, head - q_cut)], tp=other)
        wire.all_sent("wk.a", wkv.at[pl.ds(0, 3 * heads), pl.ds(0, nope)], tp=other)
        wire.all_sent("wv.b", wkv.at[pl.ds(0, 3 * heads), pl.ds(0, nope)], tp=other)
        wire.all_sent("wo.a", wo_out.at[0, pl.ds(0, 3), pl.ds(0, o_cut)], tp=other)
        wire.all_sent("wo.b", wo_out.at[0, pl.ds(0, 3), pl.ds(0, o_cut)], tp=other)
        wire.all_sent("wo.m", wo_out.at[0, pl.ds(0, 3), left_over], tp=other)
        wire.all_sent("woS", wo_out.at[0], tp=other)
        wire.all_sent("o", o_send, tp=other)
        pltpu.make_async_copy(rows.at[:, pl.ds(prefix, chunk)], c_out, load_sem.at[0]).wait()
        pltpu.make_async_copy(rot.at[:, pl.ds(prefix, chunk)], p_out, load_sem.at[1]).wait()
        pltpu.make_async_copy(o_own, o_out.at[odd], load_sem.at[2]).wait()
        pltpu.make_async_copy(wo_buf, wo_out.at[odd, 0], load_sem.at[4]).wait()


def finish_kernel(
    len_hbm, o_hbm, w_hbm, x_hbm, c_hbm, p_hbm, lat_hbm, pe_hbm, y_hbm, lat_out, pe_out, fresh, acc, x_buf, y_buf, o_buf, w_buf, c_buf, p_buf, lat_buf, pe_buf, lat_new, pe_new, len_ref, load_sem, store_sem, sems
):
    chip = lax.axis_index("tp") // 2
    quads, seqs, toks, depth = o_hbm.shape[1:]
    terms = 2 * quads
    slots = c_hbm.shape[1]
    rank = lat_hbm.shape[2]
    rope, cache_len = pe_hbm.shape[1:]
    chunk = slots * 2 * toks
    words = rank // BLOCK
    dim = x_hbm.shape[2]
    part = 2 * depth
    ring = w_buf.shape[0]

    def loads(k, with_term):
        slot = lax.rem(k, ring)
        out = [
            pltpu.make_async_copy(c_hbm.at[k], c_buf.at[slot], load_sem.at[0, slot]),
            pltpu.make_async_copy(lat_hbm.at[k], lat_buf.at[slot], load_sem.at[1, slot]),
        ]
        if with_term:
            side, quad = k // quads, lax.rem(k, quads)
            out.append(pltpu.make_async_copy(o_hbm.at[side, quad], o_buf.at[slot], load_sem.at[2, slot]))
            out.append(pltpu.make_async_copy(w_hbm.at[side, pl.ds(pl.multiple_of(quad * depth, depth), depth)], w_buf.at[slot], load_sem.at[3, slot]))
        return out

    def store(k):
        slot = lax.rem(k, ring)
        return pltpu.make_async_copy(lat_new.at[slot], lat_out.at[k], store_sem.at[slot])

    load_len = pltpu.make_async_copy(len_hbm, len_ref, sems.at[4 + dim // part])
    load_x = pltpu.make_async_copy(x_hbm, x_buf, sems.at[0])
    load_p = pltpu.make_async_copy(p_hbm, p_buf, sems.at[1])
    load_pe = pltpu.make_async_copy(pe_hbm, pe_buf, sems.at[2])
    store_pe = pltpu.make_async_copy(pe_new, pe_out, sems.at[3])

    def store_y(n):
        cols = pl.ds(n * part, part)
        return pltpu.make_async_copy(y_buf.at[:, :, cols], y_hbm.at[:, :, cols], sems.at[4 + n])


    def slot_of(j):
        return lax.rem(chip - j + slots, slots)

    def project(k, kind):
        slot = lax.rem(k, ring)
        o = o_buf[slot].reshape(seqs * toks, depth)
        for n in range(0, dim, part):
            cols = slice(n, n + part)
            y = dot(o, w_buf[slot, :, cols])
            if kind != "first":
                y = acc[:, cols] + y
            if kind == "last":
                y = y + x_buf[:, :, cols].reshape(seqs * toks, part).astype(F32)
                y_buf[:, :, cols] = y.astype(BF16).reshape(seqs, toks, part)
                store_y(n // part).start()
            else:
                acc[:, cols] = y

    def cache(k):
        at_slot = lax.rem(k, ring)
        length = len_ref[k]
        for j in range(slots):
            piece = c_buf[at_slot, slot_of(j)].reshape(2 * toks, rank).astype(F32)
            for w in range(words):
                fresh[w, BLOCK + j * 2 * toks : BLOCK + (j + 1) * 2 * toks] = piece[:, w * BLOCK : (w + 1) * BLOCK]
        lat_new[at_slot] = lat_buf[at_slot]
        base = (length // 16) * 16
        skew = length - base
        tile_row = lax.broadcasted_iota(jnp.int32, (16, BLOCK), 0)
        for i in range(chunk // 16 + 1):
            at = pl.multiple_of(jnp.minimum(base + i * 16, cache_len - 16), 16)
            for w in range(words):
                cols = slice(w * BLOCK, (w + 1) * BLOCK)
                moved = fresh[w, pl.ds(BLOCK - skew + i * 16, 16), :].astype(BF16)
                if i == 0 or i == chunk // 16:
                    local = tile_row + (at - length)
                    shown = (local >= 0) & (local < chunk) if i == 0 else (local < chunk)
                    if i == 0:
                        rest = lat_buf[at_slot, pl.ds(at, 16), cols]
                    else:
                        shown = shown & (skew > 0)
                        rest = lat_new[at_slot, pl.ds(at, 16), cols]
                    moved = jnp.where(shown, moved.astype(F32), rest.astype(F32)).astype(BF16)
                lat_new[at_slot, pl.ds(at, 16), cols] = moved

        turned = jnp.concatenate([p_buf[k // (BLOCK // rope), slot_of(j)].reshape(2 * toks, BLOCK).astype(F32).T for j in range(slots)], axis=1)
        group = lax.rem(k, BLOCK // rope)
        mine = turned[:rope]
        for g in range(1, BLOCK // rope):
            mine = jnp.where(group == g, turned[g * rope : (g + 1) * rope], mine)
        mine = jnp.concatenate([mine, jnp.zeros((rope, cache_len - chunk), F32)], axis=1)
        mine = pltpu.roll(mine, length, axis=1)
        spot = lax.broadcasted_iota(jnp.int32, (rope, cache_len), 1) - length
        pe_new[k] = jnp.where((spot >= 0) & (spot < chunk), mine, pe_buf[k].astype(F32)).astype(BF16)

    def begin(k, with_term):
        for load in loads(k, with_term):
            load.start()

    def arrived(k, with_term):
        for load in loads(k, with_term):
            load.wait()

    def work(k, kind):
        if kind != "none":
            project(k, kind)
        cache(k)
        store(k).start()

    def more(k):
        pl.when(k < terms)(lambda: begin(k, True))
        pl.when((k >= terms) & (k < seqs))(lambda: begin(k, False))

    first = loads(0, True)
    for load in first[2:] + first[:2]:
        load.start()
    load_len.start()
    load_p.start()
    load_pe.start()
    for load in first[2:]:
        load.wait()
    begin(1, True)
    begin(2, True)
    project(0, "first")
    for load in first[:2] + [load_len, load_p, load_pe]:
        load.wait()
    begin(3, True)
    cache(0)
    store(0).start()
    load_x.start()

    def middle(k, _):
        with jax.named_scope('g_wait'):
            arrived(k, True)
        more(k + ring - 1)

        @pl.when(k >= ring)
        def _():
            store(k - ring).wait()

        with jax.named_scope('g_work'):
            work(k, "middle")
        return 0

    lax.fori_loop(1, terms - 1, middle, 0)
    last = terms - 1
    arrived(last, True)
    more(last + ring - 1)
    store(last - ring).wait()
    load_x.wait()
    with jax.named_scope('g_last'):
        work(last, "last")

    def tail(k, _):
        arrived(k, False)
        store(k - ring).wait()
        with jax.named_scope('g_tail'):
            work(k, "none")
        return 0

    lax.fori_loop(terms, seqs, tail, 0)
    store_pe.start()
    for k in range(ring):
        store(seqs - ring + k).wait()
    store_pe.wait()
    for n in range(dim // part):
        store_y(n).wait()


def solution(mesh):
    size = mesh.shape["tp"]
    count = mesh.shape["dp"]
    stride = 2 ** (count.bit_length() // 2)
    paired = {"a": count % 2 == 0, "b": count % (2 * stride) == 0}

    def local_step(hidden, lengths, rope_cos, rope_sin, cache_lat, cache_pe, norm_in, w_dq, norm_q, w_dkv, norm_kv, w_uq, w_uk, w_uv, w_out):
        seqs, toks, dim = hidden.shape
        q_rank = w_dq.shape[1]
        rank, heads, nope = w_uk.shape
        rope = cache_pe.shape[2]
        cache_len = cache_lat.shape[1]
        slots = size // 2
        head = nope + rope
        quads = slots * heads // 4
        chunk = size * toks
        prefix = cache_len - chunk
        per = BLOCK // rope
        groups = seqs // per
        wide = 2 * BLOCK
        cos_t, sin_t = rope_cos.transpose(0, 2, 1), rope_sin.transpose(0, 2, 1)
        pe_t = cache_pe.transpose(0, 2, 1)
        wdkv_t = w_dkv.transpose(1, 0)
        wq_t, wk_t, wv_t = (w.transpose(1, 2, 0) for w in (w_uq, w_uk, w_uv))

        inboxes = 9 * groups + 36 + 8 + 3 + slots + 4 + quads + 1
        any_spec = pl.BlockSpec(memory_space=pl.ANY)
        c_all, p_all, o_all, wo_all = pl.pallas_call(
            functools.partial(main_kernel, (size, stride, paired)),
            in_specs=[any_spec] * 15,
            out_specs=[any_spec] * 4,
            out_shape=[
                jax.ShapeDtypeStruct((seqs, chunk, rank), BF16),
                jax.ShapeDtypeStruct((groups, chunk, BLOCK), BF16),
                jax.ShapeDtypeStruct((2, quads, seqs, toks, 4 * nope), BF16),
                jax.ShapeDtypeStruct((2, slots) + w_out.shape, BF16),
            ],
            scratch_shapes=[
                pltpu.VMEM(hidden.shape, BF16),
                pltpu.VMEM(w_dq.shape, BF16),
                pltpu.VMEM(wdkv_t.shape, BF16),
                pltpu.VMEM((groups, per * toks, dim), BF16),
                pltpu.VMEM((seqs, cache_len, rank), BF16),
                pltpu.VMEM((groups, cache_len, BLOCK), BF16),
                pltpu.VMEM((seqs, rope, prefix), BF16),
                pltpu.VMEM((seqs, rope // 2, BLOCK), F32),
                pltpu.VMEM((seqs, rope // 2, BLOCK), F32),
                pltpu.VMEM((2, seqs, toks, q_rank), BF16),
                pltpu.VMEM((slots * heads, head, q_rank), BF16),
                pltpu.VMEM((slots * heads, 2 * nope, rank), BF16),
                [pltpu.VMEM((cache_len, 4 * nope), BF16) for _ in range(2)],
                [pltpu.VMEM((4 * nope, cache_len), BF16) for _ in range(2)],
                pltpu.VMEM((2, 2, wide, wide), BF16),
                pltpu.VMEM((4 * head, wide), F32),
                [pltpu.VMEM((cache_len, wide), F32) for _ in range(4)],
                pltpu.VMEM((4, 8, wide), F32),
                [pltpu.VMEM((cache_len, wide), BF16) for _ in range(4)],
                pltpu.VMEM((4, 8, wide), F32),
                pltpu.VMEM((quads, seqs, toks, 4 * nope), BF16),
                pltpu.VMEM((quads, seqs, toks, 4 * nope), BF16),
                pltpu.VMEM(w_out.shape, BF16),
                pltpu.SMEM(lengths.shape, jnp.int32),
                pltpu.VMEM(norm_in.shape, F32),
                pltpu.VMEM(norm_q.shape, F32),
                pltpu.VMEM(norm_kv.shape, F32),
                pltpu.SemaphoreType.DMA((13 + groups,)),
                pltpu.SemaphoreType.DMA((12,)),
                pltpu.SemaphoreType.DMA((inboxes,)),
            ],
            compiler_params=pltpu.CompilerParams(collective_id=0, has_side_effects=True, vmem_limit_bytes=63 * MIB),
            cost_estimate=pl.CostEstimate(flops=70 * 10**9, bytes_accessed=40 * MIB, transcendentals=30 * 10**6),
            name="main",
        )(lengths, hidden, norm_in, w_dq, norm_q, wdkv_t, norm_kv, cos_t, sin_t, wq_t, wk_t, wv_t, w_out, cache_lat, pe_t)

        depth = 4 * nope
        ahead = 4
        y, lat_new, pe_new = pl.pallas_call(
            finish_kernel,
            in_specs=[any_spec] * 8,
            out_specs=[any_spec] * 3,
            scratch_shapes=[
                pltpu.VMEM((rank // BLOCK, chunk + 2 * BLOCK, BLOCK), F32),
                pltpu.VMEM((seqs * toks, dim), F32),
                pltpu.VMEM(hidden.shape, BF16),
                pltpu.VMEM(hidden.shape, BF16),
                pltpu.VMEM((ahead, seqs, toks, depth), BF16),
                pltpu.VMEM((ahead, depth, dim), BF16),
                pltpu.VMEM((ahead, slots, 2, toks, rank), BF16),
                pltpu.VMEM((groups, slots, 2, toks, BLOCK), BF16),
                pltpu.VMEM((ahead, cache_len, rank), BF16),
                pltpu.VMEM(pe_t.shape, BF16),
                pltpu.VMEM((ahead, cache_len, rank), BF16),
                pltpu.VMEM(pe_t.shape, BF16),
                pltpu.SMEM(lengths.shape, jnp.int32),
                pltpu.SemaphoreType.DMA((4, ahead)),
                pltpu.SemaphoreType.DMA((ahead,)),
                pltpu.SemaphoreType.DMA((5 + dim // (2 * depth),)),
            ],
            out_shape=[
                jax.ShapeDtypeStruct(hidden.shape, BF16),
                jax.ShapeDtypeStruct(cache_lat.shape, BF16),
                jax.ShapeDtypeStruct(pe_t.shape, BF16),
            ],
            compiler_params=pltpu.CompilerParams(vmem_limit_bytes=63 * MIB),
            cost_estimate=pl.CostEstimate(flops=2 * seqs * toks * dim * dim, bytes_accessed=50 * MIB, transcendentals=0),
            name="finish",
        )(
            lengths,
            o_all,
            wo_all.reshape(2, slots * w_out.shape[0], dim),
            hidden,
            c_all.reshape(seqs, slots, 2, toks, rank),
            p_all.reshape(groups, slots, 2, toks, BLOCK),
            cache_lat,
            pe_t,
        )
        return y, lat_new, pe_new.transpose(0, 2, 1)

    spec_tok = P("dp", "tp", None)
    spec_len = P("dp")
    spec_seq = P("dp", None, None)
    spec_vec = P(None)
    spec_mat = P(None, None)
    spec_head = P(None, "tp", None)
    spec_rows = P("tp", None)
    in_specs = (spec_tok, spec_len, spec_seq, spec_seq, spec_seq, spec_seq, spec_vec, spec_mat, spec_vec, spec_mat, spec_vec, spec_head, spec_head, spec_head, spec_rows)
    return jax.shard_map(local_step, mesh=mesh, in_specs=in_specs, out_specs=(spec_tok, spec_seq, spec_seq), check_vma=False)
```

```python
import functools

import jax
import jax.numpy as jnp
from jax import lax
from jax.experimental import pallas as pl
from jax.experimental.pallas import tpu as pltpu
from jax.sharding import PartitionSpec as P

BLOCK = 128
LOG2E = 1.4426950408889634
NEVER = -1e30
NORM_ROWS = 16
F32 = jnp.float32
BF16 = jnp.bfloat16
MESH = pl.DeviceIdType.MESH
MIB = 2**20


def dot(a, b):
    return lax.dot_general(a, b, (((1,), (0,)), ((), ())), preferred_element_type=F32)


def dot_t(a, b):
    return lax.dot_general(a, b, (((1,), (1,)), ((), ())), preferred_element_type=F32)


def unit(x):
    return x * lax.rsqrt(jnp.mean(x * x, axis=-1, keepdims=True) + 1e-6)


class Wire:
    def __init__(self, send_sem, recv_sem):
        self.sems = (send_sem, recv_sem)
        self.made = {}
        self.pools = {}
        self.inboxes = {}

    def add(self, name, pool, src, dst, inbox=None, **peer):
        send = self.pools.setdefault(pool, len(self.pools))
        recv = self.inboxes.setdefault(inbox or name, len(self.inboxes))
        self.made[name] = lambda: pltpu.make_async_remote_copy(
            src(), dst(), self.sems[0].at[send], self.sems[1].at[recv], device_id=peer, device_id_type=MESH
        )

    def start(self, *names):
        for name in names:
            self.made[name]().start()

    def landed(self, *names):
        for name in names:
            self.made[name]().wait_recv()

    def all_landed(self, inbox, whole, **peer):
        copy = pltpu.make_async_remote_copy(whole, whole, self.sems[0].at[0], self.sems[1].at[self.inboxes[inbox]], device_id=peer, device_id_type=MESH)
        copy.wait_recv()

    def all_sent(self, pool, whole, **peer):
        copy = pltpu.make_async_remote_copy(whole, whole, self.sems[0].at[self.pools[pool]], self.sems[1].at[0], device_id=peer, device_id_type=MESH)
        copy.wait_send()


def main_kernel(
    plan,
    len_hbm,
    x_hbm,
    g1_hbm,
    wdq_hbm,
    gq_hbm,
    wdkv_hbm,
    gkv_hbm,
    cos_hbm,
    sin_hbm,
    wq_hbm,
    wk_hbm,
    wv_hbm,
    wo_hbm,
    lat_hbm,
    pe_hbm,
    c_out,
    p_out,
    o_out,
    wo_out,
    x_buf,
    wdq,
    wdkv,
    a_buf,
    rows,
    rot,
    pe_buf,
    cos_ref,
    sin_ref,
    cq_buf,
    wq,
    wkv,
    kb,
    vb,
    qb,
    q_raw,
    sb,
    mb,
    pb,
    lb,
    o_own,
    o_send,
    wo_buf,
    len_ref,
    g1_ref,
    gq_ref,
    gkv_ref,
    load_sem,
    send_sem,
    recv_sem,
):
    size, stride, paired = plan
    me = lax.axis_index("tp")
    odd = lax.rem(me, 2)
    chip = me // 2
    right, left = lax.rem(me + 2, size), lax.rem(me + size - 2, size)
    onward = jnp.where(odd == 0, right, left)
    other = me + 1 - 2 * odd
    dp = lax.axis_index("dp")
    flip = {"a": lax.rem(dp, 2), "b": lax.rem(dp // stride, 2)}
    partner = {"a": dp + 1 - 2 * flip["a"], "b": dp + stride * (1 - 2 * flip["b"])}

    seqs, toks, dim = x_hbm.shape
    groups = rot.shape[0]
    per = seqs // groups
    rank = rows.shape[2]
    slots = size // 2
    chunk = size * toks
    prefix = rows.shape[1] - chunk
    heads = wq.shape[0] // slots
    head, q_rank = wq.shape[1:]
    rope = BLOCK // per
    half = rope // 2
    nope = head - rope
    quads = wq.shape[0] // 4
    duos = seqs // 2
    wide = 2 * BLOCK
    factor = LOG2E * head**-0.5

    loads = {}

    def load(name, src, dst):
        loads[name] = pltpu.make_async_copy(src, dst, load_sem.at[len(loads)])
        loads[name].start()

    def spot(slot, parity):
        return pl.ds(pl.multiple_of(prefix + slot * BLOCK + parity * toks, toks), toks)

    barrier = pltpu.get_barrier_semaphore()
    for peer in (left, right, other):
        pl.semaphore_signal(barrier, inc=1, device_id={"tp": peer}, device_id_type=MESH)
    for side in "ab":
        if paired[side]:
            pl.semaphore_signal(barrier, inc=1, device_id={"dp": partner[side]}, device_id_type=MESH)

    lanes_chip = pl.ds(pl.multiple_of(chip * BLOCK, BLOCK), BLOCK)
    def load_x(g):
        load(f"x{g}", x_hbm.at[pl.ds(g * per, per)], x_buf.at[pl.ds(g * per, per)])

    load("g1", g1_hbm, g1_ref)
    load_x(0)
    load("wdkv", wdkv_hbm, wdkv)
    load("gkv", gkv_hbm, gkv_ref)
    load("gq", gq_hbm, gq_ref)
    load("len", len_hbm, len_ref)
    load("cos", cos_hbm.at[:, :, lanes_chip], cos_ref)
    load("sin", sin_hbm.at[:, :, lanes_chip], sin_ref)

    wire = Wire(send_sem, recv_sem)

    def chain(name, here, there, places, via="split", whole=True):
        near_left, near_right, opposite = places
        handed = {"right": near_left, "left": near_right, "split": jnp.where(odd == 0, near_left, near_right)}[via]
        pool = name[0] if name[1].isdigit() else name[:4]
        if whole:
            wire.add(name + "R", pool, lambda: here(0), lambda: there(near_left), tp=right)
        wire.add(name + "L", pool, lambda: here(0), lambda: there(near_right), tp=left)
        wire.add(name + "O", pool, lambda: there(handed), lambda: there(opposite), tp={"right": right, "left": left, "split": onward}[via])

    for g in range(groups):
        for name, ref in (("c", lambda slot, g=g: rows.at[pl.ds(g * per, per), spot(slot, odd)]), ("p", lambda slot, g=g: rot.at[g, spot(slot, odd)])):
            name = f"{name}{g}"
            chain(name, ref, ref, (1, 3, 2), "left")
            for slot in range(slots):
                wire.add(f"{name}S{slot}", name[0], functools.partial(ref, slot), functools.partial(ref, slot), f"{name}S", tp=other)
        cq_ref = lambda g=g: cq_buf.at[odd, pl.ds(g * per, per)]
        wire.add(f"q{g}S", "q", cq_ref, cq_ref, tp=other)

    def cut(side, low, high, unit, mine):
        half_size = (high - low) // 2
        which = flip[side] if mine else 1 - flip[side]
        return pl.ds(pl.multiple_of(low + which * half_size, unit), half_size)

    q_cut = head * 2 // 3
    o_cut = wo_hbm.shape[0] * 2 // 5
    lots = {"R": (0, 3), "r": (3, heads - 3)}
    everyone = (0, heads)

    def lot_of(place, lot):
        return pl.ds(place * heads + lot[0], lot[1])

    pieces = {
        "wq.a": (lambda r, lot: wq_hbm.at[pl.ds(*lot), r], lambda place, r, lot: wq.at[lot_of(place, lot), r], ("a", 0, q_cut, 16)),
        "wq.b": (lambda r, lot: wq_hbm.at[pl.ds(*lot), r], lambda place, r, lot: wq.at[lot_of(place, lot), r], ("b", q_cut, head, 16)),
        "wk.a": (
            lambda r, lot: wk_hbm.at[pl.ds(*lot), :, r],
            lambda place, r, lot: wkv.at[lot_of(place, lot), pl.ds(0, nope), r],
            ("a", 0, rank, BLOCK),
        ),
        "wv.b": (
            lambda r, lot: wv_hbm.at[pl.ds(*lot), :, r],
            lambda place, r, lot: wkv.at[lot_of(place, lot), pl.ds(nope, nope), r],
            ("b", 0, rank, BLOCK),
        ),
        "wo.a": (lambda r, lot: wo_hbm.at[r], lambda place, r, lot: wo_out.at[odd, place, r], ("a", 0, o_cut, 16)),
        "wo.b": (lambda r, lot: wo_hbm.at[r], lambda place, r, lot: wo_out.at[odd, place, r], ("b", o_cut, 2 * o_cut, 16)),
    }
    left_over = pl.ds(2 * o_cut, wo_hbm.shape[0] - 2 * o_cut)
    chain("wo.m", lambda place: wo_hbm.at[left_over], lambda place: wo_out.at[odd, place, left_over], (1, 2, 3))
    for piece, (source, target, bounds) in pieces.items():
        side = bounds[0]
        large = piece.startswith("wo")
        for mine in (True,) if paired[side] else (True, False):
            here = lambda place, lot=everyone, source=source, bounds=bounds, mine=mine: source(cut(*bounds, mine), lot)
            there = lambda place, lot=everyone, target=target, bounds=bounds, mine=mine: target(place, cut(*bounds, mine), lot)
            name = piece + ("" if mine else "~")
            chain(name, here, there, (1, 2, 3), "split" if large else "right", large)
            if not large:
                for way, lot in lots.items():
                    wire.add(name + way, piece, functools.partial(here, 0, lot), functools.partial(there, 1, lot), tp=right)
        if paired[side]:
            for place, tag, lot in ((1, "", everyone),) if large else ((1, "", lots["R"]), (1, "r", lots["r"])):
                ref = lambda place=place, lot=lot, target=target, bounds=bounds: target(place, cut(*bounds, True), lot)
                wire.add(f"{piece}X{place}{tag}", piece, ref, ref, dp=partner[side])
            for place in (2, 3):
                ref = lambda place=place, target=target, bounds=bounds: target(place, cut(*bounds, True), everyone)
                wire.add(f"{piece}X{place}", piece, ref, ref, dp=partner[side])
    for place in range(slots - 1):
        ref = lambda place=place: wo_out.at[odd, place]
        wire.add(f"woS{place}", "woS", ref if place else lambda: wo_hbm, ref, tp=other)
    for piece in ("wo.a", "wo.b"):
        for mine in (True, False):
            ref = lambda piece=piece, mine=mine: pieces[piece][1](slots - 1, cut(*pieces[piece][2], mine), everyone)
            wire.add(f"{piece}S" + ("" if mine else "~"), "woS", ref, ref, tp=other)
    ref = lambda: wo_out.at[odd, slots - 1, left_over]
    wire.add("wo.mS", "woS", ref, ref, tp=other)
    for quad in range(quads - 1):
        wire.add(f"o{quad}S", "o", lambda quad=quad: o_send.at[quad], lambda quad=quad: o_out.at[odd, quad], tp=other)
    cut_o = seqs - 4
    for name, part in (("o.a", pl.ds(0, cut_o)), ("o.b", pl.ds(cut_o, seqs - cut_o))):
        wire.add(name + "S", "o", lambda part=part: o_send.at[quads - 1, part], lambda part=part: o_out.at[odd, quads - 1, part], tp=other)

    small = ("wk.a", "wv.b", "wq.a", "wq.b")

    def ring(which, *kinds):
        return [f"{kind}{half_name}{way}" for kind in kinds for half_name in ("", "~")[: 1 if paired[kind[-1]] else 2] for way in which]

    def across(place, *kinds):
        return [f"{kind}X{place}" for kind in kinds if paired[kind[-1]]]

    def norm(g):
        for r in range(per):
            for at in range(0, toks, NORM_ROWS):
                x = x_buf[g * per + r, at : at + NORM_ROWS].astype(F32)
                a_buf[g, r * toks + at : r * toks + at + NORM_ROWS] = (unit(x) * g1_ref[...]).astype(BF16)

    def latent(g):
        kv = dot_t(a_buf[g], wdkv[...])
        rows[g * per : (g + 1) * per, spot(0, odd), :] = (unit(kv[:, :rank]) * gkv_ref[...]).astype(BF16).reshape(per, toks, rank)
        turned = []
        for s in range(per):
            cos_pair, sin_pair = cos_ref[g * per + s], sin_ref[g * per + s]
            cos = jnp.where(odd == 1, cos_pair[:, toks:], cos_pair[:, :toks])
            sin = jnp.where(odd == 1, sin_pair[:, toks:], sin_pair[:, :toks])
            table = jnp.concatenate([cos, cos, -sin, sin], axis=0).T
            p = kv[s * toks : (s + 1) * toks, rank:]
            swapped = jnp.concatenate([p[:, half:], p[:, :half]], axis=1)
            turned.append(p * table[:, :rope] + swapped * table[:, rope:])
        rot[g, spot(0, odd), :] = jnp.concatenate(turned, axis=1).astype(BF16)

    def queries(g):
        h = jnp.concatenate([dot(a_buf[g], wdq[:, : 2 * rank]), dot(a_buf[g], wdq[:, 2 * rank :])], axis=1)
        cq_buf[odd, g * per : (g + 1) * per] = (unit(h) * gq_ref[...]).astype(BF16).reshape(per, toks, q_rank)

    loads["g1"].wait()
    with jax.named_scope('p_norm0'):
        loads["x0"].wait()
        for g in range(1, groups):
            load_x(g)
        norm(0)
    for name in ("wdkv", "cos", "sin", "gkv", "gq", "len"):
        loads[name].wait()
    load("wdq", wdq_hbm, wdq)
    load("wk", wk_hbm, wkv.at[pl.ds(0, heads), pl.ds(0, nope)])
    load("wv", wv_hbm, wkv.at[pl.ds(0, heads), pl.ds(nope, nope)])
    load("wq", wq_hbm, wq.at[pl.ds(0, heads)])
    load("pe", pe_hbm.at[:, :, pl.ds(0, prefix)], pe_buf)
    load("lat", lat_hbm.at[:, pl.ds(0, prefix)], rows.at[:, pl.ds(0, prefix)])
    with jax.named_scope('p_bar'):
        pl.semaphore_wait(barrier, 3 + paired["a"] + paired["b"])
    with jax.named_scope('p_kv'):
        for g in range(groups):
            latent(g)
            for way in ("R", "L", "S0"):
                wire.start(f"c{g}{way}", f"p{g}{way}")
            if g + 1 < groups:
                loads[f"x{g + 1}"].wait()
                norm(g + 1)
    wire.start(*ring("R", *small), *ring("r", *small))

    def hand_on(g):
        wire.landed(f"c{g}L", f"p{g}L", f"c{g}R", f"p{g}R")
        wire.start(f"c{g}O", f"p{g}O", f"c{g}S3", f"p{g}S3", f"c{g}S1", f"p{g}S1")

    with jax.named_scope('p_cq'):
        loads["wdq"].wait()
        for g in range(groups):
            queries(g)
            wire.start(f"q{g}S")
            hand_on(g)
    wire.start(*ring("L", *small, "wo.b", "wo.a"), "wo.mL", "woS0")

    loads["pe"].wait()
    for g in range(groups):
        old = pe_buf[g * per : (g + 1) * per].reshape(per * rope, prefix).astype(F32)
        for b in range(prefix // BLOCK):
            rot[g, b * BLOCK : (b + 1) * BLOCK] = old[:, b * BLOCK : (b + 1) * BLOCK].T.astype(BF16)
    qb[...] = jnp.zeros_like(qb)

    def forward(g):
        wire.landed(f"c{g}O", f"p{g}O")
        wire.start(f"c{g}S2", f"p{g}S2")

    def settle(g):
        wire.all_landed(f"c{g}S", rows.at[pl.ds(0, per), pl.ds(0, slots * toks)], tp=other)
        wire.all_landed(f"p{g}S", rot.at[0, pl.ds(0, slots * toks)], tp=other)
        if g:
            wire.landed(f"q{g}S")

    with jax.named_scope('p_rest0'):
        for name in ("wk", "wv", "wq", "lat"):
            loads[name].wait()
    row = lax.broadcasted_iota(jnp.int32, (BLOCK, wide), 0)
    lane = lax.rem(lax.broadcasted_iota(jnp.int32, (BLOCK, wide), 1), BLOCK)
    near = row <= lane

    def place(n):
        return n // duos, lax.rem(n, duos)

    def query_dot(n):
        quad, duo = place(n)
        w = wq[pl.ds(quad * 4, 4)].reshape(4 * head, q_rank)
        cq = jnp.concatenate([cq_buf[parity, 2 * duo + u] for u in range(2) for parity in range(2)], axis=0)
        q_raw[...] = dot_t(w, cq)

    def query_stage(n):
        quad, duo = place(n)
        raw = q_raw
        for u in range(2):
            slot = 2 * lax.rem(duo, 2) + u
            cos, sin = cos_ref[2 * duo + u], sin_ref[2 * duo + u]
            for h in range(4):
                pair, side = h // 2, h % 2
                q = raw[h * head : (h + 1) * head, u * BLOCK : (u + 1) * BLOCK]
                cols = slice(side * BLOCK, (side + 1) * BLOCK)
                qb[u, pair, side * nope : (side + 1) * nope, cols] = q[:nope].astype(BF16)
                lo, hi = q[nope : nope + half], q[nope + half :]
                turned = jnp.concatenate([lo * cos - hi * sin, hi * cos + lo * sin], axis=0).astype(BF16)
                start = pl.multiple_of(BLOCK + slot * rope, rope)
                stale = pl.multiple_of(BLOCK + lax.rem(slot + 2, 4) * rope, rope)
                qb[u, pair, pl.ds(start, rope), cols] = turned
                qb[u, pair, pl.ds(stale, rope), cols] = jnp.zeros_like(turned)

    def key_stage(n, t, u):
        quad, duo = place(n)
        w = wkv[pl.ds(quad * 4, 4), :nope].reshape(4 * nope, rank)
        kb[u][:t] = dot_t(rows[2 * duo + u, :t], w).astype(BF16)

    def value_stage(n, t, u):
        quad, duo = place(n)
        w = wkv[pl.ds(quad * 4, 4), nope:].reshape(4 * nope, rank)
        vb[u][:, :t] = dot_t(w, rows[2 * duo + u, :t]).astype(BF16)

    def score_stage(n, t, u, pair):
        _, duo = place(n)
        length = len_ref[2 * duo + u]
        keys = jnp.concatenate([kb[u][:t, pair * BLOCK : (pair + 1) * BLOCK], rot[duo // 2, :t]], axis=1)
        value = dot(keys, qb[u, pair])
        most = None
        for b in range(t // BLOCK):
            part = value[b * BLOCK : (b + 1) * BLOCK]
            if BLOCK <= b * BLOCK < prefix:
                part = jnp.where(row < length - b * BLOCK, part, NEVER)
            if b * BLOCK == prefix:
                part = jnp.where(near, part, NEVER)
            sb[2 * u + pair][b * BLOCK : (b + 1) * BLOCK] = part
            part = jnp.max(part.reshape(BLOCK // 8, 8, wide), axis=0)
            most = part if most is None else jnp.maximum(most, part)
        mb[2 * u + pair] = jnp.broadcast_to(jnp.max(most, axis=0, keepdims=True), (8, wide))

    def soft_stage(t, u, pair):
        i = 2 * u + pair
        most = mb[i, :1]
        total = None
        for b in range(t // BLOCK):
            x = jnp.exp2((sb[i][b * BLOCK : (b + 1) * BLOCK] - most) * factor)
            part = jnp.sum(x.reshape(BLOCK // 8, 8, wide), axis=0)
            total = part if total is None else total + part
            pb[i][b * BLOCK : (b + 1) * BLOCK] = x.astype(BF16)
        lb[i] = total

    def mix_stage(n, t, u, pair):
        quad, duo = place(n)
        i = 2 * u + pair
        inv = 1.0 / jnp.sum(lb[i], axis=0, keepdims=True)
        o = dot(vb[u][pair * BLOCK : (pair + 1) * BLOCK, :t], pb[i][:t]) * inv
        o = jnp.concatenate([o[:nope, :BLOCK], o[nope:, BLOCK:]], axis=0).T.astype(BF16)
        first, second = o[:toks], o[toks:]
        cols = slice(pair * BLOCK, (pair + 1) * BLOCK)
        o_own[quad, 2 * duo + u, :, cols] = jnp.where(odd == 1, second, first)
        o_send[quad, 2 * duo + u, :, cols] = jnp.where(odd == 1, first, second)

    units = [(u, pair) for u in range(2) for pair in range(2)]
    total = quads * duos

    def each_chip(fn):
        for c in range(slots):
            pl.when(chip == c)(lambda c=c: fn(prefix + (c + 1) * BLOCK))

    def body(b, t):
        before, ahead, later = jnp.maximum(b - 1, 0), jnp.minimum(b + 1, total - 1), jnp.minimum(b + 2, total - 1)
        mix_stage(before, t, 0, 0)
        mix_stage(before, t, 0, 1)
        mix_stage(before, t, 1, 0)
        mix_stage(before, t, 1, 1)
        soft_stage(t, 0, 0)
        score_stage(ahead, t, 0, 0)
        value_stage(b, t, 0)
        soft_stage(t, 0, 1)
        score_stage(ahead, t, 0, 1)
        key_stage(later, t, 0)
        soft_stage(t, 1, 0)
        score_stage(ahead, t, 1, 0)
        value_stage(b, t, 1)
        soft_stage(t, 1, 1)
        score_stage(ahead, t, 1, 1)
        query_dot(later)
        query_stage(later)
        key_stage(later, t, 1)

    def front(b, t):
        before, ahead = jnp.maximum(b - 1, 0), b + 1
        for u, pair in units:
            mix_stage(before, t, u, pair)
        for u in range(2):
            soft_stage(t, u, 0)
            score_stage(ahead, t, u, 0)
            value_stage(b, t, u)
            soft_stage(t, u, 1)
            score_stage(ahead, t, u, 1)

    def back(b, t):
        for u in range(2):
            key_stage(b + 2, t, u)
        query_dot(b + 2)
        query_stage(b + 2)

    def at(b, when):
        return pl.when(b == when)

    agenda = {
        0: [(None, ring("R", "wq.a", "wq.b"), across(1, "wq.a", "wq.b"))],
        2: [(None, ring("r", *small), across("1r", *small) + ring("O", *small) + ring("R", "wo.a", "wo.b") + ["wo.mR"])],
        3: [(None, ring("L", "wk.a", "wv.b"), across(2, "wk.a", "wv.b"))],
        4: [(None, across(1, *small), [])],
        5: [(None, ring("L", "wq.a"), across(2, "wq.a"))],
        7: [(None, ring("L", "wq.b"), across(2, "wq.b"))],
        9: [(None, ring("O", *small), across(3, *small))],
        10: [(None, across("1r", *small) + across(2, *small), [])],
        11: [(None, ring("L", "wo.b"), across(2, "wo.b")), (1, [], ring("O", "wo.b"))],
        13: [(None, ring("R", "wo.a"), across(1, "wo.a")), (0, [], ring("O", "wo.a"))],
        15: [(None, across(3, *small), []), (None, ring("L", "wo.a"), across(2, "wo.a")), (1, [], ring("O", "wo.a"))],
        16: [(None, ring("R", "wo.b"), across(1, "wo.b")), (0, [], ring("O", "wo.b"))],
        20: [(0, ["wo.mR"], ["wo.mO"]), (1, ["wo.mL"], ["wo.mO"])],
        22: [(0, ring("O", "wo.a"), across(3, "wo.a") + ["wo.aS"]), (1, ring("O", "wo.b"), across(3, "wo.b") + ["wo.bS"])],
        23: [
            (0, ["wo.mL"], []),
            (1, ["wo.mR"], []),
            (None, across(1, "wo.a", "wo.b") + across(2, "wo.a", "wo.b"), ["woS1", "woS2"]),
        ],
        24: [(0, ring("O", "wo.b"), across(3, "wo.b") + ["wo.bS"]), (1, ring("O", "wo.a"), across(3, "wo.a") + ["wo.aS"])],
        29: [(None, ["wo.mO"], ["wo.mS"]), (None, across(3, "wo.a", "wo.b"), ["wo.aS~", "wo.bS~", "o.aS"])],
    }
    for quad in range(quads - 1):
        agenda.setdefault((quad + 1) * duos + 1, []).append((None, [], [f"o{quad}S"]))

    def run_agenda(when):
        for parity, waits, starts in agenda[when]:

            def item(waits=waits, starts=starts):
                with jax.named_scope(f"ev_{when}"):
                    wire.landed(*waits)
                wire.start(*starts)

            if parity is None:
                item()
            else:
                pl.when(odd == parity)(item)

    bounce = pltpu.make_async_copy(wo_hbm, wo_buf, load_sem.at[3])
    span = 8

    def step(b, _):
        for first in range(0, total, span):

            @pl.when(b // span == first // span)
            def _():
                for when in sorted(agenda):
                    if first <= when < first + span and when not in (0, 2):
                        at(b, when)(functools.partial(run_agenda, when))
                if first == 0:

                    @at(b, 4)
                    def _():
                        pltpu.make_async_copy(rows.at[:, pl.ds(prefix, chunk)], c_out, load_sem.at[0]).start()
                        pltpu.make_async_copy(rot.at[:, pl.ds(prefix, chunk)], p_out, load_sem.at[1]).start()
                        bounce.start()

                    @at(b, 6)
                    def _():
                        bounce.wait()
                        pltpu.make_async_copy(wo_buf, wo_out.at[odd, 0], load_sem.at[4]).start()

        split = (b == 0) | (b == 2)

        @pl.when(split)
        def _():
            with jax.named_scope('front'):
                each_chip(functools.partial(front, b))
            for g in range(1, groups):

                @at(b, 2 * (g - 1))
                def _():
                    forward(g)
                    run_agenda(2 * (g - 1))
                    settle(g)

            with jax.named_scope('back'):
                each_chip(functools.partial(back, b))

        @pl.when(jnp.logical_not(split))
        def _():
            with jax.named_scope('body'):
                each_chip(functools.partial(body, b))

        return 0

    def lead_in(t):
        for u in range(2):
            key_stage(0, t, u)
        for u, pair in units:
            score_stage(0, t, u, pair)
        for u in range(2):
            key_stage(1, t, u)
        query_dot(1)
        query_stage(1)

    wire.landed("q0S")
    query_dot(0)
    query_stage(0)
    forward(0)
    wire.landed(*ring("R", "wk.a", "wv.b"))
    wire.start(*across(1, "wk.a", "wv.b"))
    settle(0)
    with jax.named_scope('p_lead'):
        each_chip(lead_in)
    lax.fori_loop(0, total, step, 0)

    def last(t):
        for u, pair in units:
            mix_stage(total - 1, t, u, pair)

    with jax.named_scope('p_last'):
        each_chip(last)
        wire.start("o.bS")
        pltpu.make_async_copy(o_own, o_out.at[odd], load_sem.at[2]).start()
    with jax.named_scope('f_land'):
        for place in range(slots - 1):
            wire.landed(f"woS{place}")
        wire.landed("wo.aS", "wo.bS", "wo.mS", "wo.aS~", "wo.bS~")
        for quad in range(quads - 1):
            wire.landed(f"o{quad}S")
        wire.landed("o.aS", "o.bS")
    with jax.named_scope('f_sent'):
        wire.all_sent("c", rows.at[pl.ds(0, per * groups // 2), pl.ds(0, 14 * toks)], tp=other)
        wire.all_sent("p", rot.at[pl.ds(0, groups), pl.ds(0, 7 * toks)], tp=other)
        wire.all_sent("q", cq_buf.at[odd], tp=other)
        wire.all_sent("wq.a", wq.at[pl.ds(0, 3 * heads), pl.ds(0, q_cut)], tp=other)
        wire.all_sent("wq.b", wq.at[pl.ds(0, 3 * heads), pl.ds(0, head - q_cut)], tp=other)
        wire.all_sent("wk.a", wkv.at[pl.ds(0, 3 * heads), pl.ds(0, nope)], tp=other)
        wire.all_sent("wv.b", wkv.at[pl.ds(0, 3 * heads), pl.ds(0, nope)], tp=other)
        wire.all_sent("wo.a", wo_out.at[0, pl.ds(0, 3), pl.ds(0, o_cut)], tp=other)
        wire.all_sent("wo.b", wo_out.at[0, pl.ds(0, 3), pl.ds(0, o_cut)], tp=other)
        wire.all_sent("wo.m", wo_out.at[0, pl.ds(0, 3), left_over], tp=other)
        wire.all_sent("woS", wo_out.at[0], tp=other)
        wire.all_sent("o", o_send, tp=other)
        pltpu.make_async_copy(rows.at[:, pl.ds(prefix, chunk)], c_out, load_sem.at[0]).wait()
        pltpu.make_async_copy(rot.at[:, pl.ds(prefix, chunk)], p_out, load_sem.at[1]).wait()
        pltpu.make_async_copy(o_own, o_out.at[odd], load_sem.at[2]).wait()
        pltpu.make_async_copy(wo_buf, wo_out.at[odd, 0], load_sem.at[4]).wait()


def finish_kernel(
    len_hbm, o_hbm, w_hbm, x_hbm, c_hbm, p_hbm, lat_hbm, pe_hbm, y_hbm, lat_out, pe_out, fresh, acc, x_buf, y_buf, o_buf, w_buf, c_buf, p_buf, lat_buf, pe_buf, lat_new, pe_new, len_ref, load_sem, store_sem, sems
):
    chip = lax.axis_index("tp") // 2
    quads, seqs, toks, depth = o_hbm.shape[1:]
    terms = 2 * quads
    slots = c_hbm.shape[1]
    rank = lat_hbm.shape[2]
    rope, cache_len = pe_hbm.shape[1:]
    chunk = slots * 2 * toks
    words = rank // BLOCK
    dim = x_hbm.shape[2]
    part = 2 * depth
    ring = w_buf.shape[0]

    def loads(k, with_term):
        slot = lax.rem(k, ring)
        out = [
            pltpu.make_async_copy(c_hbm.at[k], c_buf.at[slot], load_sem.at[0, slot]),
            pltpu.make_async_copy(lat_hbm.at[k], lat_buf.at[slot], load_sem.at[1, slot]),
        ]
        if with_term:
            side, quad = k // quads, lax.rem(k, quads)
            out.append(pltpu.make_async_copy(o_hbm.at[side, quad], o_buf.at[slot], load_sem.at[2, slot]))
            out.append(pltpu.make_async_copy(w_hbm.at[side, pl.ds(pl.multiple_of(quad * depth, depth), depth)], w_buf.at[slot], load_sem.at[3, slot]))
        return out

    def store(k):
        slot = lax.rem(k, ring)
        return pltpu.make_async_copy(lat_new.at[slot], lat_out.at[k], store_sem.at[slot])

    load_len = pltpu.make_async_copy(len_hbm, len_ref, sems.at[4 + dim // part])
    load_x = pltpu.make_async_copy(x_hbm, x_buf, sems.at[0])
    load_p = pltpu.make_async_copy(p_hbm, p_buf, sems.at[1])
    load_pe = pltpu.make_async_copy(pe_hbm, pe_buf, sems.at[2])
    store_pe = pltpu.make_async_copy(pe_new, pe_out, sems.at[3])

    def store_y(n):
        cols = pl.ds(n * part, part)
        return pltpu.make_async_copy(y_buf.at[:, :, cols], y_hbm.at[:, :, cols], sems.at[4 + n])


    def slot_of(j):
        return lax.rem(chip - j + slots, slots)

    def project(k, kind):
        slot = lax.rem(k, ring)
        o = o_buf[slot].reshape(seqs * toks, depth)
        for n in range(0, dim, part):
            cols = slice(n, n + part)
            y = dot(o, w_buf[slot, :, cols])
            if kind != "first":
                y = acc[:, cols] + y
            if kind == "last":
                y = y + x_buf[:, :, cols].reshape(seqs * toks, part).astype(F32)
                y_buf[:, :, cols] = y.astype(BF16).reshape(seqs, toks, part)
                store_y(n // part).start()
            else:
                acc[:, cols] = y

    def cache(k):
        at_slot = lax.rem(k, ring)
        length = len_ref[k]
        for j in range(slots):
            piece = c_buf[at_slot, slot_of(j)].reshape(2 * toks, rank).astype(F32)
            for w in range(words):
                fresh[w, BLOCK + j * 2 * toks : BLOCK + (j + 1) * 2 * toks] = piece[:, w * BLOCK : (w + 1) * BLOCK]
        lat_new[at_slot] = lat_buf[at_slot]
        base = (length // 16) * 16
        skew = length - base
        tile_row = lax.broadcasted_iota(jnp.int32, (16, BLOCK), 0)
        for i in range(chunk // 16 + 1):
            at = pl.multiple_of(jnp.minimum(base + i * 16, cache_len - 16), 16)
            for w in range(words):
                cols = slice(w * BLOCK, (w + 1) * BLOCK)
                moved = fresh[w, pl.ds(BLOCK - skew + i * 16, 16), :].astype(BF16)
                if i == 0 or i == chunk // 16:
                    local = tile_row + (at - length)
                    shown = (local >= 0) & (local < chunk) if i == 0 else (local < chunk)
                    if i == 0:
                        rest = lat_buf[at_slot, pl.ds(at, 16), cols]
                    else:
                        shown = shown & (skew > 0)
                        rest = lat_new[at_slot, pl.ds(at, 16), cols]
                    moved = jnp.where(shown, moved.astype(F32), rest.astype(F32)).astype(BF16)
                lat_new[at_slot, pl.ds(at, 16), cols] = moved

        turned = jnp.concatenate([p_buf[k // (BLOCK // rope), slot_of(j)].reshape(2 * toks, BLOCK).astype(F32).T for j in range(slots)], axis=1)
        group = lax.rem(k, BLOCK // rope)
        mine = turned[:rope]
        for g in range(1, BLOCK // rope):
            mine = jnp.where(group == g, turned[g * rope : (g + 1) * rope], mine)
        mine = jnp.concatenate([mine, jnp.zeros((rope, cache_len - chunk), F32)], axis=1)
        mine = pltpu.roll(mine, length, axis=1)
        spot = lax.broadcasted_iota(jnp.int32, (rope, cache_len), 1) - length
        pe_new[k] = jnp.where((spot >= 0) & (spot < chunk), mine, pe_buf[k].astype(F32)).astype(BF16)

    def begin(k, with_term):
        for load in loads(k, with_term):
            load.start()

    def arrived(k, with_term):
        for load in loads(k, with_term):
            load.wait()

    def work(k, kind):
        if kind != "none":
            project(k, kind)
        cache(k)
        store(k).start()

    def more(k):
        pl.when(k < terms)(lambda: begin(k, True))
        pl.when((k >= terms) & (k < seqs))(lambda: begin(k, False))

    first = loads(0, True)
    for load in first[2:] + first[:2]:
        load.start()
    load_len.start()
    load_p.start()
    load_pe.start()
    for load in first[2:]:
        load.wait()
    begin(1, True)
    begin(2, True)
    project(0, "first")
    for load in first[:2] + [load_len, load_p, load_pe]:
        load.wait()
    begin(3, True)
    cache(0)
    store(0).start()
    load_x.start()

    def middle(k, _):
        with jax.named_scope('g_wait'):
            arrived(k, True)
        more(k + ring - 1)

        @pl.when(k >= ring)
        def _():
            store(k - ring).wait()

        with jax.named_scope('g_work'):
            work(k, "middle")
        return 0

    lax.fori_loop(1, terms - 1, middle, 0)
    last = terms - 1
    arrived(last, True)
    more(last + ring - 1)
    store(last - ring).wait()
    load_x.wait()
    with jax.named_scope('g_last'):
        work(last, "last")

    def tail(k, _):
        arrived(k, False)
        store(k - ring).wait()
        with jax.named_scope('g_tail'):
            work(k, "none")
        return 0

    lax.fori_loop(terms, seqs, tail, 0)
    store_pe.start()
    for k in range(ring):
        store(seqs - ring + k).wait()
    store_pe.wait()
    for n in range(dim // part):
        store_y(n).wait()


def solution(mesh):
    size = mesh.shape["tp"]
    count = mesh.shape["dp"]
    stride = 2 ** (count.bit_length() // 2)
    paired = {"a": count % 2 == 0, "b": count % (2 * stride) == 0}

    def local_step(hidden, lengths, rope_cos, rope_sin, cache_lat, cache_pe, norm_in, w_dq, norm_q, w_dkv, norm_kv, w_uq, w_uk, w_uv, w_out):
        seqs, toks, dim = hidden.shape
        q_rank = w_dq.shape[1]
        rank, heads, nope = w_uk.shape
        rope = cache_pe.shape[2]
        cache_len = cache_lat.shape[1]
        slots = size // 2
        head = nope + rope
        quads = slots * heads // 4
        chunk = size * toks
        prefix = cache_len - chunk
        per = BLOCK // rope
        groups = seqs // per
        wide = 2 * BLOCK
        cos_t, sin_t = rope_cos.transpose(0, 2, 1), rope_sin.transpose(0, 2, 1)
        pe_t = cache_pe.transpose(0, 2, 1)
        wdkv_t = w_dkv.transpose(1, 0)
        wq_t, wk_t, wv_t = (w.transpose(1, 2, 0) for w in (w_uq, w_uk, w_uv))

        inboxes = 9 * groups + 36 + 8 + 3 + slots + 4 + quads + 1
        any_spec = pl.BlockSpec(memory_space=pl.ANY)
        c_all, p_all, o_all, wo_all = pl.pallas_call(
            functools.partial(main_kernel, (size, stride, paired)),
            in_specs=[any_spec] * 15,
            out_specs=[any_spec] * 4,
            out_shape=[
                jax.ShapeDtypeStruct((seqs, chunk, rank), BF16),
                jax.ShapeDtypeStruct((groups, chunk, BLOCK), BF16),
                jax.ShapeDtypeStruct((2, quads, seqs, toks, 4 * nope), BF16),
                jax.ShapeDtypeStruct((2, slots) + w_out.shape, BF16),
            ],
            scratch_shapes=[
                pltpu.VMEM(hidden.shape, BF16),
                pltpu.VMEM(w_dq.shape, BF16),
                pltpu.VMEM(wdkv_t.shape, BF16),
                pltpu.VMEM((groups, per * toks, dim), BF16),
                pltpu.VMEM((seqs, cache_len, rank), BF16),
                pltpu.VMEM((groups, cache_len, BLOCK), BF16),
                pltpu.VMEM((seqs, rope, prefix), BF16),
                pltpu.VMEM((seqs, rope // 2, BLOCK), F32),
                pltpu.VMEM((seqs, rope // 2, BLOCK), F32),
                pltpu.VMEM((2, seqs, toks, q_rank), BF16),
                pltpu.VMEM((slots * heads, head, q_rank), BF16),
                pltpu.VMEM((slots * heads, 2 * nope, rank), BF16),
                [pltpu.VMEM((cache_len, 4 * nope), BF16) for _ in range(2)],
                [pltpu.VMEM((4 * nope, cache_len), BF16) for _ in range(2)],
                pltpu.VMEM((2, 2, wide, wide), BF16),
                pltpu.VMEM((4 * head, wide), F32),
                [pltpu.VMEM((cache_len, wide), F32) for _ in range(4)],
                pltpu.VMEM((4, 8, wide), F32),
                [pltpu.VMEM((cache_len, wide), BF16) for _ in range(4)],
                pltpu.VMEM((4, 8, wide), F32),
                pltpu.VMEM((quads, seqs, toks, 4 * nope), BF16),
                pltpu.VMEM((quads, seqs, toks, 4 * nope), BF16),
                pltpu.VMEM(w_out.shape, BF16),
                pltpu.SMEM(lengths.shape, jnp.int32),
                pltpu.VMEM(norm_in.shape, F32),
                pltpu.VMEM(norm_q.shape, F32),
                pltpu.VMEM(norm_kv.shape, F32),
                pltpu.SemaphoreType.DMA((13 + groups,)),
                pltpu.SemaphoreType.DMA((12,)),
                pltpu.SemaphoreType.DMA((inboxes,)),
            ],
            compiler_params=pltpu.CompilerParams(collective_id=0, has_side_effects=True, vmem_limit_bytes=63 * MIB),
            cost_estimate=pl.CostEstimate(flops=70 * 10**9, bytes_accessed=40 * MIB, transcendentals=30 * 10**6),
            name="main",
        )(lengths, hidden, norm_in, w_dq, norm_q, wdkv_t, norm_kv, cos_t, sin_t, wq_t, wk_t, wv_t, w_out, cache_lat, pe_t)

        depth = 4 * nope
        ahead = 4
        y, lat_new, pe_new = pl.pallas_call(
            finish_kernel,
            in_specs=[any_spec] * 8,
            out_specs=[any_spec] * 3,
            scratch_shapes=[
                pltpu.VMEM((rank // BLOCK, chunk + 2 * BLOCK, BLOCK), F32),
                pltpu.VMEM((seqs * toks, dim), F32),
                pltpu.VMEM(hidden.shape, BF16),
                pltpu.VMEM(hidden.shape, BF16),
                pltpu.VMEM((ahead, seqs, toks, depth), BF16),
                pltpu.VMEM((ahead, depth, dim), BF16),
                pltpu.VMEM((ahead, slots, 2, toks, rank), BF16),
                pltpu.VMEM((groups, slots, 2, toks, BLOCK), BF16),
                pltpu.VMEM((ahead, cache_len, rank), BF16),
                pltpu.VMEM(pe_t.shape, BF16),
                pltpu.VMEM((ahead, cache_len, rank), BF16),
                pltpu.VMEM(pe_t.shape, BF16),
                pltpu.SMEM(lengths.shape, jnp.int32),
                pltpu.SemaphoreType.DMA((4, ahead)),
                pltpu.SemaphoreType.DMA((ahead,)),
                pltpu.SemaphoreType.DMA((5 + dim // (2 * depth),)),
            ],
            out_shape=[
                jax.ShapeDtypeStruct(hidden.shape, BF16),
                jax.ShapeDtypeStruct(cache_lat.shape, BF16),
                jax.ShapeDtypeStruct(pe_t.shape, BF16),
            ],
            compiler_params=pltpu.CompilerParams(vmem_limit_bytes=63 * MIB),
            cost_estimate=pl.CostEstimate(flops=2 * seqs * toks * dim * dim, bytes_accessed=50 * MIB, transcendentals=0),
            name="finish",
        )(
            lengths,
            o_all,
            wo_all.reshape(2, slots * w_out.shape[0], dim),
            hidden,
            c_all.reshape(seqs, slots, 2, toks, rank),
            p_all.reshape(groups, slots, 2, toks, BLOCK),
            cache_lat,
            pe_t,
        )
        return y, lat_new, pe_new.transpose(0, 2, 1)

    spec_tok = P("dp", "tp", None)
    spec_len = P("dp")
    spec_seq = P("dp", None, None)
    spec_vec = P(None)
    spec_mat = P(None, None)
    spec_head = P(None, "tp", None)
    spec_rows = P("tp", None)
    in_specs = (spec_tok, spec_len, spec_seq, spec_seq, spec_seq, spec_seq, spec_vec, spec_mat, spec_vec, spec_mat, spec_vec, spec_head, spec_head, spec_head, spec_rows)
    return jax.shard_map(local_step, mesh=mesh, in_specs=in_specs, out_specs=(spec_tok, spec_seq, spec_seq), check_vma=False)
```

```python
import functools

import jax
import jax.numpy as jnp
from jax import lax
from jax.experimental import pallas as pl
from jax.experimental.pallas import tpu as pltpu
from jax.sharding import PartitionSpec as P

BLOCK = 128
LOG2E = 1.4426950408889634
NEVER = -1e30
NORM_ROWS = 16
F32 = jnp.float32
BF16 = jnp.bfloat16
MESH = pl.DeviceIdType.MESH
MIB = 2**20


def dot(a, b):
    return lax.dot_general(a, b, (((1,), (0,)), ((), ())), preferred_element_type=F32)


def dot_t(a, b):
    return lax.dot_general(a, b, (((1,), (1,)), ((), ())), preferred_element_type=F32)


def unit(x):
    return x * lax.rsqrt(jnp.mean(x * x, axis=-1, keepdims=True) + 1e-6)


class Wire:
    def __init__(self, send_sem, recv_sem):
        self.sems = (send_sem, recv_sem)
        self.made = {}
        self.pools = {}
        self.inboxes = {}

    def add(self, name, pool, src, dst, inbox=None, **peer):
        send = self.pools.setdefault(pool, len(self.pools))
        recv = self.inboxes.setdefault(inbox or name, len(self.inboxes))
        self.made[name] = lambda: pltpu.make_async_remote_copy(
            src(), dst(), self.sems[0].at[send], self.sems[1].at[recv], device_id=peer, device_id_type=MESH
        )

    def start(self, *names):
        for name in names:
            self.made[name]().start()

    def landed(self, *names):
        for name in names:
            self.made[name]().wait_recv()

    def all_landed(self, inbox, whole, **peer):
        copy = pltpu.make_async_remote_copy(whole, whole, self.sems[0].at[0], self.sems[1].at[self.inboxes[inbox]], device_id=peer, device_id_type=MESH)
        copy.wait_recv()

    def all_sent(self, pool, whole, **peer):
        copy = pltpu.make_async_remote_copy(whole, whole, self.sems[0].at[self.pools[pool]], self.sems[1].at[0], device_id=peer, device_id_type=MESH)
        copy.wait_send()


def main_kernel(
    plan,
    len_hbm,
    x_hbm,
    g1_hbm,
    wdq_hbm,
    gq_hbm,
    wdkv_hbm,
    gkv_hbm,
    cos_hbm,
    sin_hbm,
    wq_hbm,
    wk_hbm,
    wv_hbm,
    wo_hbm,
    lat_hbm,
    pe_hbm,
    c_out,
    p_out,
    o_out,
    wo_out,
    x_buf,
    wdq,
    wdkv,
    a_buf,
    rows,
    rot,
    pe_buf,
    cos_ref,
    sin_ref,
    cq_buf,
    wq,
    wkv,
    kb,
    vb,
    qb,
    q_raw,
    sb,
    mb,
    pb,
    lb,
    o_own,
    o_send,
    wo_buf,
    len_ref,
    g1_ref,
    gq_ref,
    gkv_ref,
    load_sem,
    send_sem,
    recv_sem,
):
    size, stride, paired = plan
    me = lax.axis_index("tp")
    odd = lax.rem(me, 2)
    chip = me // 2
    right, left = lax.rem(me + 2, size), lax.rem(me + size - 2, size)
    onward = jnp.where(odd == 0, right, left)
    other = me + 1 - 2 * odd
    dp = lax.axis_index("dp")
    flip = {"a": lax.rem(dp, 2), "b": lax.rem(dp // stride, 2)}
    partner = {"a": dp + 1 - 2 * flip["a"], "b": dp + stride * (1 - 2 * flip["b"])}

    seqs, toks, dim = x_hbm.shape
    groups = rot.shape[0]
    per = seqs // groups
    rank = rows.shape[2]
    slots = size // 2
    chunk = size * toks
    prefix = rows.shape[1] - chunk
    heads = wq.shape[0] // slots
    head, q_rank = wq.shape[1:]
    rope = BLOCK // per
    half = rope // 2
    nope = head - rope
    quads = wq.shape[0] // 4
    duos = seqs // 2
    wide = 2 * BLOCK
    factor = LOG2E * head**-0.5

    loads = {}

    def load(name, src, dst):
        loads[name] = pltpu.make_async_copy(src, dst, load_sem.at[len(loads)])
        loads[name].start()

    def spot(slot, parity):
        return pl.ds(pl.multiple_of(prefix + slot * BLOCK + parity * toks, toks), toks)

    barrier = pltpu.get_barrier_semaphore()
    for peer in (left, right, other):
        pl.semaphore_signal(barrier, inc=1, device_id={"tp": peer}, device_id_type=MESH)
    for side in "ab":
        if paired[side]:
            pl.semaphore_signal(barrier, inc=1, device_id={"dp": partner[side]}, device_id_type=MESH)

    lanes_chip = pl.ds(pl.multiple_of(chip * BLOCK, BLOCK), BLOCK)
    def load_x(g):
        load(f"x{g}", x_hbm.at[pl.ds(g * per, per)], x_buf.at[pl.ds(g * per, per)])

    load("g1", g1_hbm, g1_ref)
    load_x(0)
    load("wdkv", wdkv_hbm, wdkv)
    load("gkv", gkv_hbm, gkv_ref)
    load("gq", gq_hbm, gq_ref)
    load("len", len_hbm, len_ref)
    load("cos", cos_hbm.at[:, :, lanes_chip], cos_ref)
    load("sin", sin_hbm.at[:, :, lanes_chip], sin_ref)

    wire = Wire(send_sem, recv_sem)

    def chain(name, here, there, places, via="split", whole=True):
        near_left, near_right, opposite = places
        handed = {"right": near_left, "left": near_right, "split": jnp.where(odd == 0, near_left, near_right)}[via]
        pool = name[0] if name[1].isdigit() else name[:4]
        if whole:
            wire.add(name + "R", pool, lambda: here(0), lambda: there(near_left), tp=right)
        wire.add(name + "L", pool, lambda: here(0), lambda: there(near_right), tp=left)
        wire.add(name + "O", pool, lambda: there(handed), lambda: there(opposite), tp={"right": right, "left": left, "split": onward}[via])

    for g in range(groups):
        for name, ref in (("c", lambda slot, g=g: rows.at[pl.ds(g * per, per), spot(slot, odd)]), ("p", lambda slot, g=g: rot.at[g, spot(slot, odd)])):
            name = f"{name}{g}"
            chain(name, ref, ref, (1, 3, 2), "left")
            for slot in range(slots):
                wire.add(f"{name}S{slot}", name[0], functools.partial(ref, slot), functools.partial(ref, slot), f"{name}S", tp=other)
        cq_ref = lambda g=g: cq_buf.at[odd, pl.ds(g * per, per)]
        wire.add(f"q{g}S", "q", cq_ref, cq_ref, tp=other)

    def cut(side, low, high, unit, mine):
        half_size = (high - low) // 2
        which = flip[side] if mine else 1 - flip[side]
        return pl.ds(pl.multiple_of(low + which * half_size, unit), half_size)

    q_cut = head * 2 // 3
    o_cut = wo_hbm.shape[0] * 2 // 5
    lots = {"R": (0, 3), "r": (3, heads - 3)}
    everyone = (0, heads)

    def lot_of(place, lot):
        return pl.ds(place * heads + lot[0], lot[1])

    pieces = {
        "wq.a": (lambda r, lot: wq_hbm.at[pl.ds(*lot), r], lambda place, r, lot: wq.at[lot_of(place, lot), r], ("a", 0, q_cut, 16)),
        "wq.b": (lambda r, lot: wq_hbm.at[pl.ds(*lot), r], lambda place, r, lot: wq.at[lot_of(place, lot), r], ("b", q_cut, head, 16)),
        "wk.a": (
            lambda r, lot: wk_hbm.at[pl.ds(*lot), :, r],
            lambda place, r, lot: wkv.at[lot_of(place, lot), pl.ds(0, nope), r],
            ("a", 0, rank, BLOCK),
        ),
        "wv.b": (
            lambda r, lot: wv_hbm.at[pl.ds(*lot), :, r],
            lambda place, r, lot: wkv.at[lot_of(place, lot), pl.ds(nope, nope), r],
            ("b", 0, rank, BLOCK),
        ),
        "wo.a": (lambda r, lot: wo_hbm.at[r], lambda place, r, lot: wo_out.at[odd, place, r], ("a", 0, o_cut, 16)),
        "wo.b": (lambda r, lot: wo_hbm.at[r], lambda place, r, lot: wo_out.at[odd, place, r], ("b", o_cut, 2 * o_cut, 16)),
    }
    left_over = pl.ds(2 * o_cut, wo_hbm.shape[0] - 2 * o_cut)
    chain("wo.m", lambda place: wo_hbm.at[left_over], lambda place: wo_out.at[odd, place, left_over], (1, 2, 3))
    for piece, (source, target, bounds) in pieces.items():
        side = bounds[0]
        large = piece.startswith("wo")
        for mine in (True,) if paired[side] else (True, False):
            here = lambda place, lot=everyone, source=source, bounds=bounds, mine=mine: source(cut(*bounds, mine), lot)
            there = lambda place, lot=everyone, target=target, bounds=bounds, mine=mine: target(place, cut(*bounds, mine), lot)
            name = piece + ("" if mine else "~")
            chain(name, here, there, (1, 2, 3), "split" if large else "right", large)
            if not large:
                for way, lot in lots.items():
                    wire.add(name + way, piece, functools.partial(here, 0, lot), functools.partial(there, 1, lot), tp=right)
        if paired[side]:
            for place, tag, lot in ((1, "", everyone),) if large else ((1, "", lots["R"]), (1, "r", lots["r"])):
                ref = lambda place=place, lot=lot, target=target, bounds=bounds: target(place, cut(*bounds, True), lot)
                wire.add(f"{piece}X{place}{tag}", piece, ref, ref, dp=partner[side])
            for place in (2, 3):
                ref = lambda place=place, target=target, bounds=bounds: target(place, cut(*bounds, True), everyone)
                wire.add(f"{piece}X{place}", piece, ref, ref, dp=partner[side])
    for place in range(slots - 1):
        ref = lambda place=place: wo_out.at[odd, place]
        wire.add(f"woS{place}", "woS", ref if place else lambda: wo_hbm, ref, tp=other)
    for piece in ("wo.a", "wo.b"):
        for mine in (True, False):
            ref = lambda piece=piece, mine=mine: pieces[piece][1](slots - 1, cut(*pieces[piece][2], mine), everyone)
            wire.add(f"{piece}S" + ("" if mine else "~"), "woS", ref, ref, tp=other)
    ref = lambda: wo_out.at[odd, slots - 1, left_over]
    wire.add("wo.mS", "woS", ref, ref, tp=other)
    for quad in range(quads - 1):
        wire.add(f"o{quad}S", "o", lambda quad=quad: o_send.at[quad], lambda quad=quad: o_out.at[odd, quad], tp=other)
    cut_o = seqs - 4
    for name, part in (("o.a", pl.ds(0, cut_o)), ("o.b", pl.ds(cut_o, seqs - cut_o))):
        wire.add(name + "S", "o", lambda part=part: o_send.at[quads - 1, part], lambda part=part: o_out.at[odd, quads - 1, part], tp=other)

    small = ("wk.a", "wv.b", "wq.a", "wq.b")

    def ring(which, *kinds):
        return [f"{kind}{half_name}{way}" for kind in kinds for half_name in ("", "~")[: 1 if paired[kind[-1]] else 2] for way in which]

    def across(place, *kinds):
        return [f"{kind}X{place}" for kind in kinds if paired[kind[-1]]]

    def norm(g):
        for r in range(per):
            for at in range(0, toks, NORM_ROWS):
                x = x_buf[g * per + r, at : at + NORM_ROWS].astype(F32)
                a_buf[g, r * toks + at : r * toks + at + NORM_ROWS] = (unit(x) * g1_ref[...]).astype(BF16)

    def latent(g):
        kv = dot_t(a_buf[g], wdkv[...])
        rows[g * per : (g + 1) * per, spot(0, odd), :] = (unit(kv[:, :rank]) * gkv_ref[...]).astype(BF16).reshape(per, toks, rank)
        turned = []
        for s in range(per):
            cos_pair, sin_pair = cos_ref[g * per + s], sin_ref[g * per + s]
            cos = jnp.where(odd == 1, cos_pair[:, toks:], cos_pair[:, :toks])
            sin = jnp.where(odd == 1, sin_pair[:, toks:], sin_pair[:, :toks])
            table = jnp.concatenate([cos, cos, -sin, sin], axis=0).T
            p = kv[s * toks : (s + 1) * toks, rank:]
            swapped = jnp.concatenate([p[:, half:], p[:, :half]], axis=1)
            turned.append(p * table[:, :rope] + swapped * table[:, rope:])
        rot[g, spot(0, odd), :] = jnp.concatenate(turned, axis=1).astype(BF16)

    def queries(g):
        h = jnp.concatenate([dot(a_buf[g], wdq[:, : 2 * rank]), dot(a_buf[g], wdq[:, 2 * rank :])], axis=1)
        cq_buf[odd, g * per : (g + 1) * per] = (unit(h) * gq_ref[...]).astype(BF16).reshape(per, toks, q_rank)

    loads["g1"].wait()
    loads["x0"].wait()
    for g in range(1, groups):
        load_x(g)
    norm(0)
    for name in ("wdkv", "cos", "sin", "gkv", "gq", "len"):
        loads[name].wait()
    load("wdq", wdq_hbm, wdq)
    load("wk", wk_hbm, wkv.at[pl.ds(0, heads), pl.ds(0, nope)])
    load("wv", wv_hbm, wkv.at[pl.ds(0, heads), pl.ds(nope, nope)])
    load("wq", wq_hbm, wq.at[pl.ds(0, heads)])
    load("pe", pe_hbm.at[:, :, pl.ds(0, prefix)], pe_buf)
    load("lat", lat_hbm.at[:, pl.ds(0, prefix)], rows.at[:, pl.ds(0, prefix)])
    pl.semaphore_wait(barrier, 3 + paired["a"] + paired["b"])
    for g in range(groups):
        latent(g)
        for way in ("R", "L", "S0"):
            wire.start(f"c{g}{way}", f"p{g}{way}")
        if g + 1 < groups:
            loads[f"x{g + 1}"].wait()
            norm(g + 1)
    wire.start(*ring("R", *small), *ring("r", *small))

    def hand_on(g):
        wire.landed(f"c{g}L", f"p{g}L", f"c{g}R", f"p{g}R")
        wire.start(f"c{g}O", f"p{g}O", f"c{g}S3", f"p{g}S3", f"c{g}S1", f"p{g}S1")

    loads["wdq"].wait()
    for g in range(groups):
        queries(g)
        wire.start(f"q{g}S")
        hand_on(g)
    wire.start(*ring("L", "wq.a", "wq.b", "wk.a", "wv.b", "wo.b", "wo.a"), "wo.mL", "woS0")

    loads["pe"].wait()
    for g in range(groups):
        old = pe_buf[g * per : (g + 1) * per].reshape(per * rope, prefix).astype(F32)
        for b in range(prefix // BLOCK):
            rot[g, b * BLOCK : (b + 1) * BLOCK] = old[:, b * BLOCK : (b + 1) * BLOCK].T.astype(BF16)
    qb[...] = jnp.zeros_like(qb)

    def forward(g):
        wire.landed(f"c{g}O", f"p{g}O")
        wire.start(f"c{g}S2", f"p{g}S2")

    def settle(g):
        wire.all_landed(f"c{g}S", rows.at[pl.ds(0, per), pl.ds(0, slots * toks)], tp=other)
        wire.all_landed(f"p{g}S", rot.at[0, pl.ds(0, slots * toks)], tp=other)
        if g:
            wire.landed(f"q{g}S")

    for name in ("wk", "wv", "wq", "lat"):
        loads[name].wait()
    row = lax.broadcasted_iota(jnp.int32, (BLOCK, wide), 0)
    lane = lax.rem(lax.broadcasted_iota(jnp.int32, (BLOCK, wide), 1), BLOCK)
    near = row <= lane

    def place(n):
        return n // duos, lax.rem(n, duos)

    def query_dot(n):
        quad, duo = place(n)
        w = wq[pl.ds(quad * 4, 4)].reshape(4 * head, q_rank)
        cq = jnp.concatenate([cq_buf[parity, 2 * duo + u] for u in range(2) for parity in range(2)], axis=0)
        q_raw[...] = dot_t(w, cq)

    def query_stage(n):
        quad, duo = place(n)
        raw = q_raw
        for u in range(2):
            slot = 2 * lax.rem(duo, 2) + u
            cos, sin = cos_ref[2 * duo + u], sin_ref[2 * duo + u]
            for h in range(4):
                pair, side = h // 2, h % 2
                q = raw[h * head : (h + 1) * head, u * BLOCK : (u + 1) * BLOCK]
                cols = slice(side * BLOCK, (side + 1) * BLOCK)
                qb[u, pair, side * nope : (side + 1) * nope, cols] = q[:nope].astype(BF16)
                lo, hi = q[nope : nope + half], q[nope + half :]
                turned = jnp.concatenate([lo * cos - hi * sin, hi * cos + lo * sin], axis=0).astype(BF16)
                start = pl.multiple_of(BLOCK + slot * rope, rope)
                stale = pl.multiple_of(BLOCK + lax.rem(slot + 2, 4) * rope, rope)
                qb[u, pair, pl.ds(start, rope), cols] = turned
                qb[u, pair, pl.ds(stale, rope), cols] = jnp.zeros_like(turned)

    def key_stage(n, t, u):
        quad, duo = place(n)
        w = wkv[pl.ds(quad * 4, 4), :nope].reshape(4 * nope, rank)
        kb[u][:t] = dot_t(rows[2 * duo + u, :t], w).astype(BF16)

    def value_stage(n, t, u):
        quad, duo = place(n)
        w = wkv[pl.ds(quad * 4, 4), nope:].reshape(4 * nope, rank)
        vb[u][:, :t] = dot_t(w, rows[2 * duo + u, :t]).astype(BF16)

    def score_stage(n, t, u, pair):
        _, duo = place(n)
        length = len_ref[2 * duo + u]
        keys = jnp.concatenate([kb[u][:t, pair * BLOCK : (pair + 1) * BLOCK], rot[duo // 2, :t]], axis=1)
        value = dot(keys, qb[u, pair])
        most = None
        for b in range(t // BLOCK):
            part = value[b * BLOCK : (b + 1) * BLOCK]
            if BLOCK <= b * BLOCK < prefix:
                part = jnp.where(row < length - b * BLOCK, part, NEVER)
            if b * BLOCK == prefix:
                part = jnp.where(near, part, NEVER)
            sb[2 * u + pair][b * BLOCK : (b + 1) * BLOCK] = part
            part = jnp.max(part.reshape(BLOCK // 8, 8, wide), axis=0)
            most = part if most is None else jnp.maximum(most, part)
        mb[2 * u + pair] = jnp.broadcast_to(jnp.max(most, axis=0, keepdims=True), (8, wide))

    def soft_stage(t, u, pair):
        i = 2 * u + pair
        most = mb[i, :1]
        total = None
        for b in range(t // BLOCK):
            x = jnp.exp2((sb[i][b * BLOCK : (b + 1) * BLOCK] - most) * factor)
            part = jnp.sum(x.reshape(BLOCK // 8, 8, wide), axis=0)
            total = part if total is None else total + part
            pb[i][b * BLOCK : (b + 1) * BLOCK] = x.astype(BF16)
        lb[i] = total

    def mix_stage(n, t, u, pair):
        quad, duo = place(n)
        i = 2 * u + pair
        inv = 1.0 / jnp.sum(lb[i], axis=0, keepdims=True)
        o = dot(vb[u][pair * BLOCK : (pair + 1) * BLOCK, :t], pb[i][:t]) * inv
        o = jnp.concatenate([o[:nope, :BLOCK], o[nope:, BLOCK:]], axis=0).T.astype(BF16)
        first, second = o[:toks], o[toks:]
        cols = slice(pair * BLOCK, (pair + 1) * BLOCK)
        o_own[quad, 2 * duo + u, :, cols] = jnp.where(odd == 1, second, first)
        o_send[quad, 2 * duo + u, :, cols] = jnp.where(odd == 1, first, second)

    units = [(u, pair) for u in range(2) for pair in range(2)]
    total = quads * duos

    def each_chip(fn):
        for c in range(slots):
            pl.when(chip == c)(lambda c=c: fn(prefix + (c + 1) * BLOCK))

    def body(b, t):
        before, ahead, later = jnp.maximum(b - 1, 0), jnp.minimum(b + 1, total - 1), jnp.minimum(b + 2, total - 1)
        mix_stage(before, t, 0, 0)
        mix_stage(before, t, 0, 1)
        mix_stage(before, t, 1, 0)
        mix_stage(before, t, 1, 1)
        soft_stage(t, 0, 0)
        score_stage(ahead, t, 0, 0)
        value_stage(b, t, 0)
        soft_stage(t, 0, 1)
        score_stage(ahead, t, 0, 1)
        key_stage(later, t, 0)
        soft_stage(t, 1, 0)
        score_stage(ahead, t, 1, 0)
        value_stage(b, t, 1)
        soft_stage(t, 1, 1)
        score_stage(ahead, t, 1, 1)
        query_dot(later)
        query_stage(later)
        key_stage(later, t, 1)

    def front(b, t):
        before, ahead = jnp.maximum(b - 1, 0), b + 1
        for u, pair in units:
            mix_stage(before, t, u, pair)
        for u in range(2):
            soft_stage(t, u, 0)
            score_stage(ahead, t, u, 0)
            value_stage(b, t, u)
            soft_stage(t, u, 1)
            score_stage(ahead, t, u, 1)

    def back(b, t):
        for u in range(2):
            key_stage(b + 2, t, u)
        query_dot(b + 2)
        query_stage(b + 2)

    def at(b, when):
        return pl.when(b == when)

    agenda = {
        0: [(None, ring("R", "wq.a", "wq.b"), across(1, "wq.a", "wq.b"))],
        2: [(None, ring("r", *small), across("1r", *small) + ring("O", *small) + ring("R", "wo.a", "wo.b") + ["wo.mR"])],
        4: [(None, across(1, *small) + ring("L", "wq.a"), across(2, "wq.a"))],
        6: [(None, ring("L", "wq.b"), across(2, "wq.b"))],
        8: [(None, ring("L", "wk.a", "wv.b"), across(2, "wk.a", "wv.b"))],
        10: [(None, across("1r", *small) + ring("O", *small), across(3, *small)), (None, across(2, *small), [])],
        12: [(None, ring("L", "wo.b"), across(2, "wo.b")), (1, [], ring("O", "wo.b"))],
        13: [(None, ring("R", "wo.a"), across(1, "wo.a")), (0, [], ring("O", "wo.a"))],
        16: [(None, across(3, *small), []), (None, ring("L", "wo.a"), across(2, "wo.a")), (1, [], ring("O", "wo.a"))],
        17: [(None, ring("R", "wo.b"), across(1, "wo.b")), (0, [], ring("O", "wo.b"))],
        20: [(0, ["wo.mR"], ["wo.mO"]), (1, ["wo.mL"], ["wo.mO"])],
        22: [(0, ring("O", "wo.a"), across(3, "wo.a") + ["wo.aS"]), (1, ring("O", "wo.b"), across(3, "wo.b") + ["wo.bS"])],
        23: [
            (0, ["wo.mL"], []),
            (1, ["wo.mR"], []),
            (None, across(1, "wo.a", "wo.b") + across(2, "wo.a", "wo.b"), ["woS1", "woS2"]),
        ],
        24: [(0, ring("O", "wo.b"), across(3, "wo.b") + ["wo.bS"]), (1, ring("O", "wo.a"), across(3, "wo.a") + ["wo.aS"])],
        29: [(None, ["wo.mO"], ["wo.mS"]), (None, across(3, "wo.a", "wo.b"), ["wo.aS~", "wo.bS~", "o.aS"])],
    }
    for quad in range(quads - 1):
        agenda.setdefault((quad + 1) * duos + 1, []).append((None, [], [f"o{quad}S"]))

    def run_agenda(when):
        for parity, waits, starts in agenda[when]:

            def item(waits=waits, starts=starts):
                wire.landed(*waits)
                wire.start(*starts)

            if parity is None:
                item()
            else:
                pl.when(odd == parity)(item)

    bounce = pltpu.make_async_copy(wo_hbm, wo_buf, load_sem.at[3])
    span = 8

    def step(b, _):
        for first in range(0, total, span):

            @pl.when(b // span == first // span)
            def _():
                for when in sorted(agenda):
                    if first <= when < first + span and when not in (0, 2):
                        at(b, when)(functools.partial(run_agenda, when))
                if first == 0:

                    @at(b, 4)
                    def _():
                        pltpu.make_async_copy(rows.at[:, pl.ds(prefix, chunk)], c_out, load_sem.at[0]).start()
                        pltpu.make_async_copy(rot.at[:, pl.ds(prefix, chunk)], p_out, load_sem.at[1]).start()
                        bounce.start()

                    @at(b, 6)
                    def _():
                        bounce.wait()
                        pltpu.make_async_copy(wo_buf, wo_out.at[odd, 0], load_sem.at[4]).start()

        split = (b == 0) | (b == 2)

        @pl.when(split)
        def _():
            each_chip(functools.partial(front, b))
            for g in range(1, groups):

                @at(b, 2 * (g - 1))
                def _():
                    forward(g)
                    run_agenda(2 * (g - 1))
                    settle(g)

            each_chip(functools.partial(back, b))

        @pl.when(jnp.logical_not(split))
        def _():
            each_chip(functools.partial(body, b))

        return 0

    def lead_in(t):
        for u in range(2):
            key_stage(0, t, u)
        for u, pair in units:
            score_stage(0, t, u, pair)
        for u in range(2):
            key_stage(1, t, u)
        query_dot(1)
        query_stage(1)

    wire.landed("q0S")
    query_dot(0)
    query_stage(0)
    forward(0)
    wire.landed(*ring("R", "wk.a", "wv.b"))
    wire.start(*across(1, "wk.a", "wv.b"))
    settle(0)
    each_chip(lead_in)
    lax.fori_loop(0, total, step, 0)

    def last(t):
        for u, pair in units:
            mix_stage(total - 1, t, u, pair)

    each_chip(last)
    wire.start("o.bS")
    pltpu.make_async_copy(o_own, o_out.at[odd], load_sem.at[2]).start()
    for place in range(slots - 1):
        wire.landed(f"woS{place}")
    wire.landed("wo.aS", "wo.bS", "wo.mS", "wo.aS~", "wo.bS~")
    for quad in range(quads - 1):
        wire.landed(f"o{quad}S")
    wire.landed("o.aS", "o.bS")
    wire.all_sent("c", rows.at[pl.ds(0, per * groups // 2), pl.ds(0, 14 * toks)], tp=other)
    wire.all_sent("p", rot.at[pl.ds(0, groups), pl.ds(0, 7 * toks)], tp=other)
    wire.all_sent("q", cq_buf.at[odd], tp=other)
    wire.all_sent("wq.a", wq.at[pl.ds(0, 3 * heads), pl.ds(0, q_cut)], tp=other)
    wire.all_sent("wq.b", wq.at[pl.ds(0, 3 * heads), pl.ds(0, head - q_cut)], tp=other)
    wire.all_sent("wk.a", wkv.at[pl.ds(0, 3 * heads), pl.ds(0, nope)], tp=other)
    wire.all_sent("wv.b", wkv.at[pl.ds(0, 3 * heads), pl.ds(0, nope)], tp=other)
    wire.all_sent("wo.a", wo_out.at[0, pl.ds(0, 3), pl.ds(0, o_cut)], tp=other)
    wire.all_sent("wo.b", wo_out.at[0, pl.ds(0, 3), pl.ds(0, o_cut)], tp=other)
    wire.all_sent("wo.m", wo_out.at[0, pl.ds(0, 3), left_over], tp=other)
    wire.all_sent("woS", wo_out.at[0], tp=other)
    wire.all_sent("o", o_send, tp=other)
    pltpu.make_async_copy(rows.at[:, pl.ds(prefix, chunk)], c_out, load_sem.at[0]).wait()
    pltpu.make_async_copy(rot.at[:, pl.ds(prefix, chunk)], p_out, load_sem.at[1]).wait()
    pltpu.make_async_copy(o_own, o_out.at[odd], load_sem.at[2]).wait()
    pltpu.make_async_copy(wo_buf, wo_out.at[odd, 0], load_sem.at[4]).wait()


def finish_kernel(
    len_hbm, o_hbm, w_hbm, x_hbm, c_hbm, p_hbm, lat_hbm, pe_hbm, y_hbm, lat_out, pe_out, fresh, acc, x_buf, y_buf, o_buf, w_buf, c_buf, p_buf, lat_buf, pe_buf, lat_new, pe_new, len_ref, load_sem, store_sem, sems
):
    chip = lax.axis_index("tp") // 2
    quads, seqs, toks, depth = o_hbm.shape[1:]
    terms = 2 * quads
    slots = c_hbm.shape[1]
    rank = lat_hbm.shape[2]
    rope, cache_len = pe_hbm.shape[1:]
    chunk = slots * 2 * toks
    words = rank // BLOCK
    dim = x_hbm.shape[2]
    part = 2 * depth
    ring = w_buf.shape[0]

    def loads(k, with_term):
        slot = lax.rem(k, ring)
        out = [
            pltpu.make_async_copy(c_hbm.at[k], c_buf.at[slot], load_sem.at[0, slot]),
            pltpu.make_async_copy(lat_hbm.at[k], lat_buf.at[slot], load_sem.at[1, slot]),
        ]
        if with_term:
            side, quad = k // quads, lax.rem(k, quads)
            out.append(pltpu.make_async_copy(o_hbm.at[side, quad], o_buf.at[slot], load_sem.at[2, slot]))
            out.append(pltpu.make_async_copy(w_hbm.at[side, pl.ds(pl.multiple_of(quad * depth, depth), depth)], w_buf.at[slot], load_sem.at[3, slot]))
        return out

    def store(k):
        slot = lax.rem(k, ring)
        return pltpu.make_async_copy(lat_new.at[slot], lat_out.at[k], store_sem.at[slot])

    load_len = pltpu.make_async_copy(len_hbm, len_ref, sems.at[4 + dim // part])
    load_x = pltpu.make_async_copy(x_hbm, x_buf, sems.at[0])
    load_p = pltpu.make_async_copy(p_hbm, p_buf, sems.at[1])
    load_pe = pltpu.make_async_copy(pe_hbm, pe_buf, sems.at[2])
    store_pe = pltpu.make_async_copy(pe_new, pe_out, sems.at[3])

    def store_y(n):
        cols = pl.ds(n * part, part)
        return pltpu.make_async_copy(y_buf.at[:, :, cols], y_hbm.at[:, :, cols], sems.at[4 + n])


    def slot_of(j):
        return lax.rem(chip - j + slots, slots)

    def project(k, kind):
        slot = lax.rem(k, ring)
        o = o_buf[slot].reshape(seqs * toks, depth)
        for n in range(0, dim, part):
            cols = slice(n, n + part)
            y = dot(o, w_buf[slot, :, cols])
            if kind != "first":
                y = acc[:, cols] + y
            if kind == "last":
                y = y + x_buf[:, :, cols].reshape(seqs * toks, part).astype(F32)
                y_buf[:, :, cols] = y.astype(BF16).reshape(seqs, toks, part)
                store_y(n // part).start()
            else:
                acc[:, cols] = y

    def cache(k):
        at_slot = lax.rem(k, ring)
        length = len_ref[k]
        for j in range(slots):
            piece = c_buf[at_slot, slot_of(j)].reshape(2 * toks, rank).astype(F32)
            for w in range(words):
                fresh[w, BLOCK + j * 2 * toks : BLOCK + (j + 1) * 2 * toks] = piece[:, w * BLOCK : (w + 1) * BLOCK]
        lat_new[at_slot] = lat_buf[at_slot]
        base = (length // 16) * 16
        skew = length - base
        tile_row = lax.broadcasted_iota(jnp.int32, (16, BLOCK), 0)
        for i in range(chunk // 16 + 1):
            at = pl.multiple_of(jnp.minimum(base + i * 16, cache_len - 16), 16)
            for w in range(words):
                cols = slice(w * BLOCK, (w + 1) * BLOCK)
                moved = fresh[w, pl.ds(BLOCK - skew + i * 16, 16), :].astype(BF16)
                if i == 0 or i == chunk // 16:
                    local = tile_row + (at - length)
                    shown = (local >= 0) & (local < chunk) if i == 0 else (local < chunk)
                    if i == 0:
                        rest = lat_buf[at_slot, pl.ds(at, 16), cols]
                    else:
                        shown = shown & (skew > 0)
                        rest = lat_new[at_slot, pl.ds(at, 16), cols]
                    moved = jnp.where(shown, moved.astype(F32), rest.astype(F32)).astype(BF16)
                lat_new[at_slot, pl.ds(at, 16), cols] = moved

        turned = jnp.concatenate([p_buf[k // (BLOCK // rope), slot_of(j)].reshape(2 * toks, BLOCK).astype(F32).T for j in range(slots)], axis=1)
        group = lax.rem(k, BLOCK // rope)
        mine = turned[:rope]
        for g in range(1, BLOCK // rope):
            mine = jnp.where(group == g, turned[g * rope : (g + 1) * rope], mine)
        mine = jnp.concatenate([mine, jnp.zeros((rope, cache_len - chunk), F32)], axis=1)
        mine = pltpu.roll(mine, length, axis=1)
        spot = lax.broadcasted_iota(jnp.int32, (rope, cache_len), 1) - length
        pe_new[k] = jnp.where((spot >= 0) & (spot < chunk), mine, pe_buf[k].astype(F32)).astype(BF16)

    def begin(k, with_term):
        for load in loads(k, with_term):
            load.start()

    def arrived(k, with_term):
        for load in loads(k, with_term):
            load.wait()

    def work(k, kind):
        if kind != "none":
            project(k, kind)
        cache(k)
        store(k).start()

    def more(k):
        pl.when(k < terms)(lambda: begin(k, True))
        pl.when((k >= terms) & (k < seqs))(lambda: begin(k, False))

    first = loads(0, True)
    for load in first[2:] + first[:2]:
        load.start()
    load_len.start()
    load_p.start()
    load_pe.start()
    for load in first[2:]:
        load.wait()
    begin(1, True)
    begin(2, True)
    project(0, "first")
    for load in first[:2] + [load_len, load_p, load_pe]:
        load.wait()
    begin(3, True)
    cache(0)
    store(0).start()
    load_x.start()

    def middle(k, _):
        arrived(k, True)
        more(k + ring - 1)

        @pl.when(k >= ring)
        def _():
            store(k - ring).wait()

        work(k, "middle")
        return 0

    lax.fori_loop(1, terms - 1, middle, 0)
    last = terms - 1
    arrived(last, True)
    more(last + ring - 1)
    store(last - ring).wait()
    load_x.wait()
    work(last, "last")

    def tail(k, _):
        arrived(k, False)
        store(k - ring).wait()
        work(k, "none")
        return 0

    lax.fori_loop(terms, seqs, tail, 0)
    store_pe.start()
    for k in range(ring):
        store(seqs - ring + k).wait()
    store_pe.wait()
    for n in range(dim // part):
        store_y(n).wait()


def solution(mesh):
    size = mesh.shape["tp"]
    count = mesh.shape["dp"]
    stride = 2 ** (count.bit_length() // 2)
    paired = {"a": count % 2 == 0, "b": count % (2 * stride) == 0}

    def local_step(hidden, lengths, rope_cos, rope_sin, cache_lat, cache_pe, norm_in, w_dq, norm_q, w_dkv, norm_kv, w_uq, w_uk, w_uv, w_out):
        seqs, toks, dim = hidden.shape
        q_rank = w_dq.shape[1]
        rank, heads, nope = w_uk.shape
        rope = cache_pe.shape[2]
        cache_len = cache_lat.shape[1]
        slots = size // 2
        head = nope + rope
        quads = slots * heads // 4
        chunk = size * toks
        prefix = cache_len - chunk
        per = BLOCK // rope
        groups = seqs // per
        wide = 2 * BLOCK
        cos_t, sin_t = rope_cos.transpose(0, 2, 1), rope_sin.transpose(0, 2, 1)
        pe_t = cache_pe.transpose(0, 2, 1)
        wdkv_t = w_dkv.transpose(1, 0)
        wq_t, wk_t, wv_t = (w.transpose(1, 2, 0) for w in (w_uq, w_uk, w_uv))

        inboxes = 9 * groups + 36 + 8 + 3 + slots + 4 + quads + 1
        any_spec = pl.BlockSpec(memory_space=pl.ANY)
        c_all, p_all, o_all, wo_all = pl.pallas_call(
            functools.partial(main_kernel, (size, stride, paired)),
            in_specs=[any_spec] * 15,
            out_specs=[any_spec] * 4,
            out_shape=[
                jax.ShapeDtypeStruct((seqs, chunk, rank), BF16),
                jax.ShapeDtypeStruct((groups, chunk, BLOCK), BF16),
                jax.ShapeDtypeStruct((2, quads, seqs, toks, 4 * nope), BF16),
                jax.ShapeDtypeStruct((2, slots) + w_out.shape, BF16),
            ],
            scratch_shapes=[
                pltpu.VMEM(hidden.shape, BF16),
                pltpu.VMEM(w_dq.shape, BF16),
                pltpu.VMEM(wdkv_t.shape, BF16),
                pltpu.VMEM((groups, per * toks, dim), BF16),
                pltpu.VMEM((seqs, cache_len, rank), BF16),
                pltpu.VMEM((groups, cache_len, BLOCK), BF16),
                pltpu.VMEM((seqs, rope, prefix), BF16),
                pltpu.VMEM((seqs, rope // 2, BLOCK), F32),
                pltpu.VMEM((seqs, rope // 2, BLOCK), F32),
                pltpu.VMEM((2, seqs, toks, q_rank), BF16),
                pltpu.VMEM((slots * heads, head, q_rank), BF16),
                pltpu.VMEM((slots * heads, 2 * nope, rank), BF16),
                [pltpu.VMEM((cache_len, 4 * nope), BF16) for _ in range(2)],
                [pltpu.VMEM((4 * nope, cache_len), BF16) for _ in range(2)],
                pltpu.VMEM((2, 2, wide, wide), BF16),
                pltpu.VMEM((4 * head, wide), F32),
                [pltpu.VMEM((cache_len, wide), F32) for _ in range(4)],
                pltpu.VMEM((4, 8, wide), F32),
                [pltpu.VMEM((cache_len, wide), BF16) for _ in range(4)],
                pltpu.VMEM((4, 8, wide), F32),
                pltpu.VMEM((quads, seqs, toks, 4 * nope), BF16),
                pltpu.VMEM((quads, seqs, toks, 4 * nope), BF16),
                pltpu.VMEM(w_out.shape, BF16),
                pltpu.SMEM(lengths.shape, jnp.int32),
                pltpu.VMEM(norm_in.shape, F32),
                pltpu.VMEM(norm_q.shape, F32),
                pltpu.VMEM(norm_kv.shape, F32),
                pltpu.SemaphoreType.DMA((13 + groups,)),
                pltpu.SemaphoreType.DMA((12,)),
                pltpu.SemaphoreType.DMA((inboxes,)),
            ],
            compiler_params=pltpu.CompilerParams(collective_id=0, has_side_effects=True, vmem_limit_bytes=63 * MIB),
            cost_estimate=pl.CostEstimate(flops=70 * 10**9, bytes_accessed=40 * MIB, transcendentals=30 * 10**6),
            name="main",
        )(lengths, hidden, norm_in, w_dq, norm_q, wdkv_t, norm_kv, cos_t, sin_t, wq_t, wk_t, wv_t, w_out, cache_lat, pe_t)

        depth = 4 * nope
        ahead = 4
        y, lat_new, pe_new = pl.pallas_call(
            finish_kernel,
            in_specs=[any_spec] * 8,
            out_specs=[any_spec] * 3,
            scratch_shapes=[
                pltpu.VMEM((rank // BLOCK, chunk + 2 * BLOCK, BLOCK), F32),
                pltpu.VMEM((seqs * toks, dim), F32),
                pltpu.VMEM(hidden.shape, BF16),
                pltpu.VMEM(hidden.shape, BF16),
                pltpu.VMEM((ahead, seqs, toks, depth), BF16),
                pltpu.VMEM((ahead, depth, dim), BF16),
                pltpu.VMEM((ahead, slots, 2, toks, rank), BF16),
                pltpu.VMEM((groups, slots, 2, toks, BLOCK), BF16),
                pltpu.VMEM((ahead, cache_len, rank), BF16),
                pltpu.VMEM(pe_t.shape, BF16),
                pltpu.VMEM((ahead, cache_len, rank), BF16),
                pltpu.VMEM(pe_t.shape, BF16),
                pltpu.SMEM(lengths.shape, jnp.int32),
                pltpu.SemaphoreType.DMA((4, ahead)),
                pltpu.SemaphoreType.DMA((ahead,)),
                pltpu.SemaphoreType.DMA((5 + dim // (2 * depth),)),
            ],
            out_shape=[
                jax.ShapeDtypeStruct(hidden.shape, BF16),
                jax.ShapeDtypeStruct(cache_lat.shape, BF16),
                jax.ShapeDtypeStruct(pe_t.shape, BF16),
            ],
            compiler_params=pltpu.CompilerParams(vmem_limit_bytes=63 * MIB),
            cost_estimate=pl.CostEstimate(flops=2 * seqs * toks * dim * dim, bytes_accessed=50 * MIB, transcendentals=0),
            name="finish",
        )(
            lengths,
            o_all,
            wo_all.reshape(2, slots * w_out.shape[0], dim),
            hidden,
            c_all.reshape(seqs, slots, 2, toks, rank),
            p_all.reshape(groups, slots, 2, toks, BLOCK),
            cache_lat,
            pe_t,
        )
        return y, lat_new, pe_new.transpose(0, 2, 1)

    spec_tok = P("dp", "tp", None)
    spec_len = P("dp")
    spec_seq = P("dp", None, None)
    spec_vec = P(None)
    spec_mat = P(None, None)
    spec_head = P(None, "tp", None)
    spec_rows = P("tp", None)
    in_specs = (spec_tok, spec_len, spec_seq, spec_seq, spec_seq, spec_seq, spec_vec, spec_mat, spec_vec, spec_mat, spec_vec, spec_head, spec_head, spec_head, spec_rows)
    return jax.shard_map(local_step, mesh=mesh, in_specs=in_specs, out_specs=(spec_tok, spec_seq, spec_seq), check_vma=False)
```
